32 devices in a mesh: layer: 1 (over z), tensor: 32 (over y, x, core).
Axes of the slice: x: 4, y: 4, z: 1, core: 2. Of those that a mesh axis runs over, the one named last changes fastest.
The devices are a block of a 4x4x8 slice.
Arguments:
- gradient: bfloat16 [4096, 8192], P('layer', 'tensor')
- left_stat: float32 [4096, 4096], P(('layer', 'tensor'))
- right_stat: float32 [8192, 8192], P(('layer', 'tensor'))
- left_root: bfloat16 [4096, 4096], P(('layer', 'tensor'))
- right_root: bfloat16 [8192, 8192], P(('layer', 'tensor'))
Outputs:
- output 1: float32 [4096, 4096], P(('layer', 'tensor'))
- output 2: float32 [8192, 8192], P(('layer', 'tensor'))
- output 3: float32 [4096, 8192], P('layer', 'tensor')
All inputs are finite; a program needn't handle non-finite values.
Results may differ from the reference program's by a relative error of at most 0.001.
Values are sent between devices in bfloat16 or wider.
A program may use at most 768 MiB of HBM per device.

```python
import jax
import jax.numpy as jnp

ROW_COUNT = 4096
COL_COUNT = 8192
EMA_DECAY = 0.9


def setup_inputs(seed: int = 0, part: int = 0) -> dict:
    base_key = jax.random.fold_in(jax.random.key(seed), part)
    keys = jax.random.split(base_key, 5)
    grad_scale = (ROW_COUNT * COL_COUNT) ** -0.25
    root_scale = (ROW_COUNT * COL_COUNT) ** 0.125
    gradient = grad_scale * jax.random.normal(keys[0], (ROW_COUNT, COL_COUNT), jnp.float32)
    left_hist = jax.random.normal(keys[1], (ROW_COUNT, COL_COUNT // 8), jnp.float32)
    left_stat = (0.8 * grad_scale ** 2) * jnp.dot(left_hist, left_hist.T)
    right_hist = jax.random.normal(keys[2], (COL_COUNT, ROW_COUNT // 8), jnp.float32)
    right_stat = (0.8 * grad_scale ** 2) * jnp.dot(right_hist, right_hist.T)
    left_basis = jax.random.normal(keys[3], (ROW_COUNT, ROW_COUNT // 8), jnp.float32)
    left_root = root_scale * (0.5 * jnp.eye(ROW_COUNT, dtype=jnp.float32) + jnp.dot(left_basis, left_basis.T) / ROW_COUNT)
    right_basis = jax.random.normal(keys[4], (COL_COUNT, COL_COUNT // 8), jnp.float32)
    right_prod = jnp.dot(right_basis, right_basis.T) / COL_COUNT
    right_root = root_scale * (0.5 * jnp.eye(COL_COUNT, dtype=jnp.float32) + 0.5 * (right_prod + right_prod.T))
    return {"gradient": gradient.astype(jnp.bfloat16), "left_stat": left_stat, "right_stat": right_stat, "left_root": left_root.astype(jnp.bfloat16), "right_root": right_root.astype(jnp.bfloat16)}


def reference(gradient, left_stat, right_stat, left_root, right_root):
    left_new = EMA_DECAY * left_stat + (1.0 - EMA_DECAY) * jnp.dot(gradient, gradient.T, preferred_element_type=jnp.float32)
    right_new = EMA_DECAY * right_stat + (1.0 - EMA_DECAY) * jnp.dot(gradient.T, gradient, preferred_element_type=jnp.float32)
    precond = jnp.dot(gradient, right_root, preferred_element_type=jnp.float32).astype(jnp.bfloat16)
    direction = jnp.dot(left_root, precond, preferred_element_type=jnp.float32)
    return (left_new, right_new, direction)
```

```python
import jax
import jax.numpy as jnp
from jax import lax
from jax.sharding import PartitionSpec as P

EMA_DECAY = 0.9


def solution(mesh):
    row_spec = P(("layer", "tensor"), None)
    col_spec = P("layer", "tensor")

    def local_step(grad_local, left_block, right_block, left_root_block, right_root_block):
        rows = left_block.shape[0]
        grad_full = lax.all_gather(grad_local, "tensor", axis=1, tiled=True)
        grad_full, left_root_block = lax.optimization_barrier((grad_full, left_root_block))
        left_root_full = lax.all_gather(left_root_block, "tensor", axis=0, tiled=True)
        precond = jnp.einsum("mn,cn->mc", grad_full, right_root_block, preferred_element_type=jnp.float32).astype(jnp.bfloat16)
        right_prod = jnp.einsum("mc,mn->cn", grad_local, grad_full, preferred_element_type=jnp.float32)
        right_new = EMA_DECAY * right_block + (1.0 - EMA_DECAY) * right_prod
        grad_rows = lax.dynamic_slice_in_dim(grad_full, lax.axis_index("tensor") * rows, rows, axis=0)
        left_prod = jnp.einsum("rn,mn->rm", grad_rows, grad_full, preferred_element_type=jnp.float32)
        left_new = EMA_DECAY * left_block + (1.0 - EMA_DECAY) * left_prod
        direction = jnp.dot(left_root_full, precond, preferred_element_type=jnp.float32)
        return left_new, right_new, direction

    return jax.shard_map(local_step, mesh=mesh, in_specs=(col_spec, row_spec, row_spec, row_spec, row_spec), out_specs=(row_spec, row_spec, col_spec), check_vma=False)
```

```python
import functools
import math

import jax
import jax.numpy as jnp
from jax import lax
from jax.experimental import pallas as pl
from jax.experimental.pallas import tpu as pltpu
from jax.sharding import PartitionSpec as P

EMA_DECAY = 0.9
CORES = 2
MESH = pl.DeviceIdType.MESH

ORDER = [(0, 0), (3, 0), (1, 0), (0, 3), (0, 1), (2, 0), (0, 2), (3, 3), (1, 1), (1, 3), (3, 1), (2, 3), (2, 1), (3, 2), (1, 2), (2, 2)]
UP = [
    ((0, 3), 0, True), ((0, 3), 1, False), ((3, 3), 0, True), ((1, 3), 1, False), ((0, 2), 0, False), ((3, 3), 1, False),
    ((1, 3), 0, True), ((2, 3), 0, True), ((2, 3), 1, False), ((3, 2), 0, False), ((1, 2), 0, False), ((2, 2), 0, False),
]
DOWN = [
    ((0, 1), 1, True), ((0, 1), 0, False), ((1, 1), 1, True), ((3, 1), 0, False), ((0, 2), 1, False), ((1, 1), 0, False),
    ((3, 1), 1, True), ((2, 1), 1, True), ((2, 1), 0, False), ((1, 2), 1, False), ((3, 2), 1, False), ((2, 2), 1, False),
]
ROUNDS = len(UP)
FIRST_UP = [((3, 0), 0, True), ((3, 0), 1, False), ((2, 0), 0, False)]
FIRST_DOWN = [((1, 0), 1, True), ((1, 0), 0, False), ((2, 0), 1, False)]
GRAD_ROUND_STEP = [2, 2, 8, 10, 12, 14, 17, 20, 22, 24, 26, 30]
ROOT_ROUND_STEP = [2, 2, 8, 10, 12, 14, 17, 20, 22, 24, 26, 30]
LATE = (2, 12, 14, 22, 26, 30)


def packed(values):
    return [sum(v << (2 * i) for i, v in enumerate(values[j:j + 8])) for j in (0, 8)]


FIRST_CODE = packed([o[0] for o in ORDER])
SECOND_CODE = packed([o[1] for o in ORDER])


def lookup(code, e):
    word = code[0] + (e // 8) * (code[1] - code[0])
    return lax.shift_right_logical(word, 2 * (e % 8)) & 3


def kernel(n, side, g_ref, l_ref, r_ref, lr_ref, rr_ref, lo_out, ro_out, do_out, gfull, lfull,
           lo_ref, ro_ref, do_ref, rr, gt, acc, gbuf, lbuf, rhs, xbf, g_recv, l_recv, g_send, l_send, load_sem, init_sem, out_sem):
    _, half_rows, cols = g_ref.shape
    rows = 2 * half_rows
    lrows = l_ref.shape[0]
    tile = min(1024, half_rows)

    me = lax.axis_index("tensor")
    c = me % CORES
    chip = me // CORES
    x, y = chip % side, chip // side
    f = x + c * (y - x)
    s = y + c * (x - y)
    fstep = CORES + c * CORES * (side - 1)
    sstep = CORES * side - c * CORES * (side - 1)
    twin = me + 1 - 2 * c

    def index(df, ds):
        return ((f + df) % side) * fstep + ((s + ds) % side) * sstep + c

    def twin_index(df, ds):
        return ((s + df) % side) * sstep + ((f + ds) % side) * fstep + 1 - c

    peers = {"f+": index(1, 0), "f-": index(3, 0), "s+": index(0, 1), "s-": index(0, 3), "twin": twin}
    slot_of = {name: i for i, name in enumerate(peers)}

    class Gather:
        def __init__(self, own, full, recv, send):
            self.own, self.full, self.recv, self.send_sem = own, full, recv, send
            self.count = {name: 0 for name in peers}

        def copy(self, name, b, half, own=False):
            src = self.own.at[half] if own else self.full.at[2 * b + half]
            return pltpu.make_async_remote_copy(
                src_ref=src, dst_ref=self.full.at[2 * b + half], send_sem=self.send_sem.at[slot_of[name]],
                recv_sem=self.recv.at[2 * b + half], device_id={"tensor": peers[name]}, device_id_type=MESH)

        def send(self, name, b, half, own=False):
            self.count[name] += 1
            self.copy(name, b, half, own).start()

        def wait(self, b, half):
            self.copy("twin", b, half).wait_recv()

        def start(self):
            for half in (0, 1):
                for name in ("f+", "s+"):
                    self.send(name, me, half, own=True)
                for name in ("f-", "s-"):
                    self.send(name, me, 1 - half, own=True)
            for half in (0, 1):
                self.send("twin", me, half, own=True)

        def round(self, r):
            if r < len(FIRST_UP):
                (ou, hu, on), (od, hd, _) = FIRST_UP[r], FIRST_DOWN[r]
                bu, bd = index(*ou), index(*od)
                self.wait(bu, hu)
                if on:
                    self.send("f+", bu, hu)
                self.wait(bd, hd)
                if on:
                    self.send("f-", bd, hd)
                self.send("s+", bu, hu)
                self.send("s-", bd, hd)
                self.send("s+", bd, hd)
                self.send("s-", bu, hu)
                self.send("twin", bu, hu)
                self.send("twin", bd, hd)
            (ou, hu, on), (od, hd, _) = UP[r], DOWN[r]
            bu, bd = index(*ou), index(*od)
            self.wait(bu, hu)
            if on:
                self.send("s+", bu, hu)
            self.send("twin", bu, hu)
            self.wait(bd, hd)
            if on:
                self.send("s-", bd, hd)
            self.send("twin", bd, hd)

        def drain(self):
            for name, count in self.count.items():
                whole = self.full.at[pl.ds(0, count)]
                pltpu.make_async_copy(whole, whole, self.send_sem.at[slot_of[name]]).wait()

    grad = Gather(g_ref, gfull, g_recv, g_send)
    root = Gather(lr_ref, lfull, l_recv, l_send)

    def block_of(k):
        e, other = k // 2, k % 2
        df, ds = lookup(FIRST_CODE, e), lookup(SECOND_CODE, e)
        mine = index(df, ds)
        return mine + other * (twin_index(df, ds) - mine)

    def load(gather, buf, k, sem):
        b = block_of(k)
        return pltpu.make_async_copy(gather.full.at[pl.ds(2 * b, 2)], buf.at[k % 2], sem.at[k % 2])

    def start_load(gather, buf, k, sem):
        @pl.when(k % 2 == 1)
        def _():
            b = block_of(k)
            gather.wait(b, 0)
            gather.wait(b, 1)
        load(gather, buf, k, sem).start()

    def is_late(k):
        late = k == LATE[0]
        for v in LATE[1:]:
            late = late | (k == v)
        return late

    def steps(gather, buf, sem, round_step, extra, work):
        def step(k, carry):
            for r in range(ROUNDS):
                @pl.when(k == round_step[r])
                def _():
                    gather.round(r)
            for at, fn in extra:
                pl.when(k == at)(fn)

            @pl.when(is_late(k))
            def _():
                start_load(gather, buf, k, sem)

            @pl.when((k + 1 < n) & jnp.logical_not(is_late(k + 1)))
            def _():
                start_load(gather, buf, k + 1, sem)
            load(gather, buf, k, sem).wait()
            work(k, k % 2, block_of(k))
            return carry
        lax.fori_loop(0, n, step, 0)

    first = [
        pltpu.make_async_copy(rr_ref, rr, init_sem.at[0]),
        pltpu.make_async_copy(r_ref, ro_ref, init_sem.at[1]),
        pltpu.make_async_copy(l_ref, lo_ref, init_sem.at[2]),
    ]
    own_load = pltpu.make_async_copy(g_ref, gbuf.at[0], load_sem.at[0])
    own_load.start()

    barrier = pltpu.get_barrier_semaphore()
    for peer in peers.values():
        pl.semaphore_signal(barrier, inc=1, device_id={"tensor": peer}, device_id_type=MESH)
    pl.semaphore_wait(barrier, len(peers))
    grad.start()
    for copy in first:
        copy.start()

    acc[...] = jnp.zeros_like(acc)
    own_load.wait()
    for h in (0, 1):
        gt[:, h * half_rows:(h + 1) * half_rows] = gbuf[0, h].T
    for copy in first:
        copy.wait()
    own_load.start()

    per_half = half_rows // tile

    def grad_work(k, slot, b):
        at = pl.multiple_of(b * cols, cols)
        rhs[:cols] = rr[:, pl.ds(at, cols)]
        rhs[cols:] = gbuf[slot, me // (n // 2), pl.ds(pl.multiple_of((me % (n // 2)) * lrows, lrows), lrows), :]

        def rows_step(t, carry):
            left = gbuf[slot, t // per_half, pl.ds(pl.multiple_of((t % per_half) * tile, tile), tile), :]
            out = pl.ds(pl.multiple_of(t * tile, tile), tile)
            acc[out, :] += lax.dot_general(left, rhs[...], (((1,), (1,)), ((), ())), preferred_element_type=jnp.float32)
            return carry
        lax.fori_loop(0, 2 * per_half, rows_step, 0)
        prod = jnp.dot(gt[:, :half_rows], gbuf[slot, 0], preferred_element_type=jnp.float32)
        prod += jnp.dot(gt[:, half_rows:], gbuf[slot, 1], preferred_element_type=jnp.float32)
        ro_ref[:, pl.ds(at, cols)] = EMA_DECAY * ro_ref[:, pl.ds(at, cols)] + (1.0 - EMA_DECAY) * prod
        pltpu.make_async_copy(ro_ref.at[:, pl.ds(at, cols)], ro_out.at[:, pl.ds(at, cols)], out_sem.at[0]).start()

    steps(grad, gbuf, load_sem, GRAD_ROUND_STEP, [(GRAD_ROUND_STEP[-2], root.start)], grad_work)

    pltpu.make_async_copy(lr_ref, lbuf.at[0], load_sem.at[0]).start()
    xbf[...] = acc[:, :cols].astype(jnp.bfloat16)

    def left_step(t, carry):
        at = pl.ds(pl.multiple_of(t * lrows, lrows), lrows)
        lo_ref[:, at] = EMA_DECAY * lo_ref[:, at] + (1.0 - EMA_DECAY) * acc[at, cols:].T
        return carry
    lax.fori_loop(0, rows // lrows, left_step, 0)
    left_store = pltpu.make_async_copy(lo_ref, lo_out, out_sem.at[1])
    left_store.start()

    def root_work(k, slot, b):
        left = lbuf[slot].reshape(lrows, rows)
        at = pl.ds(pl.multiple_of(b * lrows, lrows), lrows)
        do_ref[at, :] = jnp.dot(left, xbf[...], preferred_element_type=jnp.float32)
        pltpu.make_async_copy(do_ref.at[at], do_out.at[at], out_sem.at[2]).start()

    steps(root, lbuf, load_sem, ROOT_ROUND_STEP, [], root_work)
    grad.drain()
    root.drain()
    pltpu.make_async_copy(ro_ref, ro_out, out_sem.at[0]).wait()
    left_store.wait()
    pltpu.make_async_copy(do_ref, do_out, out_sem.at[2]).wait()


def solution(mesh):
    row_spec = P(("layer", "tensor"), None)
    col_spec = P("layer", "tensor")
    n = mesh.shape["tensor"]
    side = math.isqrt(n // CORES)

    def local_step(g, l, r, lr, rr):
        rows, cols = g.shape
        lrows = l.shape[0]
        hbm = pl.BlockSpec(memory_space=pltpu.HBM)
        left_new, right_new, direction, _, _ = pl.pallas_call(
            functools.partial(kernel, n, side),
            name="shampoo",
            out_shape=[
                jax.ShapeDtypeStruct(l.shape, jnp.float32),
                jax.ShapeDtypeStruct(r.shape, jnp.float32),
                jax.ShapeDtypeStruct(g.shape, jnp.float32),
                jax.ShapeDtypeStruct((2 * n, rows // 2, cols), jnp.bfloat16),
                jax.ShapeDtypeStruct((2 * n, lrows // 2, rows), jnp.bfloat16),
            ],
            in_specs=[hbm] * 5,
            out_specs=[hbm] * 5,
            scratch_shapes=[
                pltpu.VMEM(l.shape, jnp.float32),
                pltpu.VMEM(r.shape, jnp.float32),
                pltpu.VMEM(g.shape, jnp.float32),
                pltpu.VMEM(rr.shape, jnp.bfloat16),
                pltpu.VMEM((cols, rows), jnp.bfloat16),
                pltpu.VMEM((rows, cols + lrows), jnp.float32),
                pltpu.VMEM((2, 2, rows // 2, cols), jnp.bfloat16),
                pltpu.VMEM((2, 2, lrows // 2, rows), jnp.bfloat16),
                pltpu.VMEM((cols + lrows, cols), jnp.bfloat16),
                pltpu.VMEM((rows, cols), jnp.bfloat16),
                pltpu.SemaphoreType.DMA((2 * n,)),
                pltpu.SemaphoreType.DMA((2 * n,)),
                pltpu.SemaphoreType.DMA((5,)),
                pltpu.SemaphoreType.DMA((5,)),
                pltpu.SemaphoreType.DMA((2,)),
                pltpu.SemaphoreType.DMA((3,)),
                pltpu.SemaphoreType.DMA((3,)),
            ],
            compiler_params=pltpu.CompilerParams(collective_id=0, has_side_effects=True, vmem_limit_bytes=62 * 2**20),
            cost_estimate=pl.CostEstimate(flops=2 * rows * cols * (2 * n * cols + 2 * rows), bytes_accessed=2 * n * rows * cols * 3, transcendentals=0),
        )(g.reshape(2, rows // 2, cols), l, r, lr.reshape(2, lrows // 2, rows), rr)
        return left_new, right_new, direction

    return jax.shard_map(local_step, mesh=mesh, in_specs=(col_spec, row_spec, row_spec, row_spec, row_spec), out_specs=(row_spec, row_spec, col_spec), check_vma=False)
```

```python
import functools
import math

import jax
import jax.numpy as jnp
from jax import lax
from jax.experimental import pallas as pl
from jax.experimental.pallas import tpu as pltpu
from jax.sharding import PartitionSpec as P

EMA_DECAY = 0.9
CORES = 2
MESH = pl.DeviceIdType.MESH

ORDER = [(0, 0), (3, 0), (1, 0), (0, 3), (0, 1), (2, 0), (0, 2), (3, 3), (1, 1), (1, 3), (3, 1), (2, 3), (2, 1), (3, 2), (1, 2), (2, 2)]
UP = [
    ((0, 3), 0, True), ((0, 3), 1, False), ((3, 3), 0, True), ((1, 3), 1, False), ((0, 2), 0, False), ((3, 3), 1, False),
    ((1, 3), 0, True), ((2, 3), 0, True), ((2, 3), 1, False), ((3, 2), 0, False), ((1, 2), 0, False), ((2, 2), 0, False),
]
DOWN = [
    ((0, 1), 1, True), ((0, 1), 0, False), ((1, 1), 1, True), ((3, 1), 0, False), ((0, 2), 1, False), ((1, 1), 0, False),
    ((3, 1), 1, True), ((2, 1), 1, True), ((2, 1), 0, False), ((1, 2), 1, False), ((3, 2), 1, False), ((2, 2), 1, False),
]
ROUNDS = len(UP)
FIRST_UP = [((3, 0), 0, True), ((3, 0), 1, False), ((2, 0), 0, False)]
FIRST_DOWN = [((1, 0), 1, True), ((1, 0), 0, False), ((2, 0), 1, False)]
GRAD_ROUND_STEP = [2, 2, 8, 10, 12, 14, 17, 20, 22, 24, 26, 30]
ROOT_START_STEP = 29
LATE = (2, 12, 14, 22, 26, 30)


def packed(values):
    return [sum(v << (2 * i) for i, v in enumerate(values[j:j + 8])) for j in (0, 8)]


FIRST_CODE = packed([o[0] for o in ORDER])
SECOND_CODE = packed([o[1] for o in ORDER])


def lookup(code, e):
    word = code[0] + (e // 8) * (code[1] - code[0])
    return lax.shift_right_logical(word, 2 * (e % 8)) & 3


ROOT_ORDER = [(0, 0), (3, 0), (1, 0), (0, 1), (2, 0), (3, 1), (1, 1), (2, 1)]
ROOT_Y = sum(o[0] << (2 * i) for i, o in enumerate(ROOT_ORDER))
ROOT_X = sum(o[1] << (2 * i) for i, o in enumerate(ROOT_ORDER))


def kernel(n, side, g_ref, l_ref, r_ref, lr_ref, rr_ref, lo_ref, ro_ref, do_ref, gfull,
           rr, gt, acc, gbuf, rhs, xx, lroot, relay, lent,
           g_recv, g_send, load_sem, init_sem, l_recv, relay_recv, x_recv, d_recv, l_send, x_send, d_send):
    _, half_rows, cols = g_ref.shape
    rows = 2 * half_rows
    lrows = l_ref.shape[0]
    tile = min(1024, half_rows)

    me = lax.axis_index("tensor")
    c = me % CORES
    chip = me // CORES
    x, y = chip % side, chip // side
    f = x + c * (y - x)
    s = y + c * (x - y)
    fstep = CORES + c * CORES * (side - 1)
    sstep = CORES * side - c * CORES * (side - 1)
    twin = me + 1 - 2 * c

    def index(df, ds):
        return ((f + df) % side) * fstep + ((s + ds) % side) * sstep + c

    def twin_index(df, ds):
        return ((s + df) % side) * sstep + ((f + ds) % side) * fstep + 1 - c

    peers = {"f+": index(1, 0), "f-": index(3, 0), "s+": index(0, 1), "s-": index(0, 3), "twin": twin}
    slot_of = {name: i for i, name in enumerate(peers)}

    class Gather:
        def __init__(self, own, full, recv, send):
            self.own, self.full, self.recv, self.send_sem = own, full, recv, send
            self.count = {name: 0 for name in peers}

        def copy(self, name, b, half, own=False):
            src = self.own.at[half] if own else self.full.at[2 * b + half]
            return pltpu.make_async_remote_copy(
                src_ref=src, dst_ref=self.full.at[2 * b + half], send_sem=self.send_sem.at[slot_of[name]],
                recv_sem=self.recv.at[2 * b + half], device_id={"tensor": peers[name]}, device_id_type=MESH)

        def send(self, name, b, half, own=False):
            self.count[name] += 1
            self.copy(name, b, half, own).start()

        def wait(self, b, half):
            self.copy("twin", b, half).wait_recv()

        def start(self):
            for half in (0, 1):
                for name in ("f+", "s+"):
                    self.send(name, me, half, own=True)
                for name in ("f-", "s-"):
                    self.send(name, me, 1 - half, own=True)
            for half in (0, 1):
                self.send("twin", me, half, own=True)

        def round(self, r):
            if r < len(FIRST_UP):
                (ou, hu, on), (od, hd, _) = FIRST_UP[r], FIRST_DOWN[r]
                bu, bd = index(*ou), index(*od)
                self.wait(bu, hu)
                if on:
                    self.send("f+", bu, hu)
                self.wait(bd, hd)
                if on:
                    self.send("f-", bd, hd)
                self.send("s+", bu, hu)
                self.send("s-", bd, hd)
                self.send("s+", bd, hd)
                self.send("s-", bu, hu)
                self.send("twin", bu, hu)
                self.send("twin", bd, hd)
            (ou, hu, on), (od, hd, _) = UP[r], DOWN[r]
            bu, bd = index(*ou), index(*od)
            self.wait(bu, hu)
            if on:
                self.send("s+", bu, hu)
            self.send("twin", bu, hu)
            self.wait(bd, hd)
            if on:
                self.send("s-", bd, hd)
            self.send("twin", bd, hd)

        def drain(self):
            for name, count in self.count.items():
                whole = self.full.at[pl.ds(0, count)]
                pltpu.make_async_copy(whole, whole, self.send_sem.at[slot_of[name]]).wait()

    grad = Gather(g_ref, gfull, g_recv, g_send)

    def block_of(k):
        e, other = k // 2, k % 2
        df, ds = lookup(FIRST_CODE, e), lookup(SECOND_CODE, e)
        mine = index(df, ds)
        return mine + other * (twin_index(df, ds) - mine)

    def load(gather, buf, k, sem):
        b = block_of(k)
        return pltpu.make_async_copy(gather.full.at[pl.ds(2 * b, 2)], buf.at[k % 2], sem.at[k % 2])

    def start_load(gather, buf, k, sem):
        @pl.when(k % 2 == 1)
        def _():
            b = block_of(k)
            gather.wait(b, 0)
            gather.wait(b, 1)
        load(gather, buf, k, sem).start()

    def is_late(k):
        late = k == LATE[0]
        for v in LATE[1:]:
            late = late | (k == v)
        return late

    def steps(gather, buf, sem, round_step, extra, work):
        def step(k, carry):
            for r in range(ROUNDS):
                @pl.when(k == round_step[r])
                def _():
                    gather.round(r)
            for at, fn in extra:
                pl.when(k == at)(fn)

            @pl.when(is_late(k))
            def _():
                start_load(gather, buf, k, sem)

            @pl.when((k + 1 < n) & jnp.logical_not(is_late(k + 1)))
            def _():
                start_load(gather, buf, k + 1, sem)
            load(gather, buf, k, sem).wait()
            work(k, k % 2, block_of(k))
            return carry
        lax.fori_loop(0, n, step, 0)

    first = [
        pltpu.make_async_copy(rr_ref, rr, init_sem.at[0]),
        pltpu.make_async_copy(r_ref, ro_ref, init_sem.at[1]),
        pltpu.make_async_copy(l_ref, lo_ref, init_sem.at[2]),
        pltpu.make_async_copy(lr_ref, lroot.at[pl.ds(2 * ((y * (side // 2) + x // 2) * CORES + c), 2)], init_sem.at[3]),
    ]
    own_load = pltpu.make_async_copy(g_ref, gbuf.at[0], load_sem.at[0])
    own_load.start()

    barrier = pltpu.get_barrier_semaphore()
    for peer in peers.values():
        pl.semaphore_signal(barrier, inc=1, device_id={"tensor": peer}, device_id_type=MESH)
    pl.semaphore_wait(barrier, len(peers))
    grad.start()
    for copy in first:
        copy.start()

    acc[...] = jnp.zeros_like(acc)
    own_load.wait()
    for h in (0, 1):
        gt[:, h * half_rows:(h + 1) * half_rows] = gbuf[0, h].T
    for copy in first:
        copy.wait()
    own_load.start()

    per_half = half_rows // tile

    def grad_work(k, slot, b):
        at = pl.multiple_of(b * cols, cols)
        rhs[:cols] = rr[:, pl.ds(at, cols)]
        rhs[cols:] = gbuf[slot, me // (n // 2), pl.ds(pl.multiple_of((me % (n // 2)) * lrows, lrows), lrows), :]

        def rows_step(t, carry):
            left = gbuf[slot, t // per_half, pl.ds(pl.multiple_of((t % per_half) * tile, tile), tile), :]
            out = pl.ds(pl.multiple_of(t * tile, tile), tile)
            acc[out, :] += lax.dot_general(left, rhs[...], (((1,), (1,)), ((), ())), preferred_element_type=jnp.float32)
            return carry
        lax.fori_loop(0, 2 * per_half, rows_step, 0)
        prod = jnp.dot(gt[:, :half_rows], gbuf[slot, 0], preferred_element_type=jnp.float32)
        prod += jnp.dot(gt[:, half_rows:], gbuf[slot, 1], preferred_element_type=jnp.float32)
        ro_ref[:, pl.ds(at, cols)] = EMA_DECAY * ro_ref[:, pl.ds(at, cols)] + (1.0 - EMA_DECAY) * prod


    dx = 1 - 2 * c
    helper = (y * side + (x + dx + side) % side) * CORES + c
    client = (y * side + (x - dx + side) % side) * CORES + c
    up = (((y + 1) % side) * side + x) * CORES + c
    down = (((y + side - 1) % side) * side + x) * CORES + c
    half_count = lroot.shape[0]

    def root_block(dy, q, p=0):
        oy, ox = (y + dy) % side, (x + 2 * q) % side
        core = c + p * (1 - 2 * c)
        return (oy * (side // 2) + ox // 2) * CORES + core, (oy * side + ox) * CORES + core

    def root_copy(peer, sem, place, half, src=None, dst=None, recv=None):
        here = lroot.at[2 * place + half]
        return pltpu.make_async_remote_copy(
            src_ref=here if src is None else src, dst_ref=here if dst is None else dst, send_sem=l_send.at[sem],
            recv_sem=l_recv.at[2 * place + half] if recv is None else recv, device_id={"tensor": peer}, device_id_type=MESH)

    sent = [0, 0, 0, 0]

    def root_send(peer, sem, place, half, **kw):
        sent[sem] += 1
        root_copy(peer, sem, place, half, **kw).start()

    def root_wait(place, half):
        root_copy(twin, 3, place, half).wait_recv()

    own_place, _ = root_block(0, 0)
    far_place, _ = root_block(0, 1)
    passing = (y * (side // 2) + ((x - dx + side) % side) // 2) * CORES + c

    def root_start():
        for half in (0, 1):
            root_send(helper, 0, own_place, half, src=lr_ref.at[half], dst=relay.at[half], recv=relay_recv.at[half])
            root_send(up, 1, own_place, half, src=lr_ref.at[half])
            root_send(down, 2, own_place, 1 - half, src=lr_ref.at[1 - half])
        for half in (0, 1):
            root_send(twin, 3, own_place, half, src=lr_ref.at[half])

    def root_relay():
        for half in (0, 1):
            root_copy(helper, 0, own_place, half, src=lr_ref.at[half], dst=relay.at[half], recv=relay_recv.at[half]).wait_recv()
            root_send(helper, 0, passing, half, src=relay.at[half])

    def root_far():
        for half in (0, 1):
            root_wait(far_place, half)
            root_send(up, 1, far_place, half)
            root_send(down, 2, far_place, half)
            root_send(twin, 3, far_place, half)

    def root_round(r):
        q, stage = r // 3, r % 3
        if stage < 2:
            up_half = stage if q == 0 else stage
            down_half = 1 - stage if q == 0 else stage
            below, above = root_block(side - 1, q)[0], root_block(1, q)[0]
        else:
            up_half, down_half = 0, 1
            below = above = root_block(2, q)[0]
        root_wait(below, up_half)
        if stage < 2 and up_half == 0:
            root_send(up, 1, below, 0)
        root_send(twin, 3, below, up_half)
        root_wait(above, down_half)
        if stage < 2 and down_half == 1:
            root_send(down, 2, above, 1)
        root_send(twin, 3, above, down_half)

    steps(grad, gbuf, load_sem, GRAD_ROUND_STEP, [(ROOT_START_STEP, root_start)], grad_work)

    x_copy = pltpu.make_async_remote_copy(
        src_ref=xx.at[0], dst_ref=xx.at[1], send_sem=x_send.at[0], recv_sem=x_recv.at[0], device_id={"tensor": helper}, device_id_type=MESH)
    xx[0] = acc[:, :cols].astype(jnp.bfloat16)
    root_relay()
    x_copy.start()
    root_round(0)

    def left_step(t, carry):
        at = pl.ds(pl.multiple_of(t * lrows, lrows), lrows)
        lo_ref[:, at] = EMA_DECAY * lo_ref[:, at] + (1.0 - EMA_DECAY) * acc[at, cols:].T
        return carry
    lax.fori_loop(0, rows // lrows, left_step, 0)

    def at_step(i):
        e, p = i // 2, i % 2
        dy = lax.shift_right_logical(ROOT_Y, 2 * e) & 3
        q = lax.shift_right_logical(ROOT_X, 2 * e) & 3
        return root_block(dy, q, p)

    def twin_wait(i, place):
        @pl.when(i % 2 == 1)
        def _():
            root_wait(place, 0)
            root_wait(place, 1)

    def product(place, which):
        left = lroot[pl.ds(2 * place, 2)].reshape(lrows, rows)
        return jnp.dot(left, xx[which], preferred_element_type=jnp.float32)

    def rows_of(device):
        return pl.ds(pl.multiple_of(device * lrows, lrows), lrows)

    def own_rows(i):
        place, device = at_step(i)
        do_ref[rows_of(device), :] = product(place, 0)

    def lent_copy(place, device):
        return pltpu.make_async_remote_copy(
            src_ref=lent.at[place], dst_ref=do_ref.at[rows_of(device)], send_sem=d_send.at[0], recv_sem=d_recv.at[place],
            device_id={"tensor": client}, device_id_type=MESH)

    def lent_rows(i):
        place, device = at_step(i)
        lent[place] = product(place, 1)
        lent_copy(place, device).start()

    def loop(lo, hi, body):
        def step(i, carry):
            body(i)
            return carry
        lax.fori_loop(lo, hi, step, 0)

    def first_own(i):
        @pl.when(i == 2)
        def _():
            root_far()
            root_round(1)

        @pl.when(i == 8)
        def _():
            root_round(2)
        twin_wait(i, at_step(i)[0])
        own_rows(i)

    loop(0, 10, first_own)
    root_round(3)
    x_copy.wait_recv()
    loop(0, 10, lent_rows)
    root_round(4)

    def both(i):
        twin_wait(i, at_step(i)[0])
        lent_rows(i)
        own_rows(i)
    loop(10, 14, both)
    root_round(5)

    def last_lent(i):
        twin_wait(i, at_step(i)[0])
        lent_rows(i)
    loop(14, 16, last_lent)
    loop(14, 16, own_rows)

    grad.drain()
    for sem, count in enumerate(sent):
        whole = lroot.at[pl.ds(0, count)]
        pltpu.make_async_copy(whole, whole, l_send.at[sem]).wait()
    x_copy.wait_send()
    pltpu.make_async_copy(lent, lent, d_send.at[0]).wait()

    def lent_wait(i, carry):
        lent_copy(i, 0).wait_recv()
        return carry
    lax.fori_loop(0, half_count // 2, lent_wait, 0)


def store_kernel(*refs):
    count = (len(refs) - 1) // 2
    sems = refs[-1]
    pieces = 4
    for i in range(count):
        src, dst = refs[i], refs[count + i]
        step = src.shape[0] // pieces
        for j in range(pieces):
            part = pl.ds(j * step, step)
            pltpu.make_async_copy(src.at[part], dst.at[part], sems.at[i]).start()
    for i in range(count):
        pltpu.make_async_copy(refs[i], refs[count + i], sems.at[i]).wait()


def solution(mesh):
    row_spec = P(("layer", "tensor"), None)
    col_spec = P("layer", "tensor")
    n = mesh.shape["tensor"]
    side = math.isqrt(n // CORES)

    def local_step(g, l, r, lr, rr):
        rows, cols = g.shape
        lrows = l.shape[0]
        kept = n // 2
        hbm = pl.BlockSpec(memory_space=pltpu.HBM)
        vmem = pl.BlockSpec(memory_space=pltpu.VMEM)
        operands = [g.reshape(2, rows // 2, cols), l, r, lr.reshape(2, lrows // 2, rows), rr]
        left_new, right_new, direction, _ = pl.pallas_call(
            functools.partial(kernel, n, side),
            name="shampoo",
            out_shape=[
                pltpu.VMEM(l.shape, jnp.float32),
                pltpu.VMEM(r.shape, jnp.float32),
                pltpu.VMEM(g.shape, jnp.float32),
                pltpu.HBM((2 * n, rows // 2, cols), jnp.bfloat16),
            ],
            in_specs=[hbm] * 5,
            out_specs=[vmem, vmem, vmem, hbm],
            scratch_shapes=[
                pltpu.VMEM(rr.shape, jnp.bfloat16),
                pltpu.VMEM((cols, rows), jnp.bfloat16),
                pltpu.VMEM((rows, cols + lrows), jnp.float32),
                pltpu.VMEM((2, 2, rows // 2, cols), jnp.bfloat16),
                pltpu.VMEM((cols + lrows, cols), jnp.bfloat16),
                pltpu.VMEM((2, rows, cols), jnp.bfloat16),
                pltpu.VMEM((2 * kept, lrows // 2, rows), jnp.bfloat16),
                pltpu.VMEM((2, lrows // 2, rows), jnp.bfloat16),
                pltpu.VMEM((kept, lrows, cols), jnp.float32),
                pltpu.SemaphoreType.DMA((2 * n,)),
                pltpu.SemaphoreType.DMA((5,)),
                pltpu.SemaphoreType.DMA((2,)),
                pltpu.SemaphoreType.DMA((4,)),
                pltpu.SemaphoreType.DMA((2 * kept,)),
                pltpu.SemaphoreType.DMA((2,)),
                pltpu.SemaphoreType.DMA((1,)),
                pltpu.SemaphoreType.DMA((kept,)),
                pltpu.SemaphoreType.DMA((4,)),
                pltpu.SemaphoreType.DMA((1,)),
                pltpu.SemaphoreType.DMA((1,)),
            ],
            compiler_params=pltpu.CompilerParams(collective_id=0, has_side_effects=True, vmem_limit_bytes=48 * 2**20),
            cost_estimate=pl.CostEstimate(flops=2 * rows * cols * (2 * n * cols + 2 * rows), bytes_accessed=2 * n * rows * cols * 3, transcendentals=0),
        )(*[pltpu.with_memory_space_constraint(v, pltpu.HBM) for v in operands])
        results = [left_new, right_new, direction]
        return pl.pallas_call(
            store_kernel,
            name="store",
            out_shape=[jax.ShapeDtypeStruct(v.shape, v.dtype) for v in results],
            in_specs=[vmem] * 3,
            out_specs=[hbm] * 3,
            scratch_shapes=[pltpu.SemaphoreType.DMA((3,))],
            compiler_params=pltpu.CompilerParams(vmem_limit_bytes=1 * 2**20),
        )(*results)

    return jax.shard_map(local_step, mesh=mesh, in_specs=(col_spec, row_spec, row_spec, row_spec, row_spec), out_specs=(row_spec, row_spec, col_spec), check_vma=False)
```

```python
import functools
import math

import jax
import jax.numpy as jnp
from jax import lax
from jax.experimental import pallas as pl
from jax.experimental.pallas import tpu as pltpu
from jax.sharding import PartitionSpec as P

EMA_DECAY = 0.9
CORES = 2
MESH = pl.DeviceIdType.MESH

ORDER = [(int(a), int(b)) for a, b in zip("0310020311322312", "0003102313131222")]
UP = [
    ((0, 3), 0, [((0, 3), 0)]), ((0, 3), 1, []), ((3, 3), 0, [((3, 3), 0)]), ((1, 3), 1, []), ((0, 2), 0, []), ((3, 3), 1, []),
    ((1, 3), 0, [((1, 3), 0)]), ((2, 3), 0, [((2, 3), 0)]), ((2, 3), 1, []), ((3, 2), 0, []), ((1, 2), 0, []), ((2, 2), 0, []),
]
DOWN = [
    ((0, 1), 1, [((0, 1), 1)]), ((0, 1), 0, []), ((1, 1), 1, []), ((3, 1), 0, []), ((0, 2), 1, []), ((1, 1), 0, []),
    ((3, 1), 1, [((3, 1), 1), ((1, 1), 1)]), ((2, 1), 1, [((2, 1), 1)]), ((2, 1), 0, []), ((3, 2), 1, []), ((1, 2), 1, []), ((2, 2), 1, []),
]
ROUNDS = len(UP)
FIRST_UP = [((3, 0), 0, True), ((3, 0), 1, False), ((2, 0), 0, False)]
FIRST_DOWN = [((1, 0), 1, True), ((1, 0), 0, False), ((2, 0), 1, False)]
GRAD_ROUND_STEP = [2, 2, 8, 10, 12, 14, 17, 20, 22, 26, 28, 30]
ROOT_START_STEP = 30
RELAY_STEP = 31
LATE = (2, 12, 14, 22, 26, 28, 30)
MIDDLE = (3, 13, 15, 23, 27, 29, 31)


def packed(values):
    return [sum(v << (2 * i) for i, v in enumerate(values[j:j + 8])) for j in (0, 8)]


FIRST_CODE = packed([o[0] for o in ORDER])
SECOND_CODE = packed([o[1] for o in ORDER])


def lookup(code, e):
    word = code[0] + (e // 8) * (code[1] - code[0])
    return lax.shift_right_logical(word, 2 * (e % 8)) & 3


ROOT_ORDER = [(0, 0), (3, 0), (1, 0), (0, 1), (2, 0), (3, 1), (1, 1), (2, 1)]
ROOT_Y = sum(o[0] << (2 * i) for i, o in enumerate(ROOT_ORDER))
ROOT_X = sum(o[1] << (2 * i) for i, o in enumerate(ROOT_ORDER))


def kernel(n, side, g_ref, l_ref, r_ref, lr_ref, rr_ref, lo_ref, ro_ref, do_ref, gfull,
           rr, gt, acc, gbuf, rhs, xx, lroot, relay, lent,
           g_recv, g_send, load_sem, init_sem, l_recv, last_recv, relay_recv, x_recv, d_recv, l_send, x_send, d_send):
    _, half_rows, cols = g_ref.shape
    rows = 2 * half_rows
    lrows = l_ref.shape[0]
    tile = min(1024, half_rows)

    me = lax.axis_index("tensor")
    c = me % CORES
    chip = me // CORES
    x, y = chip % side, chip // side
    f = x + c * (y - x)
    s = y + c * (x - y)
    fstep = CORES + c * CORES * (side - 1)
    sstep = CORES * side - c * CORES * (side - 1)
    twin = me + 1 - 2 * c

    def index(df, ds):
        return ((f + df) % side) * fstep + ((s + ds) % side) * sstep + c

    def twin_index(df, ds):
        return ((s + df) % side) * sstep + ((f + ds) % side) * fstep + 1 - c

    peers = {"f+": index(1, 0), "f-": index(3, 0), "s+": index(0, 1), "s-": index(0, 3), "twin": twin}
    slot_of = {name: i for i, name in enumerate(peers)}

    class Gather:
        def __init__(self, own, full, recv, send):
            self.own, self.full, self.recv, self.send_sem = own, full, recv, send
            self.count = {name: 0 for name in peers}

        def copy(self, name, b, half, own=False):
            src = self.own.at[half] if own else self.full.at[2 * b + half]
            return pltpu.make_async_remote_copy(
                src_ref=src, dst_ref=self.full.at[2 * b + half], send_sem=self.send_sem.at[slot_of[name]],
                recv_sem=self.recv.at[2 * b + half], device_id={"tensor": peers[name]}, device_id_type=MESH)

        def send(self, name, b, half, own=False):
            self.count[name] += 1
            self.copy(name, b, half, own).start()

        def wait(self, b, half):
            self.copy("twin", b, half).wait_recv()

        def start(self):
            for half in (0, 1):
                for name in ("f+", "s+"):
                    self.send(name, me, half, own=True)
                for name in ("f-", "s-"):
                    self.send(name, me, 1 - half, own=True)
            for half in (0, 1):
                self.send("twin", me, half, own=True)

        def round(self, r):
            if r < len(FIRST_UP):
                (ou, hu, on), (od, hd, _) = FIRST_UP[r], FIRST_DOWN[r]
                bu, bd = index(*ou), index(*od)
                self.wait(bu, hu)
                if on:
                    self.send("f+", bu, hu)
                self.wait(bd, hd)
                if on:
                    self.send("f-", bd, hd)
                self.send("s+", bu, hu)
                self.send("s-", bd, hd)
                self.send("s+", bd, hd)
                self.send("s-", bu, hu)
                self.send("twin", bu, hu)
                self.send("twin", bd, hd)
            (ou, hu, fu), (od, hd, fd) = UP[r], DOWN[r]
            bu, bd = index(*ou), index(*od)
            self.wait(bu, hu)
            for offset, half in fu:
                self.send("s+", index(*offset), half)
            self.send("twin", bu, hu)
            self.wait(bd, hd)
            for offset, half in fd:
                self.send("s-", index(*offset), half)
            self.send("twin", bd, hd)

        def drain(self):
            for name, count in self.count.items():
                whole = self.full.at[pl.ds(0, count)]
                pltpu.make_async_copy(whole, whole, self.send_sem.at[slot_of[name]]).wait()

    grad = Gather(g_ref, gfull, g_recv, g_send)

    def block_of(k):
        e, other = k // 2, k % 2
        df, ds = lookup(FIRST_CODE, e), lookup(SECOND_CODE, e)
        mine = index(df, ds)
        return mine + other * (twin_index(df, ds) - mine)

    def load(gather, buf, k, sem):
        b = block_of(k)
        return pltpu.make_async_copy(gather.full.at[pl.ds(2 * b, 2)], buf.at[k % 2], sem.at[k % 2])

    def start_load(gather, buf, k, sem):
        @pl.when(k % 2 == 1)
        def _():
            b = block_of(k)
            with jax.named_scope("twinwait"):
                gather.wait(b, 0)
                gather.wait(b, 1)
        load(gather, buf, k, sem).start()

    def one_of(k, values):
        found = k == values[0]
        for v in values[1:]:
            found = found | (k == v)
        return found

    def steps(gather, buf, sem, round_step, extra, work):
        def step(k, carry):
            for at, fn in extra:
                pl.when(k == at)(fn)
            for r in range(ROUNDS):
                @pl.when(k == round_step[r])
                def _():
                    with jax.named_scope(f"ground{r}"):
                        gather.round(r)

            @pl.when(one_of(k, LATE))
            def _():
                start_load(gather, buf, k, sem)

            @pl.when((k + 1 < n) & jnp.logical_not(one_of(k + 1, LATE + MIDDLE)))
            def _():
                start_load(gather, buf, k + 1, sem)

            def middle():
                @pl.when(one_of(k + 1, MIDDLE))
                def _():
                    start_load(gather, buf, k + 1, sem)
            with jax.named_scope("loadwait"):
                load(gather, buf, k, sem).wait()
            with jax.named_scope("work"):
                work(k, k % 2, block_of(k), middle)
            return carry
        lax.fori_loop(0, n, step, 0)

    first = [
        pltpu.make_async_copy(rr_ref, rr, init_sem.at[0]),
        pltpu.make_async_copy(r_ref, ro_ref, init_sem.at[1]),
        pltpu.make_async_copy(l_ref, lo_ref, init_sem.at[2]),
        pltpu.make_async_copy(lr_ref, lroot.at[pl.ds(2 * ((y * (side // 2) + x // 2) * CORES + c), 2)], init_sem.at[3]),
    ]
    own_load = pltpu.make_async_copy(g_ref, gbuf.at[0], load_sem.at[0])
    own_load.start()

    barrier = pltpu.get_barrier_semaphore()
    for peer in peers.values():
        pl.semaphore_signal(barrier, inc=1, device_id={"tensor": peer}, device_id_type=MESH)
    with jax.named_scope("barrier"):
        pl.semaphore_wait(barrier, len(peers))
    grad.start()
    for copy in first:
        copy.start()

    acc[...] = jnp.zeros_like(acc)
    own_load.wait()
    for h in (0, 1):
        gt[:, h * half_rows:(h + 1) * half_rows] = gbuf[0, h].T
    for copy in first:
        copy.wait()
    own_load.start()

    per_half = half_rows // tile

    def grad_work(k, slot, b, middle):
        at = pl.multiple_of(b * cols, cols)
        rhs[:cols] = rr[:, pl.ds(at, cols)]
        rhs[cols:] = gbuf[slot, me // (n // 2), pl.ds(pl.multiple_of((me % (n // 2)) * lrows, lrows), lrows), :]

        def rows_step(t, carry):
            left = gbuf[slot, t // per_half, pl.ds(pl.multiple_of((t % per_half) * tile, tile), tile), :]
            out = pl.ds(pl.multiple_of(t * tile, tile), tile)
            acc[out, :] += lax.dot_general(left, rhs[...], (((1,), (1,)), ((), ())), preferred_element_type=jnp.float32)
            return carry
        lax.fori_loop(0, 2 * per_half, rows_step, 0)
        middle()
        prod = jnp.dot(gt[:, :half_rows], gbuf[slot, 0], preferred_element_type=jnp.float32)
        prod += jnp.dot(gt[:, half_rows:], gbuf[slot, 1], preferred_element_type=jnp.float32)
        ro_ref[:, pl.ds(at, cols)] = EMA_DECAY * ro_ref[:, pl.ds(at, cols)] + (1.0 - EMA_DECAY) * prod


    dx = 1 - 2 * c
    helper = (y * side + (x + dx + side) % side) * CORES + c
    client = (y * side + (x - dx + side) % side) * CORES + c
    up = (((y + 1) % side) * side + x) * CORES + c
    down = (((y + side - 1) % side) * side + x) * CORES + c
    half_count, root_half, _ = lroot.shape
    quarter = root_half // 2

    def root_block(dy, q, p=0):
        oy, ox = (y + dy) % side, (x + 2 * q) % side
        core = c + p * (1 - 2 * c)
        return (oy * (side // 2) + ox // 2) * CORES + core, (oy * side + ox) * CORES + core

    def root_copy(peer, sem, place, half, src=None, dst=None, recv=None, part=None):
        here = lroot.at[2 * place + half]
        if part is not None:
            here = here.at[pl.ds(part * quarter, quarter)]
        return pltpu.make_async_remote_copy(
            src_ref=here if src is None else src, dst_ref=here if dst is None else dst, send_sem=l_send.at[sem],
            recv_sem=l_recv.at[2 * place + half] if recv is None else recv, device_id={"tensor": peer}, device_id_type=MESH)

    sent = [0, 0, 0, 0]

    def root_send(peer, sem, place, half, part=None, **kw):
        sent[sem] += 1 if part is None else 0.5
        root_copy(peer, sem, place, half, part=part, **kw).start()

    def root_wait(place, half, **kw):
        root_copy(twin, 3, place, half, **kw).wait_recv()

    own_place, _ = root_block(0, 0)
    far_place, _ = root_block(0, 1)
    passing = (y * (side // 2) + ((x - dx + side) % side) // 2) * CORES + c

    def root_start():
        for half in (0, 1):
            root_send(helper, 0, own_place, half, src=lr_ref.at[half], dst=relay.at[half], recv=relay_recv.at[half])
            root_send(up, 1, own_place, half, src=lr_ref.at[half])
            root_send(down, 2, own_place, 1 - half, src=lr_ref.at[1 - half])
        for half in (0, 1):
            root_send(twin, 3, own_place, half, src=lr_ref.at[half])

    def root_relay(half):
        root_copy(helper, 0, own_place, half, src=lr_ref.at[half], dst=relay.at[half], recv=relay_recv.at[half]).wait_recv()
        root_send(helper, 0, passing, half, src=relay.at[half])

    def root_far():
        for half in (0, 1):
            root_wait(far_place, half)
            root_send(up, 1, far_place, half)
            root_send(twin, 3, far_place, half)
        for half in (1, 0):
            root_send(down, 2, far_place, half)

    def root_round(r):
        q, stage = r // 3, r % 3
        if stage == 2:
            behind = root_block(2, q)[0]
            for half in (0, 1):
                root_wait(behind, half)
                root_send(twin, 3, behind, half)
            return
        below, above = root_block(side - 1, q)[0], root_block(1, q)[0]
        root_wait(below, stage)
        if stage == 0:
            for part in (None,) if q == 0 else (0, 1):
                root_send(up, 1, below, 0, part=part, recv=last_recv.at[0] if part else None)
        root_send(twin, 3, below, stage)
        root_wait(above, 1 - stage)
        if stage == 0:
            for part in (None,) if q == 0 else (0, 1):
                root_send(down, 2, above, 1, part=part, recv=last_recv.at[1] if part else None)
        root_send(twin, 3, above, 1 - stage)

    last_place, last_device = root_block(2, 1)
    twin_place, twin_device = root_block(2, 1, 1)

    def root_last(part):
        for half in (0, 1):
            root_wait(last_place, half, part=part, recv=last_recv.at[half] if part else None)
            root_send(twin, 3, last_place, half, part=part, recv=last_recv.at[2 + half] if part else None)

    def root_last_twin(part):
        for half in (0, 1):
            root_wait(twin_place, half, part=part, recv=last_recv.at[2 + half] if part else None)

    steps(grad, gbuf, load_sem, GRAD_ROUND_STEP, [(ROOT_START_STEP, root_start), (RELAY_STEP, lambda: root_relay(0))], grad_work)

    x_copy = pltpu.make_async_remote_copy(
        src_ref=xx.at[0], dst_ref=xx.at[1], send_sem=x_send.at[0], recv_sem=x_recv.at[0], device_id={"tensor": helper}, device_id_type=MESH)
    with jax.named_scope("xfin"):
        xx[0] = acc[:, :cols].astype(jnp.bfloat16)
    with jax.named_scope("relay"):
        root_relay(1)
    x_copy.start()
    with jax.named_scope("rround0"):
        root_round(0)

    def left_step(t, carry):
        at = pl.ds(pl.multiple_of(t * lrows, lrows), lrows)
        lo_ref[:, at] = EMA_DECAY * lo_ref[:, at] + (1.0 - EMA_DECAY) * acc[at, cols:].T
        return carry
    with jax.named_scope("leftfin"):
        lax.fori_loop(0, rows // lrows, left_step, 0)

    def at_step(i):
        e, p = i // 2, i % 2
        dy = lax.shift_right_logical(ROOT_Y, 2 * e) & 3
        q = lax.shift_right_logical(ROOT_X, 2 * e) & 3
        return root_block(dy, q, p)

    def twin_wait(i, place):
        @pl.when(i % 2 == 1)
        def _():
            root_wait(place, 0)
            root_wait(place, 1)

    def product(place, which):
        left = lroot[pl.ds(2 * place, 2)].reshape(lrows, rows)
        return jnp.dot(left, xx[which], preferred_element_type=jnp.float32)

    def rows_of(device):
        return pl.ds(pl.multiple_of(device * lrows, lrows), lrows)

    def own_rows(i):
        place, device = at_step(i)
        do_ref[rows_of(device), :] = product(place, 0)

    def lent_copy(place, device):
        return pltpu.make_async_remote_copy(
            src_ref=lent.at[place], dst_ref=do_ref.at[rows_of(device)], send_sem=d_send.at[0], recv_sem=d_recv.at[place],
            device_id={"tensor": client}, device_id_type=MESH)

    def lent_rows(i):
        place, device = at_step(i)
        lent[place] = product(place, 1)
        lent_copy(place, device).start()

    def loop(lo, hi, body):
        def step(i, carry):
            body(i)
            return carry
        lax.fori_loop(lo, hi, step, 0)

    def first_own(i):
        @pl.when(i == 2)
        def _():
            with jax.named_scope("far"):
                root_far()
            with jax.named_scope("rround1"):
                root_round(1)

        @pl.when(i == 8)
        def _():
            with jax.named_scope("rround2"):
                root_round(2)
        twin_wait(i, at_step(i)[0])
        own_rows(i)

    loop(0, 10, first_own)
    with jax.named_scope("rround3"):
        root_round(3)
    with jax.named_scope("xwait"):
        x_copy.wait_recv()
    with jax.named_scope("lentloop"):
        loop(0, 10, lent_rows)
    with jax.named_scope("rround4"):
        root_round(4)

    def both(i):
        twin_wait(i, at_step(i)[0])
        lent_rows(i)
        own_rows(i)
    with jax.named_scope("both"):
        loop(10, 14, both)

    def quarter_product(place, part, which):
        rows = pl.ds(part * quarter, quarter)
        left = jnp.concatenate([lroot[2 * place, rows, :], lroot[2 * place + 1, rows, :]], axis=0)
        return jnp.dot(left, xx[which], preferred_element_type=jnp.float32)

    def lent_quarter(place, device, part):
        prod = quarter_product(place, part, 1)
        for half in (0, 1):
            at = half * root_half + part * quarter
            lent[place, pl.ds(at, quarter), :] = prod[half * quarter:(half + 1) * quarter]
            pltpu.make_async_remote_copy(
                src_ref=lent.at[place, pl.ds(at, quarter)], dst_ref=do_ref.at[pl.ds(pl.multiple_of(device * lrows, lrows) + at, quarter)],
                send_sem=d_send.at[0], recv_sem=d_recv.at[place], device_id={"tensor": client}, device_id_type=MESH).start()

    def own_quarter(place, device, part):
        prod = quarter_product(place, part, 0)
        for half in (0, 1):
            at = half * root_half + part * quarter
            do_ref[pl.ds(pl.multiple_of(device * lrows, lrows) + at, quarter), :] = prod[half * quarter:(half + 1) * quarter]

    for part in (0, 1):
        with jax.named_scope(f"last{part}"):
            root_last(part)
        lent_quarter(last_place, last_device, part)
        with jax.named_scope(f"lasttwin{part}"):
            root_last_twin(part)
        lent_quarter(twin_place, twin_device, part)
        own_quarter(last_place, last_device, part)
        own_quarter(twin_place, twin_device, part)

    with jax.named_scope("drain"):
        grad.drain()
    for sem, count in enumerate(sent):
        whole = lroot.at[pl.ds(0, int(count))]
        pltpu.make_async_copy(whole, whole, l_send.at[sem]).wait()
    x_copy.wait_send()
    pltpu.make_async_copy(lent, lent, d_send.at[0]).wait()

    def lent_wait(i, carry):
        lent_copy(i, 0).wait_recv()
        return carry
    with jax.named_scope("dwait"):
        lax.fori_loop(0, half_count // 2, lent_wait, 0)


def store_kernel(*refs):
    count = (len(refs) - 1) // 2
    sems = refs[-1]
    pieces = 4
    for i in range(count):
        src, dst = refs[i], refs[count + i]
        step = src.shape[0] // pieces
        for j in range(pieces):
            part = pl.ds(j * step, step)
            pltpu.make_async_copy(src.at[part], dst.at[part], sems.at[i]).start()
    for i in range(count):
        pltpu.make_async_copy(refs[i], refs[count + i], sems.at[i]).wait()


def solution(mesh):
    row_spec = P(("layer", "tensor"), None)
    col_spec = P("layer", "tensor")
    n = mesh.shape["tensor"]
    side = math.isqrt(n // CORES)

    def local_step(g, l, r, lr, rr):
        rows, cols = g.shape
        lrows = l.shape[0]
        kept = n // 2
        hbm = pl.BlockSpec(memory_space=pltpu.HBM)
        vmem = pl.BlockSpec(memory_space=pltpu.VMEM)
        operands = [g.reshape(2, rows // 2, cols), l, r, lr.reshape(2, lrows // 2, rows), rr]
        left_new, right_new, direction, _ = pl.pallas_call(
            functools.partial(kernel, n, side),
            name="shampoo",
            out_shape=[
                pltpu.VMEM(l.shape, jnp.float32),
                pltpu.VMEM(r.shape, jnp.float32),
                pltpu.VMEM(g.shape, jnp.float32),
                pltpu.HBM((2 * n, rows // 2, cols), jnp.bfloat16),
            ],
            in_specs=[hbm] * 5,
            out_specs=[vmem, vmem, vmem, hbm],
            scratch_shapes=[
                pltpu.VMEM(rr.shape, jnp.bfloat16),
                pltpu.VMEM((cols, rows), jnp.bfloat16),
                pltpu.VMEM((rows, cols + lrows), jnp.float32),
                pltpu.VMEM((2, 2, rows // 2, cols), jnp.bfloat16),
                pltpu.VMEM((cols + lrows, cols), jnp.bfloat16),
                pltpu.VMEM((2, rows, cols), jnp.bfloat16),
                pltpu.VMEM((2 * kept, lrows // 2, rows), jnp.bfloat16),
                pltpu.VMEM((2, lrows // 2, rows), jnp.bfloat16),
                pltpu.VMEM((kept, lrows, cols), jnp.float32),
                pltpu.SemaphoreType.DMA((2 * n,)),
                pltpu.SemaphoreType.DMA((5,)),
                pltpu.SemaphoreType.DMA((2,)),
                pltpu.SemaphoreType.DMA((4,)),
                pltpu.SemaphoreType.DMA((2 * kept,)),
                pltpu.SemaphoreType.DMA((4,)),
                pltpu.SemaphoreType.DMA((2,)),
                pltpu.SemaphoreType.DMA((1,)),
                pltpu.SemaphoreType.DMA((kept,)),
                pltpu.SemaphoreType.DMA((4,)),
                pltpu.SemaphoreType.DMA((1,)),
                pltpu.SemaphoreType.DMA((1,)),
            ],
            compiler_params=pltpu.CompilerParams(collective_id=0, has_side_effects=True, vmem_limit_bytes=48 * 2**20),
            cost_estimate=pl.CostEstimate(flops=2 * rows * cols * (2 * n * cols + 2 * rows), bytes_accessed=2 * n * rows * cols * 3, transcendentals=0),
        )(*[pltpu.with_memory_space_constraint(v, pltpu.HBM) for v in operands])
        results = [left_new, right_new, direction]
        return pl.pallas_call(
            store_kernel,
            name="store",
            out_shape=[jax.ShapeDtypeStruct(v.shape, v.dtype) for v in results],
            in_specs=[vmem] * 3,
            out_specs=[hbm] * 3,
            scratch_shapes=[pltpu.SemaphoreType.DMA((3,))],
            compiler_params=pltpu.CompilerParams(vmem_limit_bytes=1 * 2**20),
        )(*results)

    return jax.shard_map(local_step, mesh=mesh, in_specs=(col_spec, row_spec, row_spec, row_spec, row_spec), out_specs=(row_spec, row_spec, col_spec), check_vma=False)
```

```python
import functools
import math

import jax
import jax.numpy as jnp
from jax import lax
from jax.experimental import pallas as pl
from jax.experimental.pallas import tpu as pltpu
from jax.sharding import PartitionSpec as P

EMA_DECAY = 0.9
CORES = 2
MESH = pl.DeviceIdType.MESH

ORDER = [(int(a), int(b)) for a, b in zip("0310020311322312", "0003102313131222")]
UP = [
    ((0, 3), 0, [((0, 3), 0)]), ((0, 3), 1, []), ((3, 3), 0, [((3, 3), 0)]), ((1, 3), 1, []), ((0, 2), 0, []), ((3, 3), 1, []),
    ((1, 3), 0, [((1, 3), 0)]), ((2, 3), 0, [((2, 3), 0)]), ((2, 3), 1, []), ((3, 2), 0, []), ((1, 2), 0, []), ((2, 2), 0, []),
]
DOWN = [
    ((0, 1), 1, [((0, 1), 1)]), ((0, 1), 0, []), ((1, 1), 1, []), ((3, 1), 0, []), ((0, 2), 1, []), ((1, 1), 0, []),
    ((3, 1), 1, [((3, 1), 1), ((1, 1), 1)]), ((2, 1), 1, [((2, 1), 1)]), ((2, 1), 0, []), ((3, 2), 1, []), ((1, 2), 1, []), ((2, 2), 1, []),
]
ROUNDS = len(UP)
FIRST_UP = [((3, 0), 0, True), ((3, 0), 1, False), ((2, 0), 0, False)]
FIRST_DOWN = [((1, 0), 1, True), ((1, 0), 0, False), ((2, 0), 1, False)]
GRAD_ROUND_STEP = [2, 2, 8, 10, 12, 14, 17, 20, 22, 26, 28, 30]
ROOT_START_STEP = 30
RELAY_STEP = 31
LATE = (2, 12, 14, 22, 26, 28, 30)
MIDDLE = (3, 13, 15, 23, 27, 29, 31)


def packed(values):
    return [sum(v << (2 * i) for i, v in enumerate(values[j:j + 8])) for j in (0, 8)]


FIRST_CODE = packed([o[0] for o in ORDER])
SECOND_CODE = packed([o[1] for o in ORDER])


def lookup(code, e):
    word = code[0] + (e // 8) * (code[1] - code[0])
    return lax.shift_right_logical(word, 2 * (e % 8)) & 3


ROOT_ORDER = [(0, 0), (3, 0), (1, 0), (0, 1), (2, 0), (3, 1), (1, 1), (2, 1)]
ROOT_Y = sum(o[0] << (2 * i) for i, o in enumerate(ROOT_ORDER))
ROOT_X = sum(o[1] << (2 * i) for i, o in enumerate(ROOT_ORDER))


def kernel(n, side, g_ref, l_ref, r_ref, lr_ref, rr_ref, lo_ref, ro_ref, do_ref, gfull,
           rr, gt, acc, gbuf, rhs, xx, lroot, relay, lent,
           g_recv, g_send, load_sem, init_sem, l_recv, last_recv, relay_recv, x_recv, d_recv, l_send, x_send, d_send):
    _, half_rows, cols = g_ref.shape
    rows = 2 * half_rows
    lrows = l_ref.shape[0]
    tile = min(1024, half_rows)

    me = lax.axis_index("tensor")
    c = me % CORES
    chip = me // CORES
    x, y = chip % side, chip // side
    f = x + c * (y - x)
    s = y + c * (x - y)
    fstep = CORES + c * CORES * (side - 1)
    sstep = CORES * side - c * CORES * (side - 1)
    twin = me + 1 - 2 * c

    def index(df, ds):
        return ((f + df) % side) * fstep + ((s + ds) % side) * sstep + c

    def twin_index(df, ds):
        return ((s + df) % side) * sstep + ((f + ds) % side) * fstep + 1 - c

    peers = {"f+": index(1, 0), "f-": index(3, 0), "s+": index(0, 1), "s-": index(0, 3), "twin": twin}
    slot_of = {name: i for i, name in enumerate(peers)}

    class Gather:
        def __init__(self, own, full, recv, send):
            self.own, self.full, self.recv, self.send_sem = own, full, recv, send
            self.count = {name: 0 for name in peers}

        def copy(self, name, b, half, own=False):
            src = self.own.at[half] if own else self.full.at[2 * b + half]
            return pltpu.make_async_remote_copy(
                src_ref=src, dst_ref=self.full.at[2 * b + half], send_sem=self.send_sem.at[slot_of[name]],
                recv_sem=self.recv.at[2 * b + half], device_id={"tensor": peers[name]}, device_id_type=MESH)

        def send(self, name, b, half, own=False):
            self.count[name] += 1
            self.copy(name, b, half, own).start()

        def wait(self, b, half):
            self.copy("twin", b, half).wait_recv()

        def start(self):
            for half in (0, 1):
                for name in ("f+", "s+"):
                    self.send(name, me, half, own=True)
                for name in ("f-", "s-"):
                    self.send(name, me, 1 - half, own=True)
            for half in (0, 1):
                self.send("twin", me, half, own=True)

        def round(self, r):
            if r < len(FIRST_UP):
                (ou, hu, on), (od, hd, _) = FIRST_UP[r], FIRST_DOWN[r]
                bu, bd = index(*ou), index(*od)
                self.wait(bu, hu)
                if on:
                    self.send("f+", bu, hu)
                self.wait(bd, hd)
                if on:
                    self.send("f-", bd, hd)
                self.send("s+", bu, hu)
                self.send("s-", bd, hd)
                self.send("s+", bd, hd)
                self.send("s-", bu, hu)
                self.send("twin", bu, hu)
                self.send("twin", bd, hd)
            (ou, hu, fu), (od, hd, fd) = UP[r], DOWN[r]
            bu, bd = index(*ou), index(*od)
            self.wait(bu, hu)
            for offset, half in fu:
                self.send("s+", index(*offset), half)
            self.send("twin", bu, hu)
            self.wait(bd, hd)
            for offset, half in fd:
                self.send("s-", index(*offset), half)
            self.send("twin", bd, hd)

        def drain(self):
            for name, count in self.count.items():
                whole = self.full.at[pl.ds(0, count)]
                pltpu.make_async_copy(whole, whole, self.send_sem.at[slot_of[name]]).wait()

    grad = Gather(g_ref, gfull, g_recv, g_send)

    def block_of(k):
        e, other = k // 2, k % 2
        df, ds = lookup(FIRST_CODE, e), lookup(SECOND_CODE, e)
        mine = index(df, ds)
        return mine + other * (twin_index(df, ds) - mine)

    def load(gather, buf, k, sem):
        b = block_of(k)
        return pltpu.make_async_copy(gather.full.at[pl.ds(2 * b, 2)], buf.at[k % 2], sem.at[k % 2])

    def start_load(gather, buf, k, sem):
        @pl.when(k % 2 == 1)
        def _():
            b = block_of(k)
            with jax.named_scope("twinwait"):
                gather.wait(b, 0)
                gather.wait(b, 1)
        load(gather, buf, k, sem).start()

    def one_of(k, values):
        found = k == values[0]
        for v in values[1:]:
            found = found | (k == v)
        return found

    def steps(gather, buf, sem, round_step, extra, work):
        def step(k, carry):
            for at, fn in extra:
                pl.when(k == at)(fn)
            for r in range(ROUNDS):
                @pl.when(k == round_step[r])
                def _():
                    with jax.named_scope(f"ground{r}"):
                        gather.round(r)

            @pl.when(one_of(k, LATE))
            def _():
                start_load(gather, buf, k, sem)

            @pl.when((k + 1 < n) & jnp.logical_not(one_of(k + 1, LATE + MIDDLE)))
            def _():
                start_load(gather, buf, k + 1, sem)

            def middle():
                @pl.when(one_of(k + 1, MIDDLE))
                def _():
                    start_load(gather, buf, k + 1, sem)
            with jax.named_scope("loadwait"):
                load(gather, buf, k, sem).wait()
            with jax.named_scope("work"):
                work(k, k % 2, block_of(k), middle)
            return carry
        lax.fori_loop(0, n, step, 0)

    first = [
        pltpu.make_async_copy(rr_ref, rr, init_sem.at[0]),
        pltpu.make_async_copy(r_ref, ro_ref, init_sem.at[1]),
        pltpu.make_async_copy(l_ref, lo_ref, init_sem.at[2]),
        pltpu.make_async_copy(lr_ref, lroot.at[pl.ds(2 * ((y * (side // 2) + x // 2) * CORES + c), 2)], init_sem.at[3]),
    ]
    own_load = pltpu.make_async_copy(g_ref, gbuf.at[0], load_sem.at[0])
    own_load.start()

    barrier = pltpu.get_barrier_semaphore()
    for peer in peers.values():
        pl.semaphore_signal(barrier, inc=1, device_id={"tensor": peer}, device_id_type=MESH)
    with jax.named_scope("barrier"):
        pl.semaphore_wait(barrier, len(peers))
    grad.start()
    for copy in first:
        copy.start()

    acc[...] = jnp.zeros_like(acc)
    own_load.wait()
    for h in (0, 1):
        gt[:, h * half_rows:(h + 1) * half_rows] = gbuf[0, h].T
    for copy in first:
        copy.wait()
    own_load.start()

    per_half = half_rows // tile

    def grad_work(k, slot, b, middle):
        at = pl.multiple_of(b * cols, cols)
        rhs[:cols] = rr[:, pl.ds(at, cols)]
        rhs[cols:] = gbuf[slot, me // (n // 2), pl.ds(pl.multiple_of((me % (n // 2)) * lrows, lrows), lrows), :]

        def rows_step(t, carry):
            left = gbuf[slot, t // per_half, pl.ds(pl.multiple_of((t % per_half) * tile, tile), tile), :]
            out = pl.ds(pl.multiple_of(t * tile, tile), tile)
            acc[out, :] += lax.dot_general(left, rhs[...], (((1,), (1,)), ((), ())), preferred_element_type=jnp.float32)
            return carry
        lax.fori_loop(0, 2 * per_half, rows_step, 0)
        middle()
        prod = jnp.dot(gt[:, :half_rows], gbuf[slot, 0], preferred_element_type=jnp.float32)
        prod += jnp.dot(gt[:, half_rows:], gbuf[slot, 1], preferred_element_type=jnp.float32)
        ro_ref[:, pl.ds(at, cols)] = EMA_DECAY * ro_ref[:, pl.ds(at, cols)] + (1.0 - EMA_DECAY) * prod


    dx = 1 - 2 * c
    helper = (y * side + (x + dx + side) % side) * CORES + c
    client = (y * side + (x - dx + side) % side) * CORES + c
    up = (((y + 1) % side) * side + x) * CORES + c
    down = (((y + side - 1) % side) * side + x) * CORES + c
    half_count, root_half, _ = lroot.shape
    pieces = ((0, root_half - root_half // 4), (root_half - root_half // 4, root_half // 4))

    def root_block(dy, q, p=0):
        oy, ox = (y + dy) % side, (x + 2 * q) % side
        core = c + p * (1 - 2 * c)
        return (oy * (side // 2) + ox // 2) * CORES + core, (oy * side + ox) * CORES + core

    def root_copy(peer, sem, place, half, src=None, dst=None, recv=None, part=None):
        here = lroot.at[2 * place + half]
        if part is not None:
            here = here.at[pl.ds(*pieces[part])]
        return pltpu.make_async_remote_copy(
            src_ref=here if src is None else src, dst_ref=here if dst is None else dst, send_sem=l_send.at[sem],
            recv_sem=l_recv.at[2 * place + half] if recv is None else recv, device_id={"tensor": peer}, device_id_type=MESH)

    sent = [0, 0, 0, 0]

    def root_send(peer, sem, place, half, part=None, **kw):
        sent[sem] += root_half if part is None else pieces[part][1]
        root_copy(peer, sem, place, half, part=part, **kw).start()

    def root_wait(place, half, **kw):
        root_copy(twin, 3, place, half, **kw).wait_recv()

    own_place, _ = root_block(0, 0)
    far_place, _ = root_block(0, 1)
    passing = (y * (side // 2) + ((x - dx + side) % side) // 2) * CORES + c

    def root_start():
        for half in (0, 1):
            root_send(helper, 0, own_place, half, src=lr_ref.at[half], dst=relay.at[half], recv=relay_recv.at[half])
            root_send(up, 1, own_place, half, src=lr_ref.at[half])
            root_send(down, 2, own_place, 1 - half, src=lr_ref.at[1 - half])
        for half in (0, 1):
            root_send(twin, 3, own_place, half, src=lr_ref.at[half])

    def root_relay(half):
        root_copy(helper, 0, own_place, half, src=lr_ref.at[half], dst=relay.at[half], recv=relay_recv.at[half]).wait_recv()
        root_send(helper, 0, passing, half, src=relay.at[half])

    def root_far():
        for half in (0, 1):
            root_wait(far_place, half)
            root_send(up, 1, far_place, half)
            root_send(twin, 3, far_place, half)
        for half in (1, 0):
            root_send(down, 2, far_place, half)

    def root_round(r):
        q, stage = r // 3, r % 3
        if stage == 2:
            behind = root_block(2, q)[0]
            for half in (0, 1):
                root_wait(behind, half)
                root_send(twin, 3, behind, half)
            return
        below, above = root_block(side - 1, q)[0], root_block(1, q)[0]
        root_wait(below, stage)
        if stage == 0:
            for part in (None,) if q == 0 else (0, 1):
                root_send(up, 1, below, 0, part=part, recv=last_recv.at[0] if part else None)
        root_send(twin, 3, below, stage)
        root_wait(above, 1 - stage)
        if stage == 0:
            for part in (None,) if q == 0 else (0, 1):
                root_send(down, 2, above, 1, part=part, recv=last_recv.at[1] if part else None)
        root_send(twin, 3, above, 1 - stage)

    last_place, last_device = root_block(2, 1)
    twin_place, twin_device = root_block(2, 1, 1)

    def root_last(part):
        for half in (0, 1):
            root_wait(last_place, half, part=part, recv=last_recv.at[half] if part else None)
            root_send(twin, 3, last_place, half, part=part, recv=last_recv.at[2 + half] if part else None)

    def root_last_twin(part):
        for half in (0, 1):
            root_wait(twin_place, half, part=part, recv=last_recv.at[2 + half] if part else None)

    steps(grad, gbuf, load_sem, GRAD_ROUND_STEP, [(ROOT_START_STEP, root_start), (RELAY_STEP, lambda: root_relay(0))], grad_work)

    x_copy = pltpu.make_async_remote_copy(
        src_ref=xx.at[0], dst_ref=xx.at[1], send_sem=x_send.at[0], recv_sem=x_recv.at[0], device_id={"tensor": helper}, device_id_type=MESH)
    with jax.named_scope("xfin"):
        xx[0] = acc[:, :cols].astype(jnp.bfloat16)
    with jax.named_scope("relay"):
        root_relay(1)
    x_copy.start()
    with jax.named_scope("rround0"):
        root_round(0)

    def left_step(t, carry):
        at = pl.ds(pl.multiple_of(t * lrows, lrows), lrows)
        lo_ref[:, at] = EMA_DECAY * lo_ref[:, at] + (1.0 - EMA_DECAY) * acc[at, cols:].T
        return carry
    with jax.named_scope("leftfin"):
        lax.fori_loop(0, rows // lrows, left_step, 0)

    def at_step(i):
        e, p = i // 2, i % 2
        dy = lax.shift_right_logical(ROOT_Y, 2 * e) & 3
        q = lax.shift_right_logical(ROOT_X, 2 * e) & 3
        return root_block(dy, q, p)

    def twin_wait(i, place):
        @pl.when(i % 2 == 1)
        def _():
            root_wait(place, 0)
            root_wait(place, 1)

    def product(place, which):
        left = lroot[pl.ds(2 * place, 2)].reshape(lrows, rows)
        return jnp.dot(left, xx[which], preferred_element_type=jnp.float32)

    def rows_of(device):
        return pl.ds(pl.multiple_of(device * lrows, lrows), lrows)

    def own_rows(i):
        place, device = at_step(i)
        do_ref[rows_of(device), :] = product(place, 0)

    def lent_copy(place, device):
        return pltpu.make_async_remote_copy(
            src_ref=lent.at[place], dst_ref=do_ref.at[rows_of(device)], send_sem=d_send.at[0], recv_sem=d_recv.at[place],
            device_id={"tensor": client}, device_id_type=MESH)

    def lent_rows(i):
        place, device = at_step(i)
        lent[place] = product(place, 1)
        lent_copy(place, device).start()

    def loop(lo, hi, body):
        def step(i, carry):
            body(i)
            return carry
        lax.fori_loop(lo, hi, step, 0)

    def first_own(i):
        @pl.when(i == 2)
        def _():
            with jax.named_scope("far"):
                root_far()
            with jax.named_scope("rround1"):
                root_round(1)

        @pl.when(i == 8)
        def _():
            with jax.named_scope("rround2"):
                root_round(2)
        twin_wait(i, at_step(i)[0])
        own_rows(i)

    loop(0, 10, first_own)
    with jax.named_scope("rround3"):
        root_round(3)
    with jax.named_scope("xwait"):
        x_copy.wait_recv()
    with jax.named_scope("lentloop"):
        loop(0, 10, lent_rows)
    with jax.named_scope("rround4"):
        root_round(4)

    def both(i):
        twin_wait(i, at_step(i)[0])
        lent_rows(i)
        own_rows(i)
    with jax.named_scope("both"):
        loop(10, 14, both)

    def lent_piece(place, device, part):
        first, count = pieces[part]
        left = jnp.concatenate([lroot[2 * place, pl.ds(first, count), :], lroot[2 * place + 1, pl.ds(first, count), :]], axis=0)
        prod = jnp.dot(left, xx[1], preferred_element_type=jnp.float32)
        for half in (0, 1):
            at = half * root_half + first
            lent[place, pl.ds(at, count), :] = prod[half * count:(half + 1) * count]
            pltpu.make_async_remote_copy(
                src_ref=lent.at[place, pl.ds(at, count)], dst_ref=do_ref.at[pl.ds(pl.multiple_of(device * lrows, lrows) + at, count)],
                send_sem=d_send.at[0], recv_sem=d_recv.at[place], device_id={"tensor": client}, device_id_type=MESH).start()

    for part in (0, 1):
        with jax.named_scope(f"last{part}"):
            root_last(part)
        lent_piece(last_place, last_device, part)
        with jax.named_scope(f"lasttwin{part}"):
            root_last_twin(part)
        lent_piece(twin_place, twin_device, part)
    loop(14, 16, own_rows)

    with jax.named_scope("drain"):
        grad.drain()
    for sem, count in enumerate(sent):
        whole = lroot.at[pl.ds(0, count // root_half)]
        pltpu.make_async_copy(whole, whole, l_send.at[sem]).wait()
    x_copy.wait_send()
    pltpu.make_async_copy(lent, lent, d_send.at[0]).wait()

    def lent_wait(i, carry):
        lent_copy(i, 0).wait_recv()
        return carry
    with jax.named_scope("dwait"):
        lax.fori_loop(0, half_count // 2, lent_wait, 0)


def store_kernel(*refs):
    count = (len(refs) - 1) // 2
    sems = refs[-1]
    pieces = 4
    for i in range(count):
        src, dst = refs[i], refs[count + i]
        step = src.shape[0] // pieces
        for j in range(pieces):
            part = pl.ds(j * step, step)
            pltpu.make_async_copy(src.at[part], dst.at[part], sems.at[i]).start()
    for i in range(count):
        pltpu.make_async_copy(refs[i], refs[count + i], sems.at[i]).wait()


def solution(mesh):
    row_spec = P(("layer", "tensor"), None)
    col_spec = P("layer", "tensor")
    n = mesh.shape["tensor"]
    side = math.isqrt(n // CORES)

    def local_step(g, l, r, lr, rr):
        rows, cols = g.shape
        lrows = l.shape[0]
        kept = n // 2
        hbm = pl.BlockSpec(memory_space=pltpu.HBM)
        vmem = pl.BlockSpec(memory_space=pltpu.VMEM)
        operands = [g.reshape(2, rows // 2, cols), l, r, lr.reshape(2, lrows // 2, rows), rr]
        left_new, right_new, direction, _ = pl.pallas_call(
            functools.partial(kernel, n, side),
            name="shampoo",
            out_shape=[
                pltpu.VMEM(l.shape, jnp.float32),
                pltpu.VMEM(r.shape, jnp.float32),
                pltpu.VMEM(g.shape, jnp.float32),
                pltpu.HBM((2 * n, rows // 2, cols), jnp.bfloat16),
            ],
            in_specs=[hbm] * 5,
            out_specs=[vmem, vmem, vmem, hbm],
            scratch_shapes=[
                pltpu.VMEM(rr.shape, jnp.bfloat16),
                pltpu.VMEM((cols, rows), jnp.bfloat16),
                pltpu.VMEM((rows, cols + lrows), jnp.float32),
                pltpu.VMEM((2, 2, rows // 2, cols), jnp.bfloat16),
                pltpu.VMEM((cols + lrows, cols), jnp.bfloat16),
                pltpu.VMEM((2, rows, cols), jnp.bfloat16),
                pltpu.VMEM((2 * kept, lrows // 2, rows), jnp.bfloat16),
                pltpu.VMEM((2, lrows // 2, rows), jnp.bfloat16),
                pltpu.VMEM((kept, lrows, cols), jnp.float32),
                pltpu.SemaphoreType.DMA((2 * n,)),
                pltpu.SemaphoreType.DMA((5,)),
                pltpu.SemaphoreType.DMA((2,)),
                pltpu.SemaphoreType.DMA((4,)),
                pltpu.SemaphoreType.DMA((2 * kept,)),
                pltpu.SemaphoreType.DMA((4,)),
                pltpu.SemaphoreType.DMA((2,)),
                pltpu.SemaphoreType.DMA((1,)),
                pltpu.SemaphoreType.DMA((kept,)),
                pltpu.SemaphoreType.DMA((4,)),
                pltpu.SemaphoreType.DMA((1,)),
                pltpu.SemaphoreType.DMA((1,)),
            ],
            compiler_params=pltpu.CompilerParams(collective_id=0, has_side_effects=True, vmem_limit_bytes=48 * 2**20),
            cost_estimate=pl.CostEstimate(flops=2 * rows * cols * (2 * n * cols + 2 * rows), bytes_accessed=2 * n * rows * cols * 3, transcendentals=0),
        )(*[pltpu.with_memory_space_constraint(v, pltpu.HBM) for v in operands])
        results = [left_new, right_new, direction]
        return pl.pallas_call(
            store_kernel,
            name="store",
            out_shape=[jax.ShapeDtypeStruct(v.shape, v.dtype) for v in results],
            in_specs=[vmem] * 3,
            out_specs=[hbm] * 3,
            scratch_shapes=[pltpu.SemaphoreType.DMA((3,))],
            compiler_params=pltpu.CompilerParams(vmem_limit_bytes=1 * 2**20),
        )(*results)

    return jax.shard_map(local_step, mesh=mesh, in_specs=(col_spec, row_spec, row_spec, row_spec, row_spec), out_specs=(row_spec, row_spec, col_spec), check_vma=False)
```

```python
import functools
import math

import jax
import jax.numpy as jnp
from jax import lax
from jax.experimental import pallas as pl
from jax.experimental.pallas import tpu as pltpu
from jax.sharding import PartitionSpec as P

EMA_DECAY = 0.9
CORES = 2
MESH = pl.DeviceIdType.MESH

ORDER = [(int(a), int(b)) for a, b in zip("0310020311322312", "0003102313131222")]
def parcels(code):
    digits = [int(d) for d in code]
    return [((a, b), h) for a, b, h in zip(digits[0::3], digits[1::3], digits[2::3])]


UP = parcels("030031330131020331130230231320120220")
UP_ON = {0: parcels("030"), 2: parcels("330"), 6: parcels("130"), 7: parcels("230")}
DOWN = parcels("011010111310021110311211210321121221")
DOWN_ON = {0: parcels("011"), 6: parcels("311111"), 7: parcels("211")}
ROUNDS = len(UP)
FIRST_UP = parcels("300301200")
FIRST_DOWN = parcels("101100201")
GRAD_ROUND_STEP = [2, 2, 8, 10, 12, 14, 17, 20, 22, 26, 28, 30]
LAST_FORWARD = 7
SIDE_UP, SIDE_DOWN = 9, 10
ASIDE = 24
ROOT_START_STEP = 30
RELAY_STEP = 31
LATE = (2, 12, 14, 22, 26, 28, 30)
MIDDLE = (3, 13, 15, 23, 27, 29, 31)


def packed(values):
    return [sum(v << (2 * i) for i, v in enumerate(values[j:j + 8])) for j in (0, 8)]


FIRST_CODE = packed([o[0] for o in ORDER])
SECOND_CODE = packed([o[1] for o in ORDER])


def lookup(code, e):
    word = code[0] + (e // 8) * (code[1] - code[0])
    return lax.shift_right_logical(word, 2 * (e % 8)) & 3


ROOT_ORDER = [(0, 0), (3, 0), (1, 0), (0, 1), (2, 0), (3, 1), (1, 1), (2, 1)]
ROOT_Y = sum(o[0] << (2 * i) for i, o in enumerate(ROOT_ORDER))
ROOT_X = sum(o[1] << (2 * i) for i, o in enumerate(ROOT_ORDER))


def kernel(n, side, g_ref, l_ref, r_ref, lr_ref, rr_ref, lo_ref, ro_ref, do_ref, gfull,
           rr, gt, acc, gbuf, rhs, xx, lroot, relay, lent,
           g_recv, g_send, load_sem, init_sem, l_recv, last_recv, relay_recv, x_recv, d_recv, l_send, x_send, d_send):
    _, half_rows, cols = g_ref.shape
    rows = 2 * half_rows
    lrows = l_ref.shape[0]
    tile = min(1024, half_rows)
    aside_rows = half_rows * ASIDE // 128

    me = lax.axis_index("tensor")
    c = me % CORES
    chip = me // CORES
    x, y = chip % side, chip // side
    f = x + c * (y - x)
    s = y + c * (x - y)
    fstep = CORES + c * CORES * (side - 1)
    sstep = CORES * side - c * CORES * (side - 1)
    twin = me + 1 - 2 * c

    def index(df, ds):
        return ((f + df) % side) * fstep + ((s + ds) % side) * sstep + c

    def twin_index(df, ds):
        return ((s + df) % side) * sstep + ((f + ds) % side) * fstep + 1 - c

    peers = {"f+": index(1, 0), "f-": index(3, 0), "s+": index(0, 1), "s-": index(0, 3), "twin": twin}
    slot_of = {name: i for i, name in enumerate(peers)}

    class Gather:
        def __init__(self, own, full, recv, send):
            self.own, self.full, self.recv, self.send_sem = own, full, recv, send
            self.count = {name: 0 for name in peers}

        def copy(self, name, b, half, own=False, part=None):
            src = self.own.at[half] if own else self.full.at[2 * b + half]
            dst = self.full.at[2 * b + half]
            sem = slot_of[name]
            if part is not None:
                src, dst, sem = src.at[pl.ds(*part)], dst.at[pl.ds(*part)], len(peers) + sem
            return pltpu.make_async_remote_copy(
                src_ref=src, dst_ref=dst, send_sem=self.send_sem.at[sem],
                recv_sem=self.recv.at[2 * b + half], device_id={"tensor": peers[name]}, device_id_type=MESH)

        def send(self, name, b, half, own=False):
            self.count[name] += 1
            self.copy(name, b, half, own).start()

        def wait(self, b, half):
            self.copy("twin", b, half).wait_recv()

        def start(self):
            for half in (0, 1):
                for name in ("f+", "s+"):
                    self.send(name, me, half, own=True)
                for name in ("f-", "s-"):
                    self.send(name, me, 1 - half, own=True)
            for half in (0, 1):
                self.send("twin", me, half, own=True)

        def round(self, r):
            if r < len(FIRST_UP):
                (ou, hu), (od, hd) = FIRST_UP[r], FIRST_DOWN[r]
                bu, bd = index(*ou), index(*od)
                self.wait(bu, hu)
                if r == 0:
                    self.send("f+", bu, hu)
                self.wait(bd, hd)
                if r == 0:
                    self.send("f-", bd, hd)
                self.send("s+", bu, hu)
                self.send("s-", bd, hd)
                self.send("s+", bd, hd)
                self.send("s-", bu, hu)
                self.send("twin", bu, hu)
                self.send("twin", bd, hd)
            (ou, hu), (od, hd) = UP[r], DOWN[r]
            fu, fd = UP_ON.get(r, ()), DOWN_ON.get(r, ())
            bu, bd = index(*ou), index(*od)
            self.wait(bu, hu)
            for offset, half in fu:
                if r == LAST_FORWARD:
                    self.forward_last("s+", index(*offset), half)
                else:
                    self.send("s+", index(*offset), half)
            if r == SIDE_UP:
                self.aside("f+", bu, hu)
            self.send("twin", bu, hu)
            self.wait(bd, hd)
            for offset, half in fd:
                if r == LAST_FORWARD:
                    self.forward_last("s-", index(*offset), half)
                else:
                    self.send("s-", index(*offset), half)
            if r == SIDE_DOWN:
                self.aside("f-", bd, hd)
            self.send("twin", bd, hd)

        def forward_last(self, name, b, half):
            pl.when(c == 0)(lambda: self.copy(name, b, half, part=(0, half_rows - aside_rows)).start())
            pl.when(c == 1)(lambda: self.copy(name, b, half, part=(0, half_rows)).start())

        def aside(self, name, b, half):
            pl.when(c == 0)(lambda: self.copy(name, b, half, part=(half_rows - aside_rows, aside_rows)).start())

        def drain(self):
            for name, count in self.count.items():
                whole = self.full.at[pl.ds(0, count)]
                pltpu.make_async_copy(whole, whole, self.send_sem.at[slot_of[name]]).wait()

            @pl.when(c == 0)
            def _():
                for name in ("s+", "s-"):
                    self.copy(name, me, 0, part=(0, half_rows - aside_rows)).wait_send()
                for name in ("f+", "f-"):
                    self.copy(name, me, 0, part=(half_rows - aside_rows, aside_rows)).wait_send()

            @pl.when(c == 1)
            def _():
                for name in ("s+", "s-"):
                    self.copy(name, me, 0, part=(0, half_rows)).wait_send()

    grad = Gather(g_ref, gfull, g_recv, g_send)

    def block_of(k):
        e, other = k // 2, k % 2
        df, ds = lookup(FIRST_CODE, e), lookup(SECOND_CODE, e)
        mine = index(df, ds)
        return mine + other * (twin_index(df, ds) - mine)

    def load(gather, buf, k, sem):
        b = block_of(k)
        return pltpu.make_async_copy(gather.full.at[pl.ds(2 * b, 2)], buf.at[k % 2], sem.at[k % 2])

    def start_load(gather, buf, k, sem):
        @pl.when(k % 2 == 1)
        def _():
            b = block_of(k)
            with jax.named_scope("twinwait"):
                gather.wait(b, 0)
                gather.wait(b, 1)
        load(gather, buf, k, sem).start()

    def one_of(k, values):
        found = k == values[0]
        for v in values[1:]:
            found = found | (k == v)
        return found

    def steps(gather, buf, sem, round_step, extra, work):
        def step(k, carry):
            for at, fn in extra:
                pl.when(k == at)(fn)
            for r in range(ROUNDS):
                @pl.when(k == round_step[r])
                def _():
                    with jax.named_scope(f"ground{r}"):
                        gather.round(r)

            @pl.when(one_of(k, LATE))
            def _():
                start_load(gather, buf, k, sem)

            @pl.when((k + 1 < n) & jnp.logical_not(one_of(k + 1, LATE + MIDDLE)))
            def _():
                start_load(gather, buf, k + 1, sem)

            def middle():
                @pl.when(one_of(k + 1, MIDDLE))
                def _():
                    start_load(gather, buf, k + 1, sem)
            with jax.named_scope("loadwait"):
                load(gather, buf, k, sem).wait()
            with jax.named_scope("work"):
                work(k, k % 2, block_of(k), middle)
            return carry
        lax.fori_loop(0, n, step, 0)

    first = [
        pltpu.make_async_copy(rr_ref, rr, init_sem.at[0]),
        pltpu.make_async_copy(r_ref, ro_ref, init_sem.at[1]),
        pltpu.make_async_copy(l_ref, lo_ref, init_sem.at[2]),
        pltpu.make_async_copy(lr_ref, lroot.at[pl.ds(2 * ((y * (side // 2) + x // 2) * CORES + c), 2)], init_sem.at[3]),
    ]
    own_load = pltpu.make_async_copy(g_ref, gbuf.at[0], load_sem.at[0])
    own_load.start()

    barrier = pltpu.get_barrier_semaphore()
    for peer in peers.values():
        pl.semaphore_signal(barrier, inc=1, device_id={"tensor": peer}, device_id_type=MESH)
    with jax.named_scope("barrier"):
        pl.semaphore_wait(barrier, len(peers))
    grad.start()
    for copy in first:
        copy.start()

    acc[...] = jnp.zeros_like(acc)
    own_load.wait()
    for h in (0, 1):
        gt[:, h * half_rows:(h + 1) * half_rows] = gbuf[0, h].T
    for copy in first:
        copy.wait()
    own_load.start()

    per_half = half_rows // tile

    def grad_work(k, slot, b, middle):
        at = pl.multiple_of(b * cols, cols)
        rhs[:cols] = rr[:, pl.ds(at, cols)]
        rhs[cols:] = gbuf[slot, me // (n // 2), pl.ds(pl.multiple_of((me % (n // 2)) * lrows, lrows), lrows), :]

        def rows_step(t, carry):
            left = gbuf[slot, t // per_half, pl.ds(pl.multiple_of((t % per_half) * tile, tile), tile), :]
            out = pl.ds(pl.multiple_of(t * tile, tile), tile)
            acc[out, :] += lax.dot_general(left, rhs[...], (((1,), (1,)), ((), ())), preferred_element_type=jnp.float32)
            return carry
        lax.fori_loop(0, 2 * per_half, rows_step, 0)
        middle()
        prod = jnp.dot(gt[:, :half_rows], gbuf[slot, 0], preferred_element_type=jnp.float32)
        prod += jnp.dot(gt[:, half_rows:], gbuf[slot, 1], preferred_element_type=jnp.float32)
        ro_ref[:, pl.ds(at, cols)] = EMA_DECAY * ro_ref[:, pl.ds(at, cols)] + (1.0 - EMA_DECAY) * prod


    dx = 1 - 2 * c
    helper = (y * side + (x + dx + side) % side) * CORES + c
    client = (y * side + (x - dx + side) % side) * CORES + c
    up = (((y + 1) % side) * side + x) * CORES + c
    down = (((y + side - 1) % side) * side + x) * CORES + c
    half_count, root_half, _ = lroot.shape
    pieces = ((0, root_half - root_half // 4), (root_half - root_half // 4, root_half // 4))

    def root_block(dy, q, p=0):
        oy, ox = (y + dy) % side, (x + 2 * q) % side
        core = c + p * (1 - 2 * c)
        return (oy * (side // 2) + ox // 2) * CORES + core, (oy * side + ox) * CORES + core

    def root_copy(peer, sem, place, half, src=None, dst=None, recv=None, part=None):
        here = lroot.at[2 * place + half]
        if part is not None:
            here = here.at[pl.ds(*pieces[part])]
        return pltpu.make_async_remote_copy(
            src_ref=here if src is None else src, dst_ref=here if dst is None else dst, send_sem=l_send.at[sem],
            recv_sem=l_recv.at[2 * place + half] if recv is None else recv, device_id={"tensor": peer}, device_id_type=MESH)

    sent = [0, 0, 0, 0]

    def root_send(peer, sem, place, half, part=None, **kw):
        sent[sem] += root_half if part is None else pieces[part][1]
        root_copy(peer, sem, place, half, part=part, **kw).start()

    def root_wait(place, half, **kw):
        root_copy(twin, 3, place, half, **kw).wait_recv()

    own_place, _ = root_block(0, 0)
    far_place, _ = root_block(0, 1)
    passing = (y * (side // 2) + ((x - dx + side) % side) // 2) * CORES + c

    def root_start():
        for half in (0, 1):
            root_send(helper, 0, own_place, half, src=lr_ref.at[half], dst=relay.at[half], recv=relay_recv.at[half])
            root_send(up, 1, own_place, half, src=lr_ref.at[half])
            root_send(down, 2, own_place, 1 - half, src=lr_ref.at[1 - half])
        for half in (0, 1):
            root_send(twin, 3, own_place, half, src=lr_ref.at[half])

    def root_relay(half):
        root_copy(helper, 0, own_place, half, src=lr_ref.at[half], dst=relay.at[half], recv=relay_recv.at[half]).wait_recv()
        root_send(helper, 0, passing, half, src=relay.at[half])

    def root_far():
        for half in (0, 1):
            root_wait(far_place, half)
            root_send(up, 1, far_place, half)
            root_send(twin, 3, far_place, half)
        for half in (1, 0):
            root_send(down, 2, far_place, half)

    def root_round(r):
        q, stage = r // 3, r % 3
        if stage == 2:
            behind = root_block(2, q)[0]
            for half in (0, 1):
                root_wait(behind, half)
                root_send(twin, 3, behind, half)
            return
        below, above = root_block(side - 1, q)[0], root_block(1, q)[0]
        root_wait(below, stage)
        if stage == 0:
            for part in (None,) if q == 0 else (0, 1):
                root_send(up, 1, below, 0, part=part, recv=last_recv.at[0] if part else None)
        root_send(twin, 3, below, stage)
        root_wait(above, 1 - stage)
        if stage == 0:
            for part in (None,) if q == 0 else (0, 1):
                root_send(down, 2, above, 1, part=part, recv=last_recv.at[1] if part else None)
        root_send(twin, 3, above, 1 - stage)

    last_place, last_device = root_block(2, 1)
    twin_place, twin_device = root_block(2, 1, 1)

    def root_last(part):
        for half in (0, 1):
            root_wait(last_place, half, part=part, recv=last_recv.at[half] if part else None)
            root_send(twin, 3, last_place, half, part=part, recv=last_recv.at[2 + half] if part else None)

    def root_last_twin(part):
        for half in (0, 1):
            root_wait(twin_place, half, part=part, recv=last_recv.at[2 + half] if part else None)

    steps(grad, gbuf, load_sem, GRAD_ROUND_STEP, [(ROOT_START_STEP, root_start), (RELAY_STEP, lambda: root_relay(0))], grad_work)

    side_cols = cols // 2

    def x_copy(h):
        at = pl.ds(h * side_cols, side_cols)
        return pltpu.make_async_remote_copy(
            src_ref=xx.at[0, :, at], dst_ref=xx.at[1, :, at], send_sem=x_send.at[h], recv_sem=x_recv.at[h],
            device_id={"tensor": helper}, device_id_type=MESH)

    with jax.named_scope("xfin"):
        xx[0] = acc[:, :cols].astype(jnp.bfloat16)
    with jax.named_scope("relay"):
        root_relay(1)
    x_copy(0).start()
    x_copy(1).start()
    with jax.named_scope("rround0"):
        root_round(0)

    def left_step(t, carry):
        at = pl.ds(pl.multiple_of(t * lrows, lrows), lrows)
        lo_ref[:, at] = EMA_DECAY * lo_ref[:, at] + (1.0 - EMA_DECAY) * acc[at, cols:].T
        return carry
    with jax.named_scope("leftfin"):
        lax.fori_loop(0, rows // lrows, left_step, 0)

    def at_step(i):
        e, p = i // 2, i % 2
        dy = lax.shift_right_logical(ROOT_Y, 2 * e) & 3
        q = lax.shift_right_logical(ROOT_X, 2 * e) & 3
        return root_block(dy, q, p)

    def twin_wait(i, place):
        @pl.when(i % 2 == 1)
        def _():
            root_wait(place, 0)
            root_wait(place, 1)

    def product(place, which):
        left = lroot[pl.ds(2 * place, 2)].reshape(lrows, rows)
        return jnp.dot(left, xx[which], preferred_element_type=jnp.float32)

    def rows_of(device):
        return pl.ds(pl.multiple_of(device * lrows, lrows), lrows)

    def own_rows(i):
        place, device = at_step(i)
        do_ref[rows_of(device), :] = product(place, 0)

    def lent_copy(place, device):
        return pltpu.make_async_remote_copy(
            src_ref=lent.at[place], dst_ref=do_ref.at[rows_of(device)], send_sem=d_send.at[0], recv_sem=d_recv.at[place],
            device_id={"tensor": client}, device_id_type=MESH)

    def lent_rows(i):
        place, device = at_step(i)
        lent[place] = product(place, 1)
        lent_copy(place, device).start()

    def lent_side(i, h):
        place, _ = at_step(i)
        at = pl.ds(h * side_cols, side_cols)
        left = lroot[pl.ds(2 * place, 2)].reshape(lrows, rows)
        lent[place, :, at] = jnp.dot(left, xx[1, :, at], preferred_element_type=jnp.float32)

    def lent_side_copy(i, h):
        place, device = at_step(i)
        at = pl.ds(h * side_cols, side_cols)
        return pltpu.make_async_remote_copy(
            src_ref=lent.at[place, :, at], dst_ref=do_ref.at[rows_of(device), at], send_sem=d_send.at[0], recv_sem=d_recv.at[place],
            device_id={"tensor": client}, device_id_type=MESH)

    def loop(lo, hi, body):
        def step(i, carry):
            body(i)
            return carry
        lax.fori_loop(lo, hi, step, 0)

    def first_own(i):
        @pl.when(i == 2)
        def _():
            with jax.named_scope("far"):
                root_far()
            with jax.named_scope("rround1"):
                root_round(1)

        @pl.when(i == 8)
        def _():
            with jax.named_scope("rround2"):
                root_round(2)
        twin_wait(i, at_step(i)[0])
        own_rows(i)

    loop(0, 10, first_own)
    with jax.named_scope("x0wait"):
        x_copy(0).wait_recv()
    loop(0, 10, lambda i: lent_side(i, 0))
    x_copy(0).wait_send()
    with jax.named_scope("x1sent"):
        x_copy(1).wait_send()
    loop(0, 10, lambda i: lent_side_copy(i, 0).start())
    with jax.named_scope("rround3"):
        root_round(3)
    with jax.named_scope("x1wait"):
        x_copy(1).wait_recv()

    def second_side(i):
        lent_side(i, 1)
        lent_side_copy(i, 1).start()
    loop(0, 10, second_side)
    with jax.named_scope("rround4"):
        root_round(4)

    def both(i):
        twin_wait(i, at_step(i)[0])
        lent_rows(i)
        own_rows(i)
    with jax.named_scope("both"):
        loop(10, 14, both)

    def lent_piece(place, device, part):
        first, count = pieces[part]
        left = jnp.concatenate([lroot[2 * place, pl.ds(first, count), :], lroot[2 * place + 1, pl.ds(first, count), :]], axis=0)
        prod = jnp.dot(left, xx[1], preferred_element_type=jnp.float32)
        for half in (0, 1):
            at = half * root_half + first
            lent[place, pl.ds(at, count), :] = prod[half * count:(half + 1) * count]
            pltpu.make_async_remote_copy(
                src_ref=lent.at[place, pl.ds(at, count)], dst_ref=do_ref.at[pl.ds(pl.multiple_of(device * lrows, lrows) + at, count)],
                send_sem=d_send.at[0], recv_sem=d_recv.at[place], device_id={"tensor": client}, device_id_type=MESH).start()

    for part in (0, 1):
        with jax.named_scope(f"last{part}"):
            root_last(part)
        lent_piece(last_place, last_device, part)
        with jax.named_scope(f"lasttwin{part}"):
            root_last_twin(part)
        lent_piece(twin_place, twin_device, part)
    loop(14, 16, own_rows)

    with jax.named_scope("drain"):
        grad.drain()
    for sem, count in enumerate(sent):
        whole = lroot.at[pl.ds(0, count // root_half)]
        pltpu.make_async_copy(whole, whole, l_send.at[sem]).wait()
    pltpu.make_async_copy(lent, lent, d_send.at[0]).wait()

    def lent_wait(i, carry):
        lent_copy(i, 0).wait_recv()
        return carry
    with jax.named_scope("dwait"):
        lax.fori_loop(0, half_count // 2, lent_wait, 0)


def store_kernel(*refs):
    count = (len(refs) - 1) // 2
    sems = refs[-1]
    pieces = 8
    for i in range(count):
        src, dst = refs[i], refs[count + i]
        step = src.shape[0] // pieces
        for j in range(pieces):
            part = pl.ds(j * step, step)
            pltpu.make_async_copy(src.at[part], dst.at[part], sems.at[i]).start()
    for i in range(count):
        pltpu.make_async_copy(refs[i], refs[count + i], sems.at[i]).wait()


def solution(mesh):
    row_spec = P(("layer", "tensor"), None)
    col_spec = P("layer", "tensor")
    n = mesh.shape["tensor"]
    side = math.isqrt(n // CORES)

    def local_step(g, l, r, lr, rr):
        rows, cols = g.shape
        lrows = l.shape[0]
        kept = n // 2
        hbm = pl.BlockSpec(memory_space=pltpu.HBM)
        vmem = pl.BlockSpec(memory_space=pltpu.VMEM)
        operands = [g.reshape(2, rows // 2, cols), l, r, lr.reshape(2, lrows // 2, rows), rr]
        left_new, right_new, direction, _ = pl.pallas_call(
            functools.partial(kernel, n, side),
            name="shampoo",
            out_shape=[
                pltpu.VMEM(l.shape, jnp.float32),
                pltpu.VMEM(r.shape, jnp.float32),
                pltpu.VMEM(g.shape, jnp.float32),
                pltpu.HBM((2 * n, rows // 2, cols), jnp.bfloat16),
            ],
            in_specs=[hbm] * 5,
            out_specs=[vmem, vmem, vmem, hbm],
            scratch_shapes=[
                pltpu.VMEM(rr.shape, jnp.bfloat16),
                pltpu.VMEM((cols, rows), jnp.bfloat16),
                pltpu.VMEM((rows, cols + lrows), jnp.float32),
                pltpu.VMEM((2, 2, rows // 2, cols), jnp.bfloat16),
                pltpu.VMEM((cols + lrows, cols), jnp.bfloat16),
                pltpu.VMEM((2, rows, cols), jnp.bfloat16),
                pltpu.VMEM((2 * kept, lrows // 2, rows), jnp.bfloat16),
                pltpu.VMEM((2, lrows // 2, rows), jnp.bfloat16),
                pltpu.VMEM((kept, lrows, cols), jnp.float32),
                pltpu.SemaphoreType.DMA((2 * n,)),
                pltpu.SemaphoreType.DMA((10,)),
                pltpu.SemaphoreType.DMA((2,)),
                pltpu.SemaphoreType.DMA((4,)),
                pltpu.SemaphoreType.DMA((2 * kept,)),
                pltpu.SemaphoreType.DMA((4,)),
                pltpu.SemaphoreType.DMA((2,)),
                pltpu.SemaphoreType.DMA((2,)),
                pltpu.SemaphoreType.DMA((kept,)),
                pltpu.SemaphoreType.DMA((4,)),
                pltpu.SemaphoreType.DMA((2,)),
                pltpu.SemaphoreType.DMA((1,)),
            ],
            compiler_params=pltpu.CompilerParams(collective_id=0, has_side_effects=True, vmem_limit_bytes=48 * 2**20),
            cost_estimate=pl.CostEstimate(flops=2 * rows * cols * (2 * n * cols + 2 * rows), bytes_accessed=2 * n * rows * cols * 3, transcendentals=0),
        )(*[pltpu.with_memory_space_constraint(v, pltpu.HBM) for v in operands])
        results = [left_new, right_new, direction]
        return pl.pallas_call(
            store_kernel,
            name="store",
            out_shape=[jax.ShapeDtypeStruct(v.shape, v.dtype) for v in results],
            in_specs=[vmem] * 3,
            out_specs=[hbm] * 3,
            scratch_shapes=[pltpu.SemaphoreType.DMA((3,))],
            compiler_params=pltpu.CompilerParams(vmem_limit_bytes=1 * 2**20),
        )(*results)

    return jax.shard_map(local_step, mesh=mesh, in_specs=(col_spec, row_spec, row_spec, row_spec, row_spec), out_specs=(row_spec, row_spec, col_spec), check_vma=False)
```

```python
import functools
import math

import jax
import jax.numpy as jnp
from jax import lax
from jax.experimental import pallas as pl
from jax.experimental.pallas import tpu as pltpu
from jax.sharding import PartitionSpec as P

EMA_DECAY = 0.9
CORES = 2
MESH = pl.DeviceIdType.MESH

ORDER = [(int(a), int(b)) for a, b in zip("0310020311322312", "0003102313131222")]
def parcels(code):
    digits = [int(d) for d in code]
    return [((a, b), h) for a, b, h in zip(digits[0::3], digits[1::3], digits[2::3])]


UP = parcels("030031330131020331130230231320120220")
UP_ON = {0: parcels("030"), 2: parcels("330"), 6: parcels("130"), 7: parcels("230")}
DOWN = parcels("011010111310021110311211210321121221")
DOWN_ON = {0: parcels("011"), 6: parcels("311111"), 7: parcels("211")}
ROUNDS = len(UP)
FIRST_UP = parcels("300301200")
FIRST_DOWN = parcels("101100201")
GRAD_ROUND_STEP = [2, 2, 8, 10, 12, 14, 17, 20, 22, 26, 28, 30]
LAST_FORWARD = 7
SIDE_UP, SIDE_DOWN = 9, 10
ASIDE = 24
ROOT_START_STEP = 29
ROOT_ACROSS_STEP = 30
RELAY_STEP = 31
LATE = (2, 12, 14, 22, 26, 28, 30)
MIDDLE = (3, 13, 15, 23, 27, 29, 31)


def packed(values):
    return [sum(v << (2 * i) for i, v in enumerate(values[j:j + 8])) for j in (0, 8)]


FIRST_CODE = packed([o[0] for o in ORDER])
SECOND_CODE = packed([o[1] for o in ORDER])


def lookup(code, e):
    word = code[0] + (e // 8) * (code[1] - code[0])
    return lax.shift_right_logical(word, 2 * (e % 8)) & 3


ROOT_ORDER = [(0, 0), (3, 0), (1, 0), (0, 1), (2, 0), (3, 1), (1, 1), (2, 1)]
ROOT_Y = sum(o[0] << (2 * i) for i, o in enumerate(ROOT_ORDER))
ROOT_X = sum(o[1] << (2 * i) for i, o in enumerate(ROOT_ORDER))


def kernel(n, side, g_ref, l_ref, r_ref, lr_ref, rr_ref, lo_ref, ro_ref, do_ref, gfull,
           rr, gt, acc, gbuf, rhs, xx, lroot, relay, lent,
           g_recv, g_send, load_sem, init_sem, l_recv, last_recv, relay_recv, x_recv, d_recv, l_send, x_send, d_send):
    _, half_rows, cols = g_ref.shape
    rows = 2 * half_rows
    lrows = l_ref.shape[0]
    tile = min(1024, half_rows)
    aside_rows = half_rows * ASIDE // 128

    me = lax.axis_index("tensor")
    c = me % CORES
    chip = me // CORES
    x, y = chip % side, chip // side
    f = x + c * (y - x)
    s = y + c * (x - y)
    fstep = CORES + c * CORES * (side - 1)
    sstep = CORES * side - c * CORES * (side - 1)
    twin = me + 1 - 2 * c

    def index(df, ds):
        return ((f + df) % side) * fstep + ((s + ds) % side) * sstep + c

    def twin_index(df, ds):
        return ((s + df) % side) * sstep + ((f + ds) % side) * fstep + 1 - c

    peers = {"f+": index(1, 0), "f-": index(3, 0), "s+": index(0, 1), "s-": index(0, 3), "twin": twin}
    slot_of = {name: i for i, name in enumerate(peers)}

    class Gather:
        def __init__(self, own, full, recv, send):
            self.own, self.full, self.recv, self.send_sem = own, full, recv, send
            self.count = {name: 0 for name in peers}

        def copy(self, name, b, half, own=False, part=None):
            src = self.own.at[half] if own else self.full.at[2 * b + half]
            dst = self.full.at[2 * b + half]
            sem = slot_of[name]
            if part is not None:
                src, dst, sem = src.at[pl.ds(*part)], dst.at[pl.ds(*part)], len(peers) + sem
            return pltpu.make_async_remote_copy(
                src_ref=src, dst_ref=dst, send_sem=self.send_sem.at[sem],
                recv_sem=self.recv.at[2 * b + half], device_id={"tensor": peers[name]}, device_id_type=MESH)

        def send(self, name, b, half, own=False):
            self.count[name] += 1
            self.copy(name, b, half, own).start()

        def wait(self, b, half):
            self.copy("twin", b, half).wait_recv()

        def start(self):
            for half in (0, 1):
                for name in ("f+", "s+"):
                    self.send(name, me, half, own=True)
                for name in ("f-", "s-"):
                    self.send(name, me, 1 - half, own=True)
            for half in (0, 1):
                self.send("twin", me, half, own=True)

        def round(self, r):
            if r < len(FIRST_UP):
                (ou, hu), (od, hd) = FIRST_UP[r], FIRST_DOWN[r]
                bu, bd = index(*ou), index(*od)
                self.wait(bu, hu)
                if r == 0:
                    self.send("f+", bu, hu)
                self.wait(bd, hd)
                if r == 0:
                    self.send("f-", bd, hd)
                self.send("s+", bu, hu)
                self.send("s-", bd, hd)
                self.send("s+", bd, hd)
                self.send("s-", bu, hu)
                self.send("twin", bu, hu)
                self.send("twin", bd, hd)
            (ou, hu), (od, hd) = UP[r], DOWN[r]
            fu, fd = UP_ON.get(r, ()), DOWN_ON.get(r, ())
            bu, bd = index(*ou), index(*od)
            self.wait(bu, hu)
            for offset, half in fu:
                if r == LAST_FORWARD:
                    self.forward_last("s+", index(*offset), half)
                else:
                    self.send("s+", index(*offset), half)
            if r == SIDE_UP:
                self.aside("f+", bu, hu)
            self.send("twin", bu, hu)
            self.wait(bd, hd)
            for offset, half in fd:
                if r == LAST_FORWARD:
                    self.forward_last("s-", index(*offset), half)
                else:
                    self.send("s-", index(*offset), half)
            if r == SIDE_DOWN:
                self.aside("f-", bd, hd)
            self.send("twin", bd, hd)

        def forward_last(self, name, b, half):
            pl.when(c == 0)(lambda: self.copy(name, b, half, part=(0, half_rows - aside_rows)).start())
            pl.when(c == 1)(lambda: self.copy(name, b, half, part=(0, half_rows)).start())

        def aside(self, name, b, half):
            pl.when(c == 0)(lambda: self.copy(name, b, half, part=(half_rows - aside_rows, aside_rows)).start())

        def drain(self):
            for name, count in self.count.items():
                whole = self.full.at[pl.ds(0, count)]
                pltpu.make_async_copy(whole, whole, self.send_sem.at[slot_of[name]]).wait()

            @pl.when(c == 0)
            def _():
                for name in ("s+", "s-"):
                    self.copy(name, me, 0, part=(0, half_rows - aside_rows)).wait_send()
                for name in ("f+", "f-"):
                    self.copy(name, me, 0, part=(half_rows - aside_rows, aside_rows)).wait_send()

            @pl.when(c == 1)
            def _():
                for name in ("s+", "s-"):
                    self.copy(name, me, 0, part=(0, half_rows)).wait_send()

    grad = Gather(g_ref, gfull, g_recv, g_send)

    def block_of(k):
        e, other = k // 2, k % 2
        df, ds = lookup(FIRST_CODE, e), lookup(SECOND_CODE, e)
        mine = index(df, ds)
        return mine + other * (twin_index(df, ds) - mine)

    def load(gather, buf, k, sem):
        b = block_of(k)
        return pltpu.make_async_copy(gather.full.at[pl.ds(2 * b, 2)], buf.at[k % 2], sem.at[k % 2])

    def start_load(gather, buf, k, sem):
        @pl.when(k % 2 == 1)
        def _():
            b = block_of(k)
            with jax.named_scope("twinwait"):
                gather.wait(b, 0)
                gather.wait(b, 1)
        load(gather, buf, k, sem).start()

    def one_of(k, values):
        found = k == values[0]
        for v in values[1:]:
            found = found | (k == v)
        return found

    def steps(gather, buf, sem, round_step, extra, work):
        def step(k, carry):
            for at, fn in extra:
                pl.when(k == at)(fn)
            for r in range(ROUNDS):
                @pl.when(k == round_step[r])
                def _():
                    with jax.named_scope(f"ground{r}"):
                        gather.round(r)

            @pl.when(one_of(k, LATE))
            def _():
                start_load(gather, buf, k, sem)

            @pl.when((k + 1 < n) & jnp.logical_not(one_of(k + 1, LATE + MIDDLE)))
            def _():
                start_load(gather, buf, k + 1, sem)

            def middle():
                @pl.when(one_of(k + 1, MIDDLE))
                def _():
                    start_load(gather, buf, k + 1, sem)
            with jax.named_scope("loadwait"):
                load(gather, buf, k, sem).wait()
            with jax.named_scope("work"):
                work(k, k % 2, block_of(k), middle)
            return carry
        lax.fori_loop(0, n, step, 0)

    first = [
        pltpu.make_async_copy(rr_ref, rr, init_sem.at[0]),
        pltpu.make_async_copy(r_ref, ro_ref, init_sem.at[1]),
        pltpu.make_async_copy(l_ref, lo_ref, init_sem.at[2]),
        pltpu.make_async_copy(lr_ref, lroot.at[pl.ds(2 * ((y * (side // 2) + x // 2) * CORES + c), 2)], init_sem.at[3]),
    ]
    own_load = pltpu.make_async_copy(g_ref, gbuf.at[0], load_sem.at[0])
    own_load.start()

    barrier = pltpu.get_barrier_semaphore()
    for peer in peers.values():
        pl.semaphore_signal(barrier, inc=1, device_id={"tensor": peer}, device_id_type=MESH)
    with jax.named_scope("barrier"):
        pl.semaphore_wait(barrier, len(peers))
    grad.start()
    for copy in first:
        copy.start()

    acc[...] = jnp.zeros_like(acc)
    own_load.wait()
    for h in (0, 1):
        gt[:, h * half_rows:(h + 1) * half_rows] = gbuf[0, h].T
    for copy in first:
        copy.wait()
    own_load.start()

    per_half = half_rows // tile

    def grad_work(k, slot, b, middle):
        at = pl.multiple_of(b * cols, cols)
        rhs[:cols] = rr[:, pl.ds(at, cols)]
        rhs[cols:] = gbuf[slot, me // (n // 2), pl.ds(pl.multiple_of((me % (n // 2)) * lrows, lrows), lrows), :]

        def rows_step(t, carry):
            left = gbuf[slot, t // per_half, pl.ds(pl.multiple_of((t % per_half) * tile, tile), tile), :]
            out = pl.ds(pl.multiple_of(t * tile, tile), tile)
            acc[out, :] += lax.dot_general(left, rhs[...], (((1,), (1,)), ((), ())), preferred_element_type=jnp.float32)
            return carry
        lax.fori_loop(0, 2 * per_half, rows_step, 0)
        middle()
        prod = jnp.dot(gt[:, :half_rows], gbuf[slot, 0], preferred_element_type=jnp.float32)
        prod += jnp.dot(gt[:, half_rows:], gbuf[slot, 1], preferred_element_type=jnp.float32)
        ro_ref[:, pl.ds(at, cols)] = EMA_DECAY * ro_ref[:, pl.ds(at, cols)] + (1.0 - EMA_DECAY) * prod


    dx = 1 - 2 * c
    helper = (y * side + (x + dx + side) % side) * CORES + c
    client = (y * side + (x - dx + side) % side) * CORES + c
    up = (((y + 1) % side) * side + x) * CORES + c
    down = (((y + side - 1) % side) * side + x) * CORES + c
    half_count, root_half, _ = lroot.shape
    pieces = ((0, root_half - root_half // 4), (root_half - root_half // 4, root_half // 4))

    def root_block(dy, q, p=0):
        oy, ox = (y + dy) % side, (x + 2 * q) % side
        core = c + p * (1 - 2 * c)
        return (oy * (side // 2) + ox // 2) * CORES + core, (oy * side + ox) * CORES + core

    def root_copy(peer, sem, place, half, src=None, dst=None, recv=None, part=None):
        here = lroot.at[2 * place + half]
        if part is not None:
            here = here.at[pl.ds(*pieces[part])]
        return pltpu.make_async_remote_copy(
            src_ref=here if src is None else src, dst_ref=here if dst is None else dst, send_sem=l_send.at[sem],
            recv_sem=l_recv.at[2 * place + half] if recv is None else recv, device_id={"tensor": peer}, device_id_type=MESH)

    sent = [0, 0, 0, 0]

    def root_send(peer, sem, place, half, part=None, **kw):
        sent[sem] += root_half if part is None else pieces[part][1]
        root_copy(peer, sem, place, half, part=part, **kw).start()

    def root_wait(place, half, **kw):
        root_copy(twin, 3, place, half, **kw).wait_recv()

    own_place, _ = root_block(0, 0)
    far_place, _ = root_block(0, 1)
    passing = (y * (side // 2) + ((x - dx + side) % side) // 2) * CORES + c

    def root_start_across():
        for half in (0, 1):
            root_send(helper, 0, own_place, half, src=lr_ref.at[half], dst=relay.at[half], recv=relay_recv.at[half])

    def root_start():
        for half in (0, 1):
            root_send(up, 1, own_place, half, src=lr_ref.at[half])
            root_send(down, 2, own_place, 1 - half, src=lr_ref.at[1 - half])
        for half in (0, 1):
            root_send(twin, 3, own_place, half, src=lr_ref.at[half])

    def root_relay(half):
        root_copy(helper, 0, own_place, half, src=lr_ref.at[half], dst=relay.at[half], recv=relay_recv.at[half]).wait_recv()
        root_send(helper, 0, passing, half, src=relay.at[half])

    def root_far():
        for half in (0, 1):
            root_wait(far_place, half)
            root_send(up, 1, far_place, half)
            root_send(twin, 3, far_place, half)
        for half in (1, 0):
            root_send(down, 2, far_place, half)

    def root_round(r):
        q, stage = r // 3, r % 3
        if stage == 2:
            behind = root_block(2, q)[0]
            for half in (0, 1):
                root_wait(behind, half)
                root_send(twin, 3, behind, half)
            return
        below, above = root_block(side - 1, q)[0], root_block(1, q)[0]
        root_wait(below, stage)
        if stage == 0:
            for part in (None,) if q == 0 else (0, 1):
                root_send(up, 1, below, 0, part=part, recv=last_recv.at[0] if part else None)
        root_send(twin, 3, below, stage)
        root_wait(above, 1 - stage)
        if stage == 0:
            for part in (None,) if q == 0 else (0, 1):
                root_send(down, 2, above, 1, part=part, recv=last_recv.at[1] if part else None)
        root_send(twin, 3, above, 1 - stage)

    last_place, last_device = root_block(2, 1)
    twin_place, twin_device = root_block(2, 1, 1)

    def root_last(part):
        for half in (0, 1):
            root_wait(last_place, half, part=part, recv=last_recv.at[half] if part else None)
            root_send(twin, 3, last_place, half, part=part, recv=last_recv.at[2 + half] if part else None)

    def root_last_twin(part):
        for half in (0, 1):
            root_wait(twin_place, half, part=part, recv=last_recv.at[2 + half] if part else None)

    steps(grad, gbuf, load_sem, GRAD_ROUND_STEP, [(ROOT_START_STEP, root_start), (ROOT_ACROSS_STEP, root_start_across), (RELAY_STEP, lambda: root_relay(0))], grad_work)

    side_cols = cols // 2

    def x_copy(h):
        at = pl.ds(h * side_cols, side_cols)
        return pltpu.make_async_remote_copy(
            src_ref=xx.at[0, :, at], dst_ref=xx.at[1, :, at], send_sem=x_send.at[h], recv_sem=x_recv.at[h],
            device_id={"tensor": helper}, device_id_type=MESH)

    with jax.named_scope("xfin"):
        xx[0] = acc[:, :cols].astype(jnp.bfloat16)
    with jax.named_scope("relay"):
        root_relay(1)
    x_copy(0).start()
    x_copy(1).start()
    with jax.named_scope("rround0"):
        root_round(0)

    def left_step(t, carry):
        at = pl.ds(pl.multiple_of(t * lrows, lrows), lrows)
        lo_ref[:, at] = EMA_DECAY * lo_ref[:, at] + (1.0 - EMA_DECAY) * acc[at, cols:].T
        return carry
    with jax.named_scope("leftfin"):
        lax.fori_loop(0, rows // lrows, left_step, 0)

    def at_step(i):
        e, p = i // 2, i % 2
        dy = lax.shift_right_logical(ROOT_Y, 2 * e) & 3
        q = lax.shift_right_logical(ROOT_X, 2 * e) & 3
        return root_block(dy, q, p)

    def twin_wait(i, place):
        @pl.when(i % 2 == 1)
        def _():
            root_wait(place, 0)
            root_wait(place, 1)

    def product(place, which):
        left = lroot[pl.ds(2 * place, 2)].reshape(lrows, rows)
        return jnp.dot(left, xx[which], preferred_element_type=jnp.float32)

    def rows_of(device):
        return pl.ds(pl.multiple_of(device * lrows, lrows), lrows)

    def own_rows(i):
        place, device = at_step(i)
        do_ref[rows_of(device), :] = product(place, 0)

    def lent_copy(place, device):
        return pltpu.make_async_remote_copy(
            src_ref=lent.at[place], dst_ref=do_ref.at[rows_of(device)], send_sem=d_send.at[0], recv_sem=d_recv.at[place],
            device_id={"tensor": client}, device_id_type=MESH)

    def lent_rows(i):
        place, device = at_step(i)
        lent[place] = product(place, 1)
        lent_copy(place, device).start()

    def lent_side(i, h):
        place, _ = at_step(i)
        at = pl.ds(h * side_cols, side_cols)
        left = lroot[pl.ds(2 * place, 2)].reshape(lrows, rows)
        lent[place, :, at] = jnp.dot(left, xx[1, :, at], preferred_element_type=jnp.float32)

    def lent_side_copy(i, h):
        place, device = at_step(i)
        at = pl.ds(h * side_cols, side_cols)
        return pltpu.make_async_remote_copy(
            src_ref=lent.at[place, :, at], dst_ref=do_ref.at[rows_of(device), at], send_sem=d_send.at[0], recv_sem=d_recv.at[place],
            device_id={"tensor": client}, device_id_type=MESH)

    def loop(lo, hi, body):
        def step(i, carry):
            body(i)
            return carry
        lax.fori_loop(lo, hi, step, 0)

    def first_own(i):
        @pl.when(i == 2)
        def _():
            with jax.named_scope("far"):
                root_far()
            with jax.named_scope("rround1"):
                root_round(1)

        @pl.when(i == 8)
        def _():
            with jax.named_scope("rround2"):
                root_round(2)
        twin_wait(i, at_step(i)[0])
        own_rows(i)

    loop(0, 10, first_own)
    with jax.named_scope("x0wait"):
        x_copy(0).wait_recv()
    loop(0, 10, lambda i: lent_side(i, 0))
    x_copy(0).wait_send()
    with jax.named_scope("x1sent"):
        x_copy(1).wait_send()
    loop(0, 10, lambda i: lent_side_copy(i, 0).start())
    with jax.named_scope("rround3"):
        root_round(3)
    with jax.named_scope("x1wait"):
        x_copy(1).wait_recv()

    def second_side(i):
        lent_side(i, 1)
        lent_side_copy(i, 1).start()
    loop(0, 10, second_side)
    with jax.named_scope("rround4"):
        root_round(4)

    def both(i):
        twin_wait(i, at_step(i)[0])
        lent_rows(i)
        own_rows(i)
    with jax.named_scope("both"):
        loop(10, 14, both)

    def lent_piece(place, device, part):
        first, count = pieces[part]
        left = jnp.concatenate([lroot[2 * place, pl.ds(first, count), :], lroot[2 * place + 1, pl.ds(first, count), :]], axis=0)
        prod = jnp.dot(left, xx[1], preferred_element_type=jnp.float32)
        for half in (0, 1):
            at = half * root_half + first
            lent[place, pl.ds(at, count), :] = prod[half * count:(half + 1) * count]
            pltpu.make_async_remote_copy(
                src_ref=lent.at[place, pl.ds(at, count)], dst_ref=do_ref.at[pl.ds(pl.multiple_of(device * lrows, lrows) + at, count)],
                send_sem=d_send.at[0], recv_sem=d_recv.at[place], device_id={"tensor": client}, device_id_type=MESH).start()

    for part in (0, 1):
        with jax.named_scope(f"last{part}"):
            root_last(part)
        lent_piece(last_place, last_device, part)
        with jax.named_scope(f"lasttwin{part}"):
            root_last_twin(part)
        lent_piece(twin_place, twin_device, part)
    loop(14, 16, own_rows)

    with jax.named_scope("drain"):
        grad.drain()
    for sem, count in enumerate(sent):
        whole = lroot.at[pl.ds(0, count // root_half)]
        pltpu.make_async_copy(whole, whole, l_send.at[sem]).wait()
    pltpu.make_async_copy(lent, lent, d_send.at[0]).wait()

    def lent_wait(i, carry):
        lent_copy(i, 0).wait_recv()
        return carry
    with jax.named_scope("dwait"):
        lax.fori_loop(0, half_count // 2, lent_wait, 0)


def store_kernel(*refs):
    count = (len(refs) - 1) // 2
    sems = refs[-1]
    pieces = 8
    for i in range(count):
        src, dst = refs[i], refs[count + i]
        step = src.shape[0] // pieces
        for j in range(pieces):
            part = pl.ds(j * step, step)
            pltpu.make_async_copy(src.at[part], dst.at[part], sems.at[i]).start()
    for i in range(count):
        pltpu.make_async_copy(refs[i], refs[count + i], sems.at[i]).wait()


def solution(mesh):
    row_spec = P(("layer", "tensor"), None)
    col_spec = P("layer", "tensor")
    n = mesh.shape["tensor"]
    side = math.isqrt(n // CORES)

    def local_step(g, l, r, lr, rr):
        rows, cols = g.shape
        lrows = l.shape[0]
        kept = n // 2
        hbm = pl.BlockSpec(memory_space=pltpu.HBM)
        vmem = pl.BlockSpec(memory_space=pltpu.VMEM)
        operands = [g.reshape(2, rows // 2, cols), l, r, lr.reshape(2, lrows // 2, rows), rr]
        left_new, right_new, direction, _ = pl.pallas_call(
            functools.partial(kernel, n, side),
            name="shampoo",
            out_shape=[
                pltpu.VMEM(l.shape, jnp.float32),
                pltpu.VMEM(r.shape, jnp.float32),
                pltpu.VMEM(g.shape, jnp.float32),
                pltpu.HBM((2 * n, rows // 2, cols), jnp.bfloat16),
            ],
            in_specs=[hbm] * 5,
            out_specs=[vmem, vmem, vmem, hbm],
            scratch_shapes=[
                pltpu.VMEM(rr.shape, jnp.bfloat16),
                pltpu.VMEM((cols, rows), jnp.bfloat16),
                pltpu.VMEM((rows, cols + lrows), jnp.float32),
                pltpu.VMEM((2, 2, rows // 2, cols), jnp.bfloat16),
                pltpu.VMEM((cols + lrows, cols), jnp.bfloat16),
                pltpu.VMEM((2, rows, cols), jnp.bfloat16),
                pltpu.VMEM((2 * kept, lrows // 2, rows), jnp.bfloat16),
                pltpu.VMEM((2, lrows // 2, rows), jnp.bfloat16),
                pltpu.VMEM((kept, lrows, cols), jnp.float32),
                pltpu.SemaphoreType.DMA((2 * n,)),
                pltpu.SemaphoreType.DMA((10,)),
                pltpu.SemaphoreType.DMA((2,)),
                pltpu.SemaphoreType.DMA((4,)),
                pltpu.SemaphoreType.DMA((2 * kept,)),
                pltpu.SemaphoreType.DMA((4,)),
                pltpu.SemaphoreType.DMA((2,)),
                pltpu.SemaphoreType.DMA((2,)),
                pltpu.SemaphoreType.DMA((kept,)),
                pltpu.SemaphoreType.DMA((4,)),
                pltpu.SemaphoreType.DMA((2,)),
                pltpu.SemaphoreType.DMA((1,)),
            ],
            compiler_params=pltpu.CompilerParams(collective_id=0, has_side_effects=True, vmem_limit_bytes=48 * 2**20),
            cost_estimate=pl.CostEstimate(flops=2 * rows * cols * (2 * n * cols + 2 * rows), bytes_accessed=2 * n * rows * cols * 3, transcendentals=0),
        )(*[pltpu.with_memory_space_constraint(v, pltpu.HBM) for v in operands])
        results = [left_new, right_new, direction]
        return pl.pallas_call(
            store_kernel,
            name="store",
            out_shape=[jax.ShapeDtypeStruct(v.shape, v.dtype) for v in results],
            in_specs=[vmem] * 3,
            out_specs=[hbm] * 3,
            scratch_shapes=[pltpu.SemaphoreType.DMA((3,))],
            compiler_params=pltpu.CompilerParams(vmem_limit_bytes=1 * 2**20),
        )(*results)

    return jax.shard_map(local_step, mesh=mesh, in_specs=(col_spec, row_spec, row_spec, row_spec, row_spec), out_specs=(row_spec, row_spec, col_spec), check_vma=False)
```

```python
import functools
import math

import jax
import jax.numpy as jnp
from jax import lax
from jax.experimental import pallas as pl
from jax.experimental.pallas import tpu as pltpu
from jax.sharding import PartitionSpec as P

EMA_DECAY = 0.9
CORES = 2
MESH = pl.DeviceIdType.MESH

ORDER = [(int(a), int(b)) for a, b in zip("0310020311322312", "0003102313131222")]
def parcels(code):
    digits = [int(d) for d in code]
    return [((a, b), h) for a, b, h in zip(digits[0::3], digits[1::3], digits[2::3])]


UP = parcels("030031330131020331130230231320120220")
UP_ON = {0: parcels("030"), 2: parcels("330"), 6: parcels("130"), 7: parcels("230")}
DOWN = parcels("011010111310021110311211210321121221")
DOWN_ON = {0: parcels("011"), 6: parcels("311111"), 7: parcels("211")}
ROUNDS = len(UP)
FIRST_UP = parcels("300301200")
FIRST_DOWN = parcels("101100201")
GRAD_ROUND_STEP = [2, 2, 8, 10, 12, 14, 17, 20, 22, 26, 28, 30]
LAST_FORWARD = 7
SIDE_UP, SIDE_DOWN = 9, 10
ASIDE = 32
ROOT_START_STEP = 29
ROOT_ACROSS_STEP = 30
RELAY_STEP = 31
LATE = (2, 12, 14, 22, 26, 28, 30)
MIDDLE = (3, 13, 15, 23, 27, 29, 31)


def packed(values):
    return [sum(v << (2 * i) for i, v in enumerate(values[j:j + 8])) for j in (0, 8)]


FIRST_CODE = packed([o[0] for o in ORDER])
SECOND_CODE = packed([o[1] for o in ORDER])


def lookup(code, e):
    word = code[0] + (e // 8) * (code[1] - code[0])
    return lax.shift_right_logical(word, 2 * (e % 8)) & 3


ROOT_ORDER = [(0, 0), (3, 0), (1, 0), (0, 1), (2, 0), (3, 1), (1, 1), (2, 1)]
ROOT_Y = sum(o[0] << (2 * i) for i, o in enumerate(ROOT_ORDER))
ROOT_X = sum(o[1] << (2 * i) for i, o in enumerate(ROOT_ORDER))


def kernel(n, side, g_ref, l_ref, r_ref, lr_ref, rr_ref, lo_ref, ro_ref, do_ref, gfull,
           rr, gt, acc, gbuf, rhs, xx, lroot, relay, lent,
           g_recv, g_send, load_sem, init_sem, l_recv, last_recv, relay_recv, x_recv, d_recv, l_send, x_send, d_send):
    _, half_rows, cols = g_ref.shape
    rows = 2 * half_rows
    lrows = l_ref.shape[0]
    tile = min(1024, half_rows)
    aside_rows = half_rows * ASIDE // 128

    me = lax.axis_index("tensor")
    c = me % CORES
    chip = me // CORES
    x, y = chip % side, chip // side
    f = x + c * (y - x)
    s = y + c * (x - y)
    fstep = CORES + c * CORES * (side - 1)
    sstep = CORES * side - c * CORES * (side - 1)
    twin = me + 1 - 2 * c

    def index(df, ds):
        return ((f + df) % side) * fstep + ((s + ds) % side) * sstep + c

    def twin_index(df, ds):
        return ((s + df) % side) * sstep + ((f + ds) % side) * fstep + 1 - c

    peers = {"f+": index(1, 0), "f-": index(3, 0), "s+": index(0, 1), "s-": index(0, 3), "twin": twin}
    slot_of = {name: i for i, name in enumerate(peers)}

    class Gather:
        def __init__(self, own, full, recv, send):
            self.own, self.full, self.recv, self.send_sem = own, full, recv, send
            self.count = {name: 0 for name in peers}

        def copy(self, name, b, half, own=False, part=None):
            src = self.own.at[half] if own else self.full.at[2 * b + half]
            dst = self.full.at[2 * b + half]
            sem = slot_of[name]
            if part is not None:
                src, dst, sem = src.at[pl.ds(*part)], dst.at[pl.ds(*part)], len(peers) + sem
            return pltpu.make_async_remote_copy(
                src_ref=src, dst_ref=dst, send_sem=self.send_sem.at[sem],
                recv_sem=self.recv.at[2 * b + half], device_id={"tensor": peers[name]}, device_id_type=MESH)

        def send(self, name, b, half, own=False):
            self.count[name] += 1
            self.copy(name, b, half, own).start()

        def wait(self, b, half):
            self.copy("twin", b, half).wait_recv()

        def start(self):
            for half in (0, 1):
                for name in ("f+", "s+"):
                    self.send(name, me, half, own=True)
                for name in ("f-", "s-"):
                    self.send(name, me, 1 - half, own=True)
            for half in (0, 1):
                self.send("twin", me, half, own=True)

        def round(self, r):
            if r < len(FIRST_UP):
                (ou, hu), (od, hd) = FIRST_UP[r], FIRST_DOWN[r]
                bu, bd = index(*ou), index(*od)
                self.wait(bu, hu)
                if r == 0:
                    self.send("f+", bu, hu)
                self.wait(bd, hd)
                if r == 0:
                    self.send("f-", bd, hd)
                self.send("s+", bu, hu)
                self.send("s-", bd, hd)
                self.send("s+", bd, hd)
                self.send("s-", bu, hu)
                self.send("twin", bu, hu)
                self.send("twin", bd, hd)
            (ou, hu), (od, hd) = UP[r], DOWN[r]
            fu, fd = UP_ON.get(r, ()), DOWN_ON.get(r, ())
            bu, bd = index(*ou), index(*od)
            self.wait(bu, hu)
            for offset, half in fu:
                if r == LAST_FORWARD:
                    self.forward_last("s+", index(*offset), half)
                else:
                    self.send("s+", index(*offset), half)
            if r == SIDE_UP:
                self.aside("f+", bu, hu)
            self.send("twin", bu, hu)
            self.wait(bd, hd)
            for offset, half in fd:
                if r == LAST_FORWARD:
                    self.forward_last("s-", index(*offset), half)
                else:
                    self.send("s-", index(*offset), half)
            if r == SIDE_DOWN:
                self.aside("f-", bd, hd)
            self.send("twin", bd, hd)

        def forward_last(self, name, b, half):
            pl.when(c == 0)(lambda: self.copy(name, b, half, part=(0, half_rows - aside_rows)).start())
            pl.when(c == 1)(lambda: self.copy(name, b, half, part=(0, half_rows)).start())

        def aside(self, name, b, half):
            pl.when(c == 0)(lambda: self.copy(name, b, half, part=(half_rows - aside_rows, aside_rows)).start())

        def drain(self):
            for name, count in self.count.items():
                whole = self.full.at[pl.ds(0, count)]
                pltpu.make_async_copy(whole, whole, self.send_sem.at[slot_of[name]]).wait()

            @pl.when(c == 0)
            def _():
                for name in ("s+", "s-"):
                    self.copy(name, me, 0, part=(0, half_rows - aside_rows)).wait_send()
                for name in ("f+", "f-"):
                    self.copy(name, me, 0, part=(half_rows - aside_rows, aside_rows)).wait_send()

            @pl.when(c == 1)
            def _():
                for name in ("s+", "s-"):
                    self.copy(name, me, 0, part=(0, half_rows)).wait_send()

    grad = Gather(g_ref, gfull, g_recv, g_send)

    def block_of(k):
        e, other = k // 2, k % 2
        df, ds = lookup(FIRST_CODE, e), lookup(SECOND_CODE, e)
        mine = index(df, ds)
        return mine + other * (twin_index(df, ds) - mine)

    def load(gather, buf, k, sem):
        b = block_of(k)
        return pltpu.make_async_copy(gather.full.at[pl.ds(2 * b, 2)], buf.at[k % 2], sem.at[k % 2])

    def start_load(gather, buf, k, sem):
        @pl.when(k % 2 == 1)
        def _():
            b = block_of(k)
            with jax.named_scope("twinwait"):
                gather.wait(b, 0)
                gather.wait(b, 1)
        load(gather, buf, k, sem).start()

    def one_of(k, values):
        found = k == values[0]
        for v in values[1:]:
            found = found | (k == v)
        return found

    def steps(gather, buf, sem, round_step, extra, work):
        def step(k, carry):
            for at, fn in extra:
                pl.when(k == at)(fn)
            for r in range(ROUNDS):
                @pl.when(k == round_step[r])
                def _():
                    with jax.named_scope(f"ground{r}"):
                        gather.round(r)

            @pl.when(one_of(k, LATE))
            def _():
                start_load(gather, buf, k, sem)

            @pl.when((k + 1 < n) & jnp.logical_not(one_of(k + 1, LATE + MIDDLE)))
            def _():
                start_load(gather, buf, k + 1, sem)

            def middle():
                @pl.when(one_of(k + 1, MIDDLE))
                def _():
                    start_load(gather, buf, k + 1, sem)
            with jax.named_scope("loadwait"):
                load(gather, buf, k, sem).wait()
            with jax.named_scope("work"):
                work(k, k % 2, block_of(k), middle)
            return carry
        lax.fori_loop(0, n, step, 0)

    first = [
        pltpu.make_async_copy(rr_ref, rr, init_sem.at[0]),
        pltpu.make_async_copy(r_ref, ro_ref, init_sem.at[1]),
        pltpu.make_async_copy(l_ref, lo_ref, init_sem.at[2]),
        pltpu.make_async_copy(lr_ref, lroot.at[pl.ds(2 * ((y * (side // 2) + x // 2) * CORES + c), 2)], init_sem.at[3]),
    ]
    own_load = pltpu.make_async_copy(g_ref, gbuf.at[0], load_sem.at[0])
    own_load.start()

    barrier = pltpu.get_barrier_semaphore()
    for peer in peers.values():
        pl.semaphore_signal(barrier, inc=1, device_id={"tensor": peer}, device_id_type=MESH)
    with jax.named_scope("barrier"):
        pl.semaphore_wait(barrier, len(peers))
    grad.start()
    for copy in first:
        copy.start()

    acc[...] = jnp.zeros_like(acc)
    own_load.wait()
    for h in (0, 1):
        gt[:, h * half_rows:(h + 1) * half_rows] = gbuf[0, h].T
    for copy in first:
        copy.wait()
    own_load.start()

    per_half = half_rows // tile

    def grad_work(k, slot, b, middle):
        at = pl.multiple_of(b * cols, cols)
        rhs[:cols] = rr[:, pl.ds(at, cols)]
        rhs[cols:] = gbuf[slot, me // (n // 2), pl.ds(pl.multiple_of((me % (n // 2)) * lrows, lrows), lrows), :]

        def rows_step(t, carry):
            left = gbuf[slot, t // per_half, pl.ds(pl.multiple_of((t % per_half) * tile, tile), tile), :]
            out = pl.ds(pl.multiple_of(t * tile, tile), tile)
            acc[out, :] += lax.dot_general(left, rhs[...], (((1,), (1,)), ((), ())), preferred_element_type=jnp.float32)
            return carry
        lax.fori_loop(0, 2 * per_half, rows_step, 0)
        middle()
        prod = jnp.dot(gt[:, :half_rows], gbuf[slot, 0], preferred_element_type=jnp.float32)
        prod += jnp.dot(gt[:, half_rows:], gbuf[slot, 1], preferred_element_type=jnp.float32)
        ro_ref[:, pl.ds(at, cols)] = EMA_DECAY * ro_ref[:, pl.ds(at, cols)] + (1.0 - EMA_DECAY) * prod


    dx = 1 - 2 * c
    helper = (y * side + (x + dx + side) % side) * CORES + c
    client = (y * side + (x - dx + side) % side) * CORES + c
    up = (((y + 1) % side) * side + x) * CORES + c
    down = (((y + side - 1) % side) * side + x) * CORES + c
    half_count, root_half, _ = lroot.shape
    pieces = ((0, root_half - root_half // 4), (root_half - root_half // 4, root_half // 4))

    def root_block(dy, q, p=0):
        oy, ox = (y + dy) % side, (x + 2 * q) % side
        core = c + p * (1 - 2 * c)
        return (oy * (side // 2) + ox // 2) * CORES + core, (oy * side + ox) * CORES + core

    def root_copy(peer, sem, place, half, src=None, dst=None, recv=None, part=None):
        here = lroot.at[2 * place + half]
        if part is not None:
            here = here.at[pl.ds(*pieces[part])]
        return pltpu.make_async_remote_copy(
            src_ref=here if src is None else src, dst_ref=here if dst is None else dst, send_sem=l_send.at[sem],
            recv_sem=l_recv.at[2 * place + half] if recv is None else recv, device_id={"tensor": peer}, device_id_type=MESH)

    sent = [0, 0, 0, 0]

    def root_send(peer, sem, place, half, part=None, **kw):
        sent[sem] += root_half if part is None else pieces[part][1]
        root_copy(peer, sem, place, half, part=part, **kw).start()

    def root_wait(place, half, **kw):
        root_copy(twin, 3, place, half, **kw).wait_recv()

    own_place, _ = root_block(0, 0)
    far_place, _ = root_block(0, 1)
    passing = (y * (side // 2) + ((x - dx + side) % side) // 2) * CORES + c

    def root_start_across():
        for half in (0, 1):
            root_send(helper, 0, own_place, half, src=lr_ref.at[half], dst=relay.at[half], recv=relay_recv.at[half])

    def root_start():
        for half in (0, 1):
            root_send(up, 1, own_place, half, src=lr_ref.at[half])
            root_send(down, 2, own_place, 1 - half, src=lr_ref.at[1 - half])
        for half in (0, 1):
            root_send(twin, 3, own_place, half, src=lr_ref.at[half])

    def root_relay(half):
        root_copy(helper, 0, own_place, half, src=lr_ref.at[half], dst=relay.at[half], recv=relay_recv.at[half]).wait_recv()
        root_send(helper, 0, passing, half, src=relay.at[half])
        root_send(twin, 3, passing, half, src=relay.at[half], dst=relay.at[2 + half], recv=relay_recv.at[2 + half])

    def passed_rows(p):
        if p:
            for half in (0, 1):
                root_copy(twin, 3, passing, half, src=relay.at[half], dst=relay.at[2 + half], recv=relay_recv.at[2 + half]).wait_recv()
        source = (y * side + (x - (1 - 2 * p) * dx + side) % side) * CORES + c + p * (1 - 2 * c)
        left = relay[2 * p:2 * p + 2].reshape(lrows, rows)
        do_ref[rows_of(source), :] = jnp.dot(left, xx[0], preferred_element_type=jnp.float32)

    def root_far():
        for half in (0, 1):
            root_wait(far_place, half)
            root_send(up, 1, far_place, half)
            root_send(twin, 3, far_place, half)
        for half in (1, 0):
            root_send(down, 2, far_place, half)

    def root_round(r):
        q, stage = r // 3, r % 3
        if stage == 2:
            behind = root_block(2, q)[0]
            for half in (0, 1):
                root_wait(behind, half)
                root_send(twin, 3, behind, half)
            return
        below, above = root_block(side - 1, q)[0], root_block(1, q)[0]
        root_wait(below, stage)
        if stage == 0:
            for part in (None,) if q == 0 else (0, 1):
                root_send(up, 1, below, 0, part=part, recv=last_recv.at[0] if part else None)
        root_send(twin, 3, below, stage)
        root_wait(above, 1 - stage)
        if stage == 0:
            for part in (None,) if q == 0 else (0, 1):
                root_send(down, 2, above, 1, part=part, recv=last_recv.at[1] if part else None)
        root_send(twin, 3, above, 1 - stage)

    last_place, last_device = root_block(2, 1)
    twin_place, twin_device = root_block(2, 1, 1)

    def root_last(part):
        for half in (0, 1):
            root_wait(last_place, half, part=part, recv=last_recv.at[half] if part else None)
            root_send(twin, 3, last_place, half, part=part, recv=last_recv.at[2 + half] if part else None)

    def root_last_twin(part):
        for half in (0, 1):
            root_wait(twin_place, half, part=part, recv=last_recv.at[2 + half] if part else None)

    steps(grad, gbuf, load_sem, GRAD_ROUND_STEP, [(ROOT_START_STEP, root_start), (ROOT_ACROSS_STEP, root_start_across), (RELAY_STEP, lambda: root_relay(0))], grad_work)

    side_cols = cols // 2

    def x_copy(h):
        at = pl.ds(h * side_cols, side_cols)
        return pltpu.make_async_remote_copy(
            src_ref=xx.at[0, :, at], dst_ref=xx.at[1, :, at], send_sem=x_send.at[h], recv_sem=x_recv.at[h],
            device_id={"tensor": helper}, device_id_type=MESH)

    with jax.named_scope("xfin"):
        xx[0] = acc[:, :cols].astype(jnp.bfloat16)
    with jax.named_scope("relay"):
        root_relay(1)
    x_copy(0).start()
    x_copy(1).start()
    with jax.named_scope("rround0"):
        root_round(0)

    def left_step(t, carry):
        at = pl.ds(pl.multiple_of(t * lrows, lrows), lrows)
        lo_ref[:, at] = EMA_DECAY * lo_ref[:, at] + (1.0 - EMA_DECAY) * acc[at, cols:].T
        return carry
    with jax.named_scope("leftfin"):
        lax.fori_loop(0, rows // lrows, left_step, 0)

    def at_step(i):
        e, p = i // 2, i % 2
        dy = lax.shift_right_logical(ROOT_Y, 2 * e) & 3
        q = lax.shift_right_logical(ROOT_X, 2 * e) & 3
        return root_block(dy, q, p)

    def twin_wait(i, place):
        @pl.when(i % 2 == 1)
        def _():
            root_wait(place, 0)
            root_wait(place, 1)

    def product(place, which):
        left = lroot[pl.ds(2 * place, 2)].reshape(lrows, rows)
        return jnp.dot(left, xx[which], preferred_element_type=jnp.float32)

    def rows_of(device):
        return pl.ds(pl.multiple_of(device * lrows, lrows), lrows)

    def own_rows(i):
        place, device = at_step(i)
        do_ref[rows_of(device), :] = product(place, 0)

    def lent_copy(i, device):
        return pltpu.make_async_remote_copy(
            src_ref=lent.at[i], dst_ref=do_ref.at[rows_of(device)], send_sem=d_send.at[0], recv_sem=d_recv.at[i],
            device_id={"tensor": client}, device_id_type=MESH)

    def lent_rows(i):
        place, device = at_step(i)
        lent[i] = product(place, 1)
        lent_copy(i, device).start()

    def lent_side(i, h):
        place, _ = at_step(i)
        at = pl.ds(h * side_cols, side_cols)
        left = lroot[pl.ds(2 * place, 2)].reshape(lrows, rows)
        lent[i, :, at] = jnp.dot(left, xx[1, :, at], preferred_element_type=jnp.float32)

    def lent_side_copy(i, h):
        _, device = at_step(i)
        at = pl.ds(h * side_cols, side_cols)
        return pltpu.make_async_remote_copy(
            src_ref=lent.at[i, :, at], dst_ref=do_ref.at[rows_of(device), at], send_sem=d_send.at[0], recv_sem=d_recv.at[i],
            device_id={"tensor": client}, device_id_type=MESH)

    def loop(lo, hi, body):
        def step(i, carry):
            body(i)
            return carry
        lax.fori_loop(lo, hi, step, 0)

    def first_own(i):
        @pl.when(i == 2)
        def _():
            with jax.named_scope("far"):
                root_far()
            with jax.named_scope("rround1"):
                root_round(1)

        @pl.when(i == 8)
        def _():
            with jax.named_scope("rround2"):
                root_round(2)
        twin_wait(i, at_step(i)[0])
        own_rows(i)

    loop(0, 10, first_own)
    passed_rows(0)
    passed_rows(1)
    with jax.named_scope("x0wait"):
        x_copy(0).wait_recv()
    def lent_step(j):
        return j + (j + 7) // 8 + j // 5

    loop(0, 8, lambda j: lent_side(lent_step(j), 0))
    x_copy(0).wait_send()
    with jax.named_scope("x1sent"):
        x_copy(1).wait_send()
    loop(0, 8, lambda j: lent_side_copy(lent_step(j), 0).start())
    with jax.named_scope("rround3"):
        root_round(3)
    with jax.named_scope("x1wait"):
        x_copy(1).wait_recv()

    def second_side(j):
        i = lent_step(j)
        lent_side(i, 1)
        lent_side_copy(i, 1).start()
    loop(0, 8, second_side)
    with jax.named_scope("rround4"):
        root_round(4)

    def both(i):
        twin_wait(i, at_step(i)[0])
        lent_rows(i)
        own_rows(i)
    with jax.named_scope("both"):
        loop(10, 14, both)

    def lent_piece(i, place, device, part):
        first, count = pieces[part]
        left = jnp.concatenate([lroot[2 * place, pl.ds(first, count), :], lroot[2 * place + 1, pl.ds(first, count), :]], axis=0)
        prod = jnp.dot(left, xx[1], preferred_element_type=jnp.float32)
        for half in (0, 1):
            at = half * root_half + first
            lent[i, pl.ds(at, count), :] = prod[half * count:(half + 1) * count]
            pltpu.make_async_remote_copy(
                src_ref=lent.at[i, pl.ds(at, count)], dst_ref=do_ref.at[pl.ds(pl.multiple_of(device * lrows, lrows) + at, count)],
                send_sem=d_send.at[0], recv_sem=d_recv.at[i], device_id={"tensor": client}, device_id_type=MESH).start()

    for part in (0, 1):
        with jax.named_scope(f"last{part}"):
            root_last(part)
        lent_piece(14, last_place, last_device, part)
        with jax.named_scope(f"lasttwin{part}"):
            root_last_twin(part)
        lent_piece(15, twin_place, twin_device, part)
    loop(14, 16, own_rows)

    with jax.named_scope("drain"):
        grad.drain()
    for sem, count in enumerate(sent):
        whole = lroot.at[pl.ds(0, count // root_half)]
        pltpu.make_async_copy(whole, whole, l_send.at[sem]).wait()
    given = lent.at[pl.ds(0, half_count // 2 - 2)]
    pltpu.make_async_copy(given, given, d_send.at[0]).wait()
    loop(0, 8, lambda j: lent_copy(lent_step(j), 0).wait_recv())
    with jax.named_scope("dwait"):
        loop(10, half_count // 2, lambda i: lent_copy(i, 0).wait_recv())


def store_kernel(*refs):
    count = (len(refs) - 1) // 2
    sems = refs[-1]
    pieces = 8
    for i in range(count):
        src, dst = refs[i], refs[count + i]
        step = src.shape[0] // pieces
        for j in range(pieces):
            part = pl.ds(j * step, step)
            pltpu.make_async_copy(src.at[part], dst.at[part], sems.at[i]).start()
    for i in range(count):
        pltpu.make_async_copy(refs[i], refs[count + i], sems.at[i]).wait()


def solution(mesh):
    row_spec = P(("layer", "tensor"), None)
    col_spec = P("layer", "tensor")
    n = mesh.shape["tensor"]
    side = math.isqrt(n // CORES)

    def local_step(g, l, r, lr, rr):
        rows, cols = g.shape
        lrows = l.shape[0]
        kept = n // 2
        hbm = pl.BlockSpec(memory_space=pltpu.HBM)
        vmem = pl.BlockSpec(memory_space=pltpu.VMEM)
        operands = [g.reshape(2, rows // 2, cols), l, r, lr.reshape(2, lrows // 2, rows), rr]
        left_new, right_new, direction, _ = pl.pallas_call(
            functools.partial(kernel, n, side),
            name="shampoo",
            out_shape=[
                pltpu.VMEM(l.shape, jnp.float32),
                pltpu.VMEM(r.shape, jnp.float32),
                pltpu.VMEM(g.shape, jnp.float32),
                pltpu.HBM((2 * n, rows // 2, cols), jnp.bfloat16),
            ],
            in_specs=[hbm] * 5,
            out_specs=[vmem, vmem, vmem, hbm],
            scratch_shapes=[
                pltpu.VMEM(rr.shape, jnp.bfloat16),
                pltpu.VMEM((cols, rows), jnp.bfloat16),
                pltpu.VMEM((rows, cols + lrows), jnp.float32),
                pltpu.VMEM((2, 2, rows // 2, cols), jnp.bfloat16),
                pltpu.VMEM((cols + lrows, cols), jnp.bfloat16),
                pltpu.VMEM((2, rows, cols), jnp.bfloat16),
                pltpu.VMEM((2 * kept, lrows // 2, rows), jnp.bfloat16),
                pltpu.VMEM((4, lrows // 2, rows), jnp.bfloat16),
                pltpu.VMEM((kept, lrows, cols), jnp.float32),
                pltpu.SemaphoreType.DMA((2 * n,)),
                pltpu.SemaphoreType.DMA((10,)),
                pltpu.SemaphoreType.DMA((2,)),
                pltpu.SemaphoreType.DMA((4,)),
                pltpu.SemaphoreType.DMA((2 * kept,)),
                pltpu.SemaphoreType.DMA((4,)),
                pltpu.SemaphoreType.DMA((4,)),
                pltpu.SemaphoreType.DMA((2,)),
                pltpu.SemaphoreType.DMA((kept,)),
                pltpu.SemaphoreType.DMA((4,)),
                pltpu.SemaphoreType.DMA((2,)),
                pltpu.SemaphoreType.DMA((1,)),
            ],
            compiler_params=pltpu.CompilerParams(collective_id=0, has_side_effects=True, vmem_limit_bytes=48 * 2**20),
            cost_estimate=pl.CostEstimate(flops=2 * rows * cols * (2 * n * cols + 2 * rows), bytes_accessed=2 * n * rows * cols * 3, transcendentals=0),
        )(*[pltpu.with_memory_space_constraint(v, pltpu.HBM) for v in operands])
        results = [left_new, right_new, direction]
        return pl.pallas_call(
            store_kernel,
            name="store",
            out_shape=[jax.ShapeDtypeStruct(v.shape, v.dtype) for v in results],
            in_specs=[vmem] * 3,
            out_specs=[hbm] * 3,
            scratch_shapes=[pltpu.SemaphoreType.DMA((3,))],
            compiler_params=pltpu.CompilerParams(vmem_limit_bytes=1 * 2**20),
        )(*results)

    return jax.shard_map(local_step, mesh=mesh, in_specs=(col_spec, row_spec, row_spec, row_spec, row_spec), out_specs=(row_spec, row_spec, col_spec), check_vma=False)
```

```python
import functools
import math

import jax
import jax.numpy as jnp
from jax import lax
from jax.experimental import pallas as pl
from jax.experimental.pallas import tpu as pltpu
from jax.sharding import PartitionSpec as P

EMA_DECAY = 0.9
CORES = 2
MESH = pl.DeviceIdType.MESH

ORDER = [(int(a), int(b)) for a, b in zip("0310020311322312", "0003102313131222")]
def parcels(code):
    digits = [int(d) for d in code]
    return [((a, b), h) for a, b, h in zip(digits[0::3], digits[1::3], digits[2::3])]


UP = parcels("030031330131020331130230231320120220")
UP_ON = {0: parcels("030"), 2: parcels("330"), 6: parcels("130"), 7: parcels("230")}
DOWN = parcels("011010111310021110311211210321121221")
DOWN_ON = {0: parcels("011"), 6: parcels("311111"), 7: parcels("211")}
ROUNDS = len(UP)
FIRST_UP = parcels("300301200")
FIRST_DOWN = parcels("101100201")
GRAD_ROUND_STEP = [2, 2, 8, 10, 12, 14, 17, 20, 22, 26, 28, 30]
LAST_FORWARD = 7
SIDE_UP, SIDE_DOWN = 9, 10
ASIDE = 48
ROOT_START_STEP = 28
ROOT_ACROSS_STEP = 30
RELAY_STEP = 31
LATE = (2, 12, 14, 22, 26, 28, 30)
MIDDLE = (3, 13, 15, 23, 27, 29, 31)


def packed(values):
    return [sum(v << (2 * i) for i, v in enumerate(values[j:j + 8])) for j in (0, 8)]


FIRST_CODE = packed([o[0] for o in ORDER])
SECOND_CODE = packed([o[1] for o in ORDER])


def lookup(code, e):
    word = code[0] + (e // 8) * (code[1] - code[0])
    return lax.shift_right_logical(word, 2 * (e % 8)) & 3


ROOT_ORDER = [(0, 0), (3, 0), (1, 0), (0, 1), (2, 0), (3, 1), (1, 1), (2, 1)]
ROOT_Y = sum(o[0] << (2 * i) for i, o in enumerate(ROOT_ORDER))
ROOT_X = sum(o[1] << (2 * i) for i, o in enumerate(ROOT_ORDER))


def kernel(n, side, g_ref, l_ref, r_ref, lr_ref, rr_ref, lo_ref, ro_ref, do_ref, gfull,
           rr, gt, acc, gbuf, rhs, xx, lroot, relay, lent,
           g_recv, g_send, load_sem, init_sem, l_recv, last_recv, relay_recv, x_recv, d_recv, l_send, x_send, d_send):
    _, half_rows, cols = g_ref.shape
    rows = 2 * half_rows
    lrows = l_ref.shape[0]
    tile = min(1024, half_rows)
    aside_rows = half_rows * ASIDE // 128

    me = lax.axis_index("tensor")
    c = me % CORES
    chip = me // CORES
    x, y = chip % side, chip // side
    f = x + c * (y - x)
    s = y + c * (x - y)
    fstep = CORES + c * CORES * (side - 1)
    sstep = CORES * side - c * CORES * (side - 1)
    twin = me + 1 - 2 * c

    def index(df, ds):
        return ((f + df) % side) * fstep + ((s + ds) % side) * sstep + c

    def twin_index(df, ds):
        return ((s + df) % side) * sstep + ((f + ds) % side) * fstep + 1 - c

    peers = {"f+": index(1, 0), "f-": index(3, 0), "s+": index(0, 1), "s-": index(0, 3), "twin": twin}
    slot_of = {name: i for i, name in enumerate(peers)}

    class Gather:
        def __init__(self, own, full, recv, send):
            self.own, self.full, self.recv, self.send_sem = own, full, recv, send
            self.count = {name: 0 for name in peers}

        def copy(self, name, b, half, own=False, part=None):
            src = self.own.at[half] if own else self.full.at[2 * b + half]
            dst = self.full.at[2 * b + half]
            sem = slot_of[name]
            if part is not None:
                src, dst, sem = src.at[pl.ds(*part)], dst.at[pl.ds(*part)], len(peers) + sem
            return pltpu.make_async_remote_copy(
                src_ref=src, dst_ref=dst, send_sem=self.send_sem.at[sem],
                recv_sem=self.recv.at[2 * b + half], device_id={"tensor": peers[name]}, device_id_type=MESH)

        def send(self, name, b, half, own=False):
            self.count[name] += 1
            self.copy(name, b, half, own).start()

        def wait(self, b, half):
            self.copy("twin", b, half).wait_recv()

        def start(self):
            for half in (0, 1):
                for name in ("f+", "s+"):
                    self.send(name, me, half, own=True)
                for name in ("f-", "s-"):
                    self.send(name, me, 1 - half, own=True)
            for half in (0, 1):
                self.send("twin", me, half, own=True)

        def round(self, r):
            if r < len(FIRST_UP):
                (ou, hu), (od, hd) = FIRST_UP[r], FIRST_DOWN[r]
                bu, bd = index(*ou), index(*od)
                self.wait(bu, hu)
                if r == 0:
                    self.send("f+", bu, hu)
                self.wait(bd, hd)
                if r == 0:
                    self.send("f-", bd, hd)
                self.send("s+", bu, hu)
                self.send("s-", bd, hd)
                self.send("s+", bd, hd)
                self.send("s-", bu, hu)
                self.send("twin", bu, hu)
                self.send("twin", bd, hd)
            (ou, hu), (od, hd) = UP[r], DOWN[r]
            fu, fd = UP_ON.get(r, ()), DOWN_ON.get(r, ())
            bu, bd = index(*ou), index(*od)
            self.wait(bu, hu)
            for offset, half in fu:
                if r == LAST_FORWARD:
                    self.forward_last("s+", index(*offset), half)
                else:
                    self.send("s+", index(*offset), half)
            if r == SIDE_UP:
                self.aside("f+", bu, hu)
            self.send("twin", bu, hu)
            self.wait(bd, hd)
            for offset, half in fd:
                if r == LAST_FORWARD:
                    self.forward_last("s-", index(*offset), half)
                else:
                    self.send("s-", index(*offset), half)
            if r == SIDE_DOWN:
                self.aside("f-", bd, hd)
            self.send("twin", bd, hd)

        def forward_last(self, name, b, half):
            pl.when(c == 0)(lambda: self.copy(name, b, half, part=(0, half_rows - aside_rows)).start())
            pl.when(c == 1)(lambda: self.copy(name, b, half, part=(0, half_rows)).start())

        def aside(self, name, b, half):
            pl.when(c == 0)(lambda: self.copy(name, b, half, part=(half_rows - aside_rows, aside_rows)).start())

        def drain(self):
            for name, count in self.count.items():
                whole = self.full.at[pl.ds(0, count)]
                pltpu.make_async_copy(whole, whole, self.send_sem.at[slot_of[name]]).wait()

            @pl.when(c == 0)
            def _():
                for name in ("s+", "s-"):
                    self.copy(name, me, 0, part=(0, half_rows - aside_rows)).wait_send()
                for name in ("f+", "f-"):
                    self.copy(name, me, 0, part=(half_rows - aside_rows, aside_rows)).wait_send()

            @pl.when(c == 1)
            def _():
                for name in ("s+", "s-"):
                    self.copy(name, me, 0, part=(0, half_rows)).wait_send()

    grad = Gather(g_ref, gfull, g_recv, g_send)

    def block_of(k):
        e, other = k // 2, k % 2
        df, ds = lookup(FIRST_CODE, e), lookup(SECOND_CODE, e)
        mine = index(df, ds)
        return mine + other * (twin_index(df, ds) - mine)

    def load(gather, buf, k, sem):
        b = block_of(k)
        return pltpu.make_async_copy(gather.full.at[pl.ds(2 * b, 2)], buf.at[k % 2], sem.at[k % 2])

    def start_load(gather, buf, k, sem):
        @pl.when(k % 2 == 1)
        def _():
            b = block_of(k)
            with jax.named_scope("twinwait"):
                gather.wait(b, 0)
                gather.wait(b, 1)
        load(gather, buf, k, sem).start()

    def one_of(k, values):
        found = k == values[0]
        for v in values[1:]:
            found = found | (k == v)
        return found

    def steps(gather, buf, sem, round_step, extra, work):
        def step(k, carry):
            for at, fn in extra:
                pl.when(k == at)(fn)
            for r in range(ROUNDS):
                @pl.when(k == round_step[r])
                def _():
                    with jax.named_scope(f"ground{r}"):
                        gather.round(r)

            @pl.when(one_of(k, LATE))
            def _():
                start_load(gather, buf, k, sem)

            @pl.when((k + 1 < n) & jnp.logical_not(one_of(k + 1, LATE + MIDDLE)))
            def _():
                start_load(gather, buf, k + 1, sem)

            def middle():
                @pl.when(one_of(k + 1, MIDDLE))
                def _():
                    start_load(gather, buf, k + 1, sem)
            with jax.named_scope("loadwait"):
                load(gather, buf, k, sem).wait()
            with jax.named_scope("work"):
                work(k, k % 2, block_of(k), middle)
            return carry
        lax.fori_loop(0, n, step, 0)

    first = [
        pltpu.make_async_copy(rr_ref, rr, init_sem.at[0]),
        pltpu.make_async_copy(r_ref, ro_ref, init_sem.at[1]),
        pltpu.make_async_copy(l_ref, lo_ref, init_sem.at[2]),
        pltpu.make_async_copy(lr_ref, lroot.at[pl.ds(2 * ((y * (side // 2) + x // 2) * CORES + c), 2)], init_sem.at[3]),
    ]
    own_load = pltpu.make_async_copy(g_ref, gbuf.at[0], load_sem.at[0])
    own_load.start()

    barrier = pltpu.get_barrier_semaphore()
    for peer in peers.values():
        pl.semaphore_signal(barrier, inc=1, device_id={"tensor": peer}, device_id_type=MESH)
    with jax.named_scope("barrier"):
        pl.semaphore_wait(barrier, len(peers))
    grad.start()
    for copy in first:
        copy.start()

    acc[...] = jnp.zeros_like(acc)
    own_load.wait()
    for h in (0, 1):
        gt[:, h * half_rows:(h + 1) * half_rows] = gbuf[0, h].T
    for copy in first:
        copy.wait()
    own_load.start()

    per_half = half_rows // tile

    def grad_work(k, slot, b, middle):
        at = pl.multiple_of(b * cols, cols)
        rhs[:cols] = rr[:, pl.ds(at, cols)]
        rhs[cols:] = gbuf[slot, me // (n // 2), pl.ds(pl.multiple_of((me % (n // 2)) * lrows, lrows), lrows), :]

        def rows_step(t, carry):
            left = gbuf[slot, t // per_half, pl.ds(pl.multiple_of((t % per_half) * tile, tile), tile), :]
            out = pl.ds(pl.multiple_of(t * tile, tile), tile)
            acc[out, :] += lax.dot_general(left, rhs[...], (((1,), (1,)), ((), ())), preferred_element_type=jnp.float32)
            return carry
        lax.fori_loop(0, 2 * per_half, rows_step, 0)
        middle()
        prod = jnp.dot(gt[:, :half_rows], gbuf[slot, 0], preferred_element_type=jnp.float32)
        prod += jnp.dot(gt[:, half_rows:], gbuf[slot, 1], preferred_element_type=jnp.float32)
        ro_ref[:, pl.ds(at, cols)] = EMA_DECAY * ro_ref[:, pl.ds(at, cols)] + (1.0 - EMA_DECAY) * prod


    dx = 1 - 2 * c
    helper = (y * side + (x + dx + side) % side) * CORES + c
    client = (y * side + (x - dx + side) % side) * CORES + c
    up = (((y + 1) % side) * side + x) * CORES + c
    down = (((y + side - 1) % side) * side + x) * CORES + c
    half_count, root_half, _ = lroot.shape
    pieces = ((0, root_half - root_half // 4), (root_half - root_half // 4, root_half // 4))

    def root_block(dy, q, p=0):
        oy, ox = (y + dy) % side, (x + 2 * q) % side
        core = c + p * (1 - 2 * c)
        return (oy * (side // 2) + ox // 2) * CORES + core, (oy * side + ox) * CORES + core

    def root_copy(peer, sem, place, half, src=None, dst=None, recv=None, part=None):
        here = lroot.at[2 * place + half]
        if part is not None:
            here = here.at[pl.ds(*pieces[part])]
        return pltpu.make_async_remote_copy(
            src_ref=here if src is None else src, dst_ref=here if dst is None else dst, send_sem=l_send.at[sem],
            recv_sem=l_recv.at[2 * place + half] if recv is None else recv, device_id={"tensor": peer}, device_id_type=MESH)

    sent = [0, 0, 0, 0]

    def root_send(peer, sem, place, half, part=None, **kw):
        sent[sem] += root_half if part is None else pieces[part][1]
        root_copy(peer, sem, place, half, part=part, **kw).start()

    def root_wait(place, half, **kw):
        root_copy(twin, 3, place, half, **kw).wait_recv()

    own_place, _ = root_block(0, 0)
    far_place, _ = root_block(0, 1)
    passing = (y * (side // 2) + ((x - dx + side) % side) // 2) * CORES + c

    def root_start_across():
        for half in (0, 1):
            root_send(helper, 0, own_place, half, src=lr_ref.at[half], dst=relay.at[half], recv=relay_recv.at[half])

    def root_start():
        for half in (0, 1):
            root_send(up, 1, own_place, half, src=lr_ref.at[half])
            root_send(down, 2, own_place, 1 - half, src=lr_ref.at[1 - half])
        for half in (0, 1):
            root_send(twin, 3, own_place, half, src=lr_ref.at[half])

    def root_relay(half):
        root_copy(helper, 0, own_place, half, src=lr_ref.at[half], dst=relay.at[half], recv=relay_recv.at[half]).wait_recv()
        root_send(helper, 0, passing, half, src=relay.at[half])
        root_send(twin, 3, passing, half, src=relay.at[half], dst=relay.at[2 + half], recv=relay_recv.at[2 + half])

    def passed_rows(p):
        if p:
            for half in (0, 1):
                root_copy(twin, 3, passing, half, src=relay.at[half], dst=relay.at[2 + half], recv=relay_recv.at[2 + half]).wait_recv()
        source = (y * side + (x - (1 - 2 * p) * dx + side) % side) * CORES + c + p * (1 - 2 * c)
        left = relay[2 * p:2 * p + 2].reshape(lrows, rows)
        do_ref[rows_of(source), :] = jnp.dot(left, xx[0], preferred_element_type=jnp.float32)

    def root_far():
        for half in (0, 1):
            root_wait(far_place, half)
            root_send(up, 1, far_place, half)
            root_send(twin, 3, far_place, half)
        for half in (1, 0):
            root_send(down, 2, far_place, half)

    def root_round(r):
        q, stage = r // 3, r % 3
        if stage == 2:
            behind = root_block(2, q)[0]
            for half in (0, 1):
                root_wait(behind, half)
                root_send(twin, 3, behind, half)
            return
        below, above = root_block(side - 1, q)[0], root_block(1, q)[0]
        root_wait(below, stage)
        if stage == 0:
            for part in (None,) if q == 0 else (0, 1):
                root_send(up, 1, below, 0, part=part, recv=last_recv.at[0] if part else None)
        root_send(twin, 3, below, stage)
        root_wait(above, 1 - stage)
        if stage == 0:
            for part in (None,) if q == 0 else (0, 1):
                root_send(down, 2, above, 1, part=part, recv=last_recv.at[1] if part else None)
        root_send(twin, 3, above, 1 - stage)

    last_place, last_device = root_block(2, 1)
    twin_place, twin_device = root_block(2, 1, 1)

    def root_last(part):
        for half in (0, 1):
            root_wait(last_place, half, part=part, recv=last_recv.at[half] if part else None)
            root_send(twin, 3, last_place, half, part=part, recv=last_recv.at[2 + half] if part else None)

    def root_last_twin(part):
        for half in (0, 1):
            root_wait(twin_place, half, part=part, recv=last_recv.at[2 + half] if part else None)

    steps(grad, gbuf, load_sem, GRAD_ROUND_STEP, [(ROOT_START_STEP, root_start), (ROOT_ACROSS_STEP, root_start_across), (RELAY_STEP, lambda: root_relay(0))], grad_work)

    side_cols = cols // 2

    def x_copy(h):
        at = pl.ds(h * side_cols, side_cols)
        return pltpu.make_async_remote_copy(
            src_ref=xx.at[0, :, at], dst_ref=xx.at[1, :, at], send_sem=x_send.at[h], recv_sem=x_recv.at[h],
            device_id={"tensor": helper}, device_id_type=MESH)

    with jax.named_scope("xfin"):
        xx[0] = acc[:, :cols].astype(jnp.bfloat16)
    with jax.named_scope("relay"):
        root_relay(1)
    x_copy(0).start()
    x_copy(1).start()
    with jax.named_scope("rround0"):
        root_round(0)

    def left_step(t, carry):
        at = pl.ds(pl.multiple_of(t * lrows, lrows), lrows)
        lo_ref[:, at] = EMA_DECAY * lo_ref[:, at] + (1.0 - EMA_DECAY) * acc[at, cols:].T
        return carry
    with jax.named_scope("leftfin"):
        lax.fori_loop(0, rows // lrows, left_step, 0)

    def at_step(i):
        e, p = i // 2, i % 2
        dy = lax.shift_right_logical(ROOT_Y, 2 * e) & 3
        q = lax.shift_right_logical(ROOT_X, 2 * e) & 3
        return root_block(dy, q, p)

    def twin_wait(i, place):
        @pl.when(i % 2 == 1)
        def _():
            root_wait(place, 0)
            root_wait(place, 1)

    def product(place, which):
        left = lroot[pl.ds(2 * place, 2)].reshape(lrows, rows)
        return jnp.dot(left, xx[which], preferred_element_type=jnp.float32)

    def rows_of(device):
        return pl.ds(pl.multiple_of(device * lrows, lrows), lrows)

    def own_rows(i):
        place, device = at_step(i)
        do_ref[rows_of(device), :] = product(place, 0)

    def lent_copy(i, device):
        return pltpu.make_async_remote_copy(
            src_ref=lent.at[i], dst_ref=do_ref.at[rows_of(device)], send_sem=d_send.at[0], recv_sem=d_recv.at[i],
            device_id={"tensor": client}, device_id_type=MESH)

    def lent_rows(i):
        place, device = at_step(i)
        lent[i] = product(place, 1)
        lent_copy(i, device).start()

    def lent_side(i, h):
        place, _ = at_step(i)
        at = pl.ds(h * side_cols, side_cols)
        left = lroot[pl.ds(2 * place, 2)].reshape(lrows, rows)
        lent[i, :, at] = jnp.dot(left, xx[1, :, at], preferred_element_type=jnp.float32)

    def lent_side_copy(i, h):
        _, device = at_step(i)
        at = pl.ds(h * side_cols, side_cols)
        return pltpu.make_async_remote_copy(
            src_ref=lent.at[i, :, at], dst_ref=do_ref.at[rows_of(device), at], send_sem=d_send.at[0], recv_sem=d_recv.at[i],
            device_id={"tensor": client}, device_id_type=MESH)

    def loop(lo, hi, body):
        def step(i, carry):
            body(i)
            return carry
        lax.fori_loop(lo, hi, step, 0)

    def first_own(i):
        @pl.when(i == 2)
        def _():
            with jax.named_scope("far"):
                root_far()
            with jax.named_scope("rround1"):
                root_round(1)

        @pl.when(i == 8)
        def _():
            with jax.named_scope("rround2"):
                root_round(2)
        twin_wait(i, at_step(i)[0])
        own_rows(i)

    loop(0, 10, first_own)
    passed_rows(0)
    passed_rows(1)
    with jax.named_scope("x0wait"):
        x_copy(0).wait_recv()
    def lent_step(j):
        return j + (j + 7) // 8 + j // 5

    loop(0, 8, lambda j: lent_side(lent_step(j), 0))
    x_copy(0).wait_send()
    with jax.named_scope("x1sent"):
        x_copy(1).wait_send()
    loop(0, 8, lambda j: lent_side_copy(lent_step(j), 0).start())
    with jax.named_scope("rround3"):
        root_round(3)
    with jax.named_scope("x1wait"):
        x_copy(1).wait_recv()

    def second_side(j):
        i = lent_step(j)
        lent_side(i, 1)
        lent_side_copy(i, 1).start()
    loop(0, 8, second_side)
    with jax.named_scope("rround4"):
        root_round(4)

    def both(i):
        twin_wait(i, at_step(i)[0])
        lent_rows(i)
        own_rows(i)
    with jax.named_scope("both"):
        loop(10, 14, both)

    def lent_piece(i, place, device, part):
        first, count = pieces[part]
        left = jnp.concatenate([lroot[2 * place, pl.ds(first, count), :], lroot[2 * place + 1, pl.ds(first, count), :]], axis=0)
        prod = jnp.dot(left, xx[1], preferred_element_type=jnp.float32)
        for half in (0, 1):
            at = half * root_half + first
            lent[i, pl.ds(at, count), :] = prod[half * count:(half + 1) * count]
            pltpu.make_async_remote_copy(
                src_ref=lent.at[i, pl.ds(at, count)], dst_ref=do_ref.at[pl.ds(pl.multiple_of(device * lrows, lrows) + at, count)],
                send_sem=d_send.at[0], recv_sem=d_recv.at[i], device_id={"tensor": client}, device_id_type=MESH).start()

    for part in (0, 1):
        with jax.named_scope(f"last{part}"):
            root_last(part)
        lent_piece(14, last_place, last_device, part)
        with jax.named_scope(f"lasttwin{part}"):
            root_last_twin(part)
        lent_piece(15, twin_place, twin_device, part)
    loop(14, 16, own_rows)

    with jax.named_scope("drain"):
        grad.drain()
    for sem, count in enumerate(sent):
        whole = lroot.at[pl.ds(0, count // root_half)]
        pltpu.make_async_copy(whole, whole, l_send.at[sem]).wait()
    given = lent.at[pl.ds(0, half_count // 2 - 2)]
    pltpu.make_async_copy(given, given, d_send.at[0]).wait()
    loop(0, 8, lambda j: lent_copy(lent_step(j), 0).wait_recv())
    with jax.named_scope("dwait"):
        loop(10, half_count // 2, lambda i: lent_copy(i, 0).wait_recv())


def store_kernel(*refs):
    count = (len(refs) - 1) // 2
    sems = refs[-1]
    pieces = 8
    for i in range(count):
        src, dst = refs[i], refs[count + i]
        step = src.shape[0] // pieces
        for j in range(pieces):
            part = pl.ds(j * step, step)
            pltpu.make_async_copy(src.at[part], dst.at[part], sems.at[i]).start()
    for i in range(count):
        pltpu.make_async_copy(refs[i], refs[count + i], sems.at[i]).wait()


def solution(mesh):
    row_spec = P(("layer", "tensor"), None)
    col_spec = P("layer", "tensor")
    n = mesh.shape["tensor"]
    side = math.isqrt(n // CORES)

    def local_step(g, l, r, lr, rr):
        rows, cols = g.shape
        lrows = l.shape[0]
        kept = n // 2
        hbm = pl.BlockSpec(memory_space=pltpu.HBM)
        vmem = pl.BlockSpec(memory_space=pltpu.VMEM)
        operands = [g.reshape(2, rows // 2, cols), l, r, lr.reshape(2, lrows // 2, rows), rr]
        left_new, right_new, direction, _ = pl.pallas_call(
            functools.partial(kernel, n, side),
            name="shampoo",
            out_shape=[
                pltpu.VMEM(l.shape, jnp.float32),
                pltpu.VMEM(r.shape, jnp.float32),
                pltpu.VMEM(g.shape, jnp.float32),
                pltpu.HBM((2 * n, rows // 2, cols), jnp.bfloat16),
            ],
            in_specs=[hbm] * 5,
            out_specs=[vmem, vmem, vmem, hbm],
            scratch_shapes=[
                pltpu.VMEM(rr.shape, jnp.bfloat16),
                pltpu.VMEM((cols, rows), jnp.bfloat16),
                pltpu.VMEM((rows, cols + lrows), jnp.float32),
                pltpu.VMEM((2, 2, rows // 2, cols), jnp.bfloat16),
                pltpu.VMEM((cols + lrows, cols), jnp.bfloat16),
                pltpu.VMEM((2, rows, cols), jnp.bfloat16),
                pltpu.VMEM((2 * kept, lrows // 2, rows), jnp.bfloat16),
                pltpu.VMEM((4, lrows // 2, rows), jnp.bfloat16),
                pltpu.VMEM((kept, lrows, cols), jnp.float32),
                pltpu.SemaphoreType.DMA((2 * n,)),
                pltpu.SemaphoreType.DMA((10,)),
                pltpu.SemaphoreType.DMA((2,)),
                pltpu.SemaphoreType.DMA((4,)),
                pltpu.SemaphoreType.DMA((2 * kept,)),
                pltpu.SemaphoreType.DMA((4,)),
                pltpu.SemaphoreType.DMA((4,)),
                pltpu.SemaphoreType.DMA((2,)),
                pltpu.SemaphoreType.DMA((kept,)),
                pltpu.SemaphoreType.DMA((4,)),
                pltpu.SemaphoreType.DMA((2,)),
                pltpu.SemaphoreType.DMA((1,)),
            ],
            compiler_params=pltpu.CompilerParams(collective_id=0, has_side_effects=True, vmem_limit_bytes=48 * 2**20),
            cost_estimate=pl.CostEstimate(flops=2 * rows * cols * (2 * n * cols + 2 * rows), bytes_accessed=2 * n * rows * cols * 3, transcendentals=0),
        )(*[pltpu.with_memory_space_constraint(v, pltpu.HBM) for v in operands])
        results = [left_new, right_new, direction]
        return pl.pallas_call(
            store_kernel,
            name="store",
            out_shape=[jax.ShapeDtypeStruct(v.shape, v.dtype) for v in results],
            in_specs=[vmem] * 3,
            out_specs=[hbm] * 3,
            scratch_shapes=[pltpu.SemaphoreType.DMA((3,))],
            compiler_params=pltpu.CompilerParams(vmem_limit_bytes=1 * 2**20),
        )(*results)

    return jax.shard_map(local_step, mesh=mesh, in_specs=(col_spec, row_spec, row_spec, row_spec, row_spec), out_specs=(row_spec, row_spec, col_spec), check_vma=False)
```

```python
import functools
import math

import jax
import jax.numpy as jnp
from jax import lax
from jax.experimental import pallas as pl
from jax.experimental.pallas import tpu as pltpu
from jax.sharding import PartitionSpec as P

EMA_DECAY = 0.9
CORES = 2
MESH = pl.DeviceIdType.MESH

ORDER = [(int(a), int(b)) for a, b in zip("0310020311322312", "0003102313131222")]
def parcels(code):
    digits = [int(d) for d in code]
    return [((a, b), h) for a, b, h in zip(digits[0::3], digits[1::3], digits[2::3])]


UP = parcels("030031330131020331130230231320120220")
UP_ON = {0: parcels("030"), 2: parcels("330"), 6: parcels("130"), 7: parcels("230")}
DOWN = parcels("011010111310021110311211210321121221")
DOWN_ON = {0: parcels("011"), 6: parcels("311111"), 7: parcels("211")}
ROUNDS = len(UP)
FIRST_UP = parcels("300301200")
FIRST_DOWN = parcels("101100201")
GRAD_ROUND_STEP = [2, 2, 8, 10, 12, 14, 17, 20, 22, 26, 28, 30]
LAST_FORWARD = 7
SIDE_UP, SIDE_DOWN = 9, 10
ASIDE = 40
ROOT_START_STEP = 28
ROOT_ACROSS_STEP = 30
RELAY_STEP = 31
LATE = (2, 12, 14, 22, 26, 28, 30)
MIDDLE = (3, 13, 15, 23, 27, 29, 31)


def packed(values):
    return [sum(v << (2 * i) for i, v in enumerate(values[j:j + 8])) for j in (0, 8)]


FIRST_CODE = packed([o[0] for o in ORDER])
SECOND_CODE = packed([o[1] for o in ORDER])


def lookup(code, e):
    word = code[0] + (e // 8) * (code[1] - code[0])
    return lax.shift_right_logical(word, 2 * (e % 8)) & 3


ROOT_ORDER = [(0, 0), (3, 0), (1, 0), (0, 1), (2, 0), (3, 1), (1, 1), (2, 1)]
ROOT_Y = sum(o[0] << (2 * i) for i, o in enumerate(ROOT_ORDER))
ROOT_X = sum(o[1] << (2 * i) for i, o in enumerate(ROOT_ORDER))


def kernel(n, side, g_ref, l_ref, r_ref, lr_ref, rr_ref, lo_ref, ro_ref, do_ref, gfull,
           rr, gt, acc, gbuf, rhs, xx, lroot, relay, lent,
           g_recv, g_send, load_sem, init_sem, l_recv, last_recv, relay_recv, x_recv, d_recv, l_send, x_send, d_send):
    _, half_rows, cols = g_ref.shape
    rows = 2 * half_rows
    lrows = l_ref.shape[0]
    tile = min(1024, half_rows)
    aside_rows = half_rows * ASIDE // 128

    me = lax.axis_index("tensor")
    c = me % CORES
    chip = me // CORES
    x, y = chip % side, chip // side
    f = x + c * (y - x)
    s = y + c * (x - y)
    fstep = CORES + c * CORES * (side - 1)
    sstep = CORES * side - c * CORES * (side - 1)
    twin = me + 1 - 2 * c

    def index(df, ds):
        return ((f + df) % side) * fstep + ((s + ds) % side) * sstep + c

    def twin_index(df, ds):
        return ((s + df) % side) * sstep + ((f + ds) % side) * fstep + 1 - c

    peers = {"f+": index(1, 0), "f-": index(3, 0), "s+": index(0, 1), "s-": index(0, 3), "twin": twin}

    class Gather:
        def __init__(self, own, full, recv, send):
            self.own, self.full, self.recv, self.send_sem = own, full, recv, send
            self.sent = 0

        def copy(self, name, b, half, own=False, part=None):
            src = self.own.at[half] if own else self.full.at[2 * b + half]
            dst = self.full.at[2 * b + half]
            if part is not None:
                src, dst = src.at[pl.ds(*part)], dst.at[pl.ds(*part)]
            recv = self.recv.at[n + b // CORES if name == "twin" else (b // CORES) * CORES + half]
            return pltpu.make_async_remote_copy(
                src_ref=src, dst_ref=dst, send_sem=self.send_sem.at[0], recv_sem=recv, device_id={"tensor": peers[name]}, device_id_type=MESH)

        def send(self, name, b, half, own=False):
            self.sent += 1
            self.copy(name, b, half, own).start()

        def wait(self, b, half):
            self.copy("f+", b, half).wait_recv()

        def wait_twin(self, b):
            whole = self.full.at[pl.ds(2 * b, 2)]
            pltpu.make_async_copy(whole, whole, self.recv.at[n + b // CORES]).wait()

        def start(self):
            for half in (0, 1):
                for name in ("f+", "s+"):
                    self.send(name, me, half, own=True)
                for name in ("f-", "s-"):
                    self.send(name, me, 1 - half, own=True)
            for half in (0, 1):
                self.send("twin", me, half, own=True)

        def round(self, r):
            if r < len(FIRST_UP):
                (ou, hu), (od, hd) = FIRST_UP[r], FIRST_DOWN[r]
                bu, bd = index(*ou), index(*od)
                self.wait(bu, hu)
                if r == 0:
                    self.send("f+", bu, hu)
                self.wait(bd, hd)
                if r == 0:
                    self.send("f-", bd, hd)
                self.send("s+", bu, hu)
                self.send("s-", bd, hd)
                self.send("s+", bd, hd)
                self.send("s-", bu, hu)
                self.send("twin", bu, hu)
                self.send("twin", bd, hd)
            (ou, hu), (od, hd) = UP[r], DOWN[r]
            fu, fd = UP_ON.get(r, ()), DOWN_ON.get(r, ())
            bu, bd = index(*ou), index(*od)
            self.wait(bu, hu)
            for offset, half in fu:
                if r == LAST_FORWARD:
                    self.forward_last("s+", index(*offset), half)
                else:
                    self.send("s+", index(*offset), half)
            if r == SIDE_UP:
                self.aside("f+", bu, hu)
            self.send("twin", bu, hu)
            self.wait(bd, hd)
            for offset, half in fd:
                if r == LAST_FORWARD:
                    self.forward_last("s-", index(*offset), half)
                else:
                    self.send("s-", index(*offset), half)
            if r == SIDE_DOWN:
                self.aside("f-", bd, hd)
            self.send("twin", bd, hd)

        def forward_last(self, name, b, half):
            self.sent += 1
            pl.when(c == 0)(lambda: self.copy(name, b, half, part=(0, half_rows - aside_rows)).start())
            pl.when(c == 1)(lambda: self.copy(name, b, half).start())

        def aside(self, name, b, half):
            pl.when(c == 0)(lambda: self.copy(name, b, half, part=(half_rows - aside_rows, aside_rows)).start())

        def drain(self):
            whole = self.full.at[pl.ds(0, self.sent)]
            pltpu.make_async_copy(whole, whole, self.send_sem.at[0]).wait()

    grad = Gather(g_ref, gfull, g_recv, g_send)

    def block_of(k):
        e, other = k // 2, k % 2
        df, ds = lookup(FIRST_CODE, e), lookup(SECOND_CODE, e)
        mine = index(df, ds)
        return mine + other * (twin_index(df, ds) - mine)

    def load(gather, buf, k, sem):
        b = block_of(k)
        return pltpu.make_async_copy(gather.full.at[pl.ds(2 * b, 2)], buf.at[k % 2], sem.at[k % 2])

    def start_load(gather, buf, k, sem):
        @pl.when(k % 2 == 1)
        def _():
            with jax.named_scope("twinwait"):
                gather.wait_twin(block_of(k))
        load(gather, buf, k, sem).start()

    def one_of(k, values):
        found = k == values[0]
        for v in values[1:]:
            found = found | (k == v)
        return found

    def steps(gather, buf, sem, round_step, extra, work):
        def step(k, carry):
            for at, fn in extra:
                pl.when(k == at)(fn)
            for r in range(ROUNDS):
                @pl.when(k == round_step[r])
                def _():
                    with jax.named_scope(f"ground{r}"):
                        gather.round(r)

            @pl.when(one_of(k, LATE))
            def _():
                start_load(gather, buf, k, sem)

            @pl.when((k + 1 < n) & jnp.logical_not(one_of(k + 1, LATE + MIDDLE)))
            def _():
                start_load(gather, buf, k + 1, sem)

            def middle():
                @pl.when(one_of(k + 1, MIDDLE))
                def _():
                    start_load(gather, buf, k + 1, sem)
            with jax.named_scope("loadwait"):
                load(gather, buf, k, sem).wait()
            with jax.named_scope("work"):
                work(k, k % 2, block_of(k), middle)
            return carry
        lax.fori_loop(0, n, step, 0)

    first = [
        pltpu.make_async_copy(rr_ref, rr, init_sem.at[0]),
        pltpu.make_async_copy(r_ref, ro_ref, init_sem.at[1]),
        pltpu.make_async_copy(l_ref, lo_ref, init_sem.at[2]),
        pltpu.make_async_copy(lr_ref, lroot.at[pl.ds(2 * ((y * (side // 2) + x // 2) * CORES + c), 2)], init_sem.at[3]),
    ]
    own_load = pltpu.make_async_copy(g_ref, gbuf.at[0], load_sem.at[0])
    own_load.start()

    barrier = pltpu.get_barrier_semaphore()
    for peer in peers.values():
        pl.semaphore_signal(barrier, inc=1, device_id={"tensor": peer}, device_id_type=MESH)
    with jax.named_scope("barrier"):
        pl.semaphore_wait(barrier, len(peers))
    grad.start()
    for copy in first:
        copy.start()

    acc[...] = jnp.zeros_like(acc)
    own_load.wait()
    for h in (0, 1):
        gt[:, h * half_rows:(h + 1) * half_rows] = gbuf[0, h].T
    for copy in first:
        copy.wait()
    own_load.start()

    per_half = half_rows // tile

    def grad_work(k, slot, b, middle):
        at = pl.multiple_of(b * cols, cols)
        rhs[:cols] = rr[:, pl.ds(at, cols)]
        rhs[cols:] = gbuf[slot, me // (n // 2), pl.ds(pl.multiple_of((me % (n // 2)) * lrows, lrows), lrows), :]

        def rows_step(t, carry):
            left = gbuf[slot, t // per_half, pl.ds(pl.multiple_of((t % per_half) * tile, tile), tile), :]
            out = pl.ds(pl.multiple_of(t * tile, tile), tile)
            acc[out, :] += lax.dot_general(left, rhs[...], (((1,), (1,)), ((), ())), preferred_element_type=jnp.float32)
            return carry
        lax.fori_loop(0, 2 * per_half, rows_step, 0)
        middle()
        prod = jnp.dot(gt[:, :half_rows], gbuf[slot, 0], preferred_element_type=jnp.float32)
        prod += jnp.dot(gt[:, half_rows:], gbuf[slot, 1], preferred_element_type=jnp.float32)
        ro_ref[:, pl.ds(at, cols)] = EMA_DECAY * ro_ref[:, pl.ds(at, cols)] + (1.0 - EMA_DECAY) * prod


    dx = 1 - 2 * c
    helper = (y * side + (x + dx + side) % side) * CORES + c
    client = (y * side + (x - dx + side) % side) * CORES + c
    up = (((y + 1) % side) * side + x) * CORES + c
    down = (((y + side - 1) % side) * side + x) * CORES + c
    half_count, root_half, _ = lroot.shape
    pieces = ((0, root_half - root_half // 4), (root_half - root_half // 4, root_half // 4))

    def root_block(dy, q, p=0):
        oy, ox = (y + dy) % side, (x + 2 * q) % side
        core = c + p * (1 - 2 * c)
        return (oy * (side // 2) + ox // 2) * CORES + core, (oy * side + ox) * CORES + core

    def root_copy(peer, place, half, src=None, dst=None, recv=None, part=None, across=0):
        here = lroot.at[2 * place + half]
        if part is not None:
            here = here.at[pl.ds(*pieces[part])]
        if recv is None:
            recv = l_recv.at[half_count // 2 + place // CORES if peer is twin else (place // CORES) * CORES + half]
        return pltpu.make_async_remote_copy(
            src_ref=here if src is None else src, dst_ref=here if dst is None else dst, send_sem=l_send.at[across],
            recv_sem=recv, device_id={"tensor": peer}, device_id_type=MESH)

    sent = [0, 0]

    def root_send(peer, place, half, part=None, across=0, **kw):
        sent[across] += root_half if part is None else pieces[part][1]
        root_copy(peer, place, half, part=part, across=across, **kw).start()

    def root_wait(place, half, **kw):
        root_copy(up, place, half, **kw).wait_recv()

    def pair_wait(pair, sem):
        pltpu.make_async_copy(pair, pair, sem).wait()

    own_place, _ = root_block(0, 0)
    far_place, _ = root_block(0, 1)
    passing = (y * (side // 2) + ((x - dx + side) % side) // 2) * CORES + c

    def root_start_across():
        for half in (0, 1):
            root_send(helper, own_place, half, across=1, src=lr_ref.at[half], dst=relay.at[half], recv=relay_recv.at[half])

    def root_start():
        for half in (0, 1):
            root_send(up, own_place, half, src=lr_ref.at[half])
            root_send(down, own_place, 1 - half, src=lr_ref.at[1 - half])
        for half in (0, 1):
            root_send(twin, own_place, half, src=lr_ref.at[half])

    def root_relay(half):
        root_copy(helper, own_place, half, src=lr_ref.at[half], dst=relay.at[half], recv=relay_recv.at[half]).wait_recv()
        root_send(helper, passing, half, across=1, src=relay.at[half])
        root_send(twin, passing, half, across=1, src=relay.at[half], dst=relay.at[2 + half], recv=relay_recv.at[2])

    def passed_rows(p):
        if p:
            pair_wait(relay.at[pl.ds(2, 2)], relay_recv.at[2])
        source = (y * side + (x - (1 - 2 * p) * dx + side) % side) * CORES + c + p * (1 - 2 * c)
        left = relay[2 * p:2 * p + 2].reshape(lrows, rows)
        do_ref[rows_of(source), :] = jnp.dot(left, xx[0], preferred_element_type=jnp.float32)

    def root_far():
        for half in (0, 1):
            root_wait(far_place, half)
            root_send(up, far_place, half)
            root_send(twin, far_place, half)
        for half in (1, 0):
            root_send(down, far_place, half)

    def root_round(r):
        q, stage = r // 3, r % 3
        if stage == 2:
            behind = root_block(2, q)[0]
            for half in (0, 1):
                root_wait(behind, half)
                root_send(twin, behind, half)
            return
        below, above = root_block(side - 1, q)[0], root_block(1, q)[0]
        root_wait(below, stage)
        if stage == 0:
            for part in (None,) if q == 0 else (0, 1):
                root_send(up, below, 0, part=part, recv=last_recv.at[0] if part else None)
        root_send(twin, below, stage)
        root_wait(above, 1 - stage)
        if stage == 0:
            for part in (None,) if q == 0 else (0, 1):
                root_send(down, above, 1, part=part, recv=last_recv.at[1] if part else None)
        root_send(twin, above, 1 - stage)

    last_place, last_device = root_block(2, 1)
    twin_place, twin_device = root_block(2, 1, 1)

    def root_last(part):
        for half in (0, 1):
            root_wait(last_place, half, part=part, recv=last_recv.at[half] if part else None)
            root_send(twin, last_place, half, part=part, recv=last_recv.at[2] if part else None)

    def root_last_twin(part):
        pair = lroot.at[pl.ds(2 * twin_place, 2), pl.ds(*pieces[part])]
        pair_wait(pair, last_recv.at[2] if part else l_recv.at[half_count // 2 + twin_place // CORES])

    steps(grad, gbuf, load_sem, GRAD_ROUND_STEP, [(ROOT_START_STEP, root_start), (ROOT_ACROSS_STEP, root_start_across), (RELAY_STEP, lambda: root_relay(0))], grad_work)

    side_cols = cols // 2

    def x_copy(h):
        at = pl.ds(h * side_cols, side_cols)
        return pltpu.make_async_remote_copy(
            src_ref=xx.at[0, :, at], dst_ref=xx.at[1, :, at], send_sem=x_send.at[h], recv_sem=x_recv.at[h],
            device_id={"tensor": helper}, device_id_type=MESH)

    with jax.named_scope("xfin"):
        xx[0] = acc[:, :cols].astype(jnp.bfloat16)
    with jax.named_scope("relay"):
        root_relay(1)
    x_copy(0).start()
    x_copy(1).start()
    with jax.named_scope("rround0"):
        root_round(0)

    def left_step(t, carry):
        at = pl.ds(pl.multiple_of(t * lrows, lrows), lrows)
        lo_ref[:, at] = EMA_DECAY * lo_ref[:, at] + (1.0 - EMA_DECAY) * acc[at, cols:].T
        return carry
    with jax.named_scope("leftfin"):
        lax.fori_loop(0, rows // lrows, left_step, 0)

    def at_step(i):
        e, p = i // 2, i % 2
        dy = lax.shift_right_logical(ROOT_Y, 2 * e) & 3
        q = lax.shift_right_logical(ROOT_X, 2 * e) & 3
        return root_block(dy, q, p)

    def twin_wait(i, place):
        @pl.when(i % 2 == 1)
        def _():
            pair_wait(lroot.at[pl.ds(2 * place, 2)], l_recv.at[half_count // 2 + place // CORES])

    def product(place, which):
        left = lroot[pl.ds(2 * place, 2)].reshape(lrows, rows)
        return jnp.dot(left, xx[which], preferred_element_type=jnp.float32)

    def rows_of(device):
        return pl.ds(pl.multiple_of(device * lrows, lrows), lrows)

    def own_rows(i):
        place, device = at_step(i)
        do_ref[rows_of(device), :] = product(place, 0)

    def lent_copy(i, device):
        return pltpu.make_async_remote_copy(
            src_ref=lent.at[i], dst_ref=do_ref.at[rows_of(device)], send_sem=d_send.at[0], recv_sem=d_recv.at[0],
            device_id={"tensor": client}, device_id_type=MESH)

    def lent_rows(i):
        place, device = at_step(i)
        lent[i] = product(place, 1)
        lent_copy(i, device).start()

    def lent_side(i, h):
        place, _ = at_step(i)
        at = pl.ds(h * side_cols, side_cols)
        left = lroot[pl.ds(2 * place, 2)].reshape(lrows, rows)
        lent[i, :, at] = jnp.dot(left, xx[1, :, at], preferred_element_type=jnp.float32)

    def lent_side_copy(i, h):
        _, device = at_step(i)
        at = pl.ds(h * side_cols, side_cols)
        return pltpu.make_async_remote_copy(
            src_ref=lent.at[i, :, at], dst_ref=do_ref.at[rows_of(device), at], send_sem=d_send.at[0], recv_sem=d_recv.at[0],
            device_id={"tensor": client}, device_id_type=MESH)

    def loop(lo, hi, body):
        def step(i, carry):
            body(i)
            return carry
        lax.fori_loop(lo, hi, step, 0)

    def first_own(i):
        @pl.when(i == 2)
        def _():
            with jax.named_scope("far"):
                root_far()
            with jax.named_scope("rround1"):
                root_round(1)

        @pl.when(i == 8)
        def _():
            with jax.named_scope("rround2"):
                root_round(2)
        twin_wait(i, at_step(i)[0])
        own_rows(i)

    loop(0, 10, first_own)
    passed_rows(0)
    passed_rows(1)
    with jax.named_scope("x0wait"):
        x_copy(0).wait_recv()
    def lent_step(j):
        return j + (j + 7) // 8 + j // 5

    loop(0, 8, lambda j: lent_side(lent_step(j), 0))
    x_copy(0).wait_send()
    with jax.named_scope("x1sent"):
        x_copy(1).wait_send()
    loop(0, 8, lambda j: lent_side_copy(lent_step(j), 0).start())
    with jax.named_scope("rround3"):
        root_round(3)
    with jax.named_scope("x1wait"):
        x_copy(1).wait_recv()

    def second_side(j):
        i = lent_step(j)
        lent_side(i, 1)
        lent_side_copy(i, 1).start()
    loop(0, 8, second_side)
    with jax.named_scope("rround4"):
        root_round(4)

    def both(i):
        twin_wait(i, at_step(i)[0])
        lent_rows(i)
        own_rows(i)
    with jax.named_scope("both"):
        loop(10, 14, both)

    def lent_piece(i, place, device, part):
        first, count = pieces[part]
        left = jnp.concatenate([lroot[2 * place, pl.ds(first, count), :], lroot[2 * place + 1, pl.ds(first, count), :]], axis=0)
        prod = jnp.dot(left, xx[1], preferred_element_type=jnp.float32)
        for half in (0, 1):
            at = half * root_half + first
            lent[i, pl.ds(at, count), :] = prod[half * count:(half + 1) * count]
            pltpu.make_async_remote_copy(
                src_ref=lent.at[i, pl.ds(at, count)], dst_ref=do_ref.at[pl.ds(pl.multiple_of(device * lrows, lrows) + at, count)],
                send_sem=d_send.at[0], recv_sem=d_recv.at[0], device_id={"tensor": client}, device_id_type=MESH).start()

    for part in (0, 1):
        with jax.named_scope(f"last{part}"):
            root_last(part)
        lent_piece(14, last_place, last_device, part)
    for part in (0, 1):
        with jax.named_scope(f"lasttwin{part}"):
            root_last_twin(part)
        lent_piece(15, twin_place, twin_device, part)
    loop(14, 16, own_rows)

    with jax.named_scope("drain"):
        grad.drain()
    for across, count in enumerate(sent):
        whole = lroot.at[pl.ds(0, count // root_half)]
        pltpu.make_async_copy(whole, whole, l_send.at[across]).wait()
    given = lent.at[pl.ds(0, half_count // 2 - 2)]
    pltpu.make_async_copy(given, given, d_send.at[0]).wait()
    with jax.named_scope("dwait"):
        pltpu.make_async_copy(given, given, d_recv.at[0]).wait()


def store_kernel(*refs):
    count = (len(refs) - 1) // 2
    sems = refs[-1]
    pieces = 8
    for i in range(count):
        src, dst = refs[i], refs[count + i]
        step = src.shape[0] // pieces
        for j in range(pieces):
            part = pl.ds(j * step, step)
            pltpu.make_async_copy(src.at[part], dst.at[part], sems.at[i]).start()
    for i in range(count):
        pltpu.make_async_copy(refs[i], refs[count + i], sems.at[i]).wait()


def solution(mesh):
    row_spec = P(("layer", "tensor"), None)
    col_spec = P("layer", "tensor")
    n = mesh.shape["tensor"]
    side = math.isqrt(n // CORES)

    def local_step(g, l, r, lr, rr):
        rows, cols = g.shape
        lrows = l.shape[0]
        kept = n // 2
        hbm = pl.BlockSpec(memory_space=pltpu.HBM)
        vmem = pl.BlockSpec(memory_space=pltpu.VMEM)
        operands = [g.reshape(2, rows // 2, cols), l, r, lr.reshape(2, lrows // 2, rows), rr]
        left_new, right_new, direction, _ = pl.pallas_call(
            functools.partial(kernel, n, side),
            name="shampoo",
            out_shape=[
                pltpu.VMEM(l.shape, jnp.float32),
                pltpu.VMEM(r.shape, jnp.float32),
                pltpu.VMEM(g.shape, jnp.float32),
                pltpu.HBM((2 * n, rows // 2, cols), jnp.bfloat16),
            ],
            in_specs=[hbm] * 5,
            out_specs=[vmem, vmem, vmem, hbm],
            scratch_shapes=[
                pltpu.VMEM(rr.shape, jnp.bfloat16),
                pltpu.VMEM((cols, rows), jnp.bfloat16),
                pltpu.VMEM((rows, cols + lrows), jnp.float32),
                pltpu.VMEM((2, 2, rows // 2, cols), jnp.bfloat16),
                pltpu.VMEM((cols + lrows, cols), jnp.bfloat16),
                pltpu.VMEM((2, rows, cols), jnp.bfloat16),
                pltpu.VMEM((2 * kept, lrows // 2, rows), jnp.bfloat16),
                pltpu.VMEM((4, lrows // 2, rows), jnp.bfloat16),
                pltpu.VMEM((kept, lrows, cols), jnp.float32),
                pltpu.SemaphoreType.DMA((3 * n // 2,)),
                pltpu.SemaphoreType.DMA((1,)),
                pltpu.SemaphoreType.DMA((2,)),
                pltpu.SemaphoreType.DMA((4,)),
                pltpu.SemaphoreType.DMA((3 * kept // 2,)),
                pltpu.SemaphoreType.DMA((3,)),
                pltpu.SemaphoreType.DMA((3,)),
                pltpu.SemaphoreType.DMA((2,)),
                pltpu.SemaphoreType.DMA((1,)),
                pltpu.SemaphoreType.DMA((2,)),
                pltpu.SemaphoreType.DMA((2,)),
                pltpu.SemaphoreType.DMA((1,)),
            ],
            compiler_params=pltpu.CompilerParams(collective_id=0, has_side_effects=True, vmem_limit_bytes=48 * 2**20),
            cost_estimate=pl.CostEstimate(flops=2 * rows * cols * (2 * n * cols + 2 * rows), bytes_accessed=2 * n * rows * cols * 3, transcendentals=0),
        )(*[pltpu.with_memory_space_constraint(v, pltpu.HBM) for v in operands])
        results = [left_new, right_new, direction]
        return pl.pallas_call(
            store_kernel,
            name="store",
            out_shape=[jax.ShapeDtypeStruct(v.shape, v.dtype) for v in results],
            in_specs=[vmem] * 3,
            out_specs=[hbm] * 3,
            scratch_shapes=[pltpu.SemaphoreType.DMA((3,))],
            compiler_params=pltpu.CompilerParams(vmem_limit_bytes=1 * 2**20),
        )(*results)

    return jax.shard_map(local_step, mesh=mesh, in_specs=(col_spec, row_spec, row_spec, row_spec, row_spec), out_specs=(row_spec, row_spec, col_spec), check_vma=False)
```

```python
import functools
import math

import jax
import jax.numpy as jnp
from jax import lax
from jax.experimental import pallas as pl
from jax.experimental.pallas import tpu as pltpu
from jax.sharding import PartitionSpec as P

EMA_DECAY = 0.9
CORES = 2
MESH = pl.DeviceIdType.MESH

ORDER = [(int(a), int(b)) for a, b in zip("0310020311322312", "0003102313131222")]
def parcels(code):
    digits = [int(d) for d in code]
    return [((a, b), h) for a, b, h in zip(digits[0::3], digits[1::3], digits[2::3])]


UP = parcels("030031330131020331130230231320120220")
UP_ON = {0: parcels("030"), 2: parcels("330"), 6: parcels("130"), 7: parcels("230")}
DOWN = parcels("011010111310021110311211210321121221")
DOWN_ON = {0: parcels("011"), 6: parcels("311111"), 7: parcels("211")}
ROUNDS = len(UP)
FIRST_UP = parcels("300301200")
FIRST_DOWN = parcels("101100201")
GRAD_ROUND_STEP = [2, 2, 8, 10, 12, 14, 17, 20, 22, 26, 28, 30]
LAST_FORWARD = 7
SIDE_UP, SIDE_DOWN = 9, 10
ASIDE = 40
ROOT_START_STEP = 28
ROOT_ACROSS_STEP = 30
RELAY_STEP = 32


def round_of(name, offset, half):
    a, b = offset
    table, da, db = {"f+": (FIRST_UP, 3, 0), "f-": (FIRST_DOWN, 1, 0), "s+": (UP, 0, 3), "s-": (DOWN, 0, 1)}[name]
    return table.index((((a + da) % 4, (b + db) % 4), half))


def packed(values):
    return [sum(v << (2 * i) for i, v in enumerate(values[j:j + 8])) for j in (0, 8)]


FIRST_CODE = packed([o[0] for o in ORDER])
SECOND_CODE = packed([o[1] for o in ORDER])


def lookup(code, e):
    word = code[0] + (e // 8) * (code[1] - code[0])
    return lax.shift_right_logical(word, 2 * (e % 8)) & 3


ROOT_ORDER = [(0, 0), (3, 0), (1, 0), (0, 1), (2, 0), (3, 1), (1, 1), (2, 1)]
ROOT_Y = sum(o[0] << (2 * i) for i, o in enumerate(ROOT_ORDER))
FAR_TURN, LAST_TURN, TWIN_LAST, TWIN_TURN = 5, 7, 9, 10
ROOT_X = sum(o[1] << (2 * i) for i, o in enumerate(ROOT_ORDER))


def kernel(n, side, g_ref, l_ref, r_ref, lr_ref, rr_ref, lo_ref, ro_ref, do_ref, gfull,
           rr, gt, acc, gbuf, rhs, xx, lroot, relay, lent,
           g_recv, g_send, load_sem, init_sem, l_recv, relay_recv, x_recv, d_recv, l_send, x_send, d_send):
    _, half_rows, cols = g_ref.shape
    rows = 2 * half_rows
    lrows = l_ref.shape[0]
    tile = min(1024, half_rows)
    aside_rows = half_rows * ASIDE // 128

    me = lax.axis_index("tensor")
    c = me % CORES
    chip = me // CORES
    x, y = chip % side, chip // side
    f = x + c * (y - x)
    s = y + c * (x - y)
    fstep = CORES + c * CORES * (side - 1)
    sstep = CORES * side - c * CORES * (side - 1)
    twin = me + 1 - 2 * c

    def index(df, ds):
        return ((f + df) % side) * fstep + ((s + ds) % side) * sstep + c

    def twin_index(df, ds):
        return ((s + df) % side) * sstep + ((f + ds) % side) * fstep + 1 - c

    peers = {"f+": index(1, 0), "f-": index(3, 0), "s+": index(0, 1), "s-": index(0, 3), "twin": twin}

    class Gather:
        def __init__(self, own, full, recv, send):
            self.own, self.full, self.recv, self.send_sem = own, full, recv, send
            self.sent = 0

        def copy(self, name, offset, half, part=None, turn=None):
            b = index(*offset)
            src = self.own.at[half] if offset == (0, 0) else self.full.at[2 * b + half]
            dst = self.full.at[2 * b + half]
            if part is not None:
                src, dst = src.at[pl.ds(*part)], dst.at[pl.ds(*part)]
            if turn is None:
                turn = ROUNDS + b // CORES if name == "twin" else round_of(name, offset, half)
            return pltpu.make_async_remote_copy(
                src_ref=src, dst_ref=dst, send_sem=self.send_sem.at[0], recv_sem=self.recv.at[turn],
                device_id={"tensor": peers[name]}, device_id_type=MESH)

        def send(self, name, offset, half):
            self.sent += 1
            self.copy(name, offset, half).start()

        def wait(self, turn, count):
            taken = self.full.at[pl.ds(0, count)]
            pltpu.make_async_copy(taken, taken, self.recv.at[turn]).wait()

        def start(self):
            for half in (0, 1):
                for name in ("f+", "s+"):
                    self.send(name, (0, 0), half)
                for name in ("f-", "s-"):
                    self.send(name, (0, 0), 1 - half)
            for half in (0, 1):
                self.send("twin", (0, 0), half)

        def round(self, r):
            first = r < len(FIRST_UP)
            self.wait(r, 4 if first else 2)
            if first:
                above, below = FIRST_UP[r], FIRST_DOWN[r]
                if r == 0:
                    self.send("f+", *above)
                    self.send("f-", *below)
                self.send("s+", *above)
                self.send("s-", *below)
                self.send("s+", *below)
                self.send("s-", *above)
                self.send("twin", *above)
                self.send("twin", *below)
            for name, table in (("s+", UP_ON), ("s-", DOWN_ON)):
                for parcel in table.get(r, ()):
                    if r == LAST_FORWARD:
                        self.forward_last(name, *parcel)
                    else:
                        self.send(name, *parcel)
            if r == SIDE_UP:
                self.aside("f+", *UP[r])
            if r == SIDE_DOWN:
                self.aside("f-", *DOWN[r])
            self.send("twin", *UP[r])
            self.send("twin", *DOWN[r])

        def forward_last(self, name, offset, half):
            self.sent += 1
            pl.when(c == 0)(lambda: self.copy(name, offset, half, part=(0, half_rows - aside_rows)).start())
            pl.when(c == 1)(lambda: self.copy(name, offset, half).start())

        def aside(self, name, offset, half):
            part = (half_rows - aside_rows, aside_rows)
            pl.when(c == 0)(lambda: self.copy(name, offset, half, part=part, turn=ROUNDS - 1).start())

        def drain(self):
            whole = self.full.at[pl.ds(0, self.sent)]
            pltpu.make_async_copy(whole, whole, self.send_sem.at[0]).wait()

    grad = Gather(g_ref, gfull, g_recv, g_send)

    def block_of(k):
        e, other = k // 2, k % 2
        df, ds = lookup(FIRST_CODE, e), lookup(SECOND_CODE, e)
        mine = index(df, ds)
        return mine + other * (twin_index(df, ds) - mine)

    def load(gather, buf, k, sem):
        b = block_of(k)
        return pltpu.make_async_copy(gather.full.at[pl.ds(2 * b, 2)], buf.at[k % 2], sem.at[k % 2])

    def steps(gather, buf, sem, round_step, extra, work):
        def step(k, carry):
            for at, fn in extra:
                pl.when(k == at)(fn)
            for r in range(ROUNDS):
                @pl.when(k == round_step[r])
                def _():
                    with jax.named_scope(f"ground{r}"):
                        gather.round(r)

            @pl.when((k % 2 == 1) & (k < n))
            def _():
                with jax.named_scope("twinwait"):
                    gather.wait(ROUNDS + block_of(k) // CORES, 2)

            @pl.when(k < n)
            def _():
                load(gather, buf, k, sem).start()
            with jax.named_scope("loadwait"):
                load(gather, buf, k - 1, sem).wait()
            with jax.named_scope("work"):
                work((k - 1) % 2, block_of(k - 1))
            return carry
        lax.fori_loop(1, n + 1, step, 0)

    first = [
        pltpu.make_async_copy(rr_ref, rr, init_sem.at[0]),
        pltpu.make_async_copy(r_ref, ro_ref, init_sem.at[1]),
        pltpu.make_async_copy(l_ref, lo_ref, init_sem.at[2]),
        pltpu.make_async_copy(lr_ref, lroot.at[pl.ds(2 * ((y * (side // 2) + x // 2) * CORES + c), 2)], init_sem.at[3]),
    ]
    own_load = pltpu.make_async_copy(g_ref, gbuf.at[0], load_sem.at[0])
    own_load.start()

    barrier = pltpu.get_barrier_semaphore()
    for peer in peers.values():
        pl.semaphore_signal(barrier, inc=1, device_id={"tensor": peer}, device_id_type=MESH)
    with jax.named_scope("barrier"):
        pl.semaphore_wait(barrier, len(peers))
    grad.start()
    for copy in first:
        copy.start()

    acc[...] = jnp.zeros_like(acc)
    own_load.wait()
    for h in (0, 1):
        gt[:, h * half_rows:(h + 1) * half_rows] = gbuf[0, h].T
    for copy in first:
        copy.wait()
    own_load.start()

    per_half = half_rows // tile

    def grad_work(slot, b):
        at = pl.multiple_of(b * cols, cols)
        rhs[:cols] = rr[:, pl.ds(at, cols)]
        rhs[cols:] = gbuf[slot, me // (n // 2), pl.ds(pl.multiple_of((me % (n // 2)) * lrows, lrows), lrows), :]

        def rows_step(t, carry):
            left = gbuf[slot, t // per_half, pl.ds(pl.multiple_of((t % per_half) * tile, tile), tile), :]
            out = pl.ds(pl.multiple_of(t * tile, tile), tile)
            acc[out, :] += lax.dot_general(left, rhs[...], (((1,), (1,)), ((), ())), preferred_element_type=jnp.float32)
            return carry
        lax.fori_loop(0, 2 * per_half, rows_step, 0)
        prod = jnp.dot(gt[:, :half_rows], gbuf[slot, 0], preferred_element_type=jnp.float32)
        prod += jnp.dot(gt[:, half_rows:], gbuf[slot, 1], preferred_element_type=jnp.float32)
        ro_ref[:, pl.ds(at, cols)] = EMA_DECAY * ro_ref[:, pl.ds(at, cols)] + (1.0 - EMA_DECAY) * prod


    dx = 1 - 2 * c
    helper = (y * side + (x + dx + side) % side) * CORES + c
    client = (y * side + (x - dx + side) % side) * CORES + c
    up = (((y + 1) % side) * side + x) * CORES + c
    down = (((y + side - 1) % side) * side + x) * CORES + c
    half_count, root_half, _ = lroot.shape
    pieces = ((0, root_half - root_half // 4), (root_half - root_half // 4, root_half // 4))

    def root_block(dy, q, p=0):
        oy, ox = (y + dy) % side, (x + 2 * q) % side
        core = c + p * (1 - 2 * c)
        return (oy * (side // 2) + ox // 2) * CORES + core, (oy * side + ox) * CORES + core

    def root_copy(peer, place, half, src=None, dst=None, recv=None, part=None, across=0):
        here = lroot.at[2 * place + half]
        if part is not None:
            here = here.at[pl.ds(*pieces[part])]
        if peer is twin and recv is None:
            recv = l_recv.at[TWIN_TURN + place // CORES]
        return pltpu.make_async_remote_copy(
            src_ref=here if src is None else src, dst_ref=here if dst is None else dst, send_sem=l_send.at[across],
            recv_sem=l_recv.at[recv] if isinstance(recv, int) else recv, device_id={"tensor": peer}, device_id_type=MESH)

    sent = [0, 0]

    def root_send(peer, place, half, part=None, across=0, **kw):
        sent[across] += root_half if part is None else pieces[part][1]
        root_copy(peer, place, half, part=part, across=across, **kw).start()

    def pair_wait(pair, sem):
        pltpu.make_async_copy(pair, pair, sem).wait()

    own_place, _ = root_block(0, 0)
    far_place, _ = root_block(0, 1)
    passing = (y * (side // 2) + ((x - dx + side) % side) // 2) * CORES + c

    def root_start_across():
        for half in (0, 1):
            root_send(helper, own_place, half, across=1, src=lr_ref.at[half], dst=relay.at[half], recv=relay_recv.at[half])

    def root_start():
        for half in (0, 1):
            root_send(up, own_place, half, src=lr_ref.at[half], recv=half)
            root_send(down, own_place, 1 - half, src=lr_ref.at[1 - half], recv=half)
        for half in (0, 1):
            root_send(twin, own_place, half, src=lr_ref.at[half])

    def root_relay(half):
        root_copy(helper, own_place, half, src=lr_ref.at[half], dst=relay.at[half], recv=relay_recv.at[half]).wait_recv()
        root_send(helper, passing, half, across=1, src=relay.at[half], recv=FAR_TURN + half)
        root_send(twin, passing, half, across=1, src=relay.at[half], dst=relay.at[2 + half], recv=relay_recv.at[2])

    def passed_rows(p):
        if p:
            pair_wait(relay.at[pl.ds(2, 2)], relay_recv.at[2])
        source = (y * side + (x - (1 - 2 * p) * dx + side) % side) * CORES + c + p * (1 - 2 * c)
        left = relay[2 * p:2 * p + 2].reshape(lrows, rows)
        do_ref[rows_of(source), :] = jnp.dot(left, xx[0], preferred_element_type=jnp.float32)

    def root_far():
        for half in (0, 1):
            pltpu.make_async_copy(lroot.at[0], lroot.at[0], l_recv.at[FAR_TURN + half]).wait()
            root_send(up, far_place, half, recv=3 + half)
            root_send(twin, far_place, half)
        for half in (1, 0):
            root_send(down, far_place, half, recv=4 - half)

    def root_round(r):
        q, stage = r // 3, r % 3
        pair_wait(lroot.at[pl.ds(0, 2)], l_recv.at[r])
        if stage == 2:
            below = above = root_block(2, q)[0]
        else:
            below, above = root_block(side - 1, q)[0], root_block(1, q)[0]
        if stage == 0:
            for peer, place, half in ((up, below, 0), (down, above, 1)):
                if q == 0:
                    root_send(peer, place, half, recv=2)
                else:
                    for part in (0, 1):
                        root_send(peer, place, half, part=part, recv=LAST_TURN + part)
        root_send(twin, below, stage % 2)
        root_send(twin, above, 1 - stage % 2)

    last_place, last_device = root_block(2, 1)
    twin_place, twin_device = root_block(2, 1, 1)

    def root_last(part):
        pair_wait(lroot.at[pl.ds(0, 2), pl.ds(*pieces[part])], l_recv.at[LAST_TURN + part])
        for half in (0, 1):
            root_send(twin, last_place, half, part=part, recv=TWIN_LAST if part else None)

    def root_last_twin(part):
        pair = lroot.at[pl.ds(2 * twin_place, 2), pl.ds(*pieces[part])]
        pair_wait(pair, l_recv.at[TWIN_LAST if part else TWIN_TURN + twin_place // CORES])

    steps(grad, gbuf, load_sem, GRAD_ROUND_STEP, [(ROOT_START_STEP, root_start), (ROOT_ACROSS_STEP, root_start_across), (RELAY_STEP, lambda: root_relay(0))], grad_work)

    side_cols = cols // 2

    def x_copy(h):
        at = pl.ds(h * side_cols, side_cols)
        return pltpu.make_async_remote_copy(
            src_ref=xx.at[0, :, at], dst_ref=xx.at[1, :, at], send_sem=x_send.at[h], recv_sem=x_recv.at[h],
            device_id={"tensor": helper}, device_id_type=MESH)

    with jax.named_scope("xfin"):
        xx[0] = acc[:, :cols].astype(jnp.bfloat16)
    with jax.named_scope("relay"):
        root_relay(1)
    x_copy(0).start()
    x_copy(1).start()
    with jax.named_scope("rround0"):
        root_round(0)

    def left_step(t, carry):
        at = pl.ds(pl.multiple_of(t * lrows, lrows), lrows)
        lo_ref[:, at] = EMA_DECAY * lo_ref[:, at] + (1.0 - EMA_DECAY) * acc[at, cols:].T
        return carry
    with jax.named_scope("leftfin"):
        lax.fori_loop(0, rows // lrows, left_step, 0)

    def at_step(i):
        e, p = i // 2, i % 2
        dy = lax.shift_right_logical(ROOT_Y, 2 * e) & 3
        q = lax.shift_right_logical(ROOT_X, 2 * e) & 3
        return root_block(dy, q, p)

    def twin_wait(i, place):
        @pl.when(i % 2 == 1)
        def _():
            pair_wait(lroot.at[pl.ds(2 * place, 2)], l_recv.at[TWIN_TURN + place // CORES])

    def product(place, which):
        left = lroot[pl.ds(2 * place, 2)].reshape(lrows, rows)
        return jnp.dot(left, xx[which], preferred_element_type=jnp.float32)

    def rows_of(device):
        return pl.ds(pl.multiple_of(device * lrows, lrows), lrows)

    def own_rows(i):
        place, device = at_step(i)
        do_ref[rows_of(device), :] = product(place, 0)

    def lent_copy(i, device):
        return pltpu.make_async_remote_copy(
            src_ref=lent.at[i], dst_ref=do_ref.at[rows_of(device)], send_sem=d_send.at[0], recv_sem=d_recv.at[0],
            device_id={"tensor": client}, device_id_type=MESH)

    def lent_rows(i):
        place, device = at_step(i)
        lent[i] = product(place, 1)
        lent_copy(i, device).start()

    def lent_side(i, h):
        place, _ = at_step(i)
        at = pl.ds(h * side_cols, side_cols)
        left = lroot[pl.ds(2 * place, 2)].reshape(lrows, rows)
        lent[i, :, at] = jnp.dot(left, xx[1, :, at], preferred_element_type=jnp.float32)

    def lent_side_copy(i, h):
        _, device = at_step(i)
        at = pl.ds(h * side_cols, side_cols)
        return pltpu.make_async_remote_copy(
            src_ref=lent.at[i, :, at], dst_ref=do_ref.at[rows_of(device), at], send_sem=d_send.at[0], recv_sem=d_recv.at[0],
            device_id={"tensor": client}, device_id_type=MESH)

    def loop(lo, hi, body):
        def step(i, carry):
            body(i)
            return carry
        lax.fori_loop(lo, hi, step, 0)

    def first_own(i):
        @pl.when(i == 2)
        def _():
            with jax.named_scope("far"):
                root_far()
            with jax.named_scope("rround1"):
                root_round(1)

        @pl.when(i == 8)
        def _():
            with jax.named_scope("rround2"):
                root_round(2)
        twin_wait(i, at_step(i)[0])
        own_rows(i)

    loop(0, 10, first_own)
    passed_rows(0)
    passed_rows(1)
    with jax.named_scope("x0wait"):
        x_copy(0).wait_recv()
    def lent_step(j):
        return j + (j + 7) // 8 + j // 5

    loop(0, 8, lambda j: lent_side(lent_step(j), 0))
    x_copy(0).wait_send()
    with jax.named_scope("x1sent"):
        x_copy(1).wait_send()
    loop(0, 8, lambda j: lent_side_copy(lent_step(j), 0).start())
    with jax.named_scope("rround3"):
        root_round(3)
    with jax.named_scope("x1wait"):
        x_copy(1).wait_recv()

    def second_side(j):
        i = lent_step(j)
        lent_side(i, 1)
        lent_side_copy(i, 1).start()
    loop(0, 8, second_side)
    with jax.named_scope("rround4"):
        root_round(4)

    def both(i):
        twin_wait(i, at_step(i)[0])
        lent_rows(i)
        own_rows(i)
    with jax.named_scope("both"):
        loop(10, 14, both)

    def lent_piece(i, place, device, part):
        first, count = pieces[part]
        left = jnp.concatenate([lroot[2 * place, pl.ds(first, count), :], lroot[2 * place + 1, pl.ds(first, count), :]], axis=0)
        prod = jnp.dot(left, xx[1], preferred_element_type=jnp.float32)
        for half in (0, 1):
            at = half * root_half + first
            lent[i, pl.ds(at, count), :] = prod[half * count:(half + 1) * count]
            pltpu.make_async_remote_copy(
                src_ref=lent.at[i, pl.ds(at, count)], dst_ref=do_ref.at[pl.ds(pl.multiple_of(device * lrows, lrows) + at, count)],
                send_sem=d_send.at[0], recv_sem=d_recv.at[0], device_id={"tensor": client}, device_id_type=MESH).start()

    for part in (0, 1):
        with jax.named_scope(f"last{part}"):
            root_last(part)
        lent_piece(14, last_place, last_device, part)
    for part in (0, 1):
        with jax.named_scope(f"lasttwin{part}"):
            root_last_twin(part)
        lent_piece(15, twin_place, twin_device, part)
    loop(14, 16, own_rows)

    with jax.named_scope("drain"):
        grad.drain()
    for across, count in enumerate(sent):
        whole = lroot.at[pl.ds(0, count // root_half)]
        pltpu.make_async_copy(whole, whole, l_send.at[across]).wait()
    given = lent.at[pl.ds(0, half_count // 2 - 2)]
    pltpu.make_async_copy(given, given, d_send.at[0]).wait()
    with jax.named_scope("dwait"):
        pltpu.make_async_copy(given, given, d_recv.at[0]).wait()


def store_kernel(*refs):
    count = (len(refs) - 1) // 2
    sems = refs[-1]
    pieces = 8
    for i in range(count):
        src, dst = refs[i], refs[count + i]
        step = src.shape[0] // pieces
        for j in range(pieces):
            part = pl.ds(j * step, step)
            pltpu.make_async_copy(src.at[part], dst.at[part], sems.at[i]).start()
    for i in range(count):
        pltpu.make_async_copy(refs[i], refs[count + i], sems.at[i]).wait()


def solution(mesh):
    row_spec = P(("layer", "tensor"), None)
    col_spec = P("layer", "tensor")
    n = mesh.shape["tensor"]
    side = math.isqrt(n // CORES)

    def local_step(g, l, r, lr, rr):
        rows, cols = g.shape
        lrows = l.shape[0]
        kept = n // 2
        hbm = pl.BlockSpec(memory_space=pltpu.HBM)
        vmem = pl.BlockSpec(memory_space=pltpu.VMEM)
        operands = [g.reshape(2, rows // 2, cols), l, r, lr.reshape(2, lrows // 2, rows), rr]
        left_new, right_new, direction, _ = pl.pallas_call(
            functools.partial(kernel, n, side),
            name="shampoo",
            out_shape=[
                pltpu.VMEM(l.shape, jnp.float32),
                pltpu.VMEM(r.shape, jnp.float32),
                pltpu.VMEM(g.shape, jnp.float32),
                pltpu.HBM((2 * n, rows // 2, cols), jnp.bfloat16),
            ],
            in_specs=[hbm] * 5,
            out_specs=[vmem, vmem, vmem, hbm],
            scratch_shapes=[
                pltpu.VMEM(rr.shape, jnp.bfloat16),
                pltpu.VMEM((cols, rows), jnp.bfloat16),
                pltpu.VMEM((rows, cols + lrows), jnp.float32),
                pltpu.VMEM((2, 2, rows // 2, cols), jnp.bfloat16),
                pltpu.VMEM((cols + lrows, cols), jnp.bfloat16),
                pltpu.VMEM((2, rows, cols), jnp.bfloat16),
                pltpu.VMEM((2 * kept, lrows // 2, rows), jnp.bfloat16),
                pltpu.VMEM((4, lrows // 2, rows), jnp.bfloat16),
                pltpu.VMEM((kept, lrows, cols), jnp.float32),
                pltpu.SemaphoreType.DMA((ROUNDS + n // 2,)),
                pltpu.SemaphoreType.DMA((1,)),
                pltpu.SemaphoreType.DMA((2,)),
                pltpu.SemaphoreType.DMA((4,)),
                pltpu.SemaphoreType.DMA((TWIN_TURN + kept // 2,)),
                pltpu.SemaphoreType.DMA((3,)),
                pltpu.SemaphoreType.DMA((2,)),
                pltpu.SemaphoreType.DMA((1,)),
                pltpu.SemaphoreType.DMA((2,)),
                pltpu.SemaphoreType.DMA((2,)),
                pltpu.SemaphoreType.DMA((1,)),
            ],
            compiler_params=pltpu.CompilerParams(collective_id=0, has_side_effects=True, vmem_limit_bytes=48 * 2**20),
            cost_estimate=pl.CostEstimate(flops=2 * rows * cols * (2 * n * cols + 2 * rows), bytes_accessed=2 * n * rows * cols * 3, transcendentals=0),
        )(*[pltpu.with_memory_space_constraint(v, pltpu.HBM) for v in operands])
        results = [left_new, right_new, direction]
        return pl.pallas_call(
            store_kernel,
            name="store",
            out_shape=[jax.ShapeDtypeStruct(v.shape, v.dtype) for v in results],
            in_specs=[vmem] * 3,
            out_specs=[hbm] * 3,
            scratch_shapes=[pltpu.SemaphoreType.DMA((3,))],
            compiler_params=pltpu.CompilerParams(vmem_limit_bytes=1 * 2**20),
        )(*results)

    return jax.shard_map(local_step, mesh=mesh, in_specs=(col_spec, row_spec, row_spec, row_spec, row_spec), out_specs=(row_spec, row_spec, col_spec), check_vma=False)
```

```python
import functools
import math

import jax
import jax.numpy as jnp
from jax import lax
from jax.experimental import pallas as pl
from jax.experimental.pallas import tpu as pltpu
from jax.sharding import PartitionSpec as P

EMA_DECAY = 0.9
CORES = 2
MESH = pl.DeviceIdType.MESH

ORDER = [(int(a), int(b)) for a, b in zip("0310020311322312", "0003102313131222")]
def parcels(code):
    digits = [int(d) for d in code]
    return [((a, b), h) for a, b, h in zip(digits[0::3], digits[1::3], digits[2::3])]


UP = parcels("030031330131020331130230231320120220")
UP_ON = {0: parcels("030"), 2: parcels("330"), 6: parcels("130"), 7: parcels("230")}
DOWN = parcels("011010111310021110311211210321121221")
DOWN_ON = {0: parcels("011"), 6: parcels("311111"), 7: parcels("211")}
ROUNDS = len(UP)
FIRST_UP = parcels("300301200")
FIRST_DOWN = parcels("101100201")
GRAD_ROUND_STEP = [2, 2, 8, 10, 12, 14, 17, 20, 22, 26, 28, 30]
LAST_FORWARD = 7
SIDE_UP, SIDE_DOWN = 9, 10
ASIDE = 40
ROOT_START_STEP = 28
ROOT_ACROSS_STEP = 30
RELAY_STEP = 32
LATE = (2, 12, 14, 22, 26, 28, 30)


def round_of(name, offset, half):
    a, b = offset
    table, da, db = {"f+": (FIRST_UP, 3, 0), "f-": (FIRST_DOWN, 1, 0), "s+": (UP, 0, 3), "s-": (DOWN, 0, 1)}[name]
    return table.index((((a + da) % 4, (b + db) % 4), half))


def packed(values):
    return [sum(v << (2 * i) for i, v in enumerate(values[j:j + 8])) for j in (0, 8)]


FIRST_CODE = packed([o[0] for o in ORDER])
SECOND_CODE = packed([o[1] for o in ORDER])


def lookup(code, e):
    word = code[0] + (e // 8) * (code[1] - code[0])
    return lax.shift_right_logical(word, 2 * (e % 8)) & 3


ROOT_ORDER = [(0, 0), (3, 0), (1, 0), (0, 1), (2, 0), (3, 1), (1, 1), (2, 1)]
ROOT_Y = sum(o[0] << (2 * i) for i, o in enumerate(ROOT_ORDER))
FAR_TURN, LAST_TURN, TWIN_LAST, TWIN_TURN = 5, 7, 9, 10
ROOT_X = sum(o[1] << (2 * i) for i, o in enumerate(ROOT_ORDER))


def kernel(n, side, g_ref, l_ref, r_ref, lr_ref, rr_ref, lo_ref, ro_ref, do_ref, gfull,
           rr, gt, acc, gbuf, rhs, xx, lroot, relay, lent,
           g_recv, g_send, load_sem, init_sem, l_recv, relay_recv, x_recv, d_recv, l_send, x_send, d_send):
    _, half_rows, cols = g_ref.shape
    rows = 2 * half_rows
    lrows = l_ref.shape[0]
    tile = min(1024, half_rows)
    aside_rows = half_rows * ASIDE // 128

    me = lax.axis_index("tensor")
    c = me % CORES
    chip = me // CORES
    x, y = chip % side, chip // side
    f = x + c * (y - x)
    s = y + c * (x - y)
    fstep = CORES + c * CORES * (side - 1)
    sstep = CORES * side - c * CORES * (side - 1)
    twin = me + 1 - 2 * c

    def index(df, ds):
        return ((f + df) % side) * fstep + ((s + ds) % side) * sstep + c

    def twin_index(df, ds):
        return ((s + df) % side) * sstep + ((f + ds) % side) * fstep + 1 - c

    peers = {"f+": index(1, 0), "f-": index(3, 0), "s+": index(0, 1), "s-": index(0, 3), "twin": twin}

    class Gather:
        def __init__(self, own, full, recv, send):
            self.own, self.full, self.recv, self.send_sem = own, full, recv, send
            self.sent = 0

        def copy(self, name, offset, half, part=None, turn=None):
            b = index(*offset)
            src = self.own.at[half] if offset == (0, 0) else self.full.at[2 * b + half]
            dst = self.full.at[2 * b + half]
            if part is not None:
                src, dst = src.at[pl.ds(*part)], dst.at[pl.ds(*part)]
            if turn is None:
                turn = ROUNDS + b // CORES if name == "twin" else round_of(name, offset, half)
            return pltpu.make_async_remote_copy(
                src_ref=src, dst_ref=dst, send_sem=self.send_sem.at[0], recv_sem=self.recv.at[turn],
                device_id={"tensor": peers[name]}, device_id_type=MESH)

        def send(self, name, offset, half):
            self.sent += 1
            self.copy(name, offset, half).start()

        def wait(self, turn, count):
            taken = self.full.at[pl.ds(0, count)]
            pltpu.make_async_copy(taken, taken, self.recv.at[turn]).wait()

        def start(self):
            for half in (0, 1):
                for name in ("f+", "s+"):
                    self.send(name, (0, 0), half)
                for name in ("f-", "s-"):
                    self.send(name, (0, 0), 1 - half)
            for half in (0, 1):
                self.send("twin", (0, 0), half)

        def round(self, r):
            first = r < len(FIRST_UP)
            self.wait(r, 4 if first else 2)
            if first:
                above, below = FIRST_UP[r], FIRST_DOWN[r]
                if r == 0:
                    self.send("f+", *above)
                    self.send("f-", *below)
                self.send("s+", *above)
                self.send("s-", *below)
                self.send("s+", *below)
                self.send("s-", *above)
                self.send("twin", *above)
                self.send("twin", *below)
            for name, table in (("s+", UP_ON), ("s-", DOWN_ON)):
                for parcel in table.get(r, ()):
                    if r == LAST_FORWARD:
                        self.forward_last(name, *parcel)
                    else:
                        self.send(name, *parcel)
            if r == SIDE_UP:
                self.aside("f+", *UP[r])
            if r == SIDE_DOWN:
                self.aside("f-", *DOWN[r])
            self.send("twin", *UP[r])
            self.send("twin", *DOWN[r])

        def forward_last(self, name, offset, half):
            self.sent += 1
            pl.when(c == 0)(lambda: self.copy(name, offset, half, part=(0, half_rows - aside_rows)).start())
            pl.when(c == 1)(lambda: self.copy(name, offset, half).start())

        def aside(self, name, offset, half):
            part = (half_rows - aside_rows, aside_rows)
            pl.when(c == 0)(lambda: self.copy(name, offset, half, part=part, turn=ROUNDS - 1).start())

        def drain(self):
            whole = self.full.at[pl.ds(0, self.sent)]
            pltpu.make_async_copy(whole, whole, self.send_sem.at[0]).wait()

    grad = Gather(g_ref, gfull, g_recv, g_send)

    def block_of(k):
        e, other = k // 2, k % 2
        df, ds = lookup(FIRST_CODE, e), lookup(SECOND_CODE, e)
        mine = index(df, ds)
        return mine + other * (twin_index(df, ds) - mine)

    def load(gather, buf, k, sem):
        b = block_of(k)
        return pltpu.make_async_copy(gather.full.at[pl.ds(2 * b, 2)], buf.at[k % 2], sem.at[k % 2])

    def one_of(k, values):
        found = k == values[0]
        for v in values[1:]:
            found = found | (k == v)
        return found

    def steps(gather, buf, sem, round_step, early, between, after, work):
        def at_steps(k, actions):
            for at, action in actions:
                pl.when(k == at)(action)

        def step(k, carry):
            at_steps(k, early)

            @pl.when((k % 2 == 1) & (k < n))
            def _():
                with jax.named_scope("twinwait"):
                    gather.wait(ROUNDS + block_of(k) // CORES, 2)

            @pl.when(jnp.logical_not(one_of(k, LATE)) & (k < n))
            def _():
                load(gather, buf, k, sem).start()
            with jax.named_scope("loadwait"):
                load(gather, buf, k - 1, sem).wait()
            with jax.named_scope("work"):
                work((k - 1) % 2, block_of(k - 1))
            at_steps(k, between)
            for r in range(ROUNDS):
                @pl.when(k == round_step[r])
                def _():
                    with jax.named_scope(f"ground{r}"):
                        gather.round(r)
            at_steps(k, after)

            @pl.when(one_of(k, LATE))
            def _():
                load(gather, buf, k, sem).start()
            return carry
        lax.fori_loop(1, n + 1, step, 0)

    first = [
        pltpu.make_async_copy(rr_ref, rr, init_sem.at[0]),
        pltpu.make_async_copy(r_ref, ro_ref, init_sem.at[1]),
        pltpu.make_async_copy(l_ref, lo_ref, init_sem.at[2]),
        pltpu.make_async_copy(lr_ref, lroot.at[pl.ds(2 * ((y * (side // 2) + x // 2) * CORES + c), 2)], init_sem.at[3]),
    ]
    own_load = pltpu.make_async_copy(g_ref, gbuf.at[0], load_sem.at[0])
    own_load.start()

    barrier = pltpu.get_barrier_semaphore()
    for peer in peers.values():
        pl.semaphore_signal(barrier, inc=1, device_id={"tensor": peer}, device_id_type=MESH)
    with jax.named_scope("barrier"):
        pl.semaphore_wait(barrier, len(peers))
    grad.start()
    for copy in first:
        copy.start()

    acc[...] = jnp.zeros_like(acc)
    own_load.wait()
    for h in (0, 1):
        gt[:, h * half_rows:(h + 1) * half_rows] = gbuf[0, h].T
    for copy in first:
        copy.wait()
    own_load.start()

    per_half = half_rows // tile

    def grad_work(slot, b):
        at = pl.multiple_of(b * cols, cols)
        rhs[:cols] = rr[:, pl.ds(at, cols)]
        rhs[cols:] = gbuf[slot, me // (n // 2), pl.ds(pl.multiple_of((me % (n // 2)) * lrows, lrows), lrows), :]

        def rows_step(t, carry):
            left = gbuf[slot, t // per_half, pl.ds(pl.multiple_of((t % per_half) * tile, tile), tile), :]
            out = pl.ds(pl.multiple_of(t * tile, tile), tile)
            acc[out, :] += lax.dot_general(left, rhs[...], (((1,), (1,)), ((), ())), preferred_element_type=jnp.float32)
            return carry
        lax.fori_loop(0, 2 * per_half, rows_step, 0)
        prod = jnp.dot(gt[:, :half_rows], gbuf[slot, 0], preferred_element_type=jnp.float32)
        prod += jnp.dot(gt[:, half_rows:], gbuf[slot, 1], preferred_element_type=jnp.float32)
        ro_ref[:, pl.ds(at, cols)] = EMA_DECAY * ro_ref[:, pl.ds(at, cols)] + (1.0 - EMA_DECAY) * prod


    dx = 1 - 2 * c
    helper = (y * side + (x + dx + side) % side) * CORES + c
    client = (y * side + (x - dx + side) % side) * CORES + c
    up = (((y + 1) % side) * side + x) * CORES + c
    down = (((y + side - 1) % side) * side + x) * CORES + c
    half_count, root_half, _ = lroot.shape
    pieces = ((0, root_half - root_half // 4), (root_half - root_half // 4, root_half // 4))

    def root_block(dy, q, p=0):
        oy, ox = (y + dy) % side, (x + 2 * q) % side
        core = c + p * (1 - 2 * c)
        return (oy * (side // 2) + ox // 2) * CORES + core, (oy * side + ox) * CORES + core

    def root_copy(peer, place, half, src=None, dst=None, recv=None, part=None, across=0):
        here = lroot.at[2 * place + half]
        if part is not None:
            here = here.at[pl.ds(*pieces[part])]
        if peer is twin and recv is None:
            recv = l_recv.at[TWIN_TURN + place // CORES]
        return pltpu.make_async_remote_copy(
            src_ref=here if src is None else src, dst_ref=here if dst is None else dst, send_sem=l_send.at[across],
            recv_sem=l_recv.at[recv] if isinstance(recv, int) else recv, device_id={"tensor": peer}, device_id_type=MESH)

    sent = [0, 0]

    def root_send(peer, place, half, part=None, across=0, **kw):
        sent[across] += root_half if part is None else pieces[part][1]
        root_copy(peer, place, half, part=part, across=across, **kw).start()

    def pair_wait(pair, sem):
        pltpu.make_async_copy(pair, pair, sem).wait()

    own_place, _ = root_block(0, 0)
    far_place, _ = root_block(0, 1)
    passing = (y * (side // 2) + ((x - dx + side) % side) // 2) * CORES + c

    def root_start_across():
        for half in (0, 1):
            root_send(helper, own_place, half, across=1, src=lr_ref.at[half], dst=relay.at[half], recv=relay_recv.at[half])

    def root_start():
        for half in (0, 1):
            root_send(up, own_place, half, src=lr_ref.at[half], recv=half)
            root_send(down, own_place, 1 - half, src=lr_ref.at[1 - half], recv=half)
        for half in (0, 1):
            root_send(twin, own_place, half, src=lr_ref.at[half])

    def root_relay(half):
        root_copy(helper, own_place, half, src=lr_ref.at[half], dst=relay.at[half], recv=relay_recv.at[half]).wait_recv()
        root_send(helper, passing, half, across=1, src=relay.at[half], recv=FAR_TURN + half)
        root_send(twin, passing, half, across=1, src=relay.at[half], dst=relay.at[2 + half], recv=relay_recv.at[2])

    def passed_rows(p):
        if p:
            pair_wait(relay.at[pl.ds(2, 2)], relay_recv.at[2])
        source = (y * side + (x - (1 - 2 * p) * dx + side) % side) * CORES + c + p * (1 - 2 * c)
        left = relay[2 * p:2 * p + 2].reshape(lrows, rows)
        do_ref[rows_of(source), :] = jnp.dot(left, xx[0], preferred_element_type=jnp.float32)

    def root_far():
        for half in (0, 1):
            pltpu.make_async_copy(lroot.at[0], lroot.at[0], l_recv.at[FAR_TURN + half]).wait()
            root_send(up, far_place, half, recv=3 + half)
            root_send(twin, far_place, half)
        for half in (1, 0):
            root_send(down, far_place, half, recv=4 - half)

    def root_round(r):
        q, stage = r // 3, r % 3
        pair_wait(lroot.at[pl.ds(0, 2)], l_recv.at[r])
        if stage == 2:
            below = above = root_block(2, q)[0]
        else:
            below, above = root_block(side - 1, q)[0], root_block(1, q)[0]
        if stage == 0:
            for peer, place, half in ((up, below, 0), (down, above, 1)):
                if q == 0:
                    root_send(peer, place, half, recv=2)
                else:
                    for part in (0, 1):
                        root_send(peer, place, half, part=part, recv=LAST_TURN + part)
        root_send(twin, below, stage % 2)
        root_send(twin, above, 1 - stage % 2)

    last_place, last_device = root_block(2, 1)
    twin_place, twin_device = root_block(2, 1, 1)

    def root_last(part):
        pair_wait(lroot.at[pl.ds(0, 2), pl.ds(*pieces[part])], l_recv.at[LAST_TURN + part])
        for half in (0, 1):
            root_send(twin, last_place, half, part=part, recv=TWIN_LAST if part else None)

    def root_last_twin(part):
        pair = lroot.at[pl.ds(2 * twin_place, 2), pl.ds(*pieces[part])]
        pair_wait(pair, l_recv.at[TWIN_LAST if part else TWIN_TURN + twin_place // CORES])

    steps(grad, gbuf, load_sem, GRAD_ROUND_STEP, [(RELAY_STEP, lambda: root_relay(0))],
          [(ROOT_ACROSS_STEP, root_start_across)], [(ROOT_START_STEP, root_start)], grad_work)

    side_cols = cols // 2

    def x_copy(h):
        at = pl.ds(h * side_cols, side_cols)
        return pltpu.make_async_remote_copy(
            src_ref=xx.at[0, :, at], dst_ref=xx.at[1, :, at], send_sem=x_send.at[h], recv_sem=x_recv.at[h],
            device_id={"tensor": helper}, device_id_type=MESH)

    with jax.named_scope("xfin"):
        xx[0] = acc[:, :cols].astype(jnp.bfloat16)
    with jax.named_scope("relay"):
        root_relay(1)
    x_copy(0).start()
    x_copy(1).start()
    with jax.named_scope("rround0"):
        root_round(0)

    def left_step(t, carry):
        at = pl.ds(pl.multiple_of(t * lrows, lrows), lrows)
        lo_ref[:, at] = EMA_DECAY * lo_ref[:, at] + (1.0 - EMA_DECAY) * acc[at, cols:].T
        return carry
    with jax.named_scope("leftfin"):
        lax.fori_loop(0, rows // lrows, left_step, 0)

    def at_step(i):
        e, p = i // 2, i % 2
        dy = lax.shift_right_logical(ROOT_Y, 2 * e) & 3
        q = lax.shift_right_logical(ROOT_X, 2 * e) & 3
        return root_block(dy, q, p)

    def twin_wait(i, place):
        @pl.when(i % 2 == 1)
        def _():
            pair_wait(lroot.at[pl.ds(2 * place, 2)], l_recv.at[TWIN_TURN + place // CORES])

    def product(place, which):
        left = lroot[pl.ds(2 * place, 2)].reshape(lrows, rows)
        return jnp.dot(left, xx[which], preferred_element_type=jnp.float32)

    def rows_of(device):
        return pl.ds(pl.multiple_of(device * lrows, lrows), lrows)

    def own_rows(i):
        place, device = at_step(i)
        do_ref[rows_of(device), :] = product(place, 0)

    def lent_copy(i, device):
        return pltpu.make_async_remote_copy(
            src_ref=lent.at[i], dst_ref=do_ref.at[rows_of(device)], send_sem=d_send.at[0], recv_sem=d_recv.at[0],
            device_id={"tensor": client}, device_id_type=MESH)

    def lent_rows(i):
        place, device = at_step(i)
        lent[i] = product(place, 1)
        lent_copy(i, device).start()

    def lent_side(i, h):
        place, _ = at_step(i)
        at = pl.ds(h * side_cols, side_cols)
        left = lroot[pl.ds(2 * place, 2)].reshape(lrows, rows)
        lent[i, :, at] = jnp.dot(left, xx[1, :, at], preferred_element_type=jnp.float32)

    def lent_side_copy(i, h):
        _, device = at_step(i)
        at = pl.ds(h * side_cols, side_cols)
        return pltpu.make_async_remote_copy(
            src_ref=lent.at[i, :, at], dst_ref=do_ref.at[rows_of(device), at], send_sem=d_send.at[0], recv_sem=d_recv.at[0],
            device_id={"tensor": client}, device_id_type=MESH)

    def loop(lo, hi, body):
        def step(i, carry):
            body(i)
            return carry
        lax.fori_loop(lo, hi, step, 0)

    def first_own(i):
        @pl.when(i == 2)
        def _():
            with jax.named_scope("far"):
                root_far()
            with jax.named_scope("rround1"):
                root_round(1)

        @pl.when(i == 8)
        def _():
            with jax.named_scope("rround2"):
                root_round(2)
        twin_wait(i, at_step(i)[0])
        own_rows(i)

    loop(0, 10, first_own)
    passed_rows(0)
    passed_rows(1)
    with jax.named_scope("x0wait"):
        x_copy(0).wait_recv()
    def lent_step(j):
        return j + (j + 7) // 8 + j // 5

    loop(0, 8, lambda j: lent_side(lent_step(j), 0))
    x_copy(0).wait_send()
    with jax.named_scope("x1sent"):
        x_copy(1).wait_send()
    loop(0, 8, lambda j: lent_side_copy(lent_step(j), 0).start())
    with jax.named_scope("rround3"):
        root_round(3)
    with jax.named_scope("x1wait"):
        x_copy(1).wait_recv()

    def second_side(j):
        i = lent_step(j)
        lent_side(i, 1)
        lent_side_copy(i, 1).start()
    loop(0, 8, second_side)
    with jax.named_scope("rround4"):
        root_round(4)

    def both(i):
        twin_wait(i, at_step(i)[0])
        lent_rows(i)
        own_rows(i)
    with jax.named_scope("both"):
        loop(10, 14, both)

    def lent_piece(i, place, device, part):
        first, count = pieces[part]
        left = jnp.concatenate([lroot[2 * place, pl.ds(first, count), :], lroot[2 * place + 1, pl.ds(first, count), :]], axis=0)
        prod = jnp.dot(left, xx[1], preferred_element_type=jnp.float32)
        for half in (0, 1):
            at = half * root_half + first
            lent[i, pl.ds(at, count), :] = prod[half * count:(half + 1) * count]
            pltpu.make_async_remote_copy(
                src_ref=lent.at[i, pl.ds(at, count)], dst_ref=do_ref.at[pl.ds(pl.multiple_of(device * lrows, lrows) + at, count)],
                send_sem=d_send.at[0], recv_sem=d_recv.at[0], device_id={"tensor": client}, device_id_type=MESH).start()

    for part in (0, 1):
        with jax.named_scope(f"last{part}"):
            root_last(part)
        lent_piece(14, last_place, last_device, part)
    for part in (0, 1):
        with jax.named_scope(f"lasttwin{part}"):
            root_last_twin(part)
        lent_piece(15, twin_place, twin_device, part)
    loop(14, 16, own_rows)

    with jax.named_scope("drain"):
        grad.drain()
    for across, count in enumerate(sent):
        whole = lroot.at[pl.ds(0, count // root_half)]
        pltpu.make_async_copy(whole, whole, l_send.at[across]).wait()
    given = lent.at[pl.ds(0, half_count // 2 - 2)]
    pltpu.make_async_copy(given, given, d_send.at[0]).wait()
    with jax.named_scope("dwait"):
        pltpu.make_async_copy(given, given, d_recv.at[0]).wait()


def store_kernel(*refs):
    count = (len(refs) - 1) // 2
    sems = refs[-1]
    pieces = 8
    for i in range(count):
        src, dst = refs[i], refs[count + i]
        step = src.shape[0] // pieces
        for j in range(pieces):
            part = pl.ds(j * step, step)
            pltpu.make_async_copy(src.at[part], dst.at[part], sems.at[i]).start()
    for i in range(count):
        pltpu.make_async_copy(refs[i], refs[count + i], sems.at[i]).wait()


def solution(mesh):
    row_spec = P(("layer", "tensor"), None)
    col_spec = P("layer", "tensor")
    n = mesh.shape["tensor"]
    side = math.isqrt(n // CORES)

    def local_step(g, l, r, lr, rr):
        rows, cols = g.shape
        lrows = l.shape[0]
        kept = n // 2
        hbm = pl.BlockSpec(memory_space=pltpu.HBM)
        vmem = pl.BlockSpec(memory_space=pltpu.VMEM)
        operands = [g.reshape(2, rows // 2, cols), l, r, lr.reshape(2, lrows // 2, rows), rr]
        left_new, right_new, direction, _ = pl.pallas_call(
            functools.partial(kernel, n, side),
            name="shampoo",
            out_shape=[
                pltpu.VMEM(l.shape, jnp.float32),
                pltpu.VMEM(r.shape, jnp.float32),
                pltpu.VMEM(g.shape, jnp.float32),
                pltpu.HBM((2 * n, rows // 2, cols), jnp.bfloat16),
            ],
            in_specs=[hbm] * 5,
            out_specs=[vmem, vmem, vmem, hbm],
            scratch_shapes=[
                pltpu.VMEM(rr.shape, jnp.bfloat16),
                pltpu.VMEM((cols, rows), jnp.bfloat16),
                pltpu.VMEM((rows, cols + lrows), jnp.float32),
                pltpu.VMEM((2, 2, rows // 2, cols), jnp.bfloat16),
                pltpu.VMEM((cols + lrows, cols), jnp.bfloat16),
                pltpu.VMEM((2, rows, cols), jnp.bfloat16),
                pltpu.VMEM((2 * kept, lrows // 2, rows), jnp.bfloat16),
                pltpu.VMEM((4, lrows // 2, rows), jnp.bfloat16),
                pltpu.VMEM((kept, lrows, cols), jnp.float32),
                pltpu.SemaphoreType.DMA((ROUNDS + n // 2,)),
                pltpu.SemaphoreType.DMA((1,)),
                pltpu.SemaphoreType.DMA((2,)),
                pltpu.SemaphoreType.DMA((4,)),
                pltpu.SemaphoreType.DMA((TWIN_TURN + kept // 2,)),
                pltpu.SemaphoreType.DMA((3,)),
                pltpu.SemaphoreType.DMA((2,)),
                pltpu.SemaphoreType.DMA((1,)),
                pltpu.SemaphoreType.DMA((2,)),
                pltpu.SemaphoreType.DMA((2,)),
                pltpu.SemaphoreType.DMA((1,)),
            ],
            compiler_params=pltpu.CompilerParams(collective_id=0, has_side_effects=True, vmem_limit_bytes=48 * 2**20),
            cost_estimate=pl.CostEstimate(flops=2 * rows * cols * (2 * n * cols + 2 * rows), bytes_accessed=2 * n * rows * cols * 3, transcendentals=0),
        )(*[pltpu.with_memory_space_constraint(v, pltpu.HBM) for v in operands])
        results = [left_new, right_new, direction]
        return pl.pallas_call(
            store_kernel,
            name="store",
            out_shape=[jax.ShapeDtypeStruct(v.shape, v.dtype) for v in results],
            in_specs=[vmem] * 3,
            out_specs=[hbm] * 3,
            scratch_shapes=[pltpu.SemaphoreType.DMA((3,))],
            compiler_params=pltpu.CompilerParams(vmem_limit_bytes=1 * 2**20),
        )(*results)

    return jax.shard_map(local_step, mesh=mesh, in_specs=(col_spec, row_spec, row_spec, row_spec, row_spec), out_specs=(row_spec, row_spec, col_spec), check_vma=False)
```

```python
import functools
import math

import jax
import jax.numpy as jnp
from jax import lax
from jax.experimental import pallas as pl
from jax.experimental.pallas import tpu as pltpu
from jax.sharding import PartitionSpec as P

EMA_DECAY = 0.9
CORES = 2
MESH = pl.DeviceIdType.MESH

ORDER = [(int(a), int(b)) for a, b in zip("0310020311322312", "0003102313131222")]
def parcels(code):
    digits = [int(d) for d in code]
    return [((a, b), h) for a, b, h in zip(digits[0::3], digits[1::3], digits[2::3])]


UP = parcels("030031330131020331130230231320120220")
UP_ON = {0: parcels("030"), 2: parcels("330"), 6: parcels("130"), 7: parcels("230")}
DOWN = parcels("011010111310021110311211210321121221")
DOWN_ON = {0: parcels("011"), 6: parcels("311111"), 7: parcels("211")}
ROUNDS = len(UP)
FIRST_UP = parcels("300301200")
FIRST_DOWN = parcels("101100201")
GRAD_ROUND_STEP = [2, 2, 8, 10, 12, 14, 17, 20, 22, 26, 28, 30]
LAST_FORWARD = 7
SIDE_UP, SIDE_DOWN = 9, 10
ASIDE = 40
ROOT_START_STEP = 28
ROOT_ACROSS_STEP = 30
RELAY_STEP = 32
LATE = (2, 12, 14, 22, 26, 28, 30)


def round_of(name, offset, half):
    a, b = offset
    table, da, db = {"f+": (FIRST_UP, 3, 0), "f-": (FIRST_DOWN, 1, 0), "s+": (UP, 0, 3), "s-": (DOWN, 0, 1)}[name]
    return table.index((((a + da) % 4, (b + db) % 4), half))


def packed(values):
    return [sum(v << (2 * i) for i, v in enumerate(values[j:j + 8])) for j in (0, 8)]


FIRST_CODE = packed([o[0] for o in ORDER])
SECOND_CODE = packed([o[1] for o in ORDER])


def lookup(code, e):
    word = code[0] + (e // 8) * (code[1] - code[0])
    return lax.shift_right_logical(word, 2 * (e % 8)) & 3


ROOT_ORDER = [(0, 0), (3, 0), (1, 0), (0, 1), (2, 0), (3, 1), (1, 1), (2, 1)]
ROOT_Y = sum(o[0] << (2 * i) for i, o in enumerate(ROOT_ORDER))
FAR_TURN, LAST_TURN, TWIN_LAST, TWIN_TURN = 5, 7, 9, 10
ROOT_X = sum(o[1] << (2 * i) for i, o in enumerate(ROOT_ORDER))


def kernel(n, side, g_ref, l_ref, r_ref, lr_ref, rr_ref, lo_ref, ro_ref, do_ref, gfull,
           rr, gt, acc, gbuf, rhs, xx, lroot, relay, lent,
           g_recv, g_send, load_sem, init_sem, l_recv, relay_recv, x_recv, d_recv, l_send, x_send, d_send, x_gone):
    _, half_rows, cols = g_ref.shape
    rows = 2 * half_rows
    lrows = l_ref.shape[0]
    tile = min(1024, half_rows)
    aside_rows = half_rows * ASIDE // 128

    me = lax.axis_index("tensor")
    c = me % CORES
    chip = me // CORES
    x, y = chip % side, chip // side
    f = x + c * (y - x)
    s = y + c * (x - y)
    fstep = CORES + c * CORES * (side - 1)
    sstep = CORES * side - c * CORES * (side - 1)
    twin = me + 1 - 2 * c

    def index(df, ds):
        return ((f + df) % side) * fstep + ((s + ds) % side) * sstep + c

    def twin_index(df, ds):
        return ((s + df) % side) * sstep + ((f + ds) % side) * fstep + 1 - c

    peers = {"f+": index(1, 0), "f-": index(3, 0), "s+": index(0, 1), "s-": index(0, 3), "twin": twin}

    class Gather:
        def __init__(self, own, full, recv, send):
            self.own, self.full, self.recv, self.send_sem = own, full, recv, send
            self.sent = 0

        def copy(self, name, offset, half, part=None, turn=None):
            b = index(*offset)
            src = self.own.at[half] if offset == (0, 0) else self.full.at[2 * b + half]
            dst = self.full.at[2 * b + half]
            if part is not None:
                src, dst = src.at[pl.ds(*part)], dst.at[pl.ds(*part)]
            if turn is None:
                turn = ROUNDS + b // CORES if name == "twin" else round_of(name, offset, half)
            return pltpu.make_async_remote_copy(
                src_ref=src, dst_ref=dst, send_sem=self.send_sem.at[0], recv_sem=self.recv.at[turn],
                device_id={"tensor": peers[name]}, device_id_type=MESH)

        def send(self, name, offset, half):
            self.sent += 1
            self.copy(name, offset, half).start()

        def wait(self, turn, count):
            taken = self.full.at[pl.ds(0, count)]
            pltpu.make_async_copy(taken, taken, self.recv.at[turn]).wait()

        def start(self):
            for half in (0, 1):
                for name in ("f+", "s+"):
                    self.send(name, (0, 0), half)
                for name in ("f-", "s-"):
                    self.send(name, (0, 0), 1 - half)
            for half in (0, 1):
                self.send("twin", (0, 0), half)

        def round(self, r):
            first = r < len(FIRST_UP)
            self.wait(r, 4 if first else 2)
            if first:
                above, below = FIRST_UP[r], FIRST_DOWN[r]
                if r == 0:
                    self.send("f+", *above)
                    self.send("f-", *below)
                self.send("s+", *above)
                self.send("s-", *below)
                self.send("s+", *below)
                self.send("s-", *above)
                self.send("twin", *above)
                self.send("twin", *below)
            for name, table in (("s+", UP_ON), ("s-", DOWN_ON)):
                for parcel in table.get(r, ()):
                    if r == LAST_FORWARD:
                        self.forward_last(name, *parcel)
                    else:
                        self.send(name, *parcel)
            if r == SIDE_UP:
                self.aside("f+", *UP[r])
            if r == SIDE_DOWN:
                self.aside("f-", *DOWN[r])
            self.send("twin", *UP[r])
            self.send("twin", *DOWN[r])

        def forward_last(self, name, offset, half):
            self.sent += 1
            pl.when(c == 0)(lambda: self.copy(name, offset, half, part=(0, half_rows - aside_rows)).start())
            pl.when(c == 1)(lambda: self.copy(name, offset, half).start())

        def aside(self, name, offset, half):
            part = (half_rows - aside_rows, aside_rows)
            pl.when(c == 0)(lambda: self.copy(name, offset, half, part=part, turn=ROUNDS - 1).start())

        def drain(self):
            whole = self.full.at[pl.ds(0, self.sent)]
            pltpu.make_async_copy(whole, whole, self.send_sem.at[0]).wait()

    grad = Gather(g_ref, gfull, g_recv, g_send)

    def block_of(k):
        e, other = k // 2, k % 2
        df, ds = lookup(FIRST_CODE, e), lookup(SECOND_CODE, e)
        mine = index(df, ds)
        return mine + other * (twin_index(df, ds) - mine)

    def load(gather, buf, k, sem):
        b = block_of(k)
        return pltpu.make_async_copy(gather.full.at[pl.ds(2 * b, 2)], buf.at[k % 2], sem.at[k % 2])

    def one_of(k, values):
        found = k == values[0]
        for v in values[1:]:
            found = found | (k == v)
        return found

    def steps(gather, buf, sem, round_step, early, between, after, work):
        def at_steps(k, actions):
            for at, action in actions:
                pl.when(k == at)(action)

        def step(k, carry):
            at_steps(k, early)

            @pl.when((k % 2 == 1) & (k < n))
            def _():
                with jax.named_scope("twinwait"):
                    gather.wait(ROUNDS + block_of(k) // CORES, 2)

            @pl.when(jnp.logical_not(one_of(k, LATE)) & (k < n))
            def _():
                load(gather, buf, k, sem).start()
            with jax.named_scope("loadwait"):
                load(gather, buf, k - 1, sem).wait()
            with jax.named_scope("work"):
                work((k - 1) % 2, block_of(k - 1))
            at_steps(k, between)
            for r in range(ROUNDS):
                @pl.when(k == round_step[r])
                def _():
                    with jax.named_scope(f"ground{r}"):
                        gather.round(r)
            at_steps(k, after)

            @pl.when(one_of(k, LATE))
            def _():
                load(gather, buf, k, sem).start()
            return carry
        lax.fori_loop(1, n + 1, step, 0)

    first = [
        pltpu.make_async_copy(rr_ref, rr, init_sem.at[0]),
        pltpu.make_async_copy(r_ref, ro_ref, init_sem.at[1]),
        pltpu.make_async_copy(l_ref, lo_ref, init_sem.at[2]),
        pltpu.make_async_copy(lr_ref, lroot.at[pl.ds(2 * ((y * (side // 2) + x // 2) * CORES + c), 2)], init_sem.at[3]),
    ]
    own_load = pltpu.make_async_copy(g_ref, gbuf.at[0], load_sem.at[0])
    own_load.start()

    barrier = pltpu.get_barrier_semaphore()
    for peer in peers.values():
        pl.semaphore_signal(barrier, inc=1, device_id={"tensor": peer}, device_id_type=MESH)
    with jax.named_scope("barrier"):
        pl.semaphore_wait(barrier, len(peers))
    grad.start()
    for copy in first:
        copy.start()

    acc[...] = jnp.zeros_like(acc)
    own_load.wait()
    for h in (0, 1):
        gt[:, h * half_rows:(h + 1) * half_rows] = gbuf[0, h].T
    for copy in first:
        copy.wait()
    own_load.start()

    per_half = half_rows // tile

    def grad_work(slot, b):
        at = pl.multiple_of(b * cols, cols)
        rhs[:cols] = rr[:, pl.ds(at, cols)]
        rhs[cols:] = gbuf[slot, me // (n // 2), pl.ds(pl.multiple_of((me % (n // 2)) * lrows, lrows), lrows), :]

        def rows_step(t, carry):
            left = gbuf[slot, t // per_half, pl.ds(pl.multiple_of((t % per_half) * tile, tile), tile), :]
            out = pl.ds(pl.multiple_of(t * tile, tile), tile)
            acc[out, :] += lax.dot_general(left, rhs[...], (((1,), (1,)), ((), ())), preferred_element_type=jnp.float32)
            return carry
        lax.fori_loop(0, 2 * per_half, rows_step, 0)
        prod = jnp.dot(gt[:, :half_rows], gbuf[slot, 0], preferred_element_type=jnp.float32)
        prod += jnp.dot(gt[:, half_rows:], gbuf[slot, 1], preferred_element_type=jnp.float32)
        ro_ref[:, pl.ds(at, cols)] = EMA_DECAY * ro_ref[:, pl.ds(at, cols)] + (1.0 - EMA_DECAY) * prod


    dx = 1 - 2 * c
    helper = (y * side + (x + dx + side) % side) * CORES + c
    client = (y * side + (x - dx + side) % side) * CORES + c
    up = (((y + 1) % side) * side + x) * CORES + c
    down = (((y + side - 1) % side) * side + x) * CORES + c
    half_count, root_half, _ = lroot.shape
    pieces = ((0, root_half - root_half // 4), (root_half - root_half // 4, root_half // 4))

    def root_block(dy, q, p=0):
        oy, ox = (y + dy) % side, (x + 2 * q) % side
        core = c + p * (1 - 2 * c)
        return (oy * (side // 2) + ox // 2) * CORES + core, (oy * side + ox) * CORES + core

    def root_copy(peer, place, half, src=None, dst=None, recv=None, part=None, across=0):
        here = lroot.at[2 * place + half]
        if part is not None:
            here = here.at[pl.ds(*pieces[part])]
        if peer is twin and recv is None:
            recv = l_recv.at[TWIN_TURN + place // CORES]
        return pltpu.make_async_remote_copy(
            src_ref=here if src is None else src, dst_ref=here if dst is None else dst, send_sem=l_send.at[across],
            recv_sem=l_recv.at[recv] if isinstance(recv, int) else recv, device_id={"tensor": peer}, device_id_type=MESH)

    sent = [0, 0]

    def root_send(peer, place, half, part=None, across=0, **kw):
        sent[across] += root_half if part is None else pieces[part][1]
        root_copy(peer, place, half, part=part, across=across, **kw).start()

    def pair_wait(pair, sem):
        pltpu.make_async_copy(pair, pair, sem).wait()

    own_place, _ = root_block(0, 0)
    far_place, _ = root_block(0, 1)
    passing = (y * (side // 2) + ((x - dx + side) % side) // 2) * CORES + c

    def root_start_across():
        for half in (0, 1):
            root_send(helper, own_place, half, across=1, src=lr_ref.at[half], dst=relay.at[half], recv=relay_recv.at[half])

    def root_start():
        for half in (0, 1):
            root_send(up, own_place, half, src=lr_ref.at[half], recv=half)
            root_send(down, own_place, 1 - half, src=lr_ref.at[1 - half], recv=half)
        for half in (0, 1):
            root_send(twin, own_place, half, src=lr_ref.at[half])

    def root_relay(half):
        root_copy(helper, own_place, half, src=lr_ref.at[half], dst=relay.at[half], recv=relay_recv.at[half]).wait_recv()
        root_send(helper, passing, half, across=1, src=relay.at[half], recv=FAR_TURN + half)
        root_send(twin, passing, half, across=1, src=relay.at[half], dst=relay.at[2 + half], recv=relay_recv.at[2])

    def passed_rows(p):
        if p:
            pair_wait(relay.at[pl.ds(2, 2)], relay_recv.at[2])
        source = (y * side + (x - (1 - 2 * p) * dx + side) % side) * CORES + c + p * (1 - 2 * c)
        left = relay[2 * p:2 * p + 2].reshape(lrows, rows)
        do_ref[rows_of(source), :] = jnp.dot(left, xx[0], preferred_element_type=jnp.float32)

    def root_far():
        for half in (0, 1):
            pltpu.make_async_copy(lroot.at[0], lroot.at[0], l_recv.at[FAR_TURN + half]).wait()
            root_send(up, far_place, half, recv=3 + half)
            root_send(twin, far_place, half)
        for half in (1, 0):
            root_send(down, far_place, half, recv=4 - half)

    def root_round(r):
        q, stage = r // 3, r % 3
        pair_wait(lroot.at[pl.ds(0, 2)], l_recv.at[r])
        if stage == 2:
            below = above = root_block(2, q)[0]
        else:
            below, above = root_block(side - 1, q)[0], root_block(1, q)[0]
        if stage == 0:
            for peer, place, half in ((up, below, 0), (down, above, 1)):
                if q == 0:
                    root_send(peer, place, half, recv=2)
                else:
                    for part in (0, 1):
                        root_send(peer, place, half, part=part, recv=LAST_TURN + part)
        root_send(twin, below, stage % 2)
        root_send(twin, above, 1 - stage % 2)

    last_place, last_device = root_block(2, 1)
    twin_place, twin_device = root_block(2, 1, 1)

    def root_last(part):
        pair_wait(lroot.at[pl.ds(0, 2), pl.ds(*pieces[part])], l_recv.at[LAST_TURN + part])
        for half in (0, 1):
            root_send(twin, last_place, half, part=part, recv=TWIN_LAST if part else None)

    def root_last_twin(part):
        pair = lroot.at[pl.ds(2 * twin_place, 2), pl.ds(*pieces[part])]
        pair_wait(pair, l_recv.at[TWIN_LAST if part else TWIN_TURN + twin_place // CORES])

    steps(grad, gbuf, load_sem, GRAD_ROUND_STEP, [(RELAY_STEP, lambda: root_relay(0))],
          [(ROOT_ACROSS_STEP, root_start_across)], [(ROOT_START_STEP, root_start)], grad_work)

    side_cols = cols // 2

    def x_copy(h):
        at = pl.ds(h * side_cols, side_cols)
        return pltpu.make_async_remote_copy(
            src_ref=xx.at[0, :, at], dst_ref=xx.at[1, :, at], send_sem=x_send.at[h], recv_sem=x_recv.at[h],
            device_id={"tensor": helper}, device_id_type=MESH)

    with jax.named_scope("xfin"):
        xx[0] = acc[:, :cols].astype(jnp.bfloat16)
    with jax.named_scope("relay"):
        root_relay(1)
    x_copy(0).start()
    x_copy(1).start()
    with jax.named_scope("rround0"):
        root_round(0)

    def left_step(t, carry):
        at = pl.ds(pl.multiple_of(t * lrows, lrows), lrows)
        lo_ref[:, at] = EMA_DECAY * lo_ref[:, at] + (1.0 - EMA_DECAY) * acc[at, cols:].T
        return carry
    with jax.named_scope("leftfin"):
        lax.fori_loop(0, rows // lrows, left_step, 0)

    def at_step(i):
        e, p = i // 2, i % 2
        dy = lax.shift_right_logical(ROOT_Y, 2 * e) & 3
        q = lax.shift_right_logical(ROOT_X, 2 * e) & 3
        return root_block(dy, q, p)

    def twin_wait(i, place):
        @pl.when(i % 2 == 1)
        def _():
            pair_wait(lroot.at[pl.ds(2 * place, 2)], l_recv.at[TWIN_TURN + place // CORES])

    def product(place, which):
        left = lroot[pl.ds(2 * place, 2)].reshape(lrows, rows)
        return jnp.dot(left, xx[which], preferred_element_type=jnp.float32)

    def rows_of(device):
        return pl.ds(pl.multiple_of(device * lrows, lrows), lrows)

    def own_rows(i):
        place, device = at_step(i)
        do_ref[rows_of(device), :] = product(place, 0)

    def lent_copy(i, device):
        return pltpu.make_async_remote_copy(
            src_ref=lent.at[i], dst_ref=do_ref.at[rows_of(device)], send_sem=d_send.at[0], recv_sem=d_recv.at[0],
            device_id={"tensor": client}, device_id_type=MESH)

    def lent_rows(i):
        place, device = at_step(i)
        lent[i] = product(place, 1)
        lent_copy(i, device).start()

    def lent_side(i, h):
        place, _ = at_step(i)
        at = pl.ds(h * side_cols, side_cols)
        left = lroot[pl.ds(2 * place, 2)].reshape(lrows, rows)
        lent[i, :, at] = jnp.dot(left, xx[1, :, at], preferred_element_type=jnp.float32)

    def lent_side_copy(i, h):
        _, device = at_step(i)
        at = pl.ds(h * side_cols, side_cols)
        return pltpu.make_async_remote_copy(
            src_ref=lent.at[i, :, at], dst_ref=do_ref.at[rows_of(device), at], send_sem=d_send.at[0], recv_sem=d_recv.at[0],
            device_id={"tensor": client}, device_id_type=MESH)

    def loop(lo, hi, body):
        def step(i, carry):
            body(i)
            return carry
        lax.fori_loop(lo, hi, step, 0)

    def first_own(i):
        @pl.when(i == 2)
        def _():
            with jax.named_scope("far"):
                root_far()
            with jax.named_scope("rround1"):
                root_round(1)

        @pl.when(i == 8)
        def _():
            with jax.named_scope("rround2"):
                root_round(2)
        twin_wait(i, at_step(i)[0])
        own_rows(i)

    loop(0, 10, first_own)
    passed_rows(0)
    passed_rows(1)
    with jax.named_scope("x0wait"):
        x_copy(0).wait_recv()
    def lent_step(j):
        return j + (j + 7) // 8 + j // 5

    loop(0, 8, lambda j: lent_side(lent_step(j), 0))
    x_copy(0).wait_send()
    with jax.named_scope("x1sent"):
        x_copy(1).wait_send()
    pl.semaphore_signal(x_gone, inc=1, device_id={"tensor": twin}, device_id_type=MESH)
    with jax.named_scope("xgone"):
        pl.semaphore_wait(x_gone, 1)
    loop(0, 8, lambda j: lent_side_copy(lent_step(j), 0).start())
    with jax.named_scope("rround3"):
        root_round(3)
    with jax.named_scope("x1wait"):
        x_copy(1).wait_recv()

    def second_side(j):
        i = lent_step(j)
        lent_side(i, 1)
        lent_side_copy(i, 1).start()
    loop(0, 8, second_side)
    with jax.named_scope("rround4"):
        root_round(4)

    def both(i):
        twin_wait(i, at_step(i)[0])
        lent_rows(i)
        own_rows(i)
    with jax.named_scope("both"):
        loop(10, 14, both)

    def lent_piece(i, place, device, part):
        first, count = pieces[part]
        left = jnp.concatenate([lroot[2 * place, pl.ds(first, count), :], lroot[2 * place + 1, pl.ds(first, count), :]], axis=0)
        prod = jnp.dot(left, xx[1], preferred_element_type=jnp.float32)
        for half in (0, 1):
            at = half * root_half + first
            lent[i, pl.ds(at, count), :] = prod[half * count:(half + 1) * count]
            pltpu.make_async_remote_copy(
                src_ref=lent.at[i, pl.ds(at, count)], dst_ref=do_ref.at[pl.ds(pl.multiple_of(device * lrows, lrows) + at, count)],
                send_sem=d_send.at[0], recv_sem=d_recv.at[0], device_id={"tensor": client}, device_id_type=MESH).start()

    for part in (0, 1):
        with jax.named_scope(f"last{part}"):
            root_last(part)
        lent_piece(14, last_place, last_device, part)
    for part in (0, 1):
        with jax.named_scope(f"lasttwin{part}"):
            root_last_twin(part)
        lent_piece(15, twin_place, twin_device, part)
    loop(14, 16, own_rows)

    with jax.named_scope("drain"):
        grad.drain()
    for across, count in enumerate(sent):
        whole = lroot.at[pl.ds(0, count // root_half)]
        pltpu.make_async_copy(whole, whole, l_send.at[across]).wait()
    given = lent.at[pl.ds(0, half_count // 2 - 2)]
    pltpu.make_async_copy(given, given, d_send.at[0]).wait()
    with jax.named_scope("dwait"):
        pltpu.make_async_copy(given, given, d_recv.at[0]).wait()


def store_kernel(*refs):
    count = (len(refs) - 1) // 2
    sems = refs[-1]
    pieces = 8
    for i in range(count):
        src, dst = refs[i], refs[count + i]
        step = src.shape[0] // pieces
        for j in range(pieces):
            part = pl.ds(j * step, step)
            pltpu.make_async_copy(src.at[part], dst.at[part], sems.at[i]).start()
    for i in range(count):
        pltpu.make_async_copy(refs[i], refs[count + i], sems.at[i]).wait()


def solution(mesh):
    row_spec = P(("layer", "tensor"), None)
    col_spec = P("layer", "tensor")
    n = mesh.shape["tensor"]
    side = math.isqrt(n // CORES)

    def local_step(g, l, r, lr, rr):
        rows, cols = g.shape
        lrows = l.shape[0]
        kept = n // 2
        hbm = pl.BlockSpec(memory_space=pltpu.HBM)
        vmem = pl.BlockSpec(memory_space=pltpu.VMEM)
        operands = [g.reshape(2, rows // 2, cols), l, r, lr.reshape(2, lrows // 2, rows), rr]
        left_new, right_new, direction, _ = pl.pallas_call(
            functools.partial(kernel, n, side),
            name="shampoo",
            out_shape=[
                pltpu.VMEM(l.shape, jnp.float32),
                pltpu.VMEM(r.shape, jnp.float32),
                pltpu.VMEM(g.shape, jnp.float32),
                pltpu.HBM((2 * n, rows // 2, cols), jnp.bfloat16),
            ],
            in_specs=[hbm] * 5,
            out_specs=[vmem, vmem, vmem, hbm],
            scratch_shapes=[
                pltpu.VMEM(rr.shape, jnp.bfloat16),
                pltpu.VMEM((cols, rows), jnp.bfloat16),
                pltpu.VMEM((rows, cols + lrows), jnp.float32),
                pltpu.VMEM((2, 2, rows // 2, cols), jnp.bfloat16),
                pltpu.VMEM((cols + lrows, cols), jnp.bfloat16),
                pltpu.VMEM((2, rows, cols), jnp.bfloat16),
                pltpu.VMEM((2 * kept, lrows // 2, rows), jnp.bfloat16),
                pltpu.VMEM((4, lrows // 2, rows), jnp.bfloat16),
                pltpu.VMEM((kept, lrows, cols), jnp.float32),
                pltpu.SemaphoreType.DMA((ROUNDS + n // 2,)),
                pltpu.SemaphoreType.DMA((1,)),
                pltpu.SemaphoreType.DMA((2,)),
                pltpu.SemaphoreType.DMA((4,)),
                pltpu.SemaphoreType.DMA((TWIN_TURN + kept // 2,)),
                pltpu.SemaphoreType.DMA((3,)),
                pltpu.SemaphoreType.DMA((2,)),
                pltpu.SemaphoreType.DMA((1,)),
                pltpu.SemaphoreType.DMA((2,)),
                pltpu.SemaphoreType.DMA((2,)),
                pltpu.SemaphoreType.DMA((1,)),
                pltpu.SemaphoreType.REGULAR,
            ],
            compiler_params=pltpu.CompilerParams(collective_id=0, has_side_effects=True, vmem_limit_bytes=48 * 2**20),
            cost_estimate=pl.CostEstimate(flops=2 * rows * cols * (2 * n * cols + 2 * rows), bytes_accessed=2 * n * rows * cols * 3, transcendentals=0),
        )(*[pltpu.with_memory_space_constraint(v, pltpu.HBM) for v in operands])
        results = [left_new, right_new, direction]
        return pl.pallas_call(
            store_kernel,
            name="store",
            out_shape=[jax.ShapeDtypeStruct(v.shape, v.dtype) for v in results],
            in_specs=[vmem] * 3,
            out_specs=[hbm] * 3,
            scratch_shapes=[pltpu.SemaphoreType.DMA((3,))],
            compiler_params=pltpu.CompilerParams(vmem_limit_bytes=1 * 2**20),
        )(*results)

    return jax.shard_map(local_step, mesh=mesh, in_specs=(col_spec, row_spec, row_spec, row_spec, row_spec), out_specs=(row_spec, row_spec, col_spec), check_vma=False)
```

```python
import functools
import math

import jax
import jax.numpy as jnp
from jax import lax
from jax.experimental import pallas as pl
from jax.experimental.pallas import tpu as pltpu
from jax.sharding import PartitionSpec as P

EMA_DECAY = 0.9
CORES = 2
MESH = pl.DeviceIdType.MESH

ORDER = [(int(a), int(b)) for a, b in zip("0310020311322312", "0003102313131222")]
def parcels(code):
    digits = [int(d) for d in code]
    return [((a, b), h) for a, b, h in zip(digits[0::3], digits[1::3], digits[2::3])]


UP = parcels("030031330131020331130230231320120220")
UP_ON = {0: parcels("030"), 2: parcels("330"), 6: parcels("130"), 7: parcels("230")}
DOWN = parcels("011010111310021110311211210321121221")
DOWN_ON = {0: parcels("011"), 6: parcels("311111"), 7: parcels("211")}
ROUNDS = len(UP)
FIRST_UP = parcels("300301200")
FIRST_DOWN = parcels("101100201")
GRAD_ROUND_STEP = [2, 2, 8, 10, 12, 14, 17, 20, 22, 26, 28, 30]
LAST_FORWARD = 7
SIDE_UP, SIDE_DOWN = 9, 10
ASIDE = 40
ROOT_START_STEP = 28
ROOT_ACROSS_STEP = 30
RELAY_STEP = 32
LATE = (2, 12, 14, 22, 26, 28, 30)


def round_of(name, offset, half):
    a, b = offset
    table, da, db = {"f+": (FIRST_UP, 3, 0), "f-": (FIRST_DOWN, 1, 0), "s+": (UP, 0, 3), "s-": (DOWN, 0, 1)}[name]
    return table.index((((a + da) % 4, (b + db) % 4), half))


def packed(values):
    return [sum(v << (2 * i) for i, v in enumerate(values[j:j + 8])) for j in (0, 8)]


FIRST_CODE = packed([o[0] for o in ORDER])
SECOND_CODE = packed([o[1] for o in ORDER])


def lookup(code, e):
    word = code[0] + (e // 8) * (code[1] - code[0])
    return lax.shift_right_logical(word, 2 * (e % 8)) & 3


ROOT_ORDER = [(0, 0), (3, 0), (1, 0), (0, 1), (2, 0), (3, 1), (1, 1), (2, 1)]
ROOT_Y = sum(o[0] << (2 * i) for i, o in enumerate(ROOT_ORDER))
FAR_TURN, LAST_TURN, TWIN_LAST, TWIN_TURN = 5, 7, 9, 10
ROOT_X = sum(o[1] << (2 * i) for i, o in enumerate(ROOT_ORDER))


def kernel(n, side, g_ref, l_ref, r_ref, lr_ref, rr_ref, lo_ref, ro_ref, do_ref, gfull,
           rr, gt, acc, gbuf, rhs, xx, lroot, relay, lent,
           g_recv, g_send, load_sem, init_sem, l_recv, relay_recv, x_recv, d_recv, l_send, x_send, d_send, x_gone):
    _, half_rows, cols = g_ref.shape
    rows = 2 * half_rows
    lrows = l_ref.shape[0]
    tile = min(1024, half_rows)
    aside_rows = half_rows * ASIDE // 128

    me = lax.axis_index("tensor")
    c = me % CORES
    chip = me // CORES
    x, y = chip % side, chip // side
    f = x + c * (y - x)
    s = y + c * (x - y)
    fstep = CORES + c * CORES * (side - 1)
    sstep = CORES * side - c * CORES * (side - 1)
    twin = me + 1 - 2 * c

    def index(df, ds):
        return ((f + df) % side) * fstep + ((s + ds) % side) * sstep + c

    def twin_index(df, ds):
        return ((s + df) % side) * sstep + ((f + ds) % side) * fstep + 1 - c

    peers = {"f+": index(1, 0), "f-": index(3, 0), "s+": index(0, 1), "s-": index(0, 3), "twin": twin}

    class Gather:
        def __init__(self, own, full, recv, send):
            self.own, self.full, self.recv, self.send_sem = own, full, recv, send
            self.sent = 0

        def copy(self, name, offset, half, part=None, turn=None):
            b = index(*offset)
            src = self.own.at[half] if offset == (0, 0) else self.full.at[2 * b + half]
            dst = self.full.at[2 * b + half]
            if part is not None:
                src, dst = src.at[pl.ds(*part)], dst.at[pl.ds(*part)]
            if turn is None:
                turn = ROUNDS + b // CORES if name == "twin" else round_of(name, offset, half)
            return pltpu.make_async_remote_copy(
                src_ref=src, dst_ref=dst, send_sem=self.send_sem.at[0], recv_sem=self.recv.at[turn],
                device_id={"tensor": peers[name]}, device_id_type=MESH)

        def send(self, name, offset, half):
            self.sent += 1
            self.copy(name, offset, half).start()

        def wait(self, turn, count):
            taken = self.full.at[pl.ds(0, count)]
            pltpu.make_async_copy(taken, taken, self.recv.at[turn]).wait()

        def start(self):
            for half in (0, 1):
                for name in ("f+", "s+"):
                    self.send(name, (0, 0), half)
                for name in ("f-", "s-"):
                    self.send(name, (0, 0), 1 - half)
            for half in (0, 1):
                self.send("twin", (0, 0), half)

        def round(self, r):
            first = r < len(FIRST_UP)
            self.wait(r, 4 if first else 2)
            if first:
                above, below = FIRST_UP[r], FIRST_DOWN[r]
                if r == 0:
                    self.send("f+", *above)
                    self.send("f-", *below)
                self.send("s+", *above)
                self.send("s-", *below)
                self.send("s+", *below)
                self.send("s-", *above)
                self.send("twin", *above)
                self.send("twin", *below)
            for name, table in (("s+", UP_ON), ("s-", DOWN_ON)):
                for parcel in table.get(r, ()):
                    if r == LAST_FORWARD:
                        self.forward_last(name, *parcel)
                    else:
                        self.send(name, *parcel)
            if r == SIDE_UP:
                self.aside("f+", *UP[r])
            if r == SIDE_DOWN:
                self.aside("f-", *DOWN[r])
            self.send("twin", *UP[r])
            self.send("twin", *DOWN[r])

        def forward_last(self, name, offset, half):
            self.sent += 1
            pl.when(c == 0)(lambda: self.copy(name, offset, half, part=(0, half_rows - aside_rows)).start())
            pl.when(c == 1)(lambda: self.copy(name, offset, half).start())

        def aside(self, name, offset, half):
            part = (half_rows - aside_rows, aside_rows)
            pl.when(c == 0)(lambda: self.copy(name, offset, half, part=part, turn=ROUNDS - 1).start())

        def drain(self):
            whole = self.full.at[pl.ds(0, self.sent)]
            pltpu.make_async_copy(whole, whole, self.send_sem.at[0]).wait()

    grad = Gather(g_ref, gfull, g_recv, g_send)

    def block_of(k):
        e, other = k // 2, k % 2
        df, ds = lookup(FIRST_CODE, e), lookup(SECOND_CODE, e)
        mine = index(df, ds)
        return mine + other * (twin_index(df, ds) - mine)

    def load(gather, buf, k, sem):
        b = block_of(k)
        return pltpu.make_async_copy(gather.full.at[pl.ds(2 * b, 2)], buf.at[k % 2], sem.at[k % 2])

    def one_of(k, values):
        found = k == values[0]
        for v in values[1:]:
            found = found | (k == v)
        return found

    def steps(gather, buf, sem, round_step, early, between, after, work):
        def at_steps(k, actions):
            for at, action in actions:
                pl.when(k == at)(action)

        def step(k, carry):
            at_steps(k, early)

            @pl.when((k % 2 == 1) & (k < n))
            def _():
                with jax.named_scope("twinwait"):
                    gather.wait(ROUNDS + block_of(k) // CORES, 2)

            @pl.when(jnp.logical_not(one_of(k, LATE)) & (k < n))
            def _():
                load(gather, buf, k, sem).start()
            with jax.named_scope("loadwait"):
                load(gather, buf, k - 1, sem).wait()
            with jax.named_scope("work"):
                work((k - 1) % 2, block_of(k - 1))
            at_steps(k, between)
            for r in range(ROUNDS):
                @pl.when(k == round_step[r])
                def _():
                    with jax.named_scope(f"ground{r}"):
                        gather.round(r)
            at_steps(k, after)

            @pl.when(one_of(k, LATE))
            def _():
                load(gather, buf, k, sem).start()
            return carry
        lax.fori_loop(1, n + 1, step, 0)

    first = [
        pltpu.make_async_copy(rr_ref, rr, init_sem.at[0]),
        pltpu.make_async_copy(r_ref, ro_ref, init_sem.at[1]),
        pltpu.make_async_copy(l_ref, lo_ref, init_sem.at[2]),
        pltpu.make_async_copy(lr_ref, lroot.at[pl.ds(2 * ((y * (side // 2) + x // 2) * CORES + c), 2)], init_sem.at[3]),
    ]
    own_load = pltpu.make_async_copy(g_ref, gbuf.at[0], load_sem.at[0])
    own_load.start()

    barrier = pltpu.get_barrier_semaphore()
    for peer in peers.values():
        pl.semaphore_signal(barrier, inc=1, device_id={"tensor": peer}, device_id_type=MESH)
    with jax.named_scope("barrier"):
        pl.semaphore_wait(barrier, len(peers))
    grad.start()
    for copy in first:
        copy.start()

    acc[...] = jnp.zeros_like(acc)
    own_load.wait()
    for h in (0, 1):
        gt[:, h * half_rows:(h + 1) * half_rows] = gbuf[0, h].T
    for copy in first:
        copy.wait()
    own_load.start()

    per_half = half_rows // tile

    def grad_work(slot, b):
        at = pl.multiple_of(b * cols, cols)
        rhs[:cols] = rr[:, pl.ds(at, cols)]
        rhs[cols:] = gbuf[slot, me // (n // 2), pl.ds(pl.multiple_of((me % (n // 2)) * lrows, lrows), lrows), :]

        def rows_step(t, carry):
            left = gbuf[slot, t // per_half, pl.ds(pl.multiple_of((t % per_half) * tile, tile), tile), :]
            out = pl.ds(pl.multiple_of(t * tile, tile), tile)
            acc[out, :] += lax.dot_general(left, rhs[...], (((1,), (1,)), ((), ())), preferred_element_type=jnp.float32)
            return carry
        lax.fori_loop(0, 2 * per_half, rows_step, 0)
        prod = jnp.dot(gt[:, :half_rows], gbuf[slot, 0], preferred_element_type=jnp.float32)
        prod += jnp.dot(gt[:, half_rows:], gbuf[slot, 1], preferred_element_type=jnp.float32)
        ro_ref[:, pl.ds(at, cols)] = EMA_DECAY * ro_ref[:, pl.ds(at, cols)] + (1.0 - EMA_DECAY) * prod


    dx = 1 - 2 * c
    helper = (y * side + (x + dx + side) % side) * CORES + c
    client = (y * side + (x - dx + side) % side) * CORES + c
    up = (((y + 1) % side) * side + x) * CORES + c
    down = (((y + side - 1) % side) * side + x) * CORES + c
    half_count, root_half, _ = lroot.shape
    pieces = ((0, root_half - root_half // 4), (root_half - root_half // 4, root_half // 4))

    def root_block(dy, q, p=0):
        oy, ox = (y + dy) % side, (x + 2 * q) % side
        core = c + p * (1 - 2 * c)
        return (oy * (side // 2) + ox // 2) * CORES + core, (oy * side + ox) * CORES + core

    def root_copy(peer, place, half, src=None, dst=None, recv=None, part=None, across=0):
        here = lroot.at[2 * place + half]
        if part is not None:
            here = here.at[pl.ds(*pieces[part])]
        if peer is twin and recv is None:
            recv = l_recv.at[TWIN_TURN + place // CORES]
        return pltpu.make_async_remote_copy(
            src_ref=here if src is None else src, dst_ref=here if dst is None else dst, send_sem=l_send.at[across],
            recv_sem=l_recv.at[recv] if isinstance(recv, int) else recv, device_id={"tensor": peer}, device_id_type=MESH)

    sent = [0, 0]

    def root_send(peer, place, half, part=None, across=0, **kw):
        sent[across] += root_half if part is None else pieces[part][1]
        root_copy(peer, place, half, part=part, across=across, **kw).start()

    def uncounted(action):
        before = list(sent)
        action()
        sent[:] = before

    def pair_wait(pair, sem):
        pltpu.make_async_copy(pair, pair, sem).wait()

    own_place, _ = root_block(0, 0)
    far_place, _ = root_block(0, 1)
    passing = (y * (side // 2) + ((x - dx + side) % side) // 2) * CORES + c

    def root_start_across():
        for half in (0, 1):
            root_send(helper, own_place, half, across=1, src=lr_ref.at[half], dst=relay.at[half], recv=relay_recv.at[half])

    def root_start():
        for half in (0, 1):
            root_send(up, own_place, half, src=lr_ref.at[half], recv=half)
            root_send(down, own_place, 1 - half, src=lr_ref.at[1 - half], recv=half)
        for half in (0, 1):
            root_send(twin, own_place, half, src=lr_ref.at[half])

    def root_relay(half):
        root_copy(helper, own_place, half, src=lr_ref.at[half], dst=relay.at[half], recv=relay_recv.at[half]).wait_recv()
        root_send(helper, passing, half, across=1, src=relay.at[half], recv=FAR_TURN + half)
        root_send(twin, passing, half, across=1, src=relay.at[half], dst=relay.at[2 + half], recv=relay_recv.at[2])

    def passed_rows(p):
        if p:
            pair_wait(relay.at[pl.ds(2, 2)], relay_recv.at[2])
        source = (y * side + (x - (1 - 2 * p) * dx + side) % side) * CORES + c + p * (1 - 2 * c)
        left = relay[2 * p:2 * p + 2].reshape(lrows, rows)
        do_ref[rows_of(source), :] = jnp.dot(left, xx[0], preferred_element_type=jnp.float32)

    def root_far():
        for half in (0, 1):
            pltpu.make_async_copy(lroot.at[0], lroot.at[0], l_recv.at[FAR_TURN + half]).wait()
            root_send(up, far_place, half, recv=3 + half)
            root_send(twin, far_place, half)
        for half in (1, 0):
            root_send(down, far_place, half, recv=4 - half)

    def root_round(r):
        q, stage = r // 3, r % 3
        pair_wait(lroot.at[pl.ds(0, 2)], l_recv.at[r])
        if stage == 2:
            below = above = root_block(2, q)[0]
        else:
            below, above = root_block(side - 1, q)[0], root_block(1, q)[0]
        if stage == 0:
            for peer, place, half in ((up, below, 0), (down, above, 1)):
                if q == 0:
                    root_send(peer, place, half, recv=2)
                else:
                    for part in (0, 1):
                        root_send(peer, place, half, part=part, recv=LAST_TURN + part)
        root_send(twin, below, stage % 2)
        root_send(twin, above, 1 - stage % 2)

    last_place, last_device = root_block(2, 1)
    twin_place, twin_device = root_block(2, 1, 1)

    def root_last(part):
        pair_wait(lroot.at[pl.ds(0, 2), pl.ds(*pieces[part])], l_recv.at[LAST_TURN + part])
        for half in (0, 1):
            root_send(twin, last_place, half, part=part, recv=TWIN_LAST if part else None)

    def root_last_twin(part):
        pair = lroot.at[pl.ds(2 * twin_place, 2), pl.ds(*pieces[part])]
        pair_wait(pair, l_recv.at[TWIN_LAST if part else TWIN_TURN + twin_place // CORES])

    steps(grad, gbuf, load_sem, GRAD_ROUND_STEP, [(RELAY_STEP, lambda: root_relay(0))],
          [(ROOT_ACROSS_STEP, root_start_across), (ROOT_ACROSS_STEP, lambda: pl.when(c == 1)(lambda: uncounted(root_start)))],
          [(ROOT_START_STEP, lambda: pl.when(c == 0)(root_start))], grad_work)

    side_cols = cols // 2

    def x_copy(h):
        at = pl.ds(h * side_cols, side_cols)
        return pltpu.make_async_remote_copy(
            src_ref=xx.at[0, :, at], dst_ref=xx.at[1, :, at], send_sem=x_send.at[h], recv_sem=x_recv.at[h],
            device_id={"tensor": helper}, device_id_type=MESH)

    with jax.named_scope("xfin"):
        xx[0] = acc[:, :cols].astype(jnp.bfloat16)
    with jax.named_scope("relay"):
        root_relay(1)
    x_copy(0).start()
    x_copy(1).start()
    with jax.named_scope("rround0"):
        root_round(0)

    def left_step(t, carry):
        at = pl.ds(pl.multiple_of(t * lrows, lrows), lrows)
        lo_ref[:, at] = EMA_DECAY * lo_ref[:, at] + (1.0 - EMA_DECAY) * acc[at, cols:].T
        return carry
    with jax.named_scope("leftfin"):
        lax.fori_loop(0, rows // lrows, left_step, 0)

    def at_step(i):
        e, p = i // 2, i % 2
        dy = lax.shift_right_logical(ROOT_Y, 2 * e) & 3
        q = lax.shift_right_logical(ROOT_X, 2 * e) & 3
        return root_block(dy, q, p)

    def twin_wait(i, place):
        @pl.when(i % 2 == 1)
        def _():
            pair_wait(lroot.at[pl.ds(2 * place, 2)], l_recv.at[TWIN_TURN + place // CORES])

    def product(place, which):
        left = lroot[pl.ds(2 * place, 2)].reshape(lrows, rows)
        return jnp.dot(left, xx[which], preferred_element_type=jnp.float32)

    def rows_of(device):
        return pl.ds(pl.multiple_of(device * lrows, lrows), lrows)

    def own_rows(i):
        place, device = at_step(i)
        do_ref[rows_of(device), :] = product(place, 0)

    def lent_copy(i, device):
        return pltpu.make_async_remote_copy(
            src_ref=lent.at[i], dst_ref=do_ref.at[rows_of(device)], send_sem=d_send.at[0], recv_sem=d_recv.at[0],
            device_id={"tensor": client}, device_id_type=MESH)

    def lent_rows(i):
        place, device = at_step(i)
        lent[i] = product(place, 1)
        lent_copy(i, device).start()

    def lent_side(i, h):
        place, _ = at_step(i)
        at = pl.ds(h * side_cols, side_cols)
        left = lroot[pl.ds(2 * place, 2)].reshape(lrows, rows)
        lent[i, :, at] = jnp.dot(left, xx[1, :, at], preferred_element_type=jnp.float32)

    def lent_side_copy(i, h):
        _, device = at_step(i)
        at = pl.ds(h * side_cols, side_cols)
        return pltpu.make_async_remote_copy(
            src_ref=lent.at[i, :, at], dst_ref=do_ref.at[rows_of(device), at], send_sem=d_send.at[0], recv_sem=d_recv.at[0],
            device_id={"tensor": client}, device_id_type=MESH)

    def loop(lo, hi, body):
        def step(i, carry):
            body(i)
            return carry
        lax.fori_loop(lo, hi, step, 0)

    def first_own(i):
        @pl.when(i == 2)
        def _():
            with jax.named_scope("far"):
                root_far()
            with jax.named_scope("rround1"):
                root_round(1)

        @pl.when(i == 8)
        def _():
            with jax.named_scope("rround2"):
                root_round(2)
        twin_wait(i, at_step(i)[0])
        own_rows(i)

    loop(0, 10, first_own)
    passed_rows(0)
    passed_rows(1)
    with jax.named_scope("x0wait"):
        x_copy(0).wait_recv()
    def lent_step(j):
        return j + (j + 7) // 8 + j // 5

    loop(0, 8, lambda j: lent_side(lent_step(j), 0))
    x_copy(0).wait_send()
    with jax.named_scope("x1sent"):
        x_copy(1).wait_send()
    pl.semaphore_signal(x_gone, inc=1, device_id={"tensor": twin}, device_id_type=MESH)
    with jax.named_scope("xgone"):
        pl.semaphore_wait(x_gone, 1)
    loop(0, 8, lambda j: lent_side_copy(lent_step(j), 0).start())
    with jax.named_scope("rround3"):
        root_round(3)
    with jax.named_scope("x1wait"):
        x_copy(1).wait_recv()

    def second_side(j):
        i = lent_step(j)
        lent_side(i, 1)
        lent_side_copy(i, 1).start()
    loop(0, 8, second_side)
    with jax.named_scope("rround4"):
        root_round(4)

    def both(i):
        twin_wait(i, at_step(i)[0])
        lent_rows(i)
        own_rows(i)
    with jax.named_scope("both"):
        loop(10, 14, both)

    def lent_piece(i, place, device, part):
        first, count = pieces[part]
        left = jnp.concatenate([lroot[2 * place, pl.ds(first, count), :], lroot[2 * place + 1, pl.ds(first, count), :]], axis=0)
        prod = jnp.dot(left, xx[1], preferred_element_type=jnp.float32)
        for half in (0, 1):
            at = half * root_half + first
            lent[i, pl.ds(at, count), :] = prod[half * count:(half + 1) * count]
            pltpu.make_async_remote_copy(
                src_ref=lent.at[i, pl.ds(at, count)], dst_ref=do_ref.at[pl.ds(pl.multiple_of(device * lrows, lrows) + at, count)],
                send_sem=d_send.at[0], recv_sem=d_recv.at[0], device_id={"tensor": client}, device_id_type=MESH).start()

    def own_piece(part):
        with jax.named_scope(f"last{part}"):
            root_last(part)
        lent_piece(14, last_place, last_device, part)

    def twin_piece(part):
        with jax.named_scope(f"lasttwin{part}"):
            root_last_twin(part)
        lent_piece(15, twin_place, twin_device, part)

    @pl.when(c == 0)
    def _():
        own_piece(0)
        own_piece(1)
        twin_piece(0)
        twin_piece(1)

    @pl.when(c == 1)
    def _():
        uncounted(lambda: own_piece(0))
        twin_piece(0)
        twin_piece(1)
        uncounted(lambda: own_piece(1))

    loop(14, 16, own_rows)

    with jax.named_scope("drain"):
        grad.drain()
    for across, count in enumerate(sent):
        whole = lroot.at[pl.ds(0, count // root_half)]
        pltpu.make_async_copy(whole, whole, l_send.at[across]).wait()
    given = lent.at[pl.ds(0, half_count // 2 - 2)]
    pltpu.make_async_copy(given, given, d_send.at[0]).wait()
    with jax.named_scope("dwait"):
        pltpu.make_async_copy(given, given, d_recv.at[0]).wait()


def store_kernel(*refs):
    count = (len(refs) - 1) // 2
    sems = refs[-1]
    pieces = 8
    for i in range(count):
        src, dst = refs[i], refs[count + i]
        step = src.shape[0] // pieces
        for j in range(pieces):
            part = pl.ds(j * step, step)
            pltpu.make_async_copy(src.at[part], dst.at[part], sems.at[i]).start()
    for i in range(count):
        pltpu.make_async_copy(refs[i], refs[count + i], sems.at[i]).wait()


def solution(mesh):
    row_spec = P(("layer", "tensor"), None)
    col_spec = P("layer", "tensor")
    n = mesh.shape["tensor"]
    side = math.isqrt(n // CORES)

    def local_step(g, l, r, lr, rr):
        rows, cols = g.shape
        lrows = l.shape[0]
        kept = n // 2
        hbm = pl.BlockSpec(memory_space=pltpu.HBM)
        vmem = pl.BlockSpec(memory_space=pltpu.VMEM)
        operands = [g.reshape(2, rows // 2, cols), l, r, lr.reshape(2, lrows // 2, rows), rr]
        left_new, right_new, direction, _ = pl.pallas_call(
            functools.partial(kernel, n, side),
            name="shampoo",
            out_shape=[
                pltpu.VMEM(l.shape, jnp.float32),
                pltpu.VMEM(r.shape, jnp.float32),
                pltpu.VMEM(g.shape, jnp.float32),
                pltpu.HBM((2 * n, rows // 2, cols), jnp.bfloat16),
            ],
            in_specs=[hbm] * 5,
            out_specs=[vmem, vmem, vmem, hbm],
            scratch_shapes=[
                pltpu.VMEM(rr.shape, jnp.bfloat16),
                pltpu.VMEM((cols, rows), jnp.bfloat16),
                pltpu.VMEM((rows, cols + lrows), jnp.float32),
                pltpu.VMEM((2, 2, rows // 2, cols), jnp.bfloat16),
                pltpu.VMEM((cols + lrows, cols), jnp.bfloat16),
                pltpu.VMEM((2, rows, cols), jnp.bfloat16),
                pltpu.VMEM((2 * kept, lrows // 2, rows), jnp.bfloat16),
                pltpu.VMEM((4, lrows // 2, rows), jnp.bfloat16),
                pltpu.VMEM((kept, lrows, cols), jnp.float32),
                pltpu.SemaphoreType.DMA((ROUNDS + n // 2,)),
                pltpu.SemaphoreType.DMA((1,)),
                pltpu.SemaphoreType.DMA((2,)),
                pltpu.SemaphoreType.DMA((4,)),
                pltpu.SemaphoreType.DMA((TWIN_TURN + kept // 2,)),
                pltpu.SemaphoreType.DMA((3,)),
                pltpu.SemaphoreType.DMA((2,)),
                pltpu.SemaphoreType.DMA((1,)),
                pltpu.SemaphoreType.DMA((2,)),
                pltpu.SemaphoreType.DMA((2,)),
                pltpu.SemaphoreType.DMA((1,)),
                pltpu.SemaphoreType.REGULAR,
            ],
            compiler_params=pltpu.CompilerParams(collective_id=0, has_side_effects=True, vmem_limit_bytes=48 * 2**20),
            cost_estimate=pl.CostEstimate(flops=2 * rows * cols * (2 * n * cols + 2 * rows), bytes_accessed=2 * n * rows * cols * 3, transcendentals=0),
        )(*[pltpu.with_memory_space_constraint(v, pltpu.HBM) for v in operands])
        results = [left_new, right_new, direction]
        return pl.pallas_call(
            store_kernel,
            name="store",
            out_shape=[jax.ShapeDtypeStruct(v.shape, v.dtype) for v in results],
            in_specs=[vmem] * 3,
            out_specs=[hbm] * 3,
            scratch_shapes=[pltpu.SemaphoreType.DMA((3,))],
            compiler_params=pltpu.CompilerParams(vmem_limit_bytes=1 * 2**20),
        )(*results)

    return jax.shard_map(local_step, mesh=mesh, in_specs=(col_spec, row_spec, row_spec, row_spec, row_spec), out_specs=(row_spec, row_spec, col_spec), check_vma=False)
```

```python
import functools
import math

import jax
import jax.numpy as jnp
from jax import lax
from jax.experimental import pallas as pl
from jax.experimental.pallas import tpu as pltpu
from jax.sharding import PartitionSpec as P

EMA_DECAY = 0.9
CORES = 2
MESH = pl.DeviceIdType.MESH

ORDER = [(int(a), int(b)) for a, b in zip("0310020311322312", "0003102313131222")]
def parcels(code):
    digits = [int(d) for d in code]
    return [((a, b), h) for a, b, h in zip(digits[0::3], digits[1::3], digits[2::3])]


UP = parcels("030031330131020331130230231320120220")
UP_ON = {0: parcels("030"), 2: parcels("330"), 6: parcels("130"), 7: parcels("230")}
DOWN = parcels("011010111310021110311211210321121221")
DOWN_ON = {0: parcels("011"), 6: parcels("311111"), 7: parcels("211")}
ROUNDS = len(UP)
FIRST_UP = parcels("300301200")
FIRST_DOWN = parcels("101100201")
GRAD_ROUND_STEP = [2, 2, 8, 10, 12, 14, 17, 20, 22, 26, 28, 30]
LAST_FORWARD = 7
SIDE_UP, SIDE_DOWN = 9, 10
ASIDE = 30
ROOT_START_STEP = 28
ROOT_ACROSS_STEP = 30
RELAY_STEP = 32
LATE = (2, 12, 14, 22, 26, 28, 30)


def round_of(name, offset, half):
    a, b = offset
    table, da, db = {"f+": (FIRST_UP, 3, 0), "f-": (FIRST_DOWN, 1, 0), "s+": (UP, 0, 3), "s-": (DOWN, 0, 1)}[name]
    return table.index((((a + da) % 4, (b + db) % 4), half))


def packed(values):
    return [sum(v << (2 * i) for i, v in enumerate(values[j:j + 8])) for j in (0, 8)]


FIRST_CODE = packed([o[0] for o in ORDER])
SECOND_CODE = packed([o[1] for o in ORDER])


def lookup(code, e):
    word = code[0] + (e // 8) * (code[1] - code[0])
    return lax.shift_right_logical(word, 2 * (e % 8)) & 3


ROOT_ORDER = [(0, 0), (3, 0), (1, 0), (0, 1), (2, 0), (3, 1), (1, 1), (2, 1)]
ROOT_Y = sum(o[0] << (2 * i) for i, o in enumerate(ROOT_ORDER))
FAR_TURN, LAST_TURN, TWIN_LAST, TWIN_TURN = 5, 7, 9, 10
ROOT_X = sum(o[1] << (2 * i) for i, o in enumerate(ROOT_ORDER))


def kernel(n, side, g_ref, l_ref, r_ref, lr_ref, rr_ref, lo_ref, ro_ref, do_ref, gfull,
           rr, gt, acc, gbuf, rhs, xx, lroot, relay, lent,
           g_recv, g_send, load_sem, init_sem, l_recv, relay_recv, x_recv, d_recv, l_send, x_send, d_send, x_gone):
    _, half_rows, cols = g_ref.shape
    rows = 2 * half_rows
    lrows = l_ref.shape[0]
    tile = min(1024, half_rows)
    aside_rows = half_rows * ASIDE // 128

    me = lax.axis_index("tensor")
    c = me % CORES
    chip = me // CORES
    x, y = chip % side, chip // side
    f = x + c * (y - x)
    s = y + c * (x - y)
    fstep = CORES + c * CORES * (side - 1)
    sstep = CORES * side - c * CORES * (side - 1)
    twin = me + 1 - 2 * c

    def index(df, ds):
        return ((f + df) % side) * fstep + ((s + ds) % side) * sstep + c

    def twin_index(df, ds):
        return ((s + df) % side) * sstep + ((f + ds) % side) * fstep + 1 - c

    peers = {"f+": index(1, 0), "f-": index(3, 0), "s+": index(0, 1), "s-": index(0, 3), "twin": twin}

    class Gather:
        def __init__(self, own, full, recv, send):
            self.own, self.full, self.recv, self.send_sem = own, full, recv, send
            self.sent = 0

        def copy(self, name, offset, half, part=None, turn=None):
            b = index(*offset)
            src = self.own.at[half] if offset == (0, 0) else self.full.at[2 * b + half]
            dst = self.full.at[2 * b + half]
            if part is not None:
                src, dst = src.at[pl.ds(*part)], dst.at[pl.ds(*part)]
            if turn is None:
                turn = ROUNDS + b // CORES if name == "twin" else round_of(name, offset, half)
            return pltpu.make_async_remote_copy(
                src_ref=src, dst_ref=dst, send_sem=self.send_sem.at[0], recv_sem=self.recv.at[turn],
                device_id={"tensor": peers[name]}, device_id_type=MESH)

        def send(self, name, offset, half):
            self.sent += 1
            self.copy(name, offset, half).start()

        def wait(self, turn, count):
            taken = self.full.at[pl.ds(0, count)]
            pltpu.make_async_copy(taken, taken, self.recv.at[turn]).wait()

        def start(self):
            for half in (0, 1):
                for name in ("f+", "s+"):
                    self.send(name, (0, 0), half)
                for name in ("f-", "s-"):
                    self.send(name, (0, 0), 1 - half)
            for half in (0, 1):
                self.send("twin", (0, 0), half)

        def round(self, r):
            first = r < len(FIRST_UP)
            self.wait(r, 4 if first else 2)
            if first:
                above, below = FIRST_UP[r], FIRST_DOWN[r]
                if r == 0:
                    self.send("f+", *above)
                    self.send("f-", *below)
                self.send("s+", *above)
                self.send("s-", *below)
                self.send("s+", *below)
                self.send("s-", *above)
                self.send("twin", *above)
                self.send("twin", *below)
            for name, table in (("s+", UP_ON), ("s-", DOWN_ON)):
                for parcel in table.get(r, ()):
                    if r == LAST_FORWARD:
                        self.forward_last(name, *parcel)
                    else:
                        self.send(name, *parcel)
            if r == SIDE_UP:
                self.aside("f+", *UP[r])
            if r == SIDE_DOWN:
                self.aside("f-", *DOWN[r])
            self.send("twin", *UP[r])
            self.send("twin", *DOWN[r])

        def forward_last(self, name, offset, half):
            self.sent += 1
            pl.when(c == 0)(lambda: self.copy(name, offset, half, part=(0, half_rows - aside_rows)).start())
            pl.when(c == 1)(lambda: self.copy(name, offset, half).start())

        def aside(self, name, offset, half):
            part = (half_rows - aside_rows, aside_rows)
            pl.when(c == 0)(lambda: self.copy(name, offset, half, part=part, turn=ROUNDS - 1).start())

        def drain(self):
            whole = self.full.at[pl.ds(0, self.sent)]
            pltpu.make_async_copy(whole, whole, self.send_sem.at[0]).wait()

    grad = Gather(g_ref, gfull, g_recv, g_send)

    def block_of(k):
        e, other = k // 2, k % 2
        df, ds = lookup(FIRST_CODE, e), lookup(SECOND_CODE, e)
        mine = index(df, ds)
        return mine + other * (twin_index(df, ds) - mine)

    def load(gather, buf, k, sem):
        b = block_of(k)
        return pltpu.make_async_copy(gather.full.at[pl.ds(2 * b, 2)], buf.at[k % 2], sem.at[k % 2])

    def one_of(k, values):
        found = k == values[0]
        for v in values[1:]:
            found = found | (k == v)
        return found

    def steps(gather, buf, sem, round_step, early, between, after, work):
        def at_steps(k, actions):
            for at, action in actions:
                pl.when(k == at)(action)

        def step(k, carry):
            at_steps(k, early)

            @pl.when((k % 2 == 1) & (k < n))
            def _():
                with jax.named_scope("twinwait"):
                    gather.wait(ROUNDS + block_of(k) // CORES, 2)

            @pl.when(jnp.logical_not(one_of(k, LATE)) & (k < n))
            def _():
                load(gather, buf, k, sem).start()
            with jax.named_scope("loadwait"):
                load(gather, buf, k - 1, sem).wait()
            with jax.named_scope("work"):
                work((k - 1) % 2, block_of(k - 1))
            at_steps(k, between)
            for r in range(ROUNDS):
                @pl.when(k == round_step[r])
                def _():
                    with jax.named_scope(f"ground{r}"):
                        gather.round(r)
            at_steps(k, after)

            @pl.when(one_of(k, LATE))
            def _():
                load(gather, buf, k, sem).start()
            return carry
        lax.fori_loop(1, n + 1, step, 0)

    first = [
        pltpu.make_async_copy(rr_ref, rr, init_sem.at[0]),
        pltpu.make_async_copy(r_ref, ro_ref, init_sem.at[1]),
        pltpu.make_async_copy(l_ref, lo_ref, init_sem.at[2]),
        pltpu.make_async_copy(lr_ref, lroot.at[pl.ds(2 * ((y * (side // 2) + x // 2) * CORES + c), 2)], init_sem.at[3]),
    ]
    own_load = pltpu.make_async_copy(g_ref, gbuf.at[0], load_sem.at[0])
    own_load.start()

    barrier = pltpu.get_barrier_semaphore()
    for peer in peers.values():
        pl.semaphore_signal(barrier, inc=1, device_id={"tensor": peer}, device_id_type=MESH)
    with jax.named_scope("barrier"):
        pl.semaphore_wait(barrier, len(peers))
    grad.start()
    for copy in first:
        copy.start()

    acc[...] = jnp.zeros_like(acc)
    own_load.wait()
    for h in (0, 1):
        gt[:, h * half_rows:(h + 1) * half_rows] = gbuf[0, h].T
    for copy in first:
        copy.wait()
    own_load.start()

    per_half = half_rows // tile

    def grad_work(slot, b):
        at = pl.multiple_of(b * cols, cols)
        rhs[:cols] = rr[:, pl.ds(at, cols)]
        rhs[cols:] = gbuf[slot, me // (n // 2), pl.ds(pl.multiple_of((me % (n // 2)) * lrows, lrows), lrows), :]

        def rows_step(t, carry):
            left = gbuf[slot, t // per_half, pl.ds(pl.multiple_of((t % per_half) * tile, tile), tile), :]
            out = pl.ds(pl.multiple_of(t * tile, tile), tile)
            acc[out, :] += lax.dot_general(left, rhs[...], (((1,), (1,)), ((), ())), preferred_element_type=jnp.float32)
            return carry
        lax.fori_loop(0, 2 * per_half, rows_step, 0)
        prod = jnp.dot(gt[:, :half_rows], gbuf[slot, 0], preferred_element_type=jnp.float32)
        prod += jnp.dot(gt[:, half_rows:], gbuf[slot, 1], preferred_element_type=jnp.float32)
        ro_ref[:, pl.ds(at, cols)] = EMA_DECAY * ro_ref[:, pl.ds(at, cols)] + (1.0 - EMA_DECAY) * prod


    dx = 1 - 2 * c
    helper = (y * side + (x + dx + side) % side) * CORES + c
    client = (y * side + (x - dx + side) % side) * CORES + c
    up = (((y + 1) % side) * side + x) * CORES + c
    down = (((y + side - 1) % side) * side + x) * CORES + c
    half_count, root_half, _ = lroot.shape
    pieces = ((0, root_half - root_half // 4), (root_half - root_half // 4, root_half // 4))

    def root_block(dy, q, p=0):
        oy, ox = (y + dy) % side, (x + 2 * q) % side
        core = c + p * (1 - 2 * c)
        return (oy * (side // 2) + ox // 2) * CORES + core, (oy * side + ox) * CORES + core

    def root_copy(peer, place, half, src=None, dst=None, recv=None, part=None, across=0):
        here = lroot.at[2 * place + half]
        if part is not None:
            here = here.at[pl.ds(*pieces[part])]
        if peer is twin and recv is None:
            recv = l_recv.at[TWIN_TURN + place // CORES]
        return pltpu.make_async_remote_copy(
            src_ref=here if src is None else src, dst_ref=here if dst is None else dst, send_sem=l_send.at[across],
            recv_sem=l_recv.at[recv] if isinstance(recv, int) else recv, device_id={"tensor": peer}, device_id_type=MESH)

    sent = [0, 0]

    def root_send(peer, place, half, part=None, across=0, **kw):
        sent[across] += root_half if part is None else pieces[part][1]
        root_copy(peer, place, half, part=part, across=across, **kw).start()

    def uncounted(action):
        before = list(sent)
        action()
        sent[:] = before

    def pair_wait(pair, sem):
        pltpu.make_async_copy(pair, pair, sem).wait()

    own_place, _ = root_block(0, 0)
    far_place, _ = root_block(0, 1)
    passing = (y * (side // 2) + ((x - dx + side) % side) // 2) * CORES + c

    def root_start_across():
        for half in (0, 1):
            root_send(helper, own_place, half, across=1, src=lr_ref.at[half], dst=relay.at[half], recv=relay_recv.at[half])

    def root_start():
        for half in (0, 1):
            root_send(up, own_place, half, src=lr_ref.at[half], recv=half)
            root_send(down, own_place, 1 - half, src=lr_ref.at[1 - half], recv=half)
        for half in (0, 1):
            root_send(twin, own_place, half, src=lr_ref.at[half])

    def root_relay(half):
        root_copy(helper, own_place, half, src=lr_ref.at[half], dst=relay.at[half], recv=relay_recv.at[half]).wait_recv()
        root_send(helper, passing, half, across=1, src=relay.at[half], recv=FAR_TURN + half)
        root_send(twin, passing, half, across=1, src=relay.at[half], dst=relay.at[2 + half], recv=relay_recv.at[2])

    def passed_rows(p):
        if p:
            pair_wait(relay.at[pl.ds(2, 2)], relay_recv.at[2])
        source = (y * side + (x - (1 - 2 * p) * dx + side) % side) * CORES + c + p * (1 - 2 * c)
        left = relay[2 * p:2 * p + 2].reshape(lrows, rows)
        do_ref[rows_of(source), :] = jnp.dot(left, xx[0], preferred_element_type=jnp.float32)

    def root_far():
        for half in (0, 1):
            pltpu.make_async_copy(lroot.at[0], lroot.at[0], l_recv.at[FAR_TURN + half]).wait()
            root_send(up, far_place, half, recv=3 + half)
            root_send(twin, far_place, half)
        for half in (1, 0):
            root_send(down, far_place, half, recv=4 - half)

    def root_round(r):
        q, stage = r // 3, r % 3
        pair_wait(lroot.at[pl.ds(0, 2)], l_recv.at[r])
        if stage == 2:
            below = above = root_block(2, q)[0]
        else:
            below, above = root_block(side - 1, q)[0], root_block(1, q)[0]
        if stage == 0:
            for peer, place, half in ((up, below, 0), (down, above, 1)):
                if q == 0:
                    root_send(peer, place, half, recv=2)
                else:
                    for part in (0, 1):
                        root_send(peer, place, half, part=part, recv=LAST_TURN + part)
        root_send(twin, below, stage % 2)
        root_send(twin, above, 1 - stage % 2)

    last_place, last_device = root_block(2, 1)
    twin_place, twin_device = root_block(2, 1, 1)

    def root_last(part):
        pair_wait(lroot.at[pl.ds(0, 2), pl.ds(*pieces[part])], l_recv.at[LAST_TURN + part])
        for half in (0, 1):
            root_send(twin, last_place, half, part=part, recv=TWIN_LAST if part else None)

    def root_last_twin(part):
        pair = lroot.at[pl.ds(2 * twin_place, 2), pl.ds(*pieces[part])]
        pair_wait(pair, l_recv.at[TWIN_LAST if part else TWIN_TURN + twin_place // CORES])

    steps(grad, gbuf, load_sem, GRAD_ROUND_STEP, [(RELAY_STEP, lambda: root_relay(0))],
          [(ROOT_ACROSS_STEP, root_start_across), (ROOT_ACROSS_STEP, lambda: pl.when(c == 1)(lambda: uncounted(root_start)))],
          [(ROOT_START_STEP, lambda: pl.when(c == 0)(root_start))], grad_work)

    side_cols = cols // 2

    def x_copy(h):
        at = pl.ds(h * side_cols, side_cols)
        return pltpu.make_async_remote_copy(
            src_ref=xx.at[0, :, at], dst_ref=xx.at[1, :, at], send_sem=x_send.at[h], recv_sem=x_recv.at[h],
            device_id={"tensor": helper}, device_id_type=MESH)

    with jax.named_scope("xfin"):
        xx[0] = acc[:, :cols].astype(jnp.bfloat16)
    with jax.named_scope("relay"):
        root_relay(1)
    x_copy(0).start()
    x_copy(1).start()
    with jax.named_scope("rround0"):
        root_round(0)

    def left_step(t, carry):
        at = pl.ds(pl.multiple_of(t * lrows, lrows), lrows)
        lo_ref[:, at] = EMA_DECAY * lo_ref[:, at] + (1.0 - EMA_DECAY) * acc[at, cols:].T
        return carry
    with jax.named_scope("leftfin"):
        lax.fori_loop(0, rows // lrows, left_step, 0)

    def at_step(i):
        e, p = i // 2, i % 2
        dy = lax.shift_right_logical(ROOT_Y, 2 * e) & 3
        q = lax.shift_right_logical(ROOT_X, 2 * e) & 3
        return root_block(dy, q, p)

    def twin_wait(i, place):
        @pl.when(i % 2 == 1)
        def _():
            pair_wait(lroot.at[pl.ds(2 * place, 2)], l_recv.at[TWIN_TURN + place // CORES])

    def product(place, which):
        left = lroot[pl.ds(2 * place, 2)].reshape(lrows, rows)
        return jnp.dot(left, xx[which], preferred_element_type=jnp.float32)

    def rows_of(device):
        return pl.ds(pl.multiple_of(device * lrows, lrows), lrows)

    def own_rows(i):
        place, device = at_step(i)
        do_ref[rows_of(device), :] = product(place, 0)

    def lent_copy(i, device):
        return pltpu.make_async_remote_copy(
            src_ref=lent.at[i], dst_ref=do_ref.at[rows_of(device)], send_sem=d_send.at[0], recv_sem=d_recv.at[0],
            device_id={"tensor": client}, device_id_type=MESH)

    def lent_rows(i):
        place, device = at_step(i)
        lent[i] = product(place, 1)
        lent_copy(i, device).start()

    def lent_side(i, h):
        place, _ = at_step(i)
        at = pl.ds(h * side_cols, side_cols)
        left = lroot[pl.ds(2 * place, 2)].reshape(lrows, rows)
        lent[i, :, at] = jnp.dot(left, xx[1, :, at], preferred_element_type=jnp.float32)

    def lent_side_copy(i, h):
        _, device = at_step(i)
        at = pl.ds(h * side_cols, side_cols)
        return pltpu.make_async_remote_copy(
            src_ref=lent.at[i, :, at], dst_ref=do_ref.at[rows_of(device), at], send_sem=d_send.at[0], recv_sem=d_recv.at[0],
            device_id={"tensor": client}, device_id_type=MESH)

    def loop(lo, hi, body):
        def step(i, carry):
            body(i)
            return carry
        lax.fori_loop(lo, hi, step, 0)

    def first_own(i):
        @pl.when(i == 2)
        def _():
            with jax.named_scope("far"):
                root_far()
            with jax.named_scope("rround1"):
                root_round(1)

        @pl.when(i == 8)
        def _():
            with jax.named_scope("rround2"):
                root_round(2)
        twin_wait(i, at_step(i)[0])
        own_rows(i)

    loop(0, 10, first_own)
    passed_rows(0)
    passed_rows(1)
    with jax.named_scope("x0wait"):
        x_copy(0).wait_recv()
    def lent_step(j):
        return j + (j + 7) // 8 + j // 5

    loop(0, 8, lambda j: lent_side(lent_step(j), 0))
    x_copy(0).wait_send()
    with jax.named_scope("x1sent"):
        x_copy(1).wait_send()
    pl.semaphore_signal(x_gone, inc=1, device_id={"tensor": twin}, device_id_type=MESH)
    with jax.named_scope("xgone"):
        pl.semaphore_wait(x_gone, 1)
    loop(0, 8, lambda j: lent_side_copy(lent_step(j), 0).start())
    with jax.named_scope("rround3"):
        root_round(3)
    with jax.named_scope("x1wait"):
        x_copy(1).wait_recv()

    def second_side(j):
        i = lent_step(j)
        lent_side(i, 1)
        lent_side_copy(i, 1).start()
    loop(0, 8, second_side)
    with jax.named_scope("rround4"):
        root_round(4)

    def both(i):
        twin_wait(i, at_step(i)[0])
        lent_rows(i)
        own_rows(i)
    with jax.named_scope("both"):
        loop(10, 14, both)

    def lent_piece(i, place, device, part):
        first, count = pieces[part]
        left = jnp.concatenate([lroot[2 * place, pl.ds(first, count), :], lroot[2 * place + 1, pl.ds(first, count), :]], axis=0)
        prod = jnp.dot(left, xx[1], preferred_element_type=jnp.float32)
        for half in (0, 1):
            at = half * root_half + first
            lent[i, pl.ds(at, count), :] = prod[half * count:(half + 1) * count]
            pltpu.make_async_remote_copy(
                src_ref=lent.at[i, pl.ds(at, count)], dst_ref=do_ref.at[pl.ds(pl.multiple_of(device * lrows, lrows) + at, count)],
                send_sem=d_send.at[0], recv_sem=d_recv.at[0], device_id={"tensor": client}, device_id_type=MESH).start()

    def own_piece(part):
        with jax.named_scope(f"last{part}"):
            root_last(part)
        lent_piece(14, last_place, last_device, part)

    def twin_piece(part):
        with jax.named_scope(f"lasttwin{part}"):
            root_last_twin(part)
        lent_piece(15, twin_place, twin_device, part)

    @pl.when(c == 0)
    def _():
        own_piece(0)
        own_piece(1)
        twin_piece(0)
        twin_piece(1)

    @pl.when(c == 1)
    def _():
        uncounted(lambda: own_piece(0))
        twin_piece(0)
        twin_piece(1)
        uncounted(lambda: own_piece(1))

    loop(14, 16, own_rows)

    with jax.named_scope("drain"):
        grad.drain()
    for across, count in enumerate(sent):
        whole = lroot.at[pl.ds(0, count // root_half)]
        pltpu.make_async_copy(whole, whole, l_send.at[across]).wait()
    given = lent.at[pl.ds(0, half_count // 2 - 2)]
    pltpu.make_async_copy(given, given, d_send.at[0]).wait()
    with jax.named_scope("dwait"):
        pltpu.make_async_copy(given, given, d_recv.at[0]).wait()


def store_kernel(*refs):
    count = (len(refs) - 1) // 2
    sems = refs[-1]
    pieces = 8
    for i in range(count):
        src, dst = refs[i], refs[count + i]
        step = src.shape[0] // pieces
        for j in range(pieces):
            part = pl.ds(j * step, step)
            pltpu.make_async_copy(src.at[part], dst.at[part], sems.at[i]).start()
    for i in range(count):
        pltpu.make_async_copy(refs[i], refs[count + i], sems.at[i]).wait()


def solution(mesh):
    row_spec = P(("layer", "tensor"), None)
    col_spec = P("layer", "tensor")
    n = mesh.shape["tensor"]
    side = math.isqrt(n // CORES)

    def local_step(g, l, r, lr, rr):
        rows, cols = g.shape
        lrows = l.shape[0]
        kept = n // 2
        hbm = pl.BlockSpec(memory_space=pltpu.HBM)
        vmem = pl.BlockSpec(memory_space=pltpu.VMEM)
        operands = [g.reshape(2, rows // 2, cols), l, r, lr.reshape(2, lrows // 2, rows), rr]
        left_new, right_new, direction, _ = pl.pallas_call(
            functools.partial(kernel, n, side),
            name="shampoo",
            out_shape=[
                pltpu.VMEM(l.shape, jnp.float32),
                pltpu.VMEM(r.shape, jnp.float32),
                pltpu.VMEM(g.shape, jnp.float32),
                pltpu.HBM((2 * n, rows // 2, cols), jnp.bfloat16),
            ],
            in_specs=[hbm] * 5,
            out_specs=[vmem, vmem, vmem, hbm],
            scratch_shapes=[
                pltpu.VMEM(rr.shape, jnp.bfloat16),
                pltpu.VMEM((cols, rows), jnp.bfloat16),
                pltpu.VMEM((rows, cols + lrows), jnp.float32),
                pltpu.VMEM((2, 2, rows // 2, cols), jnp.bfloat16),
                pltpu.VMEM((cols + lrows, cols), jnp.bfloat16),
                pltpu.VMEM((2, rows, cols), jnp.bfloat16),
                pltpu.VMEM((2 * kept, lrows // 2, rows), jnp.bfloat16),
                pltpu.VMEM((4, lrows // 2, rows), jnp.bfloat16),
                pltpu.VMEM((kept, lrows, cols), jnp.float32),
                pltpu.SemaphoreType.DMA((ROUNDS + n // 2,)),
                pltpu.SemaphoreType.DMA((1,)),
                pltpu.SemaphoreType.DMA((2,)),
                pltpu.SemaphoreType.DMA((4,)),
                pltpu.SemaphoreType.DMA((TWIN_TURN + kept // 2,)),
                pltpu.SemaphoreType.DMA((3,)),
                pltpu.SemaphoreType.DMA((2,)),
                pltpu.SemaphoreType.DMA((1,)),
                pltpu.SemaphoreType.DMA((2,)),
                pltpu.SemaphoreType.DMA((2,)),
                pltpu.SemaphoreType.DMA((1,)),
                pltpu.SemaphoreType.REGULAR,
            ],
            compiler_params=pltpu.CompilerParams(collective_id=0, has_side_effects=True, vmem_limit_bytes=48 * 2**20),
            cost_estimate=pl.CostEstimate(flops=2 * rows * cols * (2 * n * cols + 2 * rows), bytes_accessed=2 * n * rows * cols * 3, transcendentals=0),
        )(*[pltpu.with_memory_space_constraint(v, pltpu.HBM) for v in operands])
        results = [left_new, right_new, direction]
        return pl.pallas_call(
            store_kernel,
            name="store",
            out_shape=[jax.ShapeDtypeStruct(v.shape, v.dtype) for v in results],
            in_specs=[vmem] * 3,
            out_specs=[hbm] * 3,
            scratch_shapes=[pltpu.SemaphoreType.DMA((3,))],
            compiler_params=pltpu.CompilerParams(vmem_limit_bytes=1 * 2**20),
        )(*results)

    return jax.shard_map(local_step, mesh=mesh, in_specs=(col_spec, row_spec, row_spec, row_spec, row_spec), out_specs=(row_spec, row_spec, col_spec), check_vma=False)
```

```python
import functools
import math

import jax
import jax.numpy as jnp
from jax import lax
from jax.experimental import pallas as pl
from jax.experimental.pallas import tpu as pltpu
from jax.sharding import PartitionSpec as P

EMA_DECAY = 0.9
CORES = 2
MESH = pl.DeviceIdType.MESH

ORDER = [(int(a), int(b)) for a, b in zip("0310020311322312", "0003102313131222")]
def parcels(code):
    digits = [int(d) for d in code]
    return [((a, b), h) for a, b, h in zip(digits[0::3], digits[1::3], digits[2::3])]


UP = parcels("030031330131020331130230231320120220")
UP_ON = {0: parcels("030"), 2: parcels("330"), 6: parcels("130"), 7: parcels("230")}
DOWN = parcels("011010111310021110311211210321121221")
DOWN_ON = {0: parcels("011"), 6: parcels("311111"), 7: parcels("211")}
ROUNDS = len(UP)
FIRST_UP = parcels("300301200")
FIRST_DOWN = parcels("101100201")
GRAD_ROUND_STEP = [2, 2, 8, 10, 12, 14, 17, 20, 22, 26, 28, 30]
LAST_FORWARD = 7
SIDE_UP, SIDE_DOWN = 9, 10
ASIDE = 36
ROOT_START_STEP = 28
ROOT_ACROSS_STEP = 30
RELAY_STEP = 32
LATE = (2, 12, 14, 22, 26, 28, 30)


def round_of(name, offset, half):
    a, b = offset
    table, da, db = {"f+": (FIRST_UP, 3, 0), "f-": (FIRST_DOWN, 1, 0), "s+": (UP, 0, 3), "s-": (DOWN, 0, 1)}[name]
    return table.index((((a + da) % 4, (b + db) % 4), half))


def packed(values):
    return [sum(v << (2 * i) for i, v in enumerate(values[j:j + 8])) for j in (0, 8)]


FIRST_CODE = packed([o[0] for o in ORDER])
SECOND_CODE = packed([o[1] for o in ORDER])


def lookup(code, e):
    word = code[0] + (e // 8) * (code[1] - code[0])
    return lax.shift_right_logical(word, 2 * (e % 8)) & 3


ROOT_ORDER = [(0, 0), (3, 0), (1, 0), (0, 1), (2, 0), (3, 1), (1, 1), (2, 1)]
ROOT_Y = sum(o[0] << (2 * i) for i, o in enumerate(ROOT_ORDER))
FAR_TURN, LAST_TURN, TWIN_LAST, TWIN_TURN = 5, 7, 9, 10
ROOT_X = sum(o[1] << (2 * i) for i, o in enumerate(ROOT_ORDER))


def kernel(n, side, g_ref, l_ref, r_ref, lr_ref, rr_ref, lo_ref, ro_ref, do_ref, gfull,
           rr, gt, acc, gbuf, rhs, xx, lroot, relay, lent,
           g_recv, g_send, load_sem, init_sem, l_recv, relay_recv, x_recv, d_recv, l_send, x_send, d_send, x_gone):
    _, half_rows, cols = g_ref.shape
    rows = 2 * half_rows
    lrows = l_ref.shape[0]
    tile = min(1024, half_rows)
    aside_rows = half_rows * ASIDE // 128

    me = lax.axis_index("tensor")
    c = me % CORES
    chip = me // CORES
    x, y = chip % side, chip // side
    f = x + c * (y - x)
    s = y + c * (x - y)
    fstep = CORES + c * CORES * (side - 1)
    sstep = CORES * side - c * CORES * (side - 1)
    twin = me + 1 - 2 * c

    def index(df, ds):
        return ((f + df) % side) * fstep + ((s + ds) % side) * sstep + c

    def twin_index(df, ds):
        return ((s + df) % side) * sstep + ((f + ds) % side) * fstep + 1 - c

    peers = {"f+": index(1, 0), "f-": index(3, 0), "s+": index(0, 1), "s-": index(0, 3), "twin": twin}

    class Gather:
        def __init__(self, own, full, recv, send):
            self.own, self.full, self.recv, self.send_sem = own, full, recv, send
            self.sent = 0

        def copy(self, name, offset, half, part=None, turn=None):
            b = index(*offset)
            src = self.own.at[half] if offset == (0, 0) else self.full.at[2 * b + half]
            dst = self.full.at[2 * b + half]
            if part is not None:
                src, dst = src.at[pl.ds(*part)], dst.at[pl.ds(*part)]
            if turn is None:
                turn = ROUNDS + b // CORES if name == "twin" else round_of(name, offset, half)
            return pltpu.make_async_remote_copy(
                src_ref=src, dst_ref=dst, send_sem=self.send_sem.at[0], recv_sem=self.recv.at[turn],
                device_id={"tensor": peers[name]}, device_id_type=MESH)

        def send(self, name, offset, half):
            self.sent += 1
            self.copy(name, offset, half).start()

        def wait(self, turn, count):
            taken = self.full.at[pl.ds(0, count)]
            pltpu.make_async_copy(taken, taken, self.recv.at[turn]).wait()

        def start(self):
            for half in (0, 1):
                for name in ("f+", "s+"):
                    self.send(name, (0, 0), half)
                for name in ("f-", "s-"):
                    self.send(name, (0, 0), 1 - half)
            for half in (0, 1):
                self.send("twin", (0, 0), half)

        def round(self, r):
            first = r < len(FIRST_UP)
            self.wait(r, 4 if first else 2)
            if first:
                above, below = FIRST_UP[r], FIRST_DOWN[r]
                if r == 0:
                    self.send("f+", *above)
                    self.send("f-", *below)
                self.send("s+", *above)
                self.send("s-", *below)
                self.send("s+", *below)
                self.send("s-", *above)
                self.send("twin", *above)
                self.send("twin", *below)
            for name, table in (("s+", UP_ON), ("s-", DOWN_ON)):
                for parcel in table.get(r, ()):
                    if r == LAST_FORWARD:
                        self.forward_last(name, *parcel)
                    else:
                        self.send(name, *parcel)
            if r == SIDE_UP:
                self.aside("f+", *UP[r])
            if r == SIDE_DOWN:
                self.aside("f-", *DOWN[r])
            self.send("twin", *UP[r])
            self.send("twin", *DOWN[r])

        def forward_last(self, name, offset, half):
            self.sent += 1
            pl.when(c == 0)(lambda: self.copy(name, offset, half, part=(0, half_rows - aside_rows)).start())
            pl.when(c == 1)(lambda: self.copy(name, offset, half).start())

        def aside(self, name, offset, half):
            part = (half_rows - aside_rows, aside_rows)
            pl.when(c == 0)(lambda: self.copy(name, offset, half, part=part, turn=ROUNDS - 1).start())

        def drain(self):
            whole = self.full.at[pl.ds(0, self.sent)]
            pltpu.make_async_copy(whole, whole, self.send_sem.at[0]).wait()

    grad = Gather(g_ref, gfull, g_recv, g_send)

    def block_of(k):
        e, other = k // 2, k % 2
        df, ds = lookup(FIRST_CODE, e), lookup(SECOND_CODE, e)
        mine = index(df, ds)
        return mine + other * (twin_index(df, ds) - mine)

    def load(gather, buf, k, sem):
        b = block_of(k)
        return pltpu.make_async_copy(gather.full.at[pl.ds(2 * b, 2)], buf.at[k % 2], sem.at[k % 2])

    def one_of(k, values):
        found = k == values[0]
        for v in values[1:]:
            found = found | (k == v)
        return found

    def steps(gather, buf, sem, round_step, early, between, after, work):
        def at_steps(k, actions):
            for at, action in actions:
                pl.when(k == at)(action)

        def step(k, carry):
            at_steps(k, early)

            @pl.when((k % 2 == 1) & (k < n))
            def _():
                gather.wait(ROUNDS + block_of(k) // CORES, 2)

            @pl.when(jnp.logical_not(one_of(k, LATE)) & (k < n))
            def _():
                load(gather, buf, k, sem).start()
            load(gather, buf, k - 1, sem).wait()
            work((k - 1) % 2, block_of(k - 1))
            at_steps(k, between)
            for r in range(ROUNDS):
                @pl.when(k == round_step[r])
                def _():
                    gather.round(r)
            at_steps(k, after)

            @pl.when(one_of(k, LATE))
            def _():
                load(gather, buf, k, sem).start()
            return carry
        lax.fori_loop(1, n + 1, step, 0)

    barrier = pltpu.get_barrier_semaphore()
    for peer in peers.values():
        pl.semaphore_signal(barrier, inc=1, device_id={"tensor": peer}, device_id_type=MESH)

    first = [
        pltpu.make_async_copy(rr_ref, rr, init_sem.at[0]),
        pltpu.make_async_copy(r_ref, ro_ref, init_sem.at[1]),
        pltpu.make_async_copy(l_ref, lo_ref, init_sem.at[2]),
        pltpu.make_async_copy(lr_ref, lroot.at[pl.ds(2 * ((y * (side // 2) + x // 2) * CORES + c), 2)], init_sem.at[3]),
    ]
    own_load = pltpu.make_async_copy(g_ref, gbuf.at[0], load_sem.at[0])
    own_load.start()

    pl.semaphore_wait(barrier, len(peers))
    grad.start()
    for copy in first:
        copy.start()

    acc[...] = jnp.zeros_like(acc)
    own_load.wait()
    for h in (0, 1):
        gt[:, h * half_rows:(h + 1) * half_rows] = gbuf[0, h].T
    for copy in first:
        copy.wait()
    own_load.start()

    per_half = half_rows // tile

    def grad_work(slot, b):
        at = pl.multiple_of(b * cols, cols)
        rhs[:cols] = rr[:, pl.ds(at, cols)]
        rhs[cols:] = gbuf[slot, me // (n // 2), pl.ds(pl.multiple_of((me % (n // 2)) * lrows, lrows), lrows), :]

        def rows_step(t, carry):
            left = gbuf[slot, t // per_half, pl.ds(pl.multiple_of((t % per_half) * tile, tile), tile), :]
            out = pl.ds(pl.multiple_of(t * tile, tile), tile)
            acc[out, :] += lax.dot_general(left, rhs[...], (((1,), (1,)), ((), ())), preferred_element_type=jnp.float32)
            return carry
        lax.fori_loop(0, 2 * per_half, rows_step, 0)
        prod = jnp.dot(gt[:, :half_rows], gbuf[slot, 0], preferred_element_type=jnp.float32)
        prod += jnp.dot(gt[:, half_rows:], gbuf[slot, 1], preferred_element_type=jnp.float32)
        ro_ref[:, pl.ds(at, cols)] = EMA_DECAY * ro_ref[:, pl.ds(at, cols)] + (1.0 - EMA_DECAY) * prod


    dx = 1 - 2 * c
    helper = (y * side + (x + dx + side) % side) * CORES + c
    client = (y * side + (x - dx + side) % side) * CORES + c
    up = (((y + 1) % side) * side + x) * CORES + c
    down = (((y + side - 1) % side) * side + x) * CORES + c
    half_count, root_half, _ = lroot.shape
    pieces = ((0, root_half - root_half // 4), (root_half - root_half // 4, root_half // 4))

    def root_block(dy, q, p=0):
        oy, ox = (y + dy) % side, (x + 2 * q) % side
        core = c + p * (1 - 2 * c)
        return (oy * (side // 2) + ox // 2) * CORES + core, (oy * side + ox) * CORES + core

    def root_copy(peer, place, half, src=None, dst=None, recv=None, part=None, across=0):
        here = lroot.at[2 * place + half]
        if part is not None:
            here = here.at[pl.ds(*pieces[part])]
        if peer is twin and recv is None:
            recv = l_recv.at[TWIN_TURN + place // CORES]
        return pltpu.make_async_remote_copy(
            src_ref=here if src is None else src, dst_ref=here if dst is None else dst, send_sem=l_send.at[across],
            recv_sem=l_recv.at[recv] if isinstance(recv, int) else recv, device_id={"tensor": peer}, device_id_type=MESH)

    sent = [0, 0]

    def root_send(peer, place, half, part=None, across=0, **kw):
        sent[across] += root_half if part is None else pieces[part][1]
        root_copy(peer, place, half, part=part, across=across, **kw).start()

    def uncounted(action):
        before = list(sent)
        action()
        sent[:] = before

    def pair_wait(pair, sem):
        pltpu.make_async_copy(pair, pair, sem).wait()

    own_place, _ = root_block(0, 0)
    far_place, _ = root_block(0, 1)
    passing = (y * (side // 2) + ((x - dx + side) % side) // 2) * CORES + c

    def root_start_across():
        for half in (0, 1):
            root_send(helper, own_place, half, across=1, src=lr_ref.at[half], dst=relay.at[half], recv=relay_recv.at[half])

    def root_start():
        for half in (0, 1):
            root_send(up, own_place, half, src=lr_ref.at[half], recv=half)
            root_send(down, own_place, 1 - half, src=lr_ref.at[1 - half], recv=half)
        for half in (0, 1):
            root_send(twin, own_place, half, src=lr_ref.at[half])

    def root_relay(half):
        root_copy(helper, own_place, half, src=lr_ref.at[half], dst=relay.at[half], recv=relay_recv.at[half]).wait_recv()
        root_send(helper, passing, half, across=1, src=relay.at[half], recv=FAR_TURN + half)
        root_send(twin, passing, half, across=1, src=relay.at[half], dst=relay.at[2 + half], recv=relay_recv.at[2])

    def passed_rows(p):
        if p:
            pair_wait(relay.at[pl.ds(2, 2)], relay_recv.at[2])
        source = (y * side + (x - (1 - 2 * p) * dx + side) % side) * CORES + c + p * (1 - 2 * c)
        left = relay[2 * p:2 * p + 2].reshape(lrows, rows)
        do_ref[rows_of(source), :] = jnp.dot(left, xx[0], preferred_element_type=jnp.float32)

    def root_far():
        for half in (0, 1):
            pltpu.make_async_copy(lroot.at[0], lroot.at[0], l_recv.at[FAR_TURN + half]).wait()
            root_send(up, far_place, half, recv=3 + half)
            root_send(twin, far_place, half)
        for half in (1, 0):
            root_send(down, far_place, half, recv=4 - half)

    def root_round(r):
        q, stage = r // 3, r % 3
        pair_wait(lroot.at[pl.ds(0, 2)], l_recv.at[r])
        if stage == 2:
            below = above = root_block(2, q)[0]
        else:
            below, above = root_block(side - 1, q)[0], root_block(1, q)[0]
        if stage == 0:
            for peer, place, half in ((up, below, 0), (down, above, 1)):
                if q == 0:
                    root_send(peer, place, half, recv=2)
                else:
                    for part in (0, 1):
                        root_send(peer, place, half, part=part, recv=LAST_TURN + part)
        root_send(twin, below, stage % 2)
        root_send(twin, above, 1 - stage % 2)

    last_place, last_device = root_block(2, 1)
    twin_place, twin_device = root_block(2, 1, 1)

    def root_last(part):
        pair_wait(lroot.at[pl.ds(0, 2), pl.ds(*pieces[part])], l_recv.at[LAST_TURN + part])
        for half in (0, 1):
            root_send(twin, last_place, half, part=part, recv=TWIN_LAST if part else None)

    def root_last_twin(part):
        pair = lroot.at[pl.ds(2 * twin_place, 2), pl.ds(*pieces[part])]
        pair_wait(pair, l_recv.at[TWIN_LAST if part else TWIN_TURN + twin_place // CORES])

    steps(grad, gbuf, load_sem, GRAD_ROUND_STEP, [(RELAY_STEP, lambda: root_relay(0))],
          [(ROOT_ACROSS_STEP, root_start_across), (ROOT_ACROSS_STEP, lambda: pl.when(c == 1)(lambda: uncounted(root_start)))],
          [(ROOT_START_STEP, lambda: pl.when(c == 0)(root_start))], grad_work)

    side_cols = cols // 2

    def x_copy(h):
        at = pl.ds(h * side_cols, side_cols)
        return pltpu.make_async_remote_copy(
            src_ref=xx.at[0, :, at], dst_ref=xx.at[1, :, at], send_sem=x_send.at[h], recv_sem=x_recv.at[h],
            device_id={"tensor": helper}, device_id_type=MESH)

    xx[0] = acc[:, :cols].astype(jnp.bfloat16)
    root_relay(1)
    x_copy(0).start()
    x_copy(1).start()
    root_round(0)

    def left_step(t, carry):
        at = pl.ds(pl.multiple_of(t * lrows, lrows), lrows)
        lo_ref[:, at] = EMA_DECAY * lo_ref[:, at] + (1.0 - EMA_DECAY) * acc[at, cols:].T
        return carry
    lax.fori_loop(0, rows // lrows, left_step, 0)

    def at_step(i):
        e, p = i // 2, i % 2
        dy = lax.shift_right_logical(ROOT_Y, 2 * e) & 3
        q = lax.shift_right_logical(ROOT_X, 2 * e) & 3
        return root_block(dy, q, p)

    def twin_wait(i, place):
        @pl.when(i % 2 == 1)
        def _():
            pair_wait(lroot.at[pl.ds(2 * place, 2)], l_recv.at[TWIN_TURN + place // CORES])

    def product(place, which):
        left = lroot[pl.ds(2 * place, 2)].reshape(lrows, rows)
        return jnp.dot(left, xx[which], preferred_element_type=jnp.float32)

    def rows_of(device):
        return pl.ds(pl.multiple_of(device * lrows, lrows), lrows)

    def own_rows(i):
        place, device = at_step(i)
        do_ref[rows_of(device), :] = product(place, 0)

    def lent_copy(i, device):
        return pltpu.make_async_remote_copy(
            src_ref=lent.at[i], dst_ref=do_ref.at[rows_of(device)], send_sem=d_send.at[0], recv_sem=d_recv.at[0],
            device_id={"tensor": client}, device_id_type=MESH)

    def lent_rows(i):
        place, device = at_step(i)
        lent[i] = product(place, 1)
        lent_copy(i, device).start()

    def lent_side(i, h):
        place, _ = at_step(i)
        at = pl.ds(h * side_cols, side_cols)
        left = lroot[pl.ds(2 * place, 2)].reshape(lrows, rows)
        lent[i, :, at] = jnp.dot(left, xx[1, :, at], preferred_element_type=jnp.float32)

    def lent_side_copy(i, h):
        _, device = at_step(i)
        at = pl.ds(h * side_cols, side_cols)
        return pltpu.make_async_remote_copy(
            src_ref=lent.at[i, :, at], dst_ref=do_ref.at[rows_of(device), at], send_sem=d_send.at[0], recv_sem=d_recv.at[0],
            device_id={"tensor": client}, device_id_type=MESH)

    def loop(lo, hi, body):
        def step(i, carry):
            body(i)
            return carry
        lax.fori_loop(lo, hi, step, 0)

    def first_own(i):
        @pl.when(i == 2)
        def _():
            root_far()
            root_round(1)

        @pl.when(i == 8)
        def _():
            root_round(2)
        twin_wait(i, at_step(i)[0])
        own_rows(i)

    loop(0, 10, first_own)
    passed_rows(0)
    passed_rows(1)
    x_copy(0).wait_recv()
    def lent_step(j):
        return j + (j + 7) // 8 + j // 5

    loop(0, 8, lambda j: lent_side(lent_step(j), 0))
    x_copy(0).wait_send()
    x_copy(1).wait_send()
    pl.semaphore_signal(x_gone, inc=1, device_id={"tensor": twin}, device_id_type=MESH)
    pl.semaphore_wait(x_gone, 1)
    loop(0, 8, lambda j: lent_side_copy(lent_step(j), 0).start())
    root_round(3)
    x_copy(1).wait_recv()

    def second_side(j):
        i = lent_step(j)
        lent_side(i, 1)
        lent_side_copy(i, 1).start()
    loop(0, 8, second_side)
    root_round(4)

    def both(i):
        twin_wait(i, at_step(i)[0])
        lent_rows(i)
        own_rows(i)
    loop(10, 14, both)

    def lent_piece(i, place, device, part):
        first, count = pieces[part]
        left = jnp.concatenate([lroot[2 * place, pl.ds(first, count), :], lroot[2 * place + 1, pl.ds(first, count), :]], axis=0)
        prod = jnp.dot(left, xx[1], preferred_element_type=jnp.float32)
        for half in (0, 1):
            at = half * root_half + first
            lent[i, pl.ds(at, count), :] = prod[half * count:(half + 1) * count]
            pltpu.make_async_remote_copy(
                src_ref=lent.at[i, pl.ds(at, count)], dst_ref=do_ref.at[pl.ds(pl.multiple_of(device * lrows, lrows) + at, count)],
                send_sem=d_send.at[0], recv_sem=d_recv.at[0], device_id={"tensor": client}, device_id_type=MESH).start()

    def own_piece(part):
        root_last(part)
        lent_piece(14, last_place, last_device, part)

    def twin_piece(part):
        root_last_twin(part)
        lent_piece(15, twin_place, twin_device, part)

    @pl.when(c == 0)
    def _():
        own_piece(0)
        own_piece(1)
        twin_piece(0)
        twin_piece(1)

    @pl.when(c == 1)
    def _():
        uncounted(lambda: own_piece(0))
        twin_piece(0)
        twin_piece(1)
        uncounted(lambda: own_piece(1))

    loop(14, 16, own_rows)

    grad.drain()
    for across, count in enumerate(sent):
        whole = lroot.at[pl.ds(0, count // root_half)]
        pltpu.make_async_copy(whole, whole, l_send.at[across]).wait()
    given = lent.at[pl.ds(0, half_count // 2 - 2)]
    pltpu.make_async_copy(given, given, d_send.at[0]).wait()
    pltpu.make_async_copy(given, given, d_recv.at[0]).wait()


def store_kernel(*refs):
    count = (len(refs) - 1) // 2
    sems = refs[-1]
    pieces = 8
    for i in range(count):
        src, dst = refs[i], refs[count + i]
        step = src.shape[0] // pieces
        for j in range(pieces):
            part = pl.ds(j * step, step)
            pltpu.make_async_copy(src.at[part], dst.at[part], sems.at[i]).start()
    for i in range(count):
        pltpu.make_async_copy(refs[i], refs[count + i], sems.at[i]).wait()


def solution(mesh):
    row_spec = P(("layer", "tensor"), None)
    col_spec = P("layer", "tensor")
    n = mesh.shape["tensor"]
    side = math.isqrt(n // CORES)

    def local_step(g, l, r, lr, rr):
        rows, cols = g.shape
        lrows = l.shape[0]
        kept = n // 2
        hbm = pl.BlockSpec(memory_space=pltpu.HBM)
        vmem = pl.BlockSpec(memory_space=pltpu.VMEM)
        operands = [g.reshape(2, rows // 2, cols), l, r, lr.reshape(2, lrows // 2, rows), rr]
        left_new, right_new, direction, _ = pl.pallas_call(
            functools.partial(kernel, n, side),
            name="shampoo",
            out_shape=[
                pltpu.VMEM(l.shape, jnp.float32),
                pltpu.VMEM(r.shape, jnp.float32),
                pltpu.VMEM(g.shape, jnp.float32),
                pltpu.HBM((2 * n, rows // 2, cols), jnp.bfloat16),
            ],
            in_specs=[hbm] * 5,
            out_specs=[vmem, vmem, vmem, hbm],
            scratch_shapes=[
                pltpu.VMEM(rr.shape, jnp.bfloat16),
                pltpu.VMEM((cols, rows), jnp.bfloat16),
                pltpu.VMEM((rows, cols + lrows), jnp.float32),
                pltpu.VMEM((2, 2, rows // 2, cols), jnp.bfloat16),
                pltpu.VMEM((cols + lrows, cols), jnp.bfloat16),
                pltpu.VMEM((2, rows, cols), jnp.bfloat16),
                pltpu.VMEM((2 * kept, lrows // 2, rows), jnp.bfloat16),
                pltpu.VMEM((4, lrows // 2, rows), jnp.bfloat16),
                pltpu.VMEM((kept, lrows, cols), jnp.float32),
                pltpu.SemaphoreType.DMA((ROUNDS + n // 2,)),
                pltpu.SemaphoreType.DMA((1,)),
                pltpu.SemaphoreType.DMA((2,)),
                pltpu.SemaphoreType.DMA((4,)),
                pltpu.SemaphoreType.DMA((TWIN_TURN + kept // 2,)),
                pltpu.SemaphoreType.DMA((3,)),
                pltpu.SemaphoreType.DMA((2,)),
                pltpu.SemaphoreType.DMA((1,)),
                pltpu.SemaphoreType.DMA((2,)),
                pltpu.SemaphoreType.DMA((2,)),
                pltpu.SemaphoreType.DMA((1,)),
                pltpu.SemaphoreType.REGULAR,
            ],
            compiler_params=pltpu.CompilerParams(collective_id=0, has_side_effects=True, vmem_limit_bytes=48 * 2**20),
            cost_estimate=pl.CostEstimate(flops=2 * rows * cols * (2 * n * cols + 2 * rows), bytes_accessed=2 * n * rows * cols * 3, transcendentals=0),
        )(*[pltpu.with_memory_space_constraint(v, pltpu.HBM) for v in operands])
        results = [left_new, right_new, direction]
        return pl.pallas_call(
            store_kernel,
            name="store",
            out_shape=[jax.ShapeDtypeStruct(v.shape, v.dtype) for v in results],
            in_specs=[vmem] * 3,
            out_specs=[hbm] * 3,
            scratch_shapes=[pltpu.SemaphoreType.DMA((3,))],
            compiler_params=pltpu.CompilerParams(vmem_limit_bytes=1 * 2**20),
        )(*results)

    return jax.shard_map(local_step, mesh=mesh, in_specs=(col_spec, row_spec, row_spec, row_spec, row_spec), out_specs=(row_spec, row_spec, col_spec), check_vma=False)
```

```python
import functools
import math

import jax
import jax.numpy as jnp
from jax import lax
from jax.experimental import pallas as pl
from jax.experimental.pallas import tpu as pltpu
from jax.sharding import PartitionSpec as P

EMA_DECAY = 0.9
CORES = 2
MESH = pl.DeviceIdType.MESH

ORDER = [(int(a), int(b)) for a, b in zip("0310020311322312", "0003102313131222")]
def parcels(code):
    digits = [int(d) for d in code]
    return [((a, b), h) for a, b, h in zip(digits[0::3], digits[1::3], digits[2::3])]


UP = parcels("030031330131020331130230231320120220")
UP_ON = {0: parcels("030"), 2: parcels("330"), 6: parcels("130"), 7: parcels("230")}
DOWN = parcels("011010111310021110311211210321121221")
DOWN_ON = {0: parcels("011"), 6: parcels("311111"), 7: parcels("211")}
ROUNDS = len(UP)
FIRST_UP = parcels("300301200")
FIRST_DOWN = parcels("101100201")
GRAD_ROUND_STEP = [2, 2, 8, 10, 12, 14, 17, 20, 22, 26, 28, 30]
LAST_FORWARD = 7
SIDE_UP, SIDE_DOWN = 9, 10
ASIDE = 36
ROOT_START_STEP = 28
ROOT_ACROSS_STEP = 30
RELAY_STEP = 32
LATE = (2, 12, 14, 22, 26, 28, 30)


def round_of(name, offset, half):
    a, b = offset
    table, da, db = {"f+": (FIRST_UP, 3, 0), "f-": (FIRST_DOWN, 1, 0), "s+": (UP, 0, 3), "s-": (DOWN, 0, 1)}[name]
    return table.index((((a + da) % 4, (b + db) % 4), half))


def packed(values):
    return [sum(v << (2 * i) for i, v in enumerate(values[j:j + 8])) for j in (0, 8)]


FIRST_CODE = packed([o[0] for o in ORDER])
SECOND_CODE = packed([o[1] for o in ORDER])


def lookup(code, e):
    word = code[0] + (e // 8) * (code[1] - code[0])
    return lax.shift_right_logical(word, 2 * (e % 8)) & 3


ROOT_ORDER = [(0, 0), (3, 0), (1, 0), (0, 1), (2, 0), (3, 1), (1, 1), (2, 1)]
ROOT_Y = sum(o[0] << (2 * i) for i, o in enumerate(ROOT_ORDER))
FAR_TURN, LAST_TURN, ROOT_TURNS = 5, 7, 9
ROOT_X = sum(o[1] << (2 * i) for i, o in enumerate(ROOT_ORDER))


def kernel(n, side, g_ref, l_ref, r_ref, lr_ref, rr_ref, lo_ref, ro_ref, do_ref, gfull,
           rr, gt, acc, gbuf, rhs, xx, lroot, relay, lent,
           g_recv, g_send, load_sem, l_recv, relay_recv, x_recv, d_recv, l_send, x_send, d_send, x_gone):
    _, half_rows, cols = g_ref.shape
    rows = 2 * half_rows
    lrows = l_ref.shape[0]
    tile = min(1024, half_rows)
    aside_rows = half_rows * ASIDE // 128

    me = lax.axis_index("tensor")
    c = me % CORES
    chip = me // CORES
    x, y = chip % side, chip // side
    f = x + c * (y - x)
    s = y + c * (x - y)
    fstep = CORES + c * CORES * (side - 1)
    sstep = CORES * side - c * CORES * (side - 1)
    twin = me + 1 - 2 * c

    def index(df, ds):
        return ((f + df) % side) * fstep + ((s + ds) % side) * sstep + c

    def twin_index(df, ds):
        return ((s + df) % side) * sstep + ((f + ds) % side) * fstep + 1 - c

    peers = {"f+": index(1, 0), "f-": index(3, 0), "s+": index(0, 1), "s-": index(0, 3), "twin": twin}

    class Gather:
        def __init__(self, own, full, recv, send):
            self.own, self.full, self.recv, self.send_sem = own, full, recv, send
            self.sent = 0

        def copy(self, name, offset, half, part=None, turn=None):
            b = index(*offset)
            src = self.own.at[half] if offset == (0, 0) else self.full.at[2 * b + half]
            dst = self.full.at[2 * b + half]
            if part is not None:
                src, dst = src.at[pl.ds(*part)], dst.at[pl.ds(*part)]
            if turn is None:
                turn = ROUNDS + ORDER.index(offset) if name == "twin" else round_of(name, offset, half)
            return pltpu.make_async_remote_copy(
                src_ref=src, dst_ref=dst, send_sem=self.send_sem.at[0], recv_sem=self.recv.at[turn],
                device_id={"tensor": peers[name]}, device_id_type=MESH)

        def send(self, name, offset, half):
            self.sent += 1
            self.copy(name, offset, half).start()

        def wait(self, turn, count):
            taken = self.full.at[pl.ds(0, count)]
            pltpu.make_async_copy(taken, taken, self.recv.at[turn]).wait()

        def start(self):
            for half in (0, 1):
                for name in ("f+", "s+"):
                    self.send(name, (0, 0), half)
                for name in ("f-", "s-"):
                    self.send(name, (0, 0), 1 - half)
            for half in (0, 1):
                self.send("twin", (0, 0), half)

        def round(self, r):
            first = r < len(FIRST_UP)
            self.wait(r, 4 if first else 2)
            if first:
                above, below = FIRST_UP[r], FIRST_DOWN[r]
                if r == 0:
                    self.send("f+", *above)
                    self.send("f-", *below)
                self.send("s+", *above)
                self.send("s-", *below)
                self.send("s+", *below)
                self.send("s-", *above)
                self.send("twin", *above)
                self.send("twin", *below)
            for name, table in (("s+", UP_ON), ("s-", DOWN_ON)):
                for parcel in table.get(r, ()):
                    if r == LAST_FORWARD:
                        self.forward_last(name, *parcel)
                    else:
                        self.send(name, *parcel)
            if r == SIDE_UP:
                self.aside("f+", *UP[r])
            if r == SIDE_DOWN:
                self.aside("f-", *DOWN[r])
            self.send("twin", *UP[r])
            self.send("twin", *DOWN[r])

        def forward_last(self, name, offset, half):
            self.sent += 1
            pl.when(c == 0)(lambda: self.copy(name, offset, half, part=(0, half_rows - aside_rows)).start())
            pl.when(c == 1)(lambda: self.copy(name, offset, half).start())

        def aside(self, name, offset, half):
            part = (half_rows - aside_rows, aside_rows)
            pl.when(c == 0)(lambda: self.copy(name, offset, half, part=part, turn=ROUNDS - 1).start())

        def drain(self):
            whole = self.full.at[pl.ds(0, self.sent)]
            pltpu.make_async_copy(whole, whole, self.send_sem.at[0]).wait()

    grad = Gather(g_ref, gfull, g_recv, g_send)

    def block_of(k):
        e, other = k // 2, k % 2
        df, ds = lookup(FIRST_CODE, e), lookup(SECOND_CODE, e)
        mine = index(df, ds)
        return mine + other * (twin_index(df, ds) - mine)

    def load(gather, buf, k, sem):
        b = block_of(k)
        return pltpu.make_async_copy(gather.full.at[pl.ds(2 * b, 2)], buf.at[k % 2], sem.at[k % 2])

    def one_of(k, values):
        found = k == values[0]
        for v in values[1:]:
            found = found | (k == v)
        return found

    def steps(gather, buf, sem, round_step, early, between, after, work):
        def at_steps(k, actions):
            for at, action in actions:
                pl.when(k == at)(action)

        def step(k, carry):
            at_steps(k, early)

            @pl.when((k % 2 == 1) & (k < n))
            def _():
                gather.wait(ROUNDS + k // 2, 2)

            @pl.when(jnp.logical_not(one_of(k, LATE)) & (k < n))
            def _():
                load(gather, buf, k, sem).start()
            load(gather, buf, k - 1, sem).wait()
            work((k - 1) % 2, block_of(k - 1))
            at_steps(k, between)
            for r in range(ROUNDS):
                @pl.when(k == round_step[r])
                def _():
                    gather.round(r)
            at_steps(k, after)

            @pl.when(one_of(k, LATE))
            def _():
                load(gather, buf, k, sem).start()
            return carry
        lax.fori_loop(1, n + 1, step, 0)

    barrier = pltpu.get_barrier_semaphore()
    for peer in peers.values():
        pl.semaphore_signal(barrier, inc=1, device_id={"tensor": peer}, device_id_type=MESH)

    first = [
        pltpu.make_async_copy(rr_ref, rr, x_send.at[0]),
        pltpu.make_async_copy(r_ref, ro_ref, x_send.at[1]),
        pltpu.make_async_copy(l_ref, lo_ref, d_send.at[0]),
        pltpu.make_async_copy(lr_ref, lroot.at[pl.ds(2 * ((y * (side // 2) + x // 2) * CORES + c), 2)], l_send.at[0]),
    ]
    own_load = pltpu.make_async_copy(g_ref, gbuf.at[0], load_sem.at[0])
    own_load.start()

    pl.semaphore_wait(barrier, len(peers))
    grad.start()
    for copy in first:
        copy.start()

    acc[...] = jnp.zeros_like(acc)
    own_load.wait()
    for h in (0, 1):
        gt[:, h * half_rows:(h + 1) * half_rows] = gbuf[0, h].T
    for copy in first:
        copy.wait()
    own_load.start()

    per_half = half_rows // tile

    def grad_work(slot, b):
        at = pl.multiple_of(b * cols, cols)
        rhs[:cols] = rr[:, pl.ds(at, cols)]
        rhs[cols:] = gbuf[slot, me // (n // 2), pl.ds(pl.multiple_of((me % (n // 2)) * lrows, lrows), lrows), :]

        def rows_step(t, carry):
            left = gbuf[slot, t // per_half, pl.ds(pl.multiple_of((t % per_half) * tile, tile), tile), :]
            out = pl.ds(pl.multiple_of(t * tile, tile), tile)
            acc[out, :] += lax.dot_general(left, rhs[...], (((1,), (1,)), ((), ())), preferred_element_type=jnp.float32)
            return carry
        lax.fori_loop(0, 2 * per_half, rows_step, 0)
        prod = jnp.dot(gt[:, :half_rows], gbuf[slot, 0], preferred_element_type=jnp.float32)
        prod += jnp.dot(gt[:, half_rows:], gbuf[slot, 1], preferred_element_type=jnp.float32)
        ro_ref[:, pl.ds(at, cols)] = EMA_DECAY * ro_ref[:, pl.ds(at, cols)] + (1.0 - EMA_DECAY) * prod


    dx = 1 - 2 * c
    helper = (y * side + (x + dx + side) % side) * CORES + c
    client = (y * side + (x - dx + side) % side) * CORES + c
    up = (((y + 1) % side) * side + x) * CORES + c
    down = (((y + side - 1) % side) * side + x) * CORES + c
    half_count, root_half, _ = lroot.shape
    pieces = ((0, root_half - root_half // 4), (root_half - root_half // 4, root_half // 4))

    def root_block(dy, q, p=0):
        oy, ox = (y + dy) % side, (x + 2 * q) % side
        core = c + p * (1 - 2 * c)
        return (oy * (side // 2) + ox // 2) * CORES + core, (oy * side + ox) * CORES + core

    def twin_turn(place):
        return g_recv.at[ROUNDS + 1 + place // CORES]

    twin_last = g_recv.at[ROUNDS + 1 + half_count // 4]

    def root_copy(peer, place, half, src=None, dst=None, recv=None, part=None, across=0):
        here = lroot.at[2 * place + half]
        if part is not None:
            here = here.at[pl.ds(*pieces[part])]
        if peer is twin and recv is None:
            recv = twin_turn(place)
        return pltpu.make_async_remote_copy(
            src_ref=here if src is None else src, dst_ref=here if dst is None else dst, send_sem=l_send.at[across],
            recv_sem=l_recv.at[recv] if isinstance(recv, int) else recv, device_id={"tensor": peer}, device_id_type=MESH)

    sent = [0, 0]

    def root_send(peer, place, half, part=None, across=0, **kw):
        sent[across] += root_half if part is None else pieces[part][1]
        root_copy(peer, place, half, part=part, across=across, **kw).start()

    def uncounted(action):
        before = list(sent)
        action()
        sent[:] = before

    def pair_wait(pair, sem):
        pltpu.make_async_copy(pair, pair, sem).wait()

    own_place, _ = root_block(0, 0)
    far_place, _ = root_block(0, 1)
    passing = (y * (side // 2) + ((x - dx + side) % side) // 2) * CORES + c

    def root_start_across():
        for half in (0, 1):
            root_send(helper, own_place, half, across=1, src=lr_ref.at[half], dst=relay.at[half], recv=relay_recv.at[half])

    def root_start():
        for half in (0, 1):
            root_send(up, own_place, half, src=lr_ref.at[half], recv=half)
            root_send(down, own_place, 1 - half, src=lr_ref.at[1 - half], recv=half)
        for half in (0, 1):
            root_send(twin, own_place, half, src=lr_ref.at[half])

    def root_relay(half):
        root_copy(helper, own_place, half, src=lr_ref.at[half], dst=relay.at[half], recv=relay_recv.at[half]).wait_recv()
        root_send(helper, passing, half, across=1, src=relay.at[half], recv=FAR_TURN + half)
        root_send(twin, passing, half, across=1, src=relay.at[half], dst=relay.at[2 + half], recv=relay_recv.at[2])

    def passed_rows(p):
        if p:
            pair_wait(relay.at[pl.ds(2, 2)], relay_recv.at[2])
        source = (y * side + (x - (1 - 2 * p) * dx + side) % side) * CORES + c + p * (1 - 2 * c)
        left = relay[2 * p:2 * p + 2].reshape(lrows, rows)
        do_ref[rows_of(source), :] = jnp.dot(left, xx[0], preferred_element_type=jnp.float32)

    def root_far():
        for half in (0, 1):
            pltpu.make_async_copy(lroot.at[0], lroot.at[0], l_recv.at[FAR_TURN + half]).wait()
            root_send(up, far_place, half, recv=3 + half)
            root_send(twin, far_place, half)
        for half in (1, 0):
            root_send(down, far_place, half, recv=4 - half)

    def root_round(r):
        q, stage = r // 3, r % 3
        pair_wait(lroot.at[pl.ds(0, 2)], l_recv.at[r])
        if stage == 2:
            below = above = root_block(2, q)[0]
        else:
            below, above = root_block(side - 1, q)[0], root_block(1, q)[0]
        if stage == 0:
            for peer, place, half in ((up, below, 0), (down, above, 1)):
                if q == 0:
                    root_send(peer, place, half, recv=2)
                else:
                    for part in (0, 1):
                        root_send(peer, place, half, part=part, recv=LAST_TURN + part)
        root_send(twin, below, stage % 2)
        root_send(twin, above, 1 - stage % 2)

    last_place, last_device = root_block(2, 1)
    twin_place, twin_device = root_block(2, 1, 1)

    def root_last(part):
        pair_wait(lroot.at[pl.ds(0, 2), pl.ds(*pieces[part])], l_recv.at[LAST_TURN + part])
        for half in (0, 1):
            root_send(twin, last_place, half, part=part, recv=twin_last if part else None)

    def root_last_twin(part):
        pair = lroot.at[pl.ds(2 * twin_place, 2), pl.ds(*pieces[part])]
        pair_wait(pair, twin_last if part else twin_turn(twin_place))

    steps(grad, gbuf, load_sem, GRAD_ROUND_STEP, [(RELAY_STEP, lambda: root_relay(0))],
          [(ROOT_ACROSS_STEP, root_start_across), (ROOT_ACROSS_STEP, lambda: pl.when(c == 1)(lambda: uncounted(root_start)))],
          [(ROOT_START_STEP, lambda: pl.when(c == 0)(root_start))], grad_work)

    side_cols = cols // 2

    def x_copy(h):
        at = pl.ds(h * side_cols, side_cols)
        return pltpu.make_async_remote_copy(
            src_ref=xx.at[0, :, at], dst_ref=xx.at[1, :, at], send_sem=x_send.at[h], recv_sem=x_recv.at[h],
            device_id={"tensor": helper}, device_id_type=MESH)

    xx[0] = acc[:, :cols].astype(jnp.bfloat16)
    root_relay(1)
    x_copy(0).start()
    x_copy(1).start()
    root_round(0)

    def left_step(t, carry):
        at = pl.ds(pl.multiple_of(t * lrows, lrows), lrows)
        lo_ref[:, at] = EMA_DECAY * lo_ref[:, at] + (1.0 - EMA_DECAY) * acc[at, cols:].T
        return carry
    lax.fori_loop(0, rows // lrows, left_step, 0)

    def at_step(i):
        e, p = i // 2, i % 2
        dy = lax.shift_right_logical(ROOT_Y, 2 * e) & 3
        q = lax.shift_right_logical(ROOT_X, 2 * e) & 3
        return root_block(dy, q, p)

    def twin_wait(i, place):
        @pl.when(i % 2 == 1)
        def _():
            pair_wait(lroot.at[pl.ds(2 * place, 2)], twin_turn(place))

    def product(place, which):
        left = lroot[pl.ds(2 * place, 2)].reshape(lrows, rows)
        return jnp.dot(left, xx[which], preferred_element_type=jnp.float32)

    def rows_of(device):
        return pl.ds(pl.multiple_of(device * lrows, lrows), lrows)

    def own_rows(i):
        place, device = at_step(i)
        do_ref[rows_of(device), :] = product(place, 0)

    def lent_copy(i, device):
        return pltpu.make_async_remote_copy(
            src_ref=lent.at[i], dst_ref=do_ref.at[rows_of(device)], send_sem=d_send.at[0], recv_sem=d_recv.at[0],
            device_id={"tensor": client}, device_id_type=MESH)

    def lent_rows(i):
        place, device = at_step(i)
        lent[i] = product(place, 1)
        lent_copy(i, device).start()

    def lent_side(i, h):
        place, _ = at_step(i)
        at = pl.ds(h * side_cols, side_cols)
        left = lroot[pl.ds(2 * place, 2)].reshape(lrows, rows)
        lent[i, :, at] = jnp.dot(left, xx[1, :, at], preferred_element_type=jnp.float32)

    def lent_side_copy(i, h):
        _, device = at_step(i)
        at = pl.ds(h * side_cols, side_cols)
        return pltpu.make_async_remote_copy(
            src_ref=lent.at[i, :, at], dst_ref=do_ref.at[rows_of(device), at], send_sem=d_send.at[0], recv_sem=d_recv.at[0],
            device_id={"tensor": client}, device_id_type=MESH)

    def loop(lo, hi, body):
        def step(i, carry):
            body(i)
            return carry
        lax.fori_loop(lo, hi, step, 0)

    def first_own(i):
        @pl.when(i == 2)
        def _():
            root_far()
            root_round(1)

        @pl.when(i == 8)
        def _():
            root_round(2)
        twin_wait(i, at_step(i)[0])
        own_rows(i)

    loop(0, 10, first_own)
    passed_rows(0)
    passed_rows(1)
    x_copy(0).wait_recv()
    def lent_step(j):
        return j + (j + 7) // 8 + j // 5

    loop(0, 8, lambda j: lent_side(lent_step(j), 0))
    x_copy(0).wait_send()
    x_copy(1).wait_send()
    pl.semaphore_signal(x_gone, inc=1, device_id={"tensor": twin}, device_id_type=MESH)
    pl.semaphore_wait(x_gone, 1)
    loop(0, 8, lambda j: lent_side_copy(lent_step(j), 0).start())
    root_round(3)
    x_copy(1).wait_recv()

    def second_side(j):
        i = lent_step(j)
        lent_side(i, 1)
        lent_side_copy(i, 1).start()
    loop(0, 8, second_side)
    root_round(4)

    def both(i):
        twin_wait(i, at_step(i)[0])
        lent_rows(i)
        own_rows(i)
    loop(10, 14, both)

    def lent_piece(i, place, device, part):
        first, count = pieces[part]
        left = jnp.concatenate([lroot[2 * place, pl.ds(first, count), :], lroot[2 * place + 1, pl.ds(first, count), :]], axis=0)
        prod = jnp.dot(left, xx[1], preferred_element_type=jnp.float32)
        for half in (0, 1):
            at = half * root_half + first
            lent[i, pl.ds(at, count), :] = prod[half * count:(half + 1) * count]
            pltpu.make_async_remote_copy(
                src_ref=lent.at[i, pl.ds(at, count)], dst_ref=do_ref.at[pl.ds(pl.multiple_of(device * lrows, lrows) + at, count)],
                send_sem=d_send.at[0], recv_sem=d_recv.at[0], device_id={"tensor": client}, device_id_type=MESH).start()

    def own_piece(part):
        root_last(part)
        lent_piece(14, last_place, last_device, part)

    def twin_piece(part):
        root_last_twin(part)
        lent_piece(15, twin_place, twin_device, part)

    @pl.when(c == 0)
    def _():
        own_piece(0)
        own_piece(1)
        twin_piece(0)
        twin_piece(1)

    @pl.when(c == 1)
    def _():
        uncounted(lambda: own_piece(0))
        twin_piece(0)
        twin_piece(1)
        uncounted(lambda: own_piece(1))

    loop(14, 16, own_rows)

    grad.drain()
    for across, count in enumerate(sent):
        whole = lroot.at[pl.ds(0, count // root_half)]
        pltpu.make_async_copy(whole, whole, l_send.at[across]).wait()
    given = lent.at[pl.ds(0, half_count // 2 - 2)]
    pltpu.make_async_copy(given, given, d_send.at[0]).wait()
    pltpu.make_async_copy(given, given, d_recv.at[0]).wait()


def store_kernel(*refs):
    count = (len(refs) - 1) // 2
    sems = refs[-1]
    pieces = 8
    for i in range(count):
        src, dst = refs[i], refs[count + i]
        step = src.shape[0] // pieces
        for j in range(pieces):
            part = pl.ds(j * step, step)
            pltpu.make_async_copy(src.at[part], dst.at[part], sems.at[i]).start()
    for i in range(count):
        pltpu.make_async_copy(refs[i], refs[count + i], sems.at[i]).wait()


def solution(mesh):
    row_spec = P(("layer", "tensor"), None)
    col_spec = P("layer", "tensor")
    n = mesh.shape["tensor"]
    side = math.isqrt(n // CORES)

    def local_step(g, l, r, lr, rr):
        rows, cols = g.shape
        lrows = l.shape[0]
        kept = n // 2
        hbm = pl.BlockSpec(memory_space=pltpu.HBM)
        vmem = pl.BlockSpec(memory_space=pltpu.VMEM)
        operands = [g.reshape(2, rows // 2, cols), l, r, lr.reshape(2, lrows // 2, rows), rr]
        left_new, right_new, direction, _ = pl.pallas_call(
            functools.partial(kernel, n, side),
            name="shampoo",
            out_shape=[
                pltpu.VMEM(l.shape, jnp.float32),
                pltpu.VMEM(r.shape, jnp.float32),
                pltpu.VMEM(g.shape, jnp.float32),
                pltpu.HBM((2 * n, rows // 2, cols), jnp.bfloat16),
            ],
            in_specs=[hbm] * 5,
            out_specs=[vmem, vmem, vmem, hbm],
            scratch_shapes=[
                pltpu.VMEM(rr.shape, jnp.bfloat16),
                pltpu.VMEM((cols, rows), jnp.bfloat16),
                pltpu.VMEM((rows, cols + lrows), jnp.float32),
                pltpu.VMEM((2, 2, rows // 2, cols), jnp.bfloat16),
                pltpu.VMEM((cols + lrows, cols), jnp.bfloat16),
                pltpu.VMEM((2, rows, cols), jnp.bfloat16),
                pltpu.VMEM((2 * kept, lrows // 2, rows), jnp.bfloat16),
                pltpu.VMEM((4, lrows // 2, rows), jnp.bfloat16),
                pltpu.VMEM((kept, lrows, cols), jnp.float32),
                pltpu.SemaphoreType.DMA((ROUNDS + n // 2,)),
                pltpu.SemaphoreType.DMA((1,)),
                pltpu.SemaphoreType.DMA((2,)),
                pltpu.SemaphoreType.DMA((ROOT_TURNS,)),
                pltpu.SemaphoreType.DMA((3,)),
                pltpu.SemaphoreType.DMA((2,)),
                pltpu.SemaphoreType.DMA((1,)),
                pltpu.SemaphoreType.DMA((2,)),
                pltpu.SemaphoreType.DMA((2,)),
                pltpu.SemaphoreType.DMA((1,)),
                pltpu.SemaphoreType.REGULAR,
            ],
            compiler_params=pltpu.CompilerParams(collective_id=0, has_side_effects=True, vmem_limit_bytes=48 * 2**20),
            cost_estimate=pl.CostEstimate(flops=2 * rows * cols * (2 * n * cols + 2 * rows), bytes_accessed=2 * n * rows * cols * 3, transcendentals=0),
        )(*[pltpu.with_memory_space_constraint(v, pltpu.HBM) for v in operands])
        results = [left_new, right_new, direction]
        return pl.pallas_call(
            store_kernel,
            name="store",
            out_shape=[jax.ShapeDtypeStruct(v.shape, v.dtype) for v in results],
            in_specs=[vmem] * 3,
            out_specs=[hbm] * 3,
            scratch_shapes=[pltpu.SemaphoreType.DMA((3,))],
            compiler_params=pltpu.CompilerParams(vmem_limit_bytes=1 * 2**20),
        )(*results)

    return jax.shard_map(local_step, mesh=mesh, in_specs=(col_spec, row_spec, row_spec, row_spec, row_spec), out_specs=(row_spec, row_spec, col_spec), check_vma=False)
```

```python
import functools
import math

import jax
import jax.numpy as jnp
from jax import lax
from jax.experimental import pallas as pl
from jax.experimental.pallas import tpu as pltpu
from jax.sharding import PartitionSpec as P

EMA_DECAY = 0.9
CORES = 2
MESH = pl.DeviceIdType.MESH

ORDER = [(int(a), int(b)) for a, b in zip("0310020311322312", "0003102313131222")]
def parcels(code):
    digits = [int(d) for d in code]
    return [((a, b), h) for a, b, h in zip(digits[0::3], digits[1::3], digits[2::3])]


UP = parcels("030031330131020331130230231320120220")
UP_ON = {0: parcels("030"), 2: parcels("330"), 6: parcels("130"), 7: parcels("230")}
DOWN = parcels("011010111310021110311211210321121221")
DOWN_ON = {0: parcels("011"), 6: parcels("311111"), 7: parcels("211")}
ROUNDS = len(UP)
FIRST_UP = parcels("300301200")
FIRST_DOWN = parcels("101100201")
GRAD_ROUND_STEP = [2, 2, 8, 10, 12, 14, 17, 20, 22, 26, 28, 30]
LAST_FORWARD = 7
SIDE_UP, SIDE_DOWN = 9, 10
ASIDE = 33
ROOT_START_STEP = 28
ROOT_ACROSS_STEP = 30
RELAY_STEP = 32
LATE = (2, 12, 14, 22, 26, 28, 30)


def round_of(name, offset, half):
    a, b = offset
    table, da, db = {"f+": (FIRST_UP, 3, 0), "f-": (FIRST_DOWN, 1, 0), "s+": (UP, 0, 3), "s-": (DOWN, 0, 1)}[name]
    return table.index((((a + da) % 4, (b + db) % 4), half))


def packed(values):
    return [sum(v << (2 * i) for i, v in enumerate(values[j:j + 8])) for j in (0, 8)]


FIRST_CODE = packed([o[0] for o in ORDER])
SECOND_CODE = packed([o[1] for o in ORDER])


def lookup(code, e):
    word = code[0] + (e // 8) * (code[1] - code[0])
    return lax.shift_right_logical(word, 2 * (e % 8)) & 3


ROOT_ORDER = [(0, 0), (3, 0), (1, 0), (0, 1), (2, 0), (3, 1), (1, 1), (2, 1)]
ROOT_Y = sum(o[0] << (2 * i) for i, o in enumerate(ROOT_ORDER))
FAR_TURN, LAST_TURN, ROOT_TURNS = 5, 7, 9
ROOT_X = sum(o[1] << (2 * i) for i, o in enumerate(ROOT_ORDER))


def kernel(n, side, g_ref, l_ref, r_ref, lr_ref, rr_ref, lo_ref, ro_ref, do_ref, gfull,
           rr, gt, acc, gbuf, rhs, xx, lroot, relay, lent,
           g_recv, g_send, load_sem, l_recv, relay_recv, x_recv, d_recv, l_send, x_send, d_send, x_gone):
    _, half_rows, cols = g_ref.shape
    rows = 2 * half_rows
    lrows = l_ref.shape[0]
    tile = min(1024, half_rows)
    aside_rows = half_rows * ASIDE // 128

    me = lax.axis_index("tensor")
    c = me % CORES
    chip = me // CORES
    x, y = chip % side, chip // side
    f = x + c * (y - x)
    s = y + c * (x - y)
    fstep = CORES + c * CORES * (side - 1)
    sstep = CORES * side - c * CORES * (side - 1)
    twin = me + 1 - 2 * c

    def index(df, ds):
        return ((f + df) % side) * fstep + ((s + ds) % side) * sstep + c

    def twin_index(df, ds):
        return ((s + df) % side) * sstep + ((f + ds) % side) * fstep + 1 - c

    peers = {"f+": index(1, 0), "f-": index(3, 0), "s+": index(0, 1), "s-": index(0, 3), "twin": twin}

    class Gather:
        def __init__(self, own, full, recv, send):
            self.own, self.full, self.recv, self.send_sem = own, full, recv, send
            self.sent = 0

        def copy(self, name, offset, half, part=None, turn=None):
            b = index(*offset)
            src = self.own.at[half] if offset == (0, 0) else self.full.at[2 * b + half]
            dst = self.full.at[2 * b + half]
            if part is not None:
                src, dst = src.at[pl.ds(*part)], dst.at[pl.ds(*part)]
            if turn is None:
                turn = ROUNDS + ORDER.index(offset) if name == "twin" else round_of(name, offset, half)
            return pltpu.make_async_remote_copy(
                src_ref=src, dst_ref=dst, send_sem=self.send_sem.at[0], recv_sem=self.recv.at[turn],
                device_id={"tensor": peers[name]}, device_id_type=MESH)

        def send(self, name, offset, half):
            self.sent += 1
            self.copy(name, offset, half).start()

        def wait(self, turn, count):
            taken = self.full.at[pl.ds(0, count)]
            pltpu.make_async_copy(taken, taken, self.recv.at[turn]).wait()

        def start(self):
            for half in (0, 1):
                for name in ("f+", "s+"):
                    self.send(name, (0, 0), half)
                for name in ("f-", "s-"):
                    self.send(name, (0, 0), 1 - half)
            for half in (0, 1):
                self.send("twin", (0, 0), half)

        def round(self, r):
            first = r < len(FIRST_UP)
            self.wait(r, 4 if first else 2)
            if first:
                above, below = FIRST_UP[r], FIRST_DOWN[r]
                if r == 0:
                    self.send("f+", *above)
                    self.send("f-", *below)
                self.send("s+", *above)
                self.send("s-", *below)
                self.send("s+", *below)
                self.send("s-", *above)
                self.send("twin", *above)
                self.send("twin", *below)
            for name, table in (("s+", UP_ON), ("s-", DOWN_ON)):
                for parcel in table.get(r, ()):
                    if r == LAST_FORWARD:
                        self.forward_last(name, *parcel)
                    else:
                        self.send(name, *parcel)
            if r == SIDE_UP:
                self.aside("f+", *UP[r])
            if r == SIDE_DOWN:
                self.aside("f-", *DOWN[r])
            self.send("twin", *UP[r])
            self.send("twin", *DOWN[r])

        def forward_last(self, name, offset, half):
            self.sent += 1
            pl.when(c == 0)(lambda: self.copy(name, offset, half, part=(0, half_rows - aside_rows)).start())
            pl.when(c == 1)(lambda: self.copy(name, offset, half).start())

        def aside(self, name, offset, half):
            part = (half_rows - aside_rows, aside_rows)
            pl.when(c == 0)(lambda: self.copy(name, offset, half, part=part, turn=ROUNDS - 1).start())

        def drain(self):
            whole = self.full.at[pl.ds(0, self.sent)]
            pltpu.make_async_copy(whole, whole, self.send_sem.at[0]).wait()

    grad = Gather(g_ref, gfull, g_recv, g_send)

    def block_of(k):
        e, other = k // 2, k % 2
        df, ds = lookup(FIRST_CODE, e), lookup(SECOND_CODE, e)
        mine = index(df, ds)
        return mine + other * (twin_index(df, ds) - mine)

    def load(gather, buf, k, sem):
        b = block_of(k)
        return pltpu.make_async_copy(gather.full.at[pl.ds(2 * b, 2)], buf.at[k % 2], sem.at[k % 2])

    def one_of(k, values):
        found = k == values[0]
        for v in values[1:]:
            found = found | (k == v)
        return found

    def steps(gather, buf, sem, round_step, early, between, after, work):
        def at_steps(k, actions):
            for at, action in actions:
                pl.when(k == at)(action)

        def step(k, carry):
            at_steps(k, early)

            @pl.when((k % 2 == 1) & (k < n))
            def _():
                gather.wait(ROUNDS + k // 2, 2)

            @pl.when(jnp.logical_not(one_of(k, LATE)) & (k < n))
            def _():
                load(gather, buf, k, sem).start()
            load(gather, buf, k - 1, sem).wait()
            work((k - 1) % 2, block_of(k - 1))
            at_steps(k, between)
            for r in range(ROUNDS):
                @pl.when(k == round_step[r])
                def _():
                    gather.round(r)
            at_steps(k, after)

            @pl.when(one_of(k, LATE))
            def _():
                load(gather, buf, k, sem).start()
            return carry
        lax.fori_loop(1, n + 1, step, 0)

    barrier = pltpu.get_barrier_semaphore()
    for peer in peers.values():
        pl.semaphore_signal(barrier, inc=1, device_id={"tensor": peer}, device_id_type=MESH)

    first = [
        pltpu.make_async_copy(rr_ref, rr, x_send.at[0]),
        pltpu.make_async_copy(r_ref, ro_ref, x_send.at[1]),
        pltpu.make_async_copy(l_ref, lo_ref, d_send.at[0]),
        pltpu.make_async_copy(lr_ref, lroot.at[pl.ds(2 * ((y * (side // 2) + x // 2) * CORES + c), 2)], l_send.at[0]),
    ]
    own_load = pltpu.make_async_copy(g_ref, gbuf.at[0], load_sem.at[0])
    own_load.start()

    pl.semaphore_wait(barrier, len(peers))
    grad.start()
    for copy in first:
        copy.start()

    acc[...] = jnp.zeros_like(acc)
    own_load.wait()
    for h in (0, 1):
        gt[:, h * half_rows:(h + 1) * half_rows] = gbuf[0, h].T
    for copy in first:
        copy.wait()
    own_load.start()

    per_half = half_rows // tile

    def grad_work(slot, b):
        at = pl.multiple_of(b * cols, cols)
        rhs[:cols] = rr[:, pl.ds(at, cols)]
        rhs[cols:] = gbuf[slot, me // (n // 2), pl.ds(pl.multiple_of((me % (n // 2)) * lrows, lrows), lrows), :]

        def rows_step(t, carry):
            left = gbuf[slot, t // per_half, pl.ds(pl.multiple_of((t % per_half) * tile, tile), tile), :]
            out = pl.ds(pl.multiple_of(t * tile, tile), tile)
            acc[out, :] += lax.dot_general(left, rhs[...], (((1,), (1,)), ((), ())), preferred_element_type=jnp.float32)
            return carry
        lax.fori_loop(0, 2 * per_half, rows_step, 0)
        prod = jnp.dot(gt[:, :half_rows], gbuf[slot, 0], preferred_element_type=jnp.float32)
        prod += jnp.dot(gt[:, half_rows:], gbuf[slot, 1], preferred_element_type=jnp.float32)
        ro_ref[:, pl.ds(at, cols)] = EMA_DECAY * ro_ref[:, pl.ds(at, cols)] + (1.0 - EMA_DECAY) * prod


    dx = 1 - 2 * c
    helper = (y * side + (x + dx + side) % side) * CORES + c
    client = (y * side + (x - dx + side) % side) * CORES + c
    up = (((y + 1) % side) * side + x) * CORES + c
    down = (((y + side - 1) % side) * side + x) * CORES + c
    half_count, root_half, _ = lroot.shape
    pieces = ((0, root_half - root_half // 4), (root_half - root_half // 4, root_half // 4))

    def root_block(dy, q, p=0):
        oy, ox = (y + dy) % side, (x + 2 * q) % side
        core = c + p * (1 - 2 * c)
        return (oy * (side // 2) + ox // 2) * CORES + core, (oy * side + ox) * CORES + core

    def twin_turn(place):
        return g_recv.at[ROUNDS + 1 + place // CORES]

    twin_last = g_recv.at[ROUNDS + 1 + half_count // 4]

    def root_copy(peer, place, half, src=None, dst=None, recv=None, part=None, across=0):
        here = lroot.at[2 * place + half]
        if part is not None:
            here = here.at[pl.ds(*pieces[part])]
        if peer is twin and recv is None:
            recv = twin_turn(place)
        return pltpu.make_async_remote_copy(
            src_ref=here if src is None else src, dst_ref=here if dst is None else dst, send_sem=l_send.at[across],
            recv_sem=l_recv.at[recv] if isinstance(recv, int) else recv, device_id={"tensor": peer}, device_id_type=MESH)

    sent = [0, 0]

    def root_send(peer, place, half, part=None, across=0, **kw):
        sent[across] += root_half if part is None else pieces[part][1]
        root_copy(peer, place, half, part=part, across=across, **kw).start()

    def uncounted(action):
        before = list(sent)
        action()
        sent[:] = before

    def pair_wait(pair, sem):
        pltpu.make_async_copy(pair, pair, sem).wait()

    own_place, _ = root_block(0, 0)
    far_place, _ = root_block(0, 1)
    passing = (y * (side // 2) + ((x - dx + side) % side) // 2) * CORES + c

    def root_start_across():
        for half in (0, 1):
            root_send(helper, own_place, half, across=1, src=lr_ref.at[half], dst=relay.at[half], recv=relay_recv.at[half])

    def root_start():
        for half in (0, 1):
            root_send(up, own_place, half, src=lr_ref.at[half], recv=half)
            root_send(down, own_place, 1 - half, src=lr_ref.at[1 - half], recv=half)
        for half in (0, 1):
            root_send(twin, own_place, half, src=lr_ref.at[half])

    def root_relay(half):
        root_copy(helper, own_place, half, src=lr_ref.at[half], dst=relay.at[half], recv=relay_recv.at[half]).wait_recv()
        root_send(helper, passing, half, across=1, src=relay.at[half], recv=FAR_TURN + half)
        root_send(twin, passing, half, across=1, src=relay.at[half], dst=relay.at[2 + half], recv=relay_recv.at[2])

    def passed_rows(p):
        if p:
            pair_wait(relay.at[pl.ds(2, 2)], relay_recv.at[2])
        source = (y * side + (x - (1 - 2 * p) * dx + side) % side) * CORES + c + p * (1 - 2 * c)
        left = relay[2 * p:2 * p + 2].reshape(lrows, rows)
        do_ref[rows_of(source), :] = jnp.dot(left, xx[0], preferred_element_type=jnp.float32)

    def root_far():
        for half in (0, 1):
            pltpu.make_async_copy(lroot.at[0], lroot.at[0], l_recv.at[FAR_TURN + half]).wait()
            root_send(up, far_place, half, recv=3 + half)
            root_send(twin, far_place, half)
        for half in (1, 0):
            root_send(down, far_place, half, recv=4 - half)

    def root_round(r):
        q, stage = r // 3, r % 3
        pair_wait(lroot.at[pl.ds(0, 2)], l_recv.at[r])
        if stage == 2:
            below = above = root_block(2, q)[0]
        else:
            below, above = root_block(side - 1, q)[0], root_block(1, q)[0]
        if stage == 0:
            for peer, place, half in ((up, below, 0), (down, above, 1)):
                if q == 0:
                    root_send(peer, place, half, recv=2)
                else:
                    for part in (0, 1):
                        root_send(peer, place, half, part=part, recv=LAST_TURN + part)
        root_send(twin, below, stage % 2)
        root_send(twin, above, 1 - stage % 2)

    last_place, last_device = root_block(2, 1)
    twin_place, twin_device = root_block(2, 1, 1)

    def root_last(part):
        pair_wait(lroot.at[pl.ds(0, 2), pl.ds(*pieces[part])], l_recv.at[LAST_TURN + part])
        for half in (0, 1):
            root_send(twin, last_place, half, part=part, recv=twin_last if part else None)

    def root_last_twin(part):
        pair = lroot.at[pl.ds(2 * twin_place, 2), pl.ds(*pieces[part])]
        pair_wait(pair, twin_last if part else twin_turn(twin_place))

    steps(grad, gbuf, load_sem, GRAD_ROUND_STEP, [(RELAY_STEP, lambda: root_relay(0))],
          [(ROOT_ACROSS_STEP, root_start_across), (ROOT_ACROSS_STEP, lambda: pl.when(c == 1)(lambda: uncounted(root_start)))],
          [(ROOT_START_STEP, lambda: pl.when(c == 0)(root_start))], grad_work)

    side_cols = cols // 2

    def x_copy(h):
        at = pl.ds(h * side_cols, side_cols)
        return pltpu.make_async_remote_copy(
            src_ref=xx.at[0, :, at], dst_ref=xx.at[1, :, at], send_sem=x_send.at[h], recv_sem=x_recv.at[h],
            device_id={"tensor": helper}, device_id_type=MESH)

    xx[0] = acc[:, :cols].astype(jnp.bfloat16)
    root_relay(1)
    x_copy(0).start()
    x_copy(1).start()
    root_round(0)

    def left_step(t, carry):
        at = pl.ds(pl.multiple_of(t * lrows, lrows), lrows)
        lo_ref[:, at] = EMA_DECAY * lo_ref[:, at] + (1.0 - EMA_DECAY) * acc[at, cols:].T
        return carry
    lax.fori_loop(0, rows // lrows, left_step, 0)

    def at_step(i):
        e, p = i // 2, i % 2
        dy = lax.shift_right_logical(ROOT_Y, 2 * e) & 3
        q = lax.shift_right_logical(ROOT_X, 2 * e) & 3
        return root_block(dy, q, p)

    def twin_wait(i, place):
        @pl.when(i % 2 == 1)
        def _():
            pair_wait(lroot.at[pl.ds(2 * place, 2)], twin_turn(place))

    def product(place, which):
        left = lroot[pl.ds(2 * place, 2)].reshape(lrows, rows)
        return jnp.dot(left, xx[which], preferred_element_type=jnp.float32)

    def rows_of(device):
        return pl.ds(pl.multiple_of(device * lrows, lrows), lrows)

    def own_rows(i):
        place, device = at_step(i)
        do_ref[rows_of(device), :] = product(place, 0)

    def lent_copy(i, device):
        return pltpu.make_async_remote_copy(
            src_ref=lent.at[i], dst_ref=do_ref.at[rows_of(device)], send_sem=d_send.at[0], recv_sem=d_recv.at[0],
            device_id={"tensor": client}, device_id_type=MESH)

    def lent_rows(i):
        place, device = at_step(i)
        lent[i] = product(place, 1)
        lent_copy(i, device).start()

    def lent_side(i, h):
        place, _ = at_step(i)
        at = pl.ds(h * side_cols, side_cols)
        left = lroot[pl.ds(2 * place, 2)].reshape(lrows, rows)
        lent[i, :, at] = jnp.dot(left, xx[1, :, at], preferred_element_type=jnp.float32)

    def lent_side_copy(i, h):
        _, device = at_step(i)
        at = pl.ds(h * side_cols, side_cols)
        return pltpu.make_async_remote_copy(
            src_ref=lent.at[i, :, at], dst_ref=do_ref.at[rows_of(device), at], send_sem=d_send.at[0], recv_sem=d_recv.at[0],
            device_id={"tensor": client}, device_id_type=MESH)

    def loop(lo, hi, body):
        def step(i, carry):
            body(i)
            return carry
        lax.fori_loop(lo, hi, step, 0)

    def first_own(i):
        @pl.when(i == 2)
        def _():
            root_far()
            root_round(1)

        @pl.when(i == 8)
        def _():
            root_round(2)
        twin_wait(i, at_step(i)[0])
        own_rows(i)

    loop(0, 10, first_own)
    passed_rows(0)
    passed_rows(1)
    x_copy(0).wait_recv()
    def lent_step(j):
        return j + (j + 7) // 8 + j // 5

    loop(0, 8, lambda j: lent_side(lent_step(j), 0))
    x_copy(0).wait_send()
    x_copy(1).wait_send()
    pl.semaphore_signal(x_gone, inc=1, device_id={"tensor": twin}, device_id_type=MESH)
    pl.semaphore_wait(x_gone, 1)
    loop(0, 8, lambda j: lent_side_copy(lent_step(j), 0).start())
    root_round(3)
    x_copy(1).wait_recv()

    def second_side(j):
        i = lent_step(j)
        lent_side(i, 1)
        lent_side_copy(i, 1).start()
    loop(0, 8, second_side)
    root_round(4)

    def both(i):
        twin_wait(i, at_step(i)[0])
        lent_rows(i)
        own_rows(i)
    loop(10, 14, both)

    def lent_piece(i, place, device, part):
        first, count = pieces[part]
        left = jnp.concatenate([lroot[2 * place, pl.ds(first, count), :], lroot[2 * place + 1, pl.ds(first, count), :]], axis=0)
        prod = jnp.dot(left, xx[1], preferred_element_type=jnp.float32)
        for half in (0, 1):
            at = half * root_half + first
            lent[i, pl.ds(at, count), :] = prod[half * count:(half + 1) * count]
            pltpu.make_async_remote_copy(
                src_ref=lent.at[i, pl.ds(at, count)], dst_ref=do_ref.at[pl.ds(pl.multiple_of(device * lrows, lrows) + at, count)],
                send_sem=d_send.at[0], recv_sem=d_recv.at[0], device_id={"tensor": client}, device_id_type=MESH).start()

    def own_piece(part):
        root_last(part)
        lent_piece(14, last_place, last_device, part)

    def twin_piece(part):
        root_last_twin(part)
        lent_piece(15, twin_place, twin_device, part)

    @pl.when(c == 0)
    def _():
        own_piece(0)
        own_piece(1)
        twin_piece(0)
        twin_piece(1)

    @pl.when(c == 1)
    def _():
        uncounted(lambda: own_piece(0))
        twin_piece(0)
        twin_piece(1)
        uncounted(lambda: own_piece(1))

    loop(14, 16, own_rows)

    grad.drain()
    for across, count in enumerate(sent):
        whole = lroot.at[pl.ds(0, count // root_half)]
        pltpu.make_async_copy(whole, whole, l_send.at[across]).wait()
    given = lent.at[pl.ds(0, half_count // 2 - 2)]
    pltpu.make_async_copy(given, given, d_send.at[0]).wait()
    pltpu.make_async_copy(given, given, d_recv.at[0]).wait()


def store_kernel(*refs):
    count = (len(refs) - 1) // 2
    sems = refs[-1]
    pieces = 16
    for i in range(count):
        src, dst = refs[i], refs[count + i]
        step = src.shape[0] // pieces
        for j in range(pieces):
            part = pl.ds(j * step, step)
            pltpu.make_async_copy(src.at[part], dst.at[part], sems.at[i]).start()
    for i in range(count):
        pltpu.make_async_copy(refs[i], refs[count + i], sems.at[i]).wait()


def solution(mesh):
    row_spec = P(("layer", "tensor"), None)
    col_spec = P("layer", "tensor")
    n = mesh.shape["tensor"]
    side = math.isqrt(n // CORES)

    def local_step(g, l, r, lr, rr):
        rows, cols = g.shape
        lrows = l.shape[0]
        kept = n // 2
        hbm = pl.BlockSpec(memory_space=pltpu.HBM)
        vmem = pl.BlockSpec(memory_space=pltpu.VMEM)
        operands = [g.reshape(2, rows // 2, cols), l, r, lr.reshape(2, lrows // 2, rows), rr]
        left_new, right_new, direction, _ = pl.pallas_call(
            functools.partial(kernel, n, side),
            name="shampoo",
            out_shape=[
                pltpu.VMEM(l.shape, jnp.float32),
                pltpu.VMEM(r.shape, jnp.float32),
                pltpu.VMEM(g.shape, jnp.float32),
                pltpu.HBM((2 * n, rows // 2, cols), jnp.bfloat16),
            ],
            in_specs=[hbm] * 5,
            out_specs=[vmem, vmem, vmem, hbm],
            scratch_shapes=[
                pltpu.VMEM(rr.shape, jnp.bfloat16),
                pltpu.VMEM((cols, rows), jnp.bfloat16),
                pltpu.VMEM((rows, cols + lrows), jnp.float32),
                pltpu.VMEM((2, 2, rows // 2, cols), jnp.bfloat16),
                pltpu.VMEM((cols + lrows, cols), jnp.bfloat16),
                pltpu.VMEM((2, rows, cols), jnp.bfloat16),
                pltpu.VMEM((2 * kept, lrows // 2, rows), jnp.bfloat16),
                pltpu.VMEM((4, lrows // 2, rows), jnp.bfloat16),
                pltpu.VMEM((kept, lrows, cols), jnp.float32),
                pltpu.SemaphoreType.DMA((ROUNDS + n // 2,)),
                pltpu.SemaphoreType.DMA((1,)),
                pltpu.SemaphoreType.DMA((2,)),
                pltpu.SemaphoreType.DMA((ROOT_TURNS,)),
                pltpu.SemaphoreType.DMA((3,)),
                pltpu.SemaphoreType.DMA((2,)),
                pltpu.SemaphoreType.DMA((1,)),
                pltpu.SemaphoreType.DMA((2,)),
                pltpu.SemaphoreType.DMA((2,)),
                pltpu.SemaphoreType.DMA((1,)),
                pltpu.SemaphoreType.REGULAR,
            ],
            compiler_params=pltpu.CompilerParams(collective_id=0, has_side_effects=True, vmem_limit_bytes=48 * 2**20),
            cost_estimate=pl.CostEstimate(flops=2 * rows * cols * (2 * n * cols + 2 * rows), bytes_accessed=2 * n * rows * cols * 3, transcendentals=0),
        )(*[pltpu.with_memory_space_constraint(v, pltpu.HBM) for v in operands])
        results = [left_new, right_new, direction]
        return pl.pallas_call(
            store_kernel,
            name="store",
            out_shape=[jax.ShapeDtypeStruct(v.shape, v.dtype) for v in results],
            in_specs=[vmem] * 3,
            out_specs=[hbm] * 3,
            scratch_shapes=[pltpu.SemaphoreType.DMA((3,))],
            compiler_params=pltpu.CompilerParams(vmem_limit_bytes=1 * 2**20),
        )(*results)

    return jax.shard_map(local_step, mesh=mesh, in_specs=(col_spec, row_spec, row_spec, row_spec, row_spec), out_specs=(row_spec, row_spec, col_spec), check_vma=False)
```

```python
import functools
import math

import jax
import jax.numpy as jnp
from jax import lax
from jax.experimental import pallas as pl
from jax.experimental.pallas import tpu as pltpu
from jax.sharding import PartitionSpec as P

EMA_DECAY = 0.9
CORES = 2
MESH = pl.DeviceIdType.MESH

ORDER = [(int(a), int(b)) for a, b in zip("0310020311322312", "0003102313131222")]
def parcels(code):
    digits = [int(d) for d in code]
    return [((a, b), h) for a, b, h in zip(digits[0::3], digits[1::3], digits[2::3])]


UP = parcels("030031330131020331130230231320120220")
UP_ON = {0: parcels("030"), 2: parcels("330"), 6: parcels("130"), 7: parcels("230")}
DOWN = parcels("011010111310021110311211210321121221")
DOWN_ON = {0: parcels("011"), 6: parcels("311111"), 7: parcels("211")}
ROUNDS = len(UP)
FIRST_UP = parcels("300301200")
FIRST_DOWN = parcels("101100201")
GRAD_ROUND_STEP = [2, 2, 8, 10, 12, 14, 17, 20, 22, 26, 28, 30]
LAST_FORWARD = 7
SIDE_UP, SIDE_DOWN = 9, 10
ASIDE = {"+": 29, "-": 37}
ROOT_START_STEP = 28
ROOT_ACROSS_STEP = 30
RELAY_STEP = 32
LATE = (2, 12, 14, 22, 26, 28, 30)


def round_of(name, offset, half):
    a, b = offset
    table, da, db = {"f+": (FIRST_UP, 3, 0), "f-": (FIRST_DOWN, 1, 0), "s+": (UP, 0, 3), "s-": (DOWN, 0, 1)}[name]
    return table.index((((a + da) % 4, (b + db) % 4), half))


def packed(values):
    return [sum(v << (2 * i) for i, v in enumerate(values[j:j + 8])) for j in (0, 8)]


FIRST_CODE = packed([o[0] for o in ORDER])
SECOND_CODE = packed([o[1] for o in ORDER])


def lookup(code, e):
    word = code[0] + (e // 8) * (code[1] - code[0])
    return lax.shift_right_logical(word, 2 * (e % 8)) & 3


ROOT_ORDER = [(0, 0), (3, 0), (1, 0), (0, 1), (2, 0), (3, 1), (1, 1), (2, 1)]
ROOT_Y = sum(o[0] << (2 * i) for i, o in enumerate(ROOT_ORDER))
FAR_TURN, LAST_TURN, ROOT_TURNS = 5, 7, 9
ROOT_X = sum(o[1] << (2 * i) for i, o in enumerate(ROOT_ORDER))


def kernel(n, side, g_ref, l_ref, r_ref, lr_ref, rr_ref, lo_ref, ro_ref, do_ref, gfull,
           rr, gt, acc, gbuf, rhs, xx, lroot, relay, lent,
           g_recv, g_send, load_sem, l_recv, relay_recv, x_recv, d_recv, l_send, x_send, d_send, x_gone):
    _, half_rows, cols = g_ref.shape
    rows = 2 * half_rows
    lrows = l_ref.shape[0]
    tile = min(1024, half_rows)
    aside_rows = {way: half_rows * share // 128 for way, share in ASIDE.items()}

    me = lax.axis_index("tensor")
    c = me % CORES
    chip = me // CORES
    x, y = chip % side, chip // side
    f = x + c * (y - x)
    s = y + c * (x - y)
    fstep = CORES + c * CORES * (side - 1)
    sstep = CORES * side - c * CORES * (side - 1)
    twin = me + 1 - 2 * c

    def index(df, ds):
        return ((f + df) % side) * fstep + ((s + ds) % side) * sstep + c

    def twin_index(df, ds):
        return ((s + df) % side) * sstep + ((f + ds) % side) * fstep + 1 - c

    peers = {"f+": index(1, 0), "f-": index(3, 0), "s+": index(0, 1), "s-": index(0, 3), "twin": twin}

    class Gather:
        def __init__(self, own, full, recv, send):
            self.own, self.full, self.recv, self.send_sem = own, full, recv, send
            self.sent = 0

        def copy(self, name, offset, half, part=None, turn=None):
            b = index(*offset)
            src = self.own.at[half] if offset == (0, 0) else self.full.at[2 * b + half]
            dst = self.full.at[2 * b + half]
            if part is not None:
                src, dst = src.at[pl.ds(*part)], dst.at[pl.ds(*part)]
            if turn is None:
                turn = ROUNDS + ORDER.index(offset) if name == "twin" else round_of(name, offset, half)
            return pltpu.make_async_remote_copy(
                src_ref=src, dst_ref=dst, send_sem=self.send_sem.at[0], recv_sem=self.recv.at[turn],
                device_id={"tensor": peers[name]}, device_id_type=MESH)

        def send(self, name, offset, half):
            self.sent += 1
            self.copy(name, offset, half).start()

        def wait(self, turn, count):
            taken = self.full.at[pl.ds(0, count)]
            pltpu.make_async_copy(taken, taken, self.recv.at[turn]).wait()

        def start(self):
            for half in (0, 1):
                for name in ("f+", "s+"):
                    self.send(name, (0, 0), half)
                for name in ("f-", "s-"):
                    self.send(name, (0, 0), 1 - half)
            for half in (0, 1):
                self.send("twin", (0, 0), half)

        def round(self, r):
            first = r < len(FIRST_UP)
            self.wait(r, 4 if first else 2)
            if first:
                above, below = FIRST_UP[r], FIRST_DOWN[r]
                if r == 0:
                    self.send("f+", *above)
                    self.send("f-", *below)
                self.send("s+", *above)
                self.send("s-", *below)
                self.send("s+", *below)
                self.send("s-", *above)
                self.send("twin", *above)
                self.send("twin", *below)
            for name, table in (("s+", UP_ON), ("s-", DOWN_ON)):
                for parcel in table.get(r, ()):
                    if r == LAST_FORWARD:
                        self.forward_last(name, *parcel)
                    else:
                        self.send(name, *parcel)
            if r == SIDE_UP:
                self.aside("f+", *UP[r])
            if r == SIDE_DOWN:
                self.aside("f-", *DOWN[r])
            self.send("twin", *UP[r])
            self.send("twin", *DOWN[r])

        def forward_last(self, name, offset, half):
            self.sent += 1
            pl.when(c == 0)(lambda: self.copy(name, offset, half, part=(0, half_rows - aside_rows[name[1]])).start())
            pl.when(c == 1)(lambda: self.copy(name, offset, half).start())

        def aside(self, name, offset, half):
            count = aside_rows[name[1]]
            part = (half_rows - count, count)
            pl.when(c == 0)(lambda: self.copy(name, offset, half, part=part, turn=ROUNDS - 1).start())

        def drain(self):
            whole = self.full.at[pl.ds(0, self.sent)]
            pltpu.make_async_copy(whole, whole, self.send_sem.at[0]).wait()

    grad = Gather(g_ref, gfull, g_recv, g_send)

    def block_of(k):
        e, other = k // 2, k % 2
        df, ds = lookup(FIRST_CODE, e), lookup(SECOND_CODE, e)
        mine = index(df, ds)
        return mine + other * (twin_index(df, ds) - mine)

    def load(gather, buf, k, sem):
        b = block_of(k)
        return pltpu.make_async_copy(gather.full.at[pl.ds(2 * b, 2)], buf.at[k % 2], sem.at[k % 2])

    def one_of(k, values):
        found = k == values[0]
        for v in values[1:]:
            found = found | (k == v)
        return found

    def steps(gather, buf, sem, round_step, early, between, after, work):
        def at_steps(k, actions):
            for at, action in actions:
                pl.when(k == at)(action)

        def step(k, carry):
            at_steps(k, early)

            @pl.when((k % 2 == 1) & (k < n))
            def _():
                gather.wait(ROUNDS + k // 2, 2)

            @pl.when(jnp.logical_not(one_of(k, LATE)) & (k < n))
            def _():
                load(gather, buf, k, sem).start()
            load(gather, buf, k - 1, sem).wait()
            work((k - 1) % 2, block_of(k - 1))
            at_steps(k, between)
            for r in range(ROUNDS):
                @pl.when(k == round_step[r])
                def _():
                    gather.round(r)
            at_steps(k, after)

            @pl.when(one_of(k, LATE))
            def _():
                load(gather, buf, k, sem).start()
            return carry
        lax.fori_loop(1, n + 1, step, 0)

    barrier = pltpu.get_barrier_semaphore()
    for peer in peers.values():
        pl.semaphore_signal(barrier, inc=1, device_id={"tensor": peer}, device_id_type=MESH)

    first = [
        pltpu.make_async_copy(rr_ref, rr, x_send.at[0]),
        pltpu.make_async_copy(r_ref, ro_ref, x_send.at[1]),
        pltpu.make_async_copy(l_ref, lo_ref, d_send.at[0]),
        pltpu.make_async_copy(lr_ref, lroot.at[pl.ds(2 * ((y * (side // 2) + x // 2) * CORES + c), 2)], l_send.at[0]),
    ]
    own_load = pltpu.make_async_copy(g_ref, gbuf.at[0], load_sem.at[0])
    own_load.start()
    for copy in first:
        copy.start()

    pl.semaphore_wait(barrier, len(peers))
    grad.start()

    acc[...] = jnp.zeros_like(acc)
    own_load.wait()
    for h in (0, 1):
        gt[:, h * half_rows:(h + 1) * half_rows] = gbuf[0, h].T
    for copy in first:
        copy.wait()
    own_load.start()

    per_half = half_rows // tile

    def grad_work(slot, b):
        at = pl.multiple_of(b * cols, cols)
        rhs[:cols] = rr[:, pl.ds(at, cols)]
        rhs[cols:] = gbuf[slot, me // (n // 2), pl.ds(pl.multiple_of((me % (n // 2)) * lrows, lrows), lrows), :]

        def rows_step(t, carry):
            left = gbuf[slot, t // per_half, pl.ds(pl.multiple_of((t % per_half) * tile, tile), tile), :]
            out = pl.ds(pl.multiple_of(t * tile, tile), tile)
            acc[out, :] += lax.dot_general(left, rhs[...], (((1,), (1,)), ((), ())), preferred_element_type=jnp.float32)
            return carry
        lax.fori_loop(0, 2 * per_half, rows_step, 0)
        prod = jnp.dot(gt[:, :half_rows], gbuf[slot, 0], preferred_element_type=jnp.float32)
        prod += jnp.dot(gt[:, half_rows:], gbuf[slot, 1], preferred_element_type=jnp.float32)
        ro_ref[:, pl.ds(at, cols)] = EMA_DECAY * ro_ref[:, pl.ds(at, cols)] + (1.0 - EMA_DECAY) * prod


    dx = 1 - 2 * c
    helper = (y * side + (x + dx + side) % side) * CORES + c
    client = (y * side + (x - dx + side) % side) * CORES + c
    up = (((y + 1) % side) * side + x) * CORES + c
    down = (((y + side - 1) % side) * side + x) * CORES + c
    half_count, root_half, _ = lroot.shape
    pieces = ((0, root_half - root_half // 4), (root_half - root_half // 4, root_half // 4))

    def root_block(dy, q, p=0):
        oy, ox = (y + dy) % side, (x + 2 * q) % side
        core = c + p * (1 - 2 * c)
        return (oy * (side // 2) + ox // 2) * CORES + core, (oy * side + ox) * CORES + core

    def twin_turn(place):
        return g_recv.at[ROUNDS + 1 + place // CORES]

    twin_last = g_recv.at[ROUNDS + 1 + half_count // 4]

    def root_copy(peer, place, half, src=None, dst=None, recv=None, part=None, across=0):
        here = lroot.at[2 * place + half]
        if part is not None:
            here = here.at[pl.ds(*pieces[part])]
        if peer is twin and recv is None:
            recv = twin_turn(place)
        return pltpu.make_async_remote_copy(
            src_ref=here if src is None else src, dst_ref=here if dst is None else dst, send_sem=l_send.at[across],
            recv_sem=l_recv.at[recv] if isinstance(recv, int) else recv, device_id={"tensor": peer}, device_id_type=MESH)

    sent = [0, 0]

    def root_send(peer, place, half, part=None, across=0, **kw):
        sent[across] += root_half if part is None else pieces[part][1]
        root_copy(peer, place, half, part=part, across=across, **kw).start()

    def uncounted(action):
        before = list(sent)
        action()
        sent[:] = before

    def pair_wait(pair, sem):
        pltpu.make_async_copy(pair, pair, sem).wait()

    own_place, _ = root_block(0, 0)
    far_place, _ = root_block(0, 1)
    passing = (y * (side // 2) + ((x - dx + side) % side) // 2) * CORES + c

    def root_start_across():
        for half in (0, 1):
            root_send(helper, own_place, half, across=1, src=lr_ref.at[half], dst=relay.at[half], recv=relay_recv.at[half])

    def root_start():
        for half in (0, 1):
            root_send(up, own_place, half, src=lr_ref.at[half], recv=half)
            root_send(down, own_place, 1 - half, src=lr_ref.at[1 - half], recv=half)
        for half in (0, 1):
            root_send(twin, own_place, half, src=lr_ref.at[half])

    def root_relay(half):
        root_copy(helper, own_place, half, src=lr_ref.at[half], dst=relay.at[half], recv=relay_recv.at[half]).wait_recv()
        root_send(helper, passing, half, across=1, src=relay.at[half], recv=FAR_TURN + half)
        root_send(twin, passing, half, across=1, src=relay.at[half], dst=relay.at[2 + half], recv=relay_recv.at[2])

    def passed_rows(p):
        if p:
            pair_wait(relay.at[pl.ds(2, 2)], relay_recv.at[2])
        source = (y * side + (x - (1 - 2 * p) * dx + side) % side) * CORES + c + p * (1 - 2 * c)
        left = relay[2 * p:2 * p + 2].reshape(lrows, rows)
        do_ref[rows_of(source), :] = jnp.dot(left, xx[0], preferred_element_type=jnp.float32)

    def root_far():
        for half in (0, 1):
            pltpu.make_async_copy(lroot.at[0], lroot.at[0], l_recv.at[FAR_TURN + half]).wait()
            root_send(up, far_place, half, recv=3 + half)
            root_send(twin, far_place, half)
        for half in (1, 0):
            root_send(down, far_place, half, recv=4 - half)

    def root_round(r):
        q, stage = r // 3, r % 3
        pair_wait(lroot.at[pl.ds(0, 2)], l_recv.at[r])
        if stage == 2:
            below = above = root_block(2, q)[0]
        else:
            below, above = root_block(side - 1, q)[0], root_block(1, q)[0]
        if stage == 0:
            for peer, place, half in ((up, below, 0), (down, above, 1)):
                if q == 0:
                    root_send(peer, place, half, recv=2)
                else:
                    for part in (0, 1):
                        root_send(peer, place, half, part=part, recv=LAST_TURN + part)
        root_send(twin, below, stage % 2)
        root_send(twin, above, 1 - stage % 2)

    last_place, last_device = root_block(2, 1)
    twin_place, twin_device = root_block(2, 1, 1)

    def root_last(part):
        pair_wait(lroot.at[pl.ds(0, 2), pl.ds(*pieces[part])], l_recv.at[LAST_TURN + part])
        for half in (0, 1):
            root_send(twin, last_place, half, part=part, recv=twin_last if part else None)

    def root_last_twin(part):
        pair = lroot.at[pl.ds(2 * twin_place, 2), pl.ds(*pieces[part])]
        pair_wait(pair, twin_last if part else twin_turn(twin_place))

    steps(grad, gbuf, load_sem, GRAD_ROUND_STEP, [(RELAY_STEP, lambda: root_relay(0))],
          [(ROOT_ACROSS_STEP, root_start_across), (ROOT_ACROSS_STEP, lambda: pl.when(c == 1)(lambda: uncounted(root_start)))],
          [(ROOT_START_STEP, lambda: pl.when(c == 0)(root_start))], grad_work)

    side_cols = cols // 2

    def x_copy(h):
        at = pl.ds(h * side_cols, side_cols)
        return pltpu.make_async_remote_copy(
            src_ref=xx.at[0, :, at], dst_ref=xx.at[1, :, at], send_sem=x_send.at[h], recv_sem=x_recv.at[h],
            device_id={"tensor": helper}, device_id_type=MESH)

    xx[0] = acc[:, :cols].astype(jnp.bfloat16)
    root_relay(1)
    x_copy(0).start()
    x_copy(1).start()
    root_round(0)

    def left_step(t, carry):
        at = pl.ds(pl.multiple_of(t * lrows, lrows), lrows)
        lo_ref[:, at] = EMA_DECAY * lo_ref[:, at] + (1.0 - EMA_DECAY) * acc[at, cols:].T
        return carry
    lax.fori_loop(0, rows // lrows, left_step, 0)

    def at_step(i):
        e, p = i // 2, i % 2
        dy = lax.shift_right_logical(ROOT_Y, 2 * e) & 3
        q = lax.shift_right_logical(ROOT_X, 2 * e) & 3
        return root_block(dy, q, p)

    def twin_wait(i, place):
        @pl.when(i % 2 == 1)
        def _():
            pair_wait(lroot.at[pl.ds(2 * place, 2)], twin_turn(place))

    def product(place, which):
        left = lroot[pl.ds(2 * place, 2)].reshape(lrows, rows)
        return jnp.dot(left, xx[which], preferred_element_type=jnp.float32)

    def rows_of(device):
        return pl.ds(pl.multiple_of(device * lrows, lrows), lrows)

    def own_rows(i):
        place, device = at_step(i)
        do_ref[rows_of(device), :] = product(place, 0)

    def lent_copy(i, device):
        return pltpu.make_async_remote_copy(
            src_ref=lent.at[i], dst_ref=do_ref.at[rows_of(device)], send_sem=d_send.at[0], recv_sem=d_recv.at[0],
            device_id={"tensor": client}, device_id_type=MESH)

    def lent_rows(i):
        place, device = at_step(i)
        lent[i] = product(place, 1)
        lent_copy(i, device).start()

    def lent_side(i, h):
        place, _ = at_step(i)
        at = pl.ds(h * side_cols, side_cols)
        left = lroot[pl.ds(2 * place, 2)].reshape(lrows, rows)
        lent[i, :, at] = jnp.dot(left, xx[1, :, at], preferred_element_type=jnp.float32)

    def lent_side_copy(i, h):
        _, device = at_step(i)
        at = pl.ds(h * side_cols, side_cols)
        return pltpu.make_async_remote_copy(
            src_ref=lent.at[i, :, at], dst_ref=do_ref.at[rows_of(device), at], send_sem=d_send.at[0], recv_sem=d_recv.at[0],
            device_id={"tensor": client}, device_id_type=MESH)

    def loop(lo, hi, body):
        def step(i, carry):
            body(i)
            return carry
        lax.fori_loop(lo, hi, step, 0)

    def first_own(i):
        @pl.when(i == 2)
        def _():
            root_far()
            root_round(1)

        @pl.when(i == 8)
        def _():
            root_round(2)
        twin_wait(i, at_step(i)[0])
        own_rows(i)

    loop(0, 10, first_own)
    passed_rows(0)
    passed_rows(1)
    x_copy(0).wait_recv()
    def lent_step(j):
        return j + (j + 7) // 8 + j // 5

    loop(0, 8, lambda j: lent_side(lent_step(j), 0))
    x_copy(0).wait_send()
    x_copy(1).wait_send()
    pl.semaphore_signal(x_gone, inc=1, device_id={"tensor": twin}, device_id_type=MESH)
    pl.semaphore_wait(x_gone, 1)
    loop(0, 8, lambda j: lent_side_copy(lent_step(j), 0).start())
    root_round(3)
    x_copy(1).wait_recv()

    def second_side(j):
        i = lent_step(j)
        lent_side(i, 1)
        lent_side_copy(i, 1).start()
    loop(0, 8, second_side)
    root_round(4)

    def both(i):
        twin_wait(i, at_step(i)[0])
        lent_rows(i)
        own_rows(i)
    loop(10, 14, both)

    def lent_piece(i, place, device, part):
        first, count = pieces[part]
        left = jnp.concatenate([lroot[2 * place, pl.ds(first, count), :], lroot[2 * place + 1, pl.ds(first, count), :]], axis=0)
        prod = jnp.dot(left, xx[1], preferred_element_type=jnp.float32)
        for half in (0, 1):
            at = half * root_half + first
            lent[i, pl.ds(at, count), :] = prod[half * count:(half + 1) * count]
            pltpu.make_async_remote_copy(
                src_ref=lent.at[i, pl.ds(at, count)], dst_ref=do_ref.at[pl.ds(pl.multiple_of(device * lrows, lrows) + at, count)],
                send_sem=d_send.at[0], recv_sem=d_recv.at[0], device_id={"tensor": client}, device_id_type=MESH).start()

    def own_piece(part):
        root_last(part)
        lent_piece(14, last_place, last_device, part)

    def twin_piece(part):
        root_last_twin(part)
        lent_piece(15, twin_place, twin_device, part)

    @pl.when(c == 0)
    def _():
        own_piece(0)
        own_piece(1)
        twin_piece(0)
        twin_piece(1)

    @pl.when(c == 1)
    def _():
        uncounted(lambda: own_piece(0))
        twin_piece(0)
        twin_piece(1)
        uncounted(lambda: own_piece(1))

    loop(14, 16, own_rows)

    grad.drain()
    for across, count in enumerate(sent):
        whole = lroot.at[pl.ds(0, count // root_half)]
        pltpu.make_async_copy(whole, whole, l_send.at[across]).wait()
    given = lent.at[pl.ds(0, half_count // 2 - 2)]
    pltpu.make_async_copy(given, given, d_send.at[0]).wait()
    pltpu.make_async_copy(given, given, d_recv.at[0]).wait()


def store_kernel(*refs):
    count = (len(refs) - 1) // 2
    sems = refs[-1]
    pieces = 32
    for i in range(count):
        src, dst = refs[i], refs[count + i]
        step = src.shape[0] // pieces
        for j in range(pieces):
            part = pl.ds(j * step, step)
            pltpu.make_async_copy(src.at[part], dst.at[part], sems.at[i]).start()
    for i in range(count):
        pltpu.make_async_copy(refs[i], refs[count + i], sems.at[i]).wait()


def solution(mesh):
    row_spec = P(("layer", "tensor"), None)
    col_spec = P("layer", "tensor")
    n = mesh.shape["tensor"]
    side = math.isqrt(n // CORES)

    def local_step(g, l, r, lr, rr):
        rows, cols = g.shape
        lrows = l.shape[0]
        kept = n // 2
        hbm = pl.BlockSpec(memory_space=pltpu.HBM)
        vmem = pl.BlockSpec(memory_space=pltpu.VMEM)
        operands = [g.reshape(2, rows // 2, cols), l, r, lr.reshape(2, lrows // 2, rows), rr]
        left_new, right_new, direction, _ = pl.pallas_call(
            functools.partial(kernel, n, side),
            name="shampoo",
            out_shape=[
                pltpu.VMEM(l.shape, jnp.float32),
                pltpu.VMEM(r.shape, jnp.float32),
                pltpu.VMEM(g.shape, jnp.float32),
                pltpu.HBM((2 * n, rows // 2, cols), jnp.bfloat16),
            ],
            in_specs=[hbm] * 5,
            out_specs=[vmem, vmem, vmem, hbm],
            scratch_shapes=[
                pltpu.VMEM(rr.shape, jnp.bfloat16),
                pltpu.VMEM((cols, rows), jnp.bfloat16),
                pltpu.VMEM((rows, cols + lrows), jnp.float32),
                pltpu.VMEM((2, 2, rows // 2, cols), jnp.bfloat16),
                pltpu.VMEM((cols + lrows, cols), jnp.bfloat16),
                pltpu.VMEM((2, rows, cols), jnp.bfloat16),
                pltpu.VMEM((2 * kept, lrows // 2, rows), jnp.bfloat16),
                pltpu.VMEM((4, lrows // 2, rows), jnp.bfloat16),
                pltpu.VMEM((kept, lrows, cols), jnp.float32),
                pltpu.SemaphoreType.DMA((ROUNDS + n // 2,)),
                pltpu.SemaphoreType.DMA((1,)),
                pltpu.SemaphoreType.DMA((2,)),
                pltpu.SemaphoreType.DMA((ROOT_TURNS,)),
                pltpu.SemaphoreType.DMA((3,)),
                pltpu.SemaphoreType.DMA((2,)),
                pltpu.SemaphoreType.DMA((1,)),
                pltpu.SemaphoreType.DMA((2,)),
                pltpu.SemaphoreType.DMA((2,)),
                pltpu.SemaphoreType.DMA((1,)),
                pltpu.SemaphoreType.REGULAR,
            ],
            compiler_params=pltpu.CompilerParams(collective_id=0, has_side_effects=True, vmem_limit_bytes=48 * 2**20),
            cost_estimate=pl.CostEstimate(flops=2 * rows * cols * (2 * n * cols + 2 * rows), bytes_accessed=2 * n * rows * cols * 3, transcendentals=0),
        )(*[pltpu.with_memory_space_constraint(v, pltpu.HBM) for v in operands])
        results = [left_new, right_new, direction]
        return pl.pallas_call(
            store_kernel,
            name="store",
            out_shape=[jax.ShapeDtypeStruct(v.shape, v.dtype) for v in results],
            in_specs=[vmem] * 3,
            out_specs=[hbm] * 3,
            scratch_shapes=[pltpu.SemaphoreType.DMA((3,))],
            compiler_params=pltpu.CompilerParams(vmem_limit_bytes=1 * 2**20),
        )(*results)

    return jax.shard_map(local_step, mesh=mesh, in_specs=(col_spec, row_spec, row_spec, row_spec, row_spec), out_specs=(row_spec, row_spec, col_spec), check_vma=False)
```

```python
import functools
import math

import jax
import jax.numpy as jnp
from jax import lax
from jax.experimental import pallas as pl
from jax.experimental.pallas import tpu as pltpu
from jax.sharding import PartitionSpec as P

EMA_DECAY = 0.9
CORES = 2
MESH = pl.DeviceIdType.MESH

ORDER = [(int(a), int(b)) for a, b in zip("0310020311322312", "0003102313131222")]
def parcels(code):
    digits = [int(d) for d in code]
    return [((a, b), h) for a, b, h in zip(digits[0::3], digits[1::3], digits[2::3])]


UP = parcels("030031330131020331130230231320120220")
UP_ON = {0: parcels("030"), 2: parcels("330"), 6: parcels("130"), 7: parcels("230")}
DOWN = parcels("011010111310021110311211210321121221")
DOWN_ON = {0: parcels("011"), 6: parcels("311111"), 7: parcels("211")}
ROUNDS = len(UP)
FIRST_UP = parcels("300301200")
FIRST_DOWN = parcels("101100201")
GRAD_ROUND_STEP = [2, 2, 8, 10, 12, 14, 17, 20, 22, 26, 28, 30]
LAST_FORWARD = 7
SIDE_UP, SIDE_DOWN = 9, 10
ASIDE = {"+": 33, "-": 33}
ROOT_START_STEP = 28
ROOT_ACROSS_STEP = 30
RELAY_STEP = 32
LATE = (2, 12, 14, 22, 26, 28, 30)


def round_of(name, offset, half):
    a, b = offset
    table, da, db = {"f+": (FIRST_UP, 3, 0), "f-": (FIRST_DOWN, 1, 0), "s+": (UP, 0, 3), "s-": (DOWN, 0, 1)}[name]
    return table.index((((a + da) % 4, (b + db) % 4), half))


def packed(values):
    return [sum(v << (2 * i) for i, v in enumerate(values[j:j + 8])) for j in (0, 8)]


FIRST_CODE = packed([o[0] for o in ORDER])
SECOND_CODE = packed([o[1] for o in ORDER])


def lookup(code, e):
    word = code[0] + (e // 8) * (code[1] - code[0])
    return lax.shift_right_logical(word, 2 * (e % 8)) & 3


ROOT_ORDER = [(0, 0), (3, 0), (1, 0), (0, 1), (2, 0), (3, 1), (1, 1), (2, 1)]
ROOT_Y = sum(o[0] << (2 * i) for i, o in enumerate(ROOT_ORDER))
FAR_TURN, LAST_TURN, ROOT_TURNS = 5, 7, 9
ROOT_X = sum(o[1] << (2 * i) for i, o in enumerate(ROOT_ORDER))


def kernel(n, side, g_ref, l_ref, r_ref, lr_ref, rr_ref, lo_ref, ro_ref, do_ref, gfull,
           rr, gt, acc, gbuf, rhs, xx, lroot, relay, lent,
           g_recv, g_send, load_sem, l_recv, relay_recv, x_recv, d_recv, l_send, x_send, d_send, x_gone):
    _, half_rows, cols = g_ref.shape
    rows = 2 * half_rows
    lrows = l_ref.shape[0]
    tile = min(1024, half_rows)
    aside_rows = {way: half_rows * share // 128 for way, share in ASIDE.items()}

    me = lax.axis_index("tensor")
    c = me % CORES
    chip = me // CORES
    x, y = chip % side, chip // side
    f = x + c * (y - x)
    s = y + c * (x - y)
    fstep = CORES + c * CORES * (side - 1)
    sstep = CORES * side - c * CORES * (side - 1)
    twin = me + 1 - 2 * c

    def index(df, ds):
        return ((f + df) % side) * fstep + ((s + ds) % side) * sstep + c

    def twin_index(df, ds):
        return ((s + df) % side) * sstep + ((f + ds) % side) * fstep + 1 - c

    peers = {"f+": index(1, 0), "f-": index(3, 0), "s+": index(0, 1), "s-": index(0, 3), "twin": twin}

    class Gather:
        def __init__(self, own, full, recv, send):
            self.own, self.full, self.recv, self.send_sem = own, full, recv, send
            self.sent = 0

        def copy(self, name, offset, half, part=None, turn=None):
            b = index(*offset)
            src = self.own.at[half] if offset == (0, 0) else self.full.at[2 * b + half]
            dst = self.full.at[2 * b + half]
            if part is not None:
                src, dst = src.at[pl.ds(*part)], dst.at[pl.ds(*part)]
            if turn is None:
                turn = ROUNDS + ORDER.index(offset) if name == "twin" else round_of(name, offset, half)
            return pltpu.make_async_remote_copy(
                src_ref=src, dst_ref=dst, send_sem=self.send_sem.at[0], recv_sem=self.recv.at[turn],
                device_id={"tensor": peers[name]}, device_id_type=MESH)

        def send(self, name, offset, half):
            self.sent += 1
            self.copy(name, offset, half).start()

        def wait(self, turn, count):
            taken = self.full.at[pl.ds(0, count)]
            pltpu.make_async_copy(taken, taken, self.recv.at[turn]).wait()

        def start(self):
            for half in (0, 1):
                for name in ("f+", "s+"):
                    self.send(name, (0, 0), half)
                for name in ("f-", "s-"):
                    self.send(name, (0, 0), 1 - half)
            for half in (0, 1):
                self.send("twin", (0, 0), half)

        def round(self, r):
            first = r < len(FIRST_UP)
            self.wait(r, 4 if first else 2)
            if first:
                above, below = FIRST_UP[r], FIRST_DOWN[r]
                if r == 0:
                    self.send("f+", *above)
                    self.send("f-", *below)
                self.send("s+", *above)
                self.send("s-", *below)
                self.send("s+", *below)
                self.send("s-", *above)
                self.send("twin", *above)
                self.send("twin", *below)
            for name, table in (("s+", UP_ON), ("s-", DOWN_ON)):
                for parcel in table.get(r, ()):
                    if r == LAST_FORWARD:
                        self.forward_last(name, *parcel)
                    else:
                        self.send(name, *parcel)
            if r == SIDE_UP:
                self.aside("f+", *UP[r])
            if r == SIDE_DOWN:
                self.aside("f-", *DOWN[r])
            self.send("twin", *UP[r])
            self.send("twin", *DOWN[r])

        def forward_last(self, name, offset, half):
            self.sent += 1
            pl.when(c == 0)(lambda: self.copy(name, offset, half, part=(0, half_rows - aside_rows[name[1]])).start())
            pl.when(c == 1)(lambda: self.copy(name, offset, half).start())

        def aside(self, name, offset, half):
            count = aside_rows[name[1]]
            part = (half_rows - count, count)
            pl.when(c == 0)(lambda: self.copy(name, offset, half, part=part, turn=ROUNDS - 1).start())

        def drain(self):
            whole = self.full.at[pl.ds(0, self.sent)]
            pltpu.make_async_copy(whole, whole, self.send_sem.at[0]).wait()

    grad = Gather(g_ref, gfull, g_recv, g_send)

    def block_of(k):
        e, other = k // 2, k % 2
        df, ds = lookup(FIRST_CODE, e), lookup(SECOND_CODE, e)
        mine = index(df, ds)
        return mine + other * (twin_index(df, ds) - mine)

    def load(gather, buf, k, sem):
        b = block_of(k)
        return pltpu.make_async_copy(gather.full.at[pl.ds(2 * b, 2)], buf.at[k % 2], sem.at[k % 2])

    def one_of(k, values):
        found = k == values[0]
        for v in values[1:]:
            found = found | (k == v)
        return found

    def steps(gather, buf, sem, round_step, early, between, after, work):
        def at_steps(k, actions):
            for at, action in actions:
                pl.when(k == at)(action)

        def step(k, carry):
            at_steps(k, early)

            @pl.when((k % 2 == 1) & (k < n))
            def _():
                gather.wait(ROUNDS + k // 2, 2)

            @pl.when(jnp.logical_not(one_of(k, LATE)) & (k < n))
            def _():
                load(gather, buf, k, sem).start()
            load(gather, buf, k - 1, sem).wait()
            work((k - 1) % 2, block_of(k - 1))
            at_steps(k, between)
            for r in range(ROUNDS):
                @pl.when(k == round_step[r])
                def _():
                    gather.round(r)
            at_steps(k, after)

            @pl.when(one_of(k, LATE))
            def _():
                load(gather, buf, k, sem).start()
            return carry
        lax.fori_loop(1, n + 1, step, 0)

    barrier = pltpu.get_barrier_semaphore()
    for peer in peers.values():
        pl.semaphore_signal(barrier, inc=1, device_id={"tensor": peer}, device_id_type=MESH)

    first = [
        pltpu.make_async_copy(rr_ref, rr, x_send.at[0]),
        pltpu.make_async_copy(r_ref, ro_ref, x_send.at[1]),
        pltpu.make_async_copy(l_ref, lo_ref, d_send.at[0]),
        pltpu.make_async_copy(lr_ref, lroot.at[pl.ds(2 * ((y * (side // 2) + x // 2) * CORES + c), 2)], l_send.at[0]),
    ]
    own_load = pltpu.make_async_copy(g_ref, gbuf.at[0], load_sem.at[0])
    own_load.start()
    for copy in first:
        copy.start()

    pl.semaphore_wait(barrier, len(peers))
    grad.start()

    acc[...] = jnp.zeros_like(acc)
    own_load.wait()
    for h in (0, 1):
        gt[:, h * half_rows:(h + 1) * half_rows] = gbuf[0, h].T
    for copy in first:
        copy.wait()
    own_load.start()

    per_half = half_rows // tile

    def grad_work(slot, b):
        at = pl.multiple_of(b * cols, cols)
        rhs[:cols] = rr[:, pl.ds(at, cols)]
        rhs[cols:] = gbuf[slot, me // (n // 2), pl.ds(pl.multiple_of((me % (n // 2)) * lrows, lrows), lrows), :]

        def rows_step(t, carry):
            left = gbuf[slot, t // per_half, pl.ds(pl.multiple_of((t % per_half) * tile, tile), tile), :]
            out = pl.ds(pl.multiple_of(t * tile, tile), tile)
            acc[out, :] += lax.dot_general(left, rhs[...], (((1,), (1,)), ((), ())), preferred_element_type=jnp.float32)
            return carry
        lax.fori_loop(0, 2 * per_half, rows_step, 0)
        prod = jnp.dot(gt[:, :half_rows], gbuf[slot, 0], preferred_element_type=jnp.float32)
        prod += jnp.dot(gt[:, half_rows:], gbuf[slot, 1], preferred_element_type=jnp.float32)
        ro_ref[:, pl.ds(at, cols)] = EMA_DECAY * ro_ref[:, pl.ds(at, cols)] + (1.0 - EMA_DECAY) * prod


    dx = 1 - 2 * c
    helper = (y * side + (x + dx + side) % side) * CORES + c
    client = (y * side + (x - dx + side) % side) * CORES + c
    up = (((y + 1) % side) * side + x) * CORES + c
    down = (((y + side - 1) % side) * side + x) * CORES + c
    half_count, root_half, _ = lroot.shape
    pieces = ((0, root_half - root_half // 4), (root_half - root_half // 4, root_half // 4))

    def root_block(dy, q, p=0):
        oy, ox = (y + dy) % side, (x + 2 * q) % side
        core = c + p * (1 - 2 * c)
        return (oy * (side // 2) + ox // 2) * CORES + core, (oy * side + ox) * CORES + core

    def twin_turn(place):
        return g_recv.at[ROUNDS + 1 + place // CORES]

    twin_last = g_recv.at[ROUNDS + 1 + half_count // 4]

    def root_copy(peer, place, half, src=None, dst=None, recv=None, part=None, across=0):
        here = lroot.at[2 * place + half]
        if part is not None:
            here = here.at[pl.ds(*pieces[part])]
        if peer is twin and recv is None:
            recv = twin_turn(place)
        return pltpu.make_async_remote_copy(
            src_ref=here if src is None else src, dst_ref=here if dst is None else dst, send_sem=l_send.at[across],
            recv_sem=l_recv.at[recv] if isinstance(recv, int) else recv, device_id={"tensor": peer}, device_id_type=MESH)

    sent = [0, 0]

    def root_send(peer, place, half, part=None, across=0, **kw):
        sent[across] += root_half if part is None else pieces[part][1]
        root_copy(peer, place, half, part=part, across=across, **kw).start()

    def uncounted(action):
        before = list(sent)
        action()
        sent[:] = before

    def pair_wait(pair, sem):
        pltpu.make_async_copy(pair, pair, sem).wait()

    own_place, _ = root_block(0, 0)
    far_place, _ = root_block(0, 1)
    passing = (y * (side // 2) + ((x - dx + side) % side) // 2) * CORES + c

    def root_start_across():
        for half in (0, 1):
            root_send(helper, own_place, half, across=1, src=lr_ref.at[half], dst=relay.at[half], recv=relay_recv.at[half])

    def root_start():
        for half in (0, 1):
            root_send(up, own_place, half, src=lr_ref.at[half], recv=half)
            root_send(down, own_place, 1 - half, src=lr_ref.at[1 - half], recv=half)
        for half in (0, 1):
            root_send(twin, own_place, half, src=lr_ref.at[half])

    def root_relay(half):
        root_copy(helper, own_place, half, src=lr_ref.at[half], dst=relay.at[half], recv=relay_recv.at[half]).wait_recv()
        root_send(helper, passing, half, across=1, src=relay.at[half], recv=FAR_TURN + half)
        root_send(twin, passing, half, across=1, src=relay.at[half], dst=relay.at[2 + half], recv=relay_recv.at[2])

    def passed_rows(p):
        if p:
            pair_wait(relay.at[pl.ds(2, 2)], relay_recv.at[2])
        source = (y * side + (x - (1 - 2 * p) * dx + side) % side) * CORES + c + p * (1 - 2 * c)
        left = relay[2 * p:2 * p + 2].reshape(lrows, rows)
        do_ref[rows_of(source), :] = jnp.dot(left, xx[0], preferred_element_type=jnp.float32)

    def root_far():
        for half in (0, 1):
            pltpu.make_async_copy(lroot.at[0], lroot.at[0], l_recv.at[FAR_TURN + half]).wait()
            root_send(up, far_place, half, recv=3 + half)
            root_send(twin, far_place, half)
        for half in (1, 0):
            root_send(down, far_place, half, recv=4 - half)

    def root_round(r):
        q, stage = r // 3, r % 3
        pair_wait(lroot.at[pl.ds(0, 2)], l_recv.at[r])
        if stage == 2:
            below = above = root_block(2, q)[0]
        else:
            below, above = root_block(side - 1, q)[0], root_block(1, q)[0]
        if stage == 0:
            for peer, place, half in ((up, below, 0), (down, above, 1)):
                if q == 0:
                    root_send(peer, place, half, recv=2)
                else:
                    for part in (0, 1):
                        root_send(peer, place, half, part=part, recv=LAST_TURN + part)
        root_send(twin, below, stage % 2)
        root_send(twin, above, 1 - stage % 2)

    last_place, last_device = root_block(2, 1)
    twin_place, twin_device = root_block(2, 1, 1)

    def root_last(part):
        pair_wait(lroot.at[pl.ds(0, 2), pl.ds(*pieces[part])], l_recv.at[LAST_TURN + part])
        for half in (0, 1):
            root_send(twin, last_place, half, part=part, recv=twin_last if part else None)

    def root_last_twin(part):
        pair = lroot.at[pl.ds(2 * twin_place, 2), pl.ds(*pieces[part])]
        pair_wait(pair, twin_last if part else twin_turn(twin_place))

    steps(grad, gbuf, load_sem, GRAD_ROUND_STEP, [(RELAY_STEP, lambda: root_relay(0))],
          [(ROOT_ACROSS_STEP, root_start_across), (ROOT_ACROSS_STEP, lambda: pl.when(c == 1)(lambda: uncounted(root_start)))],
          [(ROOT_START_STEP, lambda: pl.when(c == 0)(root_start))], grad_work)

    side_cols = cols // 2

    def x_copy(h):
        at = pl.ds(h * side_cols, side_cols)
        return pltpu.make_async_remote_copy(
            src_ref=xx.at[0, :, at], dst_ref=xx.at[1, :, at], send_sem=x_send.at[h], recv_sem=x_recv.at[h],
            device_id={"tensor": helper}, device_id_type=MESH)

    xx[0] = acc[:, :cols].astype(jnp.bfloat16)
    root_relay(1)
    x_copy(0).start()
    x_copy(1).start()
    root_round(0)

    def left_step(t, carry):
        at = pl.ds(pl.multiple_of(t * lrows, lrows), lrows)
        lo_ref[:, at] = EMA_DECAY * lo_ref[:, at] + (1.0 - EMA_DECAY) * acc[at, cols:].T
        return carry
    lax.fori_loop(0, rows // lrows, left_step, 0)

    def at_step(i):
        e, p = i // 2, i % 2
        dy = lax.shift_right_logical(ROOT_Y, 2 * e) & 3
        q = lax.shift_right_logical(ROOT_X, 2 * e) & 3
        return root_block(dy, q, p)

    def twin_wait(i, place):
        @pl.when(i % 2 == 1)
        def _():
            pair_wait(lroot.at[pl.ds(2 * place, 2)], twin_turn(place))

    def product(place, which):
        left = lroot[pl.ds(2 * place, 2)].reshape(lrows, rows)
        return jnp.dot(left, xx[which], preferred_element_type=jnp.float32)

    def rows_of(device):
        return pl.ds(pl.multiple_of(device * lrows, lrows), lrows)

    def own_rows(i):
        place, device = at_step(i)
        do_ref[rows_of(device), :] = product(place, 0)

    def lent_copy(i, device):
        return pltpu.make_async_remote_copy(
            src_ref=lent.at[i], dst_ref=do_ref.at[rows_of(device)], send_sem=d_send.at[0], recv_sem=d_recv.at[0],
            device_id={"tensor": client}, device_id_type=MESH)

    def lent_rows(i):
        place, device = at_step(i)
        lent[i] = product(place, 1)
        lent_copy(i, device).start()

    def lent_side(i, h):
        place, _ = at_step(i)
        at = pl.ds(h * side_cols, side_cols)
        left = lroot[pl.ds(2 * place, 2)].reshape(lrows, rows)
        lent[i, :, at] = jnp.dot(left, xx[1, :, at], preferred_element_type=jnp.float32)

    def lent_side_copy(i, h):
        _, device = at_step(i)
        at = pl.ds(h * side_cols, side_cols)
        return pltpu.make_async_remote_copy(
            src_ref=lent.at[i, :, at], dst_ref=do_ref.at[rows_of(device), at], send_sem=d_send.at[0], recv_sem=d_recv.at[0],
            device_id={"tensor": client}, device_id_type=MESH)

    def loop(lo, hi, body):
        def step(i, carry):
            body(i)
            return carry
        lax.fori_loop(lo, hi, step, 0)

    def first_own(i):
        @pl.when(i == 2)
        def _():
            root_far()
            root_round(1)

        @pl.when(i == 8)
        def _():
            root_round(2)
        twin_wait(i, at_step(i)[0])
        own_rows(i)

    loop(0, 10, first_own)
    passed_rows(0)
    passed_rows(1)
    x_copy(0).wait_recv()
    def lent_step(j):
        return j + (j + 7) // 8 + j // 5

    loop(0, 8, lambda j: lent_side(lent_step(j), 0))
    x_copy(0).wait_send()
    x_copy(1).wait_send()
    pl.semaphore_signal(x_gone, inc=1, device_id={"tensor": twin}, device_id_type=MESH)
    pl.semaphore_wait(x_gone, 1)
    loop(0, 8, lambda j: lent_side_copy(lent_step(j), 0).start())
    root_round(3)
    x_copy(1).wait_recv()

    def second_side(j):
        i = lent_step(j)
        lent_side(i, 1)
        lent_side_copy(i, 1).start()
    loop(0, 8, second_side)
    root_round(4)

    def both(i):
        twin_wait(i, at_step(i)[0])
        lent_rows(i)
        own_rows(i)
    loop(10, 14, both)

    def lent_piece(i, place, device, part):
        first, count = pieces[part]
        left = jnp.concatenate([lroot[2 * place, pl.ds(first, count), :], lroot[2 * place + 1, pl.ds(first, count), :]], axis=0)
        prod = jnp.dot(left, xx[1], preferred_element_type=jnp.float32)
        for half in (0, 1):
            at = half * root_half + first
            lent[i, pl.ds(at, count), :] = prod[half * count:(half + 1) * count]
            pltpu.make_async_remote_copy(
                src_ref=lent.at[i, pl.ds(at, count)], dst_ref=do_ref.at[pl.ds(pl.multiple_of(device * lrows, lrows) + at, count)],
                send_sem=d_send.at[0], recv_sem=d_recv.at[0], device_id={"tensor": client}, device_id_type=MESH).start()

    def own_piece(part):
        root_last(part)
        lent_piece(14, last_place, last_device, part)

    def twin_piece(part):
        root_last_twin(part)
        lent_piece(15, twin_place, twin_device, part)

    @pl.when(c == 0)
    def _():
        own_piece(0)
        own_piece(1)
        twin_piece(0)
        twin_piece(1)

    @pl.when(c == 1)
    def _():
        uncounted(lambda: own_piece(0))
        twin_piece(0)
        twin_piece(1)
        uncounted(lambda: own_piece(1))

    loop(14, 16, own_rows)

    grad.drain()
    for across, count in enumerate(sent):
        whole = lroot.at[pl.ds(0, count // root_half)]
        pltpu.make_async_copy(whole, whole, l_send.at[across]).wait()
    given = lent.at[pl.ds(0, half_count // 2 - 2)]
    pltpu.make_async_copy(given, given, d_send.at[0]).wait()
    pltpu.make_async_copy(given, given, d_recv.at[0]).wait()


def store_kernel(*refs):
    count = (len(refs) - 1) // 2
    sems = refs[-1]
    pieces = 32
    for i in range(count):
        src, dst = refs[i], refs[count + i]
        step = src.shape[0] // pieces
        for j in range(pieces):
            part = pl.ds(j * step, step)
            pltpu.make_async_copy(src.at[part], dst.at[part], sems.at[i]).start()
    for i in range(count):
        pltpu.make_async_copy(refs[i], refs[count + i], sems.at[i]).wait()


def solution(mesh):
    row_spec = P(("layer", "tensor"), None)
    col_spec = P("layer", "tensor")
    n = mesh.shape["tensor"]
    side = math.isqrt(n // CORES)

    def local_step(g, l, r, lr, rr):
        rows, cols = g.shape
        lrows = l.shape[0]
        kept = n // 2
        hbm = pl.BlockSpec(memory_space=pltpu.HBM)
        vmem = pl.BlockSpec(memory_space=pltpu.VMEM)
        operands = [g.reshape(2, rows // 2, cols), l, r, lr.reshape(2, lrows // 2, rows), rr]
        left_new, right_new, direction, _ = pl.pallas_call(
            functools.partial(kernel, n, side),
            name="shampoo",
            out_shape=[
                pltpu.VMEM(l.shape, jnp.float32),
                pltpu.VMEM(r.shape, jnp.float32),
                pltpu.VMEM(g.shape, jnp.float32),
                pltpu.HBM((2 * n, rows // 2, cols), jnp.bfloat16),
            ],
            in_specs=[hbm] * 5,
            out_specs=[vmem, vmem, vmem, hbm],
            scratch_shapes=[
                pltpu.VMEM(rr.shape, jnp.bfloat16),
                pltpu.VMEM((cols, rows), jnp.bfloat16),
                pltpu.VMEM((rows, cols + lrows), jnp.float32),
                pltpu.VMEM((2, 2, rows // 2, cols), jnp.bfloat16),
                pltpu.VMEM((cols + lrows, cols), jnp.bfloat16),
                pltpu.VMEM((2, rows, cols), jnp.bfloat16),
                pltpu.VMEM((2 * kept, lrows // 2, rows), jnp.bfloat16),
                pltpu.VMEM((4, lrows // 2, rows), jnp.bfloat16),
                pltpu.VMEM((kept, lrows, cols), jnp.float32),
                pltpu.SemaphoreType.DMA((ROUNDS + n // 2,)),
                pltpu.SemaphoreType.DMA((1,)),
                pltpu.SemaphoreType.DMA((2,)),
                pltpu.SemaphoreType.DMA((ROOT_TURNS,)),
                pltpu.SemaphoreType.DMA((3,)),
                pltpu.SemaphoreType.DMA((2,)),
                pltpu.SemaphoreType.DMA((1,)),
                pltpu.SemaphoreType.DMA((2,)),
                pltpu.SemaphoreType.DMA((2,)),
                pltpu.SemaphoreType.DMA((1,)),
                pltpu.SemaphoreType.REGULAR,
            ],
            compiler_params=pltpu.CompilerParams(collective_id=0, has_side_effects=True, vmem_limit_bytes=48 * 2**20),
            cost_estimate=pl.CostEstimate(flops=2 * rows * cols * (2 * n * cols + 2 * rows), bytes_accessed=2 * n * rows * cols * 3, transcendentals=0),
        )(*[pltpu.with_memory_space_constraint(v, pltpu.HBM) for v in operands])
        results = [left_new, right_new, direction]
        return pl.pallas_call(
            store_kernel,
            name="store",
            out_shape=[jax.ShapeDtypeStruct(v.shape, v.dtype) for v in results],
            in_specs=[vmem] * 3,
            out_specs=[hbm] * 3,
            scratch_shapes=[pltpu.SemaphoreType.DMA((3,))],
            compiler_params=pltpu.CompilerParams(vmem_limit_bytes=1 * 2**20),
        )(*results)

    return jax.shard_map(local_step, mesh=mesh, in_specs=(col_spec, row_spec, row_spec, row_spec, row_spec), out_specs=(row_spec, row_spec, col_spec), check_vma=False)
```

```python
import functools
import math

import jax
import jax.numpy as jnp
from jax import lax
from jax.experimental import pallas as pl
from jax.experimental.pallas import tpu as pltpu
from jax.sharding import PartitionSpec as P

EMA_DECAY = 0.9
CORES = 2
MESH = pl.DeviceIdType.MESH

ORDER = [(int(a), int(b)) for a, b in zip("0310020311322312", "0003102313131222")]
def parcels(code):
    digits = [int(d) for d in code]
    return [((a, b), h) for a, b, h in zip(digits[0::3], digits[1::3], digits[2::3])]


UP = parcels("030031330131020331130230231320120220")
UP_ON = {0: parcels("030"), 2: parcels("330"), 6: parcels("130"), 7: parcels("230")}
DOWN = parcels("011010111310021110311211210321121221")
DOWN_ON = {0: parcels("011"), 6: parcels("311111"), 7: parcels("211")}
ROUNDS = len(UP)
FIRST_UP = parcels("300301200")
FIRST_DOWN = parcels("101100201")
GRAD_ROUND_STEP = [2, 2, 8, 10, 12, 14, 17, 20, 22, 26, 28, 30]
LAST_FORWARD = 7
SIDE_UP, SIDE_DOWN = 9, 10
ASIDE = {"+": 33, "-": 33}
ROOT_START_STEP = 28
ROOT_ACROSS_STEP = 30
RELAY_STEP = 32
LATE = (2, 12, 14, 22, 26, 28, 30)


def round_of(name, offset, half):
    a, b = offset
    table, da, db = {"f+": (FIRST_UP, 3, 0), "f-": (FIRST_DOWN, 1, 0), "s+": (UP, 0, 3), "s-": (DOWN, 0, 1)}[name]
    return table.index((((a + da) % 4, (b + db) % 4), half))


def packed(values):
    return [sum(v << (2 * i) for i, v in enumerate(values[j:j + 8])) for j in (0, 8)]


FIRST_CODE = packed([o[0] for o in ORDER])
SECOND_CODE = packed([o[1] for o in ORDER])


def lookup(code, e):
    word = code[0] + (e // 8) * (code[1] - code[0])
    return lax.shift_right_logical(word, 2 * (e % 8)) & 3


ROOT_ORDER = [(0, 0), (3, 0), (1, 0), (0, 1), (2, 0), (3, 1), (1, 1), (2, 1)]
ROOT_Y = sum(o[0] << (2 * i) for i, o in enumerate(ROOT_ORDER))
FAR_TURN, LAST_TURN, ROOT_TURNS = 5, 7, 9
ROOT_X = sum(o[1] << (2 * i) for i, o in enumerate(ROOT_ORDER))


def kernel(n, side, g_ref, l_ref, r_ref, lr_ref, rr_ref, lo_ref, ro_ref, do_ref, gfull,
           rr, gt, acc, gbuf, rhs, xx, lroot, relay, lent,
           g_recv, g_send, load_sem, l_recv, relay_recv, x_recv, d_recv, l_send, x_send, d_send, x_gone):
    _, half_rows, cols = g_ref.shape
    rows = 2 * half_rows
    lrows = l_ref.shape[0]
    tile = min(1024, half_rows)
    aside_rows = {way: half_rows * share // 128 for way, share in ASIDE.items()}

    me = lax.axis_index("tensor")
    c = me % CORES
    chip = me // CORES
    x, y = chip % side, chip // side
    f = x + c * (y - x)
    s = y + c * (x - y)
    fstep = CORES + c * CORES * (side - 1)
    sstep = CORES * side - c * CORES * (side - 1)
    twin = me + 1 - 2 * c

    def index(df, ds):
        return ((f + df) % side) * fstep + ((s + ds) % side) * sstep + c

    def twin_index(df, ds):
        return ((s + df) % side) * sstep + ((f + ds) % side) * fstep + 1 - c

    peers = {"f+": index(1, 0), "f-": index(3, 0), "s+": index(0, 1), "s-": index(0, 3), "twin": twin}

    class Gather:
        def __init__(self, own, full, recv, send):
            self.own, self.full, self.recv, self.send_sem = own, full, recv, send
            self.sent = 0

        def copy(self, name, offset, half, part=None, turn=None):
            b = index(*offset)
            src = self.own.at[half] if offset == (0, 0) else self.full.at[2 * b + half]
            dst = self.full.at[2 * b + half]
            if part is not None:
                src, dst = src.at[pl.ds(*part)], dst.at[pl.ds(*part)]
            if turn is None:
                turn = ROUNDS + ORDER.index(offset) if name == "twin" else round_of(name, offset, half)
            return pltpu.make_async_remote_copy(
                src_ref=src, dst_ref=dst, send_sem=self.send_sem.at[0], recv_sem=self.recv.at[turn],
                device_id={"tensor": peers[name]}, device_id_type=MESH)

        def send(self, name, offset, half):
            self.sent += 1
            self.copy(name, offset, half).start()

        def wait(self, turn, count):
            taken = self.full.at[pl.ds(0, count)]
            pltpu.make_async_copy(taken, taken, self.recv.at[turn]).wait()

        def start(self):
            for half in (0, 1):
                for name in ("f+", "s+"):
                    self.send(name, (0, 0), half)
                for name in ("f-", "s-"):
                    self.send(name, (0, 0), 1 - half)
            for half in (0, 1):
                self.send("twin", (0, 0), half)

        def round(self, r):
            first = r < len(FIRST_UP)
            self.wait(r, 4 if first else 2)
            if first:
                above, below = FIRST_UP[r], FIRST_DOWN[r]
                if r == 0:
                    self.send("f+", *above)
                    self.send("f-", *below)
                self.send("s+", *above)
                self.send("s-", *below)
                self.send("s+", *below)
                self.send("s-", *above)
                self.send("twin", *above)
                self.send("twin", *below)
            for name, table in (("s+", UP_ON), ("s-", DOWN_ON)):
                for parcel in table.get(r, ()):
                    if r == LAST_FORWARD:
                        self.forward_last(name, *parcel)
                    else:
                        self.send(name, *parcel)
            if r == SIDE_UP:
                self.aside("f+", *UP[r])
            if r == SIDE_DOWN:
                self.aside("f-", *DOWN[r])
            self.send("twin", *UP[r])
            self.send("twin", *DOWN[r])

        def forward_last(self, name, offset, half):
            self.sent += 1
            pl.when(c == 0)(lambda: self.copy(name, offset, half, part=(0, half_rows - aside_rows[name[1]])).start())
            pl.when(c == 1)(lambda: self.copy(name, offset, half).start())

        def aside(self, name, offset, half):
            count = aside_rows[name[1]]
            part = (half_rows - count, count)
            pl.when(c == 0)(lambda: self.copy(name, offset, half, part=part, turn=ROUNDS - 1).start())

        def drain(self):
            whole = self.full.at[pl.ds(0, self.sent)]
            pltpu.make_async_copy(whole, whole, self.send_sem.at[0]).wait()

    grad = Gather(g_ref, gfull, g_recv, g_send)

    def block_of(k):
        e, other = k // 2, k % 2
        df, ds = lookup(FIRST_CODE, e), lookup(SECOND_CODE, e)
        mine = index(df, ds)
        return mine + other * (twin_index(df, ds) - mine)

    def load(gather, buf, k, sem):
        b = block_of(k)
        return pltpu.make_async_copy(gather.full.at[pl.ds(2 * b, 2)], buf.at[k % 2], sem.at[k % 2])

    def one_of(k, values):
        found = k == values[0]
        for v in values[1:]:
            found = found | (k == v)
        return found

    def steps(gather, buf, sem, round_step, early, between, after, work):
        def at_steps(k, actions):
            for at, action in actions:
                pl.when(k == at)(action)

        def step(k, carry):
            at_steps(k, early)

            @pl.when((k % 2 == 1) & (k < n))
            def _():
                gather.wait(ROUNDS + k // 2, 2)

            @pl.when(jnp.logical_not(one_of(k, LATE)) & (k < n))
            def _():
                load(gather, buf, k, sem).start()
            load(gather, buf, k - 1, sem).wait()
            work((k - 1) % 2, block_of(k - 1))
            at_steps(k, between)
            for r in range(ROUNDS):
                @pl.when(k == round_step[r])
                def _():
                    gather.round(r)
            at_steps(k, after)

            @pl.when(one_of(k, LATE))
            def _():
                load(gather, buf, k, sem).start()
            return carry
        lax.fori_loop(1, n + 1, step, 0)

    barrier = pltpu.get_barrier_semaphore()
    for peer in peers.values():
        pl.semaphore_signal(barrier, inc=1, device_id={"tensor": peer}, device_id_type=MESH)

    first = [
        pltpu.make_async_copy(rr_ref, rr, x_send.at[0]),
        pltpu.make_async_copy(r_ref, ro_ref, x_send.at[1]),
        pltpu.make_async_copy(l_ref, lo_ref, d_send.at[0]),
        pltpu.make_async_copy(lr_ref, lroot.at[pl.ds(2 * ((y * (side // 2) + x // 2) * CORES + c), 2)], l_send.at[0]),
    ]
    own_load = pltpu.make_async_copy(g_ref, gbuf.at[0], load_sem.at[0])
    own_load.start()
    for copy in first:
        copy.start()

    pl.semaphore_wait(barrier, len(peers))
    grad.start()

    acc[...] = jnp.zeros_like(acc)
    own_load.wait()
    for h in (0, 1):
        gt[:, h * half_rows:(h + 1) * half_rows] = gbuf[0, h].T
    for copy in first:
        copy.wait()
    own_load.start()

    per_half = half_rows // tile

    def grad_work(slot, b):
        at = pl.multiple_of(b * cols, cols)
        rhs[:cols] = rr[:, pl.ds(at, cols)]
        rhs[cols:] = gbuf[slot, me // (n // 2), pl.ds(pl.multiple_of((me % (n // 2)) * lrows, lrows), lrows), :]

        def rows_step(t, carry):
            left = gbuf[slot, t // per_half, pl.ds(pl.multiple_of((t % per_half) * tile, tile), tile), :]
            out = pl.ds(pl.multiple_of(t * tile, tile), tile)
            acc[out, :] += lax.dot_general(left, rhs[...], (((1,), (1,)), ((), ())), preferred_element_type=jnp.float32)
            return carry
        lax.fori_loop(0, 2 * per_half, rows_step, 0)
        prod = jnp.dot(gt[:, :half_rows], gbuf[slot, 0], preferred_element_type=jnp.float32)
        prod += jnp.dot(gt[:, half_rows:], gbuf[slot, 1], preferred_element_type=jnp.float32)
        ro_ref[:, pl.ds(at, cols)] = EMA_DECAY * ro_ref[:, pl.ds(at, cols)] + (1.0 - EMA_DECAY) * prod


    dx = 1 - 2 * c
    helper = (y * side + (x + dx + side) % side) * CORES + c
    client = (y * side + (x - dx + side) % side) * CORES + c
    up = (((y + 1) % side) * side + x) * CORES + c
    down = (((y + side - 1) % side) * side + x) * CORES + c
    half_count, root_half, _ = lroot.shape
    pieces = ((0, root_half - root_half // 4), (root_half - root_half // 4, root_half // 4))

    def root_block(dy, q, p=0):
        oy, ox = (y + dy) % side, (x + 2 * q) % side
        core = c + p * (1 - 2 * c)
        return (oy * (side // 2) + ox // 2) * CORES + core, (oy * side + ox) * CORES + core

    def twin_turn(place):
        return g_recv.at[ROUNDS + 1 + place // CORES]

    twin_last = g_recv.at[ROUNDS + 1 + half_count // 4]

    def root_copy(peer, place, half, src=None, dst=None, recv=None, part=None, across=0):
        here = lroot.at[2 * place + half]
        if part is not None:
            here = here.at[pl.ds(*pieces[part])]
        if peer is twin and recv is None:
            recv = twin_turn(place)
        return pltpu.make_async_remote_copy(
            src_ref=here if src is None else src, dst_ref=here if dst is None else dst, send_sem=l_send.at[across],
            recv_sem=l_recv.at[recv] if isinstance(recv, int) else recv, device_id={"tensor": peer}, device_id_type=MESH)

    sent = [0, 0]

    def root_send(peer, place, half, part=None, across=0, **kw):
        sent[across] += root_half if part is None else pieces[part][1]
        root_copy(peer, place, half, part=part, across=across, **kw).start()

    def uncounted(action):
        before = list(sent)
        action()
        sent[:] = before

    def pair_wait(pair, sem):
        pltpu.make_async_copy(pair, pair, sem).wait()

    own_place, _ = root_block(0, 0)
    far_place, _ = root_block(0, 1)
    passing = (y * (side // 2) + ((x - dx + side) % side) // 2) * CORES + c

    def root_start_across():
        for half in (0, 1):
            root_send(helper, own_place, half, across=1, src=lr_ref.at[half], dst=relay.at[half], recv=relay_recv.at[half])

    def root_start():
        for half in (0, 1):
            root_send(up, own_place, half, src=lr_ref.at[half], recv=half)
            root_send(down, own_place, 1 - half, src=lr_ref.at[1 - half], recv=half)
        for half in (0, 1):
            root_send(twin, own_place, half, src=lr_ref.at[half])

    def root_relay(half):
        root_copy(helper, own_place, half, src=lr_ref.at[half], dst=relay.at[half], recv=relay_recv.at[half]).wait_recv()
        root_send(helper, passing, half, across=1, src=relay.at[half], recv=FAR_TURN + half)
        root_send(twin, passing, half, across=1, src=relay.at[half], dst=relay.at[2 + half], recv=relay_recv.at[2])

    def passed_rows(p):
        if p:
            pair_wait(relay.at[pl.ds(2, 2)], relay_recv.at[2])
        source = (y * side + (x - (1 - 2 * p) * dx + side) % side) * CORES + c + p * (1 - 2 * c)
        left = relay[2 * p:2 * p + 2].reshape(lrows, rows)
        do_ref[rows_of(source), :] = jnp.dot(left, xx[0], preferred_element_type=jnp.float32)

    def root_far():
        for half in (0, 1):
            pltpu.make_async_copy(lroot.at[0], lroot.at[0], l_recv.at[FAR_TURN + half]).wait()
            root_send(up, far_place, half, recv=3 + half)
            root_send(twin, far_place, half)
        for half in (1, 0):
            root_send(down, far_place, half, recv=4 - half)

    def root_round(r):
        q, stage = r // 3, r % 3
        pair_wait(lroot.at[pl.ds(0, 2)], l_recv.at[r])
        if stage == 2:
            below = above = root_block(2, q)[0]
        else:
            below, above = root_block(side - 1, q)[0], root_block(1, q)[0]
        if stage == 0:
            for peer, place, half in ((up, below, 0), (down, above, 1)):
                if q == 0:
                    root_send(peer, place, half, recv=2)
                else:
                    for part in (0, 1):
                        root_send(peer, place, half, part=part, recv=LAST_TURN + part)
        root_send(twin, below, stage % 2)
        root_send(twin, above, 1 - stage % 2)

    last_place, last_device = root_block(2, 1)
    twin_place, twin_device = root_block(2, 1, 1)

    def root_last(part):
        pair_wait(lroot.at[pl.ds(0, 2), pl.ds(*pieces[part])], l_recv.at[LAST_TURN + part])
        for half in (0, 1):
            root_send(twin, last_place, half, part=part, recv=twin_last if part else None)

    def root_last_twin(part):
        pair = lroot.at[pl.ds(2 * twin_place, 2), pl.ds(*pieces[part])]
        pair_wait(pair, twin_last if part else twin_turn(twin_place))

    steps(grad, gbuf, load_sem, GRAD_ROUND_STEP, [(RELAY_STEP, lambda: root_relay(0)), (ROOT_ACROSS_STEP, lambda: pl.when(c == 1)(lambda: uncounted(root_start)))],
          [(ROOT_ACROSS_STEP, root_start_across)],
          [(ROOT_START_STEP, lambda: pl.when(c == 0)(root_start))], grad_work)

    side_cols = cols // 2

    def x_copy(h):
        at = pl.ds(h * side_cols, side_cols)
        return pltpu.make_async_remote_copy(
            src_ref=xx.at[0, :, at], dst_ref=xx.at[1, :, at], send_sem=x_send.at[h], recv_sem=x_recv.at[h],
            device_id={"tensor": helper}, device_id_type=MESH)

    xx[0] = acc[:, :cols].astype(jnp.bfloat16)
    root_relay(1)
    x_copy(0).start()
    x_copy(1).start()
    root_round(0)

    def left_step(t, carry):
        at = pl.ds(pl.multiple_of(t * lrows, lrows), lrows)
        lo_ref[:, at] = EMA_DECAY * lo_ref[:, at] + (1.0 - EMA_DECAY) * acc[at, cols:].T
        return carry
    lax.fori_loop(0, rows // lrows, left_step, 0)

    def at_step(i):
        e, p = i // 2, i % 2
        dy = lax.shift_right_logical(ROOT_Y, 2 * e) & 3
        q = lax.shift_right_logical(ROOT_X, 2 * e) & 3
        return root_block(dy, q, p)

    def twin_wait(i, place):
        @pl.when(i % 2 == 1)
        def _():
            pair_wait(lroot.at[pl.ds(2 * place, 2)], twin_turn(place))

    def product(place, which):
        left = lroot[pl.ds(2 * place, 2)].reshape(lrows, rows)
        return jnp.dot(left, xx[which], preferred_element_type=jnp.float32)

    def rows_of(device):
        return pl.ds(pl.multiple_of(device * lrows, lrows), lrows)

    def own_rows(i):
        place, device = at_step(i)
        do_ref[rows_of(device), :] = product(place, 0)

    def lent_copy(i, device):
        return pltpu.make_async_remote_copy(
            src_ref=lent.at[i], dst_ref=do_ref.at[rows_of(device)], send_sem=d_send.at[0], recv_sem=d_recv.at[0],
            device_id={"tensor": client}, device_id_type=MESH)

    def lent_rows(i):
        place, device = at_step(i)
        lent[i] = product(place, 1)
        lent_copy(i, device).start()

    def lent_side(i, h):
        place, _ = at_step(i)
        at = pl.ds(h * side_cols, side_cols)
        left = lroot[pl.ds(2 * place, 2)].reshape(lrows, rows)
        lent[i, :, at] = jnp.dot(left, xx[1, :, at], preferred_element_type=jnp.float32)

    def lent_side_copy(i, h):
        _, device = at_step(i)
        at = pl.ds(h * side_cols, side_cols)
        return pltpu.make_async_remote_copy(
            src_ref=lent.at[i, :, at], dst_ref=do_ref.at[rows_of(device), at], send_sem=d_send.at[0], recv_sem=d_recv.at[0],
            device_id={"tensor": client}, device_id_type=MESH)

    def loop(lo, hi, body):
        def step(i, carry):
            body(i)
            return carry
        lax.fori_loop(lo, hi, step, 0)

    def first_own(i):
        @pl.when(i == 2)
        def _():
            root_far()
            root_round(1)

        @pl.when(i == 8)
        def _():
            root_round(2)
        twin_wait(i, at_step(i)[0])
        own_rows(i)

    loop(0, 10, first_own)
    passed_rows(0)
    passed_rows(1)
    x_copy(0).wait_recv()
    def lent_step(j):
        return j + (j + 7) // 8 + j // 5

    loop(0, 8, lambda j: lent_side(lent_step(j), 0))
    x_copy(0).wait_send()
    x_copy(1).wait_send()
    pl.semaphore_signal(x_gone, inc=1, device_id={"tensor": twin}, device_id_type=MESH)
    pl.semaphore_wait(x_gone, 1)
    loop(0, 8, lambda j: lent_side_copy(lent_step(j), 0).start())
    root_round(3)
    x_copy(1).wait_recv()

    def second_side(j):
        i = lent_step(j)
        lent_side(i, 1)
        lent_side_copy(i, 1).start()
    loop(0, 8, second_side)
    root_round(4)

    def both(i):
        twin_wait(i, at_step(i)[0])
        lent_rows(i)
        own_rows(i)
    loop(10, 14, both)

    def lent_piece(i, place, device, part):
        first, count = pieces[part]
        left = jnp.concatenate([lroot[2 * place, pl.ds(first, count), :], lroot[2 * place + 1, pl.ds(first, count), :]], axis=0)
        prod = jnp.dot(left, xx[1], preferred_element_type=jnp.float32)
        for half in (0, 1):
            at = half * root_half + first
            lent[i, pl.ds(at, count), :] = prod[half * count:(half + 1) * count]
            pltpu.make_async_remote_copy(
                src_ref=lent.at[i, pl.ds(at, count)], dst_ref=do_ref.at[pl.ds(pl.multiple_of(device * lrows, lrows) + at, count)],
                send_sem=d_send.at[0], recv_sem=d_recv.at[0], device_id={"tensor": client}, device_id_type=MESH).start()

    def own_piece(part):
        root_last(part)
        lent_piece(14, last_place, last_device, part)

    def twin_piece(part):
        root_last_twin(part)
        lent_piece(15, twin_place, twin_device, part)

    @pl.when(c == 0)
    def _():
        own_piece(0)
        own_piece(1)
        twin_piece(0)
        twin_piece(1)

    @pl.when(c == 1)
    def _():
        uncounted(lambda: own_piece(0))
        twin_piece(0)
        twin_piece(1)
        uncounted(lambda: own_piece(1))

    loop(14, 16, own_rows)

    grad.drain()
    for across, count in enumerate(sent):
        whole = lroot.at[pl.ds(0, count // root_half)]
        pltpu.make_async_copy(whole, whole, l_send.at[across]).wait()
    given = lent.at[pl.ds(0, half_count // 2 - 2)]
    pltpu.make_async_copy(given, given, d_send.at[0]).wait()
    pltpu.make_async_copy(given, given, d_recv.at[0]).wait()


def store_kernel(*refs):
    count = (len(refs) - 1) // 2
    sems = refs[-1]
    pieces = 32
    for i in range(count):
        src, dst = refs[i], refs[count + i]
        step = src.shape[0] // pieces
        for j in range(pieces):
            part = pl.ds(j * step, step)
            pltpu.make_async_copy(src.at[part], dst.at[part], sems.at[i]).start()
    for i in range(count):
        pltpu.make_async_copy(refs[i], refs[count + i], sems.at[i]).wait()


def solution(mesh):
    row_spec = P(("layer", "tensor"), None)
    col_spec = P("layer", "tensor")
    n = mesh.shape["tensor"]
    side = math.isqrt(n // CORES)

    def local_step(g, l, r, lr, rr):
        rows, cols = g.shape
        lrows = l.shape[0]
        kept = n // 2
        hbm = pl.BlockSpec(memory_space=pltpu.HBM)
        vmem = pl.BlockSpec(memory_space=pltpu.VMEM)
        operands = [g.reshape(2, rows // 2, cols), l, r, lr.reshape(2, lrows // 2, rows), rr]
        left_new, right_new, direction, _ = pl.pallas_call(
            functools.partial(kernel, n, side),
            name="shampoo",
            out_shape=[
                pltpu.VMEM(l.shape, jnp.float32),
                pltpu.VMEM(r.shape, jnp.float32),
                pltpu.VMEM(g.shape, jnp.float32),
                pltpu.HBM((2 * n, rows // 2, cols), jnp.bfloat16),
            ],
            in_specs=[hbm] * 5,
            out_specs=[vmem, vmem, vmem, hbm],
            scratch_shapes=[
                pltpu.VMEM(rr.shape, jnp.bfloat16),
                pltpu.VMEM((cols, rows), jnp.bfloat16),
                pltpu.VMEM((rows, cols + lrows), jnp.float32),
                pltpu.VMEM((2, 2, rows // 2, cols), jnp.bfloat16),
                pltpu.VMEM((cols + lrows, cols), jnp.bfloat16),
                pltpu.VMEM((2, rows, cols), jnp.bfloat16),
                pltpu.VMEM((2 * kept, lrows // 2, rows), jnp.bfloat16),
                pltpu.VMEM((4, lrows // 2, rows), jnp.bfloat16),
                pltpu.VMEM((kept, lrows, cols), jnp.float32),
                pltpu.SemaphoreType.DMA((ROUNDS + n // 2,)),
                pltpu.SemaphoreType.DMA((1,)),
                pltpu.SemaphoreType.DMA((2,)),
                pltpu.SemaphoreType.DMA((ROOT_TURNS,)),
                pltpu.SemaphoreType.DMA((3,)),
                pltpu.SemaphoreType.DMA((2,)),
                pltpu.SemaphoreType.DMA((1,)),
                pltpu.SemaphoreType.DMA((2,)),
                pltpu.SemaphoreType.DMA((2,)),
                pltpu.SemaphoreType.DMA((1,)),
                pltpu.SemaphoreType.REGULAR,
            ],
            compiler_params=pltpu.CompilerParams(collective_id=0, has_side_effects=True, vmem_limit_bytes=48 * 2**20),
            cost_estimate=pl.CostEstimate(flops=2 * rows * cols * (2 * n * cols + 2 * rows), bytes_accessed=2 * n * rows * cols * 3, transcendentals=0),
        )(*[pltpu.with_memory_space_constraint(v, pltpu.HBM) for v in operands])
        results = [left_new, right_new, direction]
        return pl.pallas_call(
            store_kernel,
            name="store",
            out_shape=[jax.ShapeDtypeStruct(v.shape, v.dtype) for v in results],
            in_specs=[vmem] * 3,
            out_specs=[hbm] * 3,
            scratch_shapes=[pltpu.SemaphoreType.DMA((3,))],
            compiler_params=pltpu.CompilerParams(vmem_limit_bytes=1 * 2**20),
        )(*results)

    return jax.shard_map(local_step, mesh=mesh, in_specs=(col_spec, row_spec, row_spec, row_spec, row_spec), out_specs=(row_spec, row_spec, col_spec), check_vma=False)
```

```python
import functools
import math

import jax
import jax.numpy as jnp
from jax import lax
from jax.experimental import pallas as pl
from jax.experimental.pallas import tpu as pltpu
from jax.sharding import PartitionSpec as P

EMA_DECAY = 0.9
CORES = 2
MESH = pl.DeviceIdType.MESH

ORDER = [(int(a), int(b)) for a, b in zip("0310020311322312", "0003102313131222")]
def parcels(code):
    digits = [int(d) for d in code]
    return [((a, b), h) for a, b, h in zip(digits[0::3], digits[1::3], digits[2::3])]


UP = parcels("030031330131020331130230231320120220")
UP_ON = {0: parcels("030"), 2: parcels("330"), 6: parcels("130"), 7: parcels("230")}
DOWN = parcels("011010111310021110311211210321121221")
DOWN_ON = {0: parcels("011"), 6: parcels("311111"), 7: parcels("211")}
ROUNDS = len(UP)
FIRST_UP = parcels("300301200")
FIRST_DOWN = parcels("101100201")
GRAD_ROUND_STEP = [2, 2, 8, 10, 12, 14, 17, 20, 22, 26, 28, 30]
LAST_FORWARD = 7
SIDE_UP, SIDE_DOWN = 9, 10
ASIDE = {"+": 35, "-": 31}
ROOT_START_STEP = 28
ROOT_ACROSS_STEP = 30
RELAY_STEP = 32
LATE = (2, 12, 14, 22, 26, 28, 30)


def round_of(name, offset, half):
    a, b = offset
    table, da, db = {"f+": (FIRST_UP, 3, 0), "f-": (FIRST_DOWN, 1, 0), "s+": (UP, 0, 3), "s-": (DOWN, 0, 1)}[name]
    return table.index((((a + da) % 4, (b + db) % 4), half))


def packed(values):
    return [sum(v << (2 * i) for i, v in enumerate(values[j:j + 8])) for j in (0, 8)]


FIRST_CODE = packed([o[0] for o in ORDER])
SECOND_CODE = packed([o[1] for o in ORDER])


def lookup(code, e):
    word = code[0] + (e // 8) * (code[1] - code[0])
    return lax.shift_right_logical(word, 2 * (e % 8)) & 3


ROOT_ORDER = [(0, 0), (3, 0), (1, 0), (0, 1), (2, 0), (3, 1), (1, 1), (2, 1)]
ROOT_Y = sum(o[0] << (2 * i) for i, o in enumerate(ROOT_ORDER))
FAR_TURN, LAST_TURN, ROOT_TURNS = 5, 7, 9
ROOT_X = sum(o[1] << (2 * i) for i, o in enumerate(ROOT_ORDER))


def kernel(n, side, g_ref, l_ref, r_ref, lr_ref, rr_ref, lo_ref, ro_ref, do_ref, gfull,
           rr, gt, acc, gbuf, rhs, xx, lroot, relay, lent,
           g_recv, g_send, load_sem, l_recv, relay_recv, x_recv, d_recv, l_send, x_send, d_send, x_gone):
    _, half_rows, cols = g_ref.shape
    rows = 2 * half_rows
    lrows = l_ref.shape[0]
    tile = min(1024, half_rows)
    aside_rows = {way: half_rows * share // 128 for way, share in ASIDE.items()}

    me = lax.axis_index("tensor")
    c = me % CORES
    chip = me // CORES
    x, y = chip % side, chip // side
    f = x + c * (y - x)
    s = y + c * (x - y)
    fstep = CORES + c * CORES * (side - 1)
    sstep = CORES * side - c * CORES * (side - 1)
    twin = me + 1 - 2 * c

    def index(df, ds):
        return ((f + df) % side) * fstep + ((s + ds) % side) * sstep + c

    def twin_index(df, ds):
        return ((s + df) % side) * sstep + ((f + ds) % side) * fstep + 1 - c

    peers = {"f+": index(1, 0), "f-": index(3, 0), "s+": index(0, 1), "s-": index(0, 3), "twin": twin}

    class Gather:
        def __init__(self, own, full, recv, send):
            self.own, self.full, self.recv, self.send_sem = own, full, recv, send
            self.sent = 0

        def copy(self, name, offset, half, part=None, turn=None):
            b = index(*offset)
            src = self.own.at[half] if offset == (0, 0) else self.full.at[2 * b + half]
            dst = self.full.at[2 * b + half]
            if part is not None:
                src, dst = src.at[pl.ds(*part)], dst.at[pl.ds(*part)]
            if turn is None:
                turn = ROUNDS + ORDER.index(offset) if name == "twin" else round_of(name, offset, half)
            return pltpu.make_async_remote_copy(
                src_ref=src, dst_ref=dst, send_sem=self.send_sem.at[0], recv_sem=self.recv.at[turn],
                device_id={"tensor": peers[name]}, device_id_type=MESH)

        def send(self, name, offset, half):
            self.sent += 1
            self.copy(name, offset, half).start()

        def wait(self, turn, count):
            taken = self.full.at[pl.ds(0, count)]
            pltpu.make_async_copy(taken, taken, self.recv.at[turn]).wait()

        def start(self):
            for half in (0, 1):
                for name in ("f+", "s+"):
                    self.send(name, (0, 0), half)
                for name in ("f-", "s-"):
                    self.send(name, (0, 0), 1 - half)
            for half in (0, 1):
                self.send("twin", (0, 0), half)

        def round(self, r):
            first = r < len(FIRST_UP)
            self.wait(r, 4 if first else 2)
            if first:
                above, below = FIRST_UP[r], FIRST_DOWN[r]
                if r == 0:
                    self.send("f+", *above)
                    self.send("f-", *below)
                self.send("s+", *above)
                self.send("s-", *below)
                self.send("s+", *below)
                self.send("s-", *above)
                self.send("twin", *above)
                self.send("twin", *below)
            for name, table in (("s+", UP_ON), ("s-", DOWN_ON)):
                for parcel in table.get(r, ()):
                    if r == LAST_FORWARD:
                        self.forward_last(name, *parcel)
                    else:
                        self.send(name, *parcel)
            if r == SIDE_UP:
                self.aside("f+", *UP[r])
            if r == SIDE_DOWN:
                self.aside("f-", *DOWN[r])
            self.send("twin", *UP[r])
            self.send("twin", *DOWN[r])

        def forward_last(self, name, offset, half):
            self.sent += 1
            pl.when(c == 0)(lambda: self.copy(name, offset, half, part=(0, half_rows - aside_rows[name[1]])).start())
            pl.when(c == 1)(lambda: self.copy(name, offset, half).start())

        def aside(self, name, offset, half):
            count = aside_rows[name[1]]
            part = (half_rows - count, count)
            pl.when(c == 0)(lambda: self.copy(name, offset, half, part=part, turn=ROUNDS - 1).start())

        def drain(self):
            whole = self.full.at[pl.ds(0, self.sent)]
            pltpu.make_async_copy(whole, whole, self.send_sem.at[0]).wait()

    grad = Gather(g_ref, gfull, g_recv, g_send)

    def block_of(k):
        e, other = k // 2, k % 2
        df, ds = lookup(FIRST_CODE, e), lookup(SECOND_CODE, e)
        mine = index(df, ds)
        return mine + other * (twin_index(df, ds) - mine)

    def load(gather, buf, k, sem):
        b = block_of(k)
        return pltpu.make_async_copy(gather.full.at[pl.ds(2 * b, 2)], buf.at[k % 2], sem.at[k % 2])

    def one_of(k, values):
        found = k == values[0]
        for v in values[1:]:
            found = found | (k == v)
        return found

    def steps(gather, buf, sem, round_step, early, between, after, work):
        def at_steps(k, actions):
            for at, action in actions:
                pl.when(k == at)(action)

        def step(k, carry):
            at_steps(k, early)

            @pl.when((k % 2 == 1) & (k < n))
            def _():
                gather.wait(ROUNDS + k // 2, 2)

            @pl.when(jnp.logical_not(one_of(k, LATE)) & (k < n))
            def _():
                load(gather, buf, k, sem).start()
            load(gather, buf, k - 1, sem).wait()
            work((k - 1) % 2, block_of(k - 1))
            at_steps(k, between)
            for r in range(ROUNDS):
                @pl.when(k == round_step[r])
                def _():
                    gather.round(r)
            at_steps(k, after)

            @pl.when(one_of(k, LATE))
            def _():
                load(gather, buf, k, sem).start()
            return carry
        lax.fori_loop(1, n + 1, step, 0)

    barrier = pltpu.get_barrier_semaphore()
    for peer in peers.values():
        pl.semaphore_signal(barrier, inc=1, device_id={"tensor": peer}, device_id_type=MESH)

    first = [
        pltpu.make_async_copy(rr_ref, rr, x_send.at[0]),
        pltpu.make_async_copy(r_ref, ro_ref, x_send.at[1]),
        pltpu.make_async_copy(l_ref, lo_ref, d_send.at[0]),
        pltpu.make_async_copy(lr_ref, lroot.at[pl.ds(2 * ((y * (side // 2) + x // 2) * CORES + c), 2)], l_send.at[0]),
    ]
    own_load = pltpu.make_async_copy(g_ref, gbuf.at[0], load_sem.at[0])
    own_load.start()
    for copy in first:
        copy.start()

    pl.semaphore_wait(barrier, len(peers))
    grad.start()

    acc[...] = jnp.zeros_like(acc)
    own_load.wait()
    for h in (0, 1):
        gt[:, h * half_rows:(h + 1) * half_rows] = gbuf[0, h].T
    for copy in first:
        copy.wait()
    own_load.start()

    per_half = half_rows // tile

    def grad_work(slot, b):
        at = pl.multiple_of(b * cols, cols)
        rhs[:cols] = rr[:, pl.ds(at, cols)]
        rhs[cols:] = gbuf[slot, me // (n // 2), pl.ds(pl.multiple_of((me % (n // 2)) * lrows, lrows), lrows), :]

        def rows_step(t, carry):
            left = gbuf[slot, t // per_half, pl.ds(pl.multiple_of((t % per_half) * tile, tile), tile), :]
            out = pl.ds(pl.multiple_of(t * tile, tile), tile)
            acc[out, :] += lax.dot_general(left, rhs[...], (((1,), (1,)), ((), ())), preferred_element_type=jnp.float32)
            return carry
        lax.fori_loop(0, 2 * per_half, rows_step, 0)
        prod = jnp.dot(gt[:, :half_rows], gbuf[slot, 0], preferred_element_type=jnp.float32)
        prod += jnp.dot(gt[:, half_rows:], gbuf[slot, 1], preferred_element_type=jnp.float32)
        ro_ref[:, pl.ds(at, cols)] = EMA_DECAY * ro_ref[:, pl.ds(at, cols)] + (1.0 - EMA_DECAY) * prod


    dx = 1 - 2 * c
    helper = (y * side + (x + dx + side) % side) * CORES + c
    client = (y * side + (x - dx + side) % side) * CORES + c
    up = (((y + 1) % side) * side + x) * CORES + c
    down = (((y + side - 1) % side) * side + x) * CORES + c
    half_count, root_half, _ = lroot.shape
    pieces = ((0, root_half - root_half // 4), (root_half - root_half // 4, root_half // 4))

    def root_block(dy, q, p=0):
        oy, ox = (y + dy) % side, (x + 2 * q) % side
        core = c + p * (1 - 2 * c)
        return (oy * (side // 2) + ox // 2) * CORES + core, (oy * side + ox) * CORES + core

    def twin_turn(place):
        return g_recv.at[ROUNDS + 1 + place // CORES]

    twin_last = g_recv.at[ROUNDS + 1 + half_count // 4]

    def root_copy(peer, place, half, src=None, dst=None, recv=None, part=None, across=0):
        here = lroot.at[2 * place + half]
        if part is not None:
            here = here.at[pl.ds(*pieces[part])]
        if peer is twin and recv is None:
            recv = twin_turn(place)
        return pltpu.make_async_remote_copy(
            src_ref=here if src is None else src, dst_ref=here if dst is None else dst, send_sem=l_send.at[across],
            recv_sem=l_recv.at[recv] if isinstance(recv, int) else recv, device_id={"tensor": peer}, device_id_type=MESH)

    sent = [0, 0]

    def root_send(peer, place, half, part=None, across=0, **kw):
        sent[across] += root_half if part is None else pieces[part][1]
        root_copy(peer, place, half, part=part, across=across, **kw).start()

    def uncounted(action):
        before = list(sent)
        action()
        sent[:] = before

    def pair_wait(pair, sem):
        pltpu.make_async_copy(pair, pair, sem).wait()

    own_place, _ = root_block(0, 0)
    far_place, _ = root_block(0, 1)
    passing = (y * (side // 2) + ((x - dx + side) % side) // 2) * CORES + c

    def root_start_across():
        for half in (0, 1):
            root_send(helper, own_place, half, across=1, src=lr_ref.at[half], dst=relay.at[half], recv=relay_recv.at[half])

    def root_start():
        for half in (0, 1):
            root_send(up, own_place, half, src=lr_ref.at[half], recv=half)
            root_send(down, own_place, 1 - half, src=lr_ref.at[1 - half], recv=half)
        for half in (0, 1):
            root_send(twin, own_place, half, src=lr_ref.at[half])

    def root_relay(half):
        root_copy(helper, own_place, half, src=lr_ref.at[half], dst=relay.at[half], recv=relay_recv.at[half]).wait_recv()
        root_send(helper, passing, half, across=1, src=relay.at[half], recv=FAR_TURN + half)
        root_send(twin, passing, half, across=1, src=relay.at[half], dst=relay.at[2 + half], recv=relay_recv.at[2])

    def passed_rows(p):
        if p:
            pair_wait(relay.at[pl.ds(2, 2)], relay_recv.at[2])
        source = (y * side + (x - (1 - 2 * p) * dx + side) % side) * CORES + c + p * (1 - 2 * c)
        left = relay[2 * p:2 * p + 2].reshape(lrows, rows)
        do_ref[rows_of(source), :] = jnp.dot(left, xx[0], preferred_element_type=jnp.float32)

    def root_far():
        for half in (0, 1):
            pltpu.make_async_copy(lroot.at[0], lroot.at[0], l_recv.at[FAR_TURN + half]).wait()
            root_send(up, far_place, half, recv=3 + half)
            root_send(twin, far_place, half)
        for half in (1, 0):
            root_send(down, far_place, half, recv=4 - half)

    def root_round(r):
        q, stage = r // 3, r % 3
        pair_wait(lroot.at[pl.ds(0, 2)], l_recv.at[r])
        if stage == 2:
            below = above = root_block(2, q)[0]
        else:
            below, above = root_block(side - 1, q)[0], root_block(1, q)[0]
        if stage == 0:
            for peer, place, half in ((up, below, 0), (down, above, 1)):
                if q == 0:
                    root_send(peer, place, half, recv=2)
                else:
                    for part in (0, 1):
                        root_send(peer, place, half, part=part, recv=LAST_TURN + part)
        root_send(twin, below, stage % 2)
        root_send(twin, above, 1 - stage % 2)

    last_place, last_device = root_block(2, 1)
    twin_place, twin_device = root_block(2, 1, 1)

    def root_last(part):
        pair_wait(lroot.at[pl.ds(0, 2), pl.ds(*pieces[part])], l_recv.at[LAST_TURN + part])
        for half in (0, 1):
            root_send(twin, last_place, half, part=part, recv=twin_last if part else None)

    def root_last_twin(part):
        pair = lroot.at[pl.ds(2 * twin_place, 2), pl.ds(*pieces[part])]
        pair_wait(pair, twin_last if part else twin_turn(twin_place))

    steps(grad, gbuf, load_sem, GRAD_ROUND_STEP, [(RELAY_STEP, lambda: root_relay(0))],
          [(ROOT_ACROSS_STEP, root_start_across), (ROOT_ACROSS_STEP, lambda: pl.when(c == 1)(lambda: uncounted(root_start)))],
          [(ROOT_START_STEP, lambda: pl.when(c == 0)(root_start))], grad_work)

    side_cols = cols // 2

    def x_copy(h):
        at = pl.ds(h * side_cols, side_cols)
        return pltpu.make_async_remote_copy(
            src_ref=xx.at[0, :, at], dst_ref=xx.at[1, :, at], send_sem=x_send.at[h], recv_sem=x_recv.at[h],
            device_id={"tensor": helper}, device_id_type=MESH)

    xx[0] = acc[:, :cols].astype(jnp.bfloat16)
    root_relay(1)
    x_copy(0).start()
    x_copy(1).start()
    root_round(0)

    def left_step(t, carry):
        at = pl.ds(pl.multiple_of(t * lrows, lrows), lrows)
        lo_ref[:, at] = EMA_DECAY * lo_ref[:, at] + (1.0 - EMA_DECAY) * acc[at, cols:].T
        return carry
    lax.fori_loop(0, rows // lrows, left_step, 0)

    def at_step(i):
        e, p = i // 2, i % 2
        dy = lax.shift_right_logical(ROOT_Y, 2 * e) & 3
        q = lax.shift_right_logical(ROOT_X, 2 * e) & 3
        return root_block(dy, q, p)

    def twin_wait(i, place):
        @pl.when(i % 2 == 1)
        def _():
            pair_wait(lroot.at[pl.ds(2 * place, 2)], twin_turn(place))

    def product(place, which):
        left = lroot[pl.ds(2 * place, 2)].reshape(lrows, rows)
        return jnp.dot(left, xx[which], preferred_element_type=jnp.float32)

    def rows_of(device):
        return pl.ds(pl.multiple_of(device * lrows, lrows), lrows)

    def own_rows(i):
        place, device = at_step(i)
        do_ref[rows_of(device), :] = product(place, 0)

    def lent_copy(i, device):
        return pltpu.make_async_remote_copy(
            src_ref=lent.at[i], dst_ref=do_ref.at[rows_of(device)], send_sem=d_send.at[0], recv_sem=d_recv.at[0],
            device_id={"tensor": client}, device_id_type=MESH)

    def lent_rows(i):
        place, device = at_step(i)
        lent[i] = product(place, 1)
        lent_copy(i, device).start()

    def lent_side(i, h):
        place, _ = at_step(i)
        at = pl.ds(h * side_cols, side_cols)
        left = lroot[pl.ds(2 * place, 2)].reshape(lrows, rows)
        lent[i, :, at] = jnp.dot(left, xx[1, :, at], preferred_element_type=jnp.float32)

    def lent_side_copy(i, h):
        _, device = at_step(i)
        at = pl.ds(h * side_cols, side_cols)
        return pltpu.make_async_remote_copy(
            src_ref=lent.at[i, :, at], dst_ref=do_ref.at[rows_of(device), at], send_sem=d_send.at[0], recv_sem=d_recv.at[0],
            device_id={"tensor": client}, device_id_type=MESH)

    def loop(lo, hi, body):
        def step(i, carry):
            body(i)
            return carry
        lax.fori_loop(lo, hi, step, 0)

    def first_own(i):
        @pl.when(i == 2)
        def _():
            root_far()
            root_round(1)

        @pl.when(i == 8)
        def _():
            root_round(2)
        twin_wait(i, at_step(i)[0])
        own_rows(i)

    loop(0, 10, first_own)
    passed_rows(0)
    passed_rows(1)
    x_copy(0).wait_recv()
    def lent_step(j):
        return j + (j + 7) // 8 + j // 5

    loop(0, 8, lambda j: lent_side(lent_step(j), 0))
    x_copy(0).wait_send()
    x_copy(1).wait_send()
    pl.semaphore_signal(x_gone, inc=1, device_id={"tensor": twin}, device_id_type=MESH)
    pl.semaphore_wait(x_gone, 1)
    loop(0, 8, lambda j: lent_side_copy(lent_step(j), 0).start())
    root_round(3)
    x_copy(1).wait_recv()

    def second_side(j):
        i = lent_step(j)
        lent_side(i, 1)
        lent_side_copy(i, 1).start()
    loop(0, 8, second_side)
    root_round(4)

    def both(i):
        twin_wait(i, at_step(i)[0])
        lent_rows(i)
        own_rows(i)
    loop(10, 14, both)

    def lent_piece(i, place, device, part):
        first, count = pieces[part]
        left = jnp.concatenate([lroot[2 * place, pl.ds(first, count), :], lroot[2 * place + 1, pl.ds(first, count), :]], axis=0)
        prod = jnp.dot(left, xx[1], preferred_element_type=jnp.float32)
        for half in (0, 1):
            at = half * root_half + first
            lent[i, pl.ds(at, count), :] = prod[half * count:(half + 1) * count]
            pltpu.make_async_remote_copy(
                src_ref=lent.at[i, pl.ds(at, count)], dst_ref=do_ref.at[pl.ds(pl.multiple_of(device * lrows, lrows) + at, count)],
                send_sem=d_send.at[0], recv_sem=d_recv.at[0], device_id={"tensor": client}, device_id_type=MESH).start()

    def own_piece(part):
        root_last(part)
        lent_piece(14, last_place, last_device, part)

    def twin_piece(part):
        root_last_twin(part)
        lent_piece(15, twin_place, twin_device, part)

    @pl.when(c == 0)
    def _():
        own_piece(0)
        own_piece(1)
        twin_piece(0)
        twin_piece(1)

    @pl.when(c == 1)
    def _():
        uncounted(lambda: own_piece(0))
        twin_piece(0)
        twin_piece(1)
        uncounted(lambda: own_piece(1))

    loop(14, 16, own_rows)

    grad.drain()
    for across, count in enumerate(sent):
        whole = lroot.at[pl.ds(0, count // root_half)]
        pltpu.make_async_copy(whole, whole, l_send.at[across]).wait()
    given = lent.at[pl.ds(0, half_count // 2 - 2)]
    pltpu.make_async_copy(given, given, d_send.at[0]).wait()
    pltpu.make_async_copy(given, given, d_recv.at[0]).wait()


def store_kernel(*refs):
    count = (len(refs) - 1) // 2
    sems = refs[-1]
    pieces = 32
    for i in range(count):
        src, dst = refs[i], refs[count + i]
        step = src.shape[0] // pieces
        for j in range(pieces):
            part = pl.ds(j * step, step)
            pltpu.make_async_copy(src.at[part], dst.at[part], sems.at[i]).start()
    for i in range(count):
        pltpu.make_async_copy(refs[i], refs[count + i], sems.at[i]).wait()


def solution(mesh):
    row_spec = P(("layer", "tensor"), None)
    col_spec = P("layer", "tensor")
    n = mesh.shape["tensor"]
    side = math.isqrt(n // CORES)

    def local_step(g, l, r, lr, rr):
        rows, cols = g.shape
        lrows = l.shape[0]
        kept = n // 2
        hbm = pl.BlockSpec(memory_space=pltpu.HBM)
        vmem = pl.BlockSpec(memory_space=pltpu.VMEM)
        operands = [g.reshape(2, rows // 2, cols), l, r, lr.reshape(2, lrows // 2, rows), rr]
        left_new, right_new, direction, _ = pl.pallas_call(
            functools.partial(kernel, n, side),
            name="shampoo",
            out_shape=[
                pltpu.VMEM(l.shape, jnp.float32),
                pltpu.VMEM(r.shape, jnp.float32),
                pltpu.VMEM(g.shape, jnp.float32),
                pltpu.HBM((2 * n, rows // 2, cols), jnp.bfloat16),
            ],
            in_specs=[hbm] * 5,
            out_specs=[vmem, vmem, vmem, hbm],
            scratch_shapes=[
                pltpu.VMEM(rr.shape, jnp.bfloat16),
                pltpu.VMEM((cols, rows), jnp.bfloat16),
                pltpu.VMEM((rows, cols + lrows), jnp.float32),
                pltpu.VMEM((2, 2, rows // 2, cols), jnp.bfloat16),
                pltpu.VMEM((cols + lrows, cols), jnp.bfloat16),
                pltpu.VMEM((2, rows, cols), jnp.bfloat16),
                pltpu.VMEM((2 * kept, lrows // 2, rows), jnp.bfloat16),
                pltpu.VMEM((4, lrows // 2, rows), jnp.bfloat16),
                pltpu.VMEM((kept, lrows, cols), jnp.float32),
                pltpu.SemaphoreType.DMA((ROUNDS + n // 2,)),
                pltpu.SemaphoreType.DMA((1,)),
                pltpu.SemaphoreType.DMA((2,)),
                pltpu.SemaphoreType.DMA((ROOT_TURNS,)),
                pltpu.SemaphoreType.DMA((3,)),
                pltpu.SemaphoreType.DMA((2,)),
                pltpu.SemaphoreType.DMA((1,)),
                pltpu.SemaphoreType.DMA((2,)),
                pltpu.SemaphoreType.DMA((2,)),
                pltpu.SemaphoreType.DMA((1,)),
                pltpu.SemaphoreType.REGULAR,
            ],
            compiler_params=pltpu.CompilerParams(collective_id=0, has_side_effects=True, vmem_limit_bytes=48 * 2**20),
            cost_estimate=pl.CostEstimate(flops=2 * rows * cols * (2 * n * cols + 2 * rows), bytes_accessed=2 * n * rows * cols * 3, transcendentals=0),
        )(*[pltpu.with_memory_space_constraint(v, pltpu.HBM) for v in operands])
        results = [left_new, right_new, direction]
        return pl.pallas_call(
            store_kernel,
            name="store",
            out_shape=[jax.ShapeDtypeStruct(v.shape, v.dtype) for v in results],
            in_specs=[vmem] * 3,
            out_specs=[hbm] * 3,
            scratch_shapes=[pltpu.SemaphoreType.DMA((3,))],
            compiler_params=pltpu.CompilerParams(vmem_limit_bytes=1 * 2**20),
        )(*results)

    return jax.shard_map(local_step, mesh=mesh, in_specs=(col_spec, row_spec, row_spec, row_spec, row_spec), out_specs=(row_spec, row_spec, col_spec), check_vma=False)
```

```python
import functools
import math

import jax
import jax.numpy as jnp
from jax import lax
from jax.experimental import pallas as pl
from jax.experimental.pallas import tpu as pltpu
from jax.sharding import PartitionSpec as P

EMA_DECAY = 0.9
CORES = 2
MESH = pl.DeviceIdType.MESH

ORDER = [(int(a), int(b)) for a, b in zip("0310020311322312", "0003102313131222")]
def parcels(code):
    digits = [int(d) for d in code]
    return [((a, b), h) for a, b, h in zip(digits[0::3], digits[1::3], digits[2::3])]


UP = parcels("030031330131020331130230231320120220")
UP_ON = {0: parcels("030"), 2: parcels("330"), 6: parcels("130"), 7: parcels("230")}
DOWN = parcels("011010111310021110311211210321121221")
DOWN_ON = {0: parcels("011"), 6: parcels("311111"), 7: parcels("211")}
ROUNDS = len(UP)
FIRST_UP = parcels("300301200")
FIRST_DOWN = parcels("101100201")
GRAD_ROUND_STEP = [2, 2, 8, 10, 12, 14, 17, 20, 22, 26, 28, 30]
LAST_FORWARD = 7
SIDE_UP, SIDE_DOWN = 9, 10
ASIDE = {"+": 33, "-": 33}
ROOT_START_STEP = 28
ROOT_ACROSS_STEP = 30
RELAY_STEP = 32
LATE = (2, 12, 14, 22, 26, 28, 30)


def round_of(name, offset, half):
    a, b = offset
    table, da, db = {"f+": (FIRST_UP, 3, 0), "f-": (FIRST_DOWN, 1, 0), "s+": (UP, 0, 3), "s-": (DOWN, 0, 1)}[name]
    return table.index((((a + da) % 4, (b + db) % 4), half))


def packed(values):
    return [sum(v << (2 * i) for i, v in enumerate(values[j:j + 8])) for j in (0, 8)]


FIRST_CODE = packed([o[0] for o in ORDER])
SECOND_CODE = packed([o[1] for o in ORDER])


def lookup(code, e):
    word = code[0] + (e // 8) * (code[1] - code[0])
    return lax.shift_right_logical(word, 2 * (e % 8)) & 3


ROOT_ORDER = [(0, 0), (3, 0), (1, 0), (0, 1), (2, 0), (3, 1), (1, 1), (2, 1)]
ROOT_Y = sum(o[0] << (2 * i) for i, o in enumerate(ROOT_ORDER))
FAR_TURN, LAST_TURN, ROOT_TURNS = 5, 7, 9
ROOT_X = sum(o[1] << (2 * i) for i, o in enumerate(ROOT_ORDER))


def kernel(n, side, g_ref, l_ref, r_ref, lr_ref, rr_ref, lo_ref, ro_ref, do_ref, gfull,
           rr, gt, acc, gbuf, rhs, xx, lroot, relay, lent,
           g_recv, g_send, load_sem, l_recv, relay_recv, x_recv, d_recv, l_send, x_send, d_send, x_gone):
    _, half_rows, cols = g_ref.shape
    rows = 2 * half_rows
    lrows = l_ref.shape[0]
    tile = min(1024, half_rows)
    aside_rows = {way: half_rows * share // 128 for way, share in ASIDE.items()}

    me = lax.axis_index("tensor")
    c = me % CORES
    chip = me // CORES
    x, y = chip % side, chip // side
    f = x + c * (y - x)
    s = y + c * (x - y)
    fstep = CORES + c * CORES * (side - 1)
    sstep = CORES * side - c * CORES * (side - 1)
    twin = me + 1 - 2 * c

    def index(df, ds):
        return ((f + df) % side) * fstep + ((s + ds) % side) * sstep + c

    def twin_index(df, ds):
        return ((s + df) % side) * sstep + ((f + ds) % side) * fstep + 1 - c

    peers = {"f+": index(1, 0), "f-": index(3, 0), "s+": index(0, 1), "s-": index(0, 3), "twin": twin}

    class Gather:
        def __init__(self, own, full, recv, send):
            self.own, self.full, self.recv, self.send_sem = own, full, recv, send
            self.sent = 0

        def copy(self, name, offset, half, part=None, turn=None):
            b = index(*offset)
            src = self.own.at[half] if offset == (0, 0) else self.full.at[2 * b + half]
            dst = self.full.at[2 * b + half]
            if part is not None:
                src, dst = src.at[pl.ds(*part)], dst.at[pl.ds(*part)]
            if turn is None:
                turn = ROUNDS + ORDER.index(offset) if name == "twin" else round_of(name, offset, half)
            return pltpu.make_async_remote_copy(
                src_ref=src, dst_ref=dst, send_sem=self.send_sem.at[0], recv_sem=self.recv.at[turn],
                device_id={"tensor": peers[name]}, device_id_type=MESH)

        def send(self, name, offset, half):
            self.sent += 1
            self.copy(name, offset, half).start()

        def wait(self, turn, count):
            taken = self.full.at[pl.ds(0, count)]
            pltpu.make_async_copy(taken, taken, self.recv.at[turn]).wait()

        def start(self):
            for half in (0, 1):
                for name in ("f+", "s+"):
                    self.send(name, (0, 0), half)
                for name in ("f-", "s-"):
                    self.send(name, (0, 0), 1 - half)
            for half in (0, 1):
                self.send("twin", (0, 0), half)

        def round(self, r):
            first = r < len(FIRST_UP)
            self.wait(r, 4 if first else 2)
            if first:
                above, below = FIRST_UP[r], FIRST_DOWN[r]
                if r == 0:
                    self.send("f+", *above)
                    self.send("f-", *below)
                self.send("s+", *above)
                self.send("s-", *below)
                self.send("s+", *below)
                self.send("s-", *above)
                self.send("twin", *above)
                self.send("twin", *below)
            for name, table in (("s+", UP_ON), ("s-", DOWN_ON)):
                for parcel in table.get(r, ()):
                    if r == LAST_FORWARD:
                        self.forward_last(name, *parcel)
                    else:
                        self.send(name, *parcel)
            if r == SIDE_UP:
                self.aside("f+", *UP[r])
            if r == SIDE_DOWN:
                self.aside("f-", *DOWN[r])
            self.send("twin", *UP[r])
            self.send("twin", *DOWN[r])

        def forward_last(self, name, offset, half):
            self.sent += 1
            pl.when(c == 0)(lambda: self.copy(name, offset, half, part=(0, half_rows - aside_rows[name[1]])).start())
            pl.when(c == 1)(lambda: self.copy(name, offset, half).start())

        def aside(self, name, offset, half):
            count = aside_rows[name[1]]
            part = (half_rows - count, count)
            pl.when(c == 0)(lambda: self.copy(name, offset, half, part=part, turn=ROUNDS - 1).start())

        def drain(self):
            whole = self.full.at[pl.ds(0, self.sent)]
            pltpu.make_async_copy(whole, whole, self.send_sem.at[0]).wait()

    grad = Gather(g_ref, gfull, g_recv, g_send)

    def block_of(k):
        e, other = k // 2, k % 2
        df, ds = lookup(FIRST_CODE, e), lookup(SECOND_CODE, e)
        mine = index(df, ds)
        return mine + other * (twin_index(df, ds) - mine)

    def load(gather, buf, k, sem):
        b = block_of(k)
        return pltpu.make_async_copy(gather.full.at[pl.ds(2 * b, 2)], buf.at[k % 2], sem.at[k % 2])

    def one_of(k, values):
        found = k == values[0]
        for v in values[1:]:
            found = found | (k == v)
        return found

    def steps(gather, buf, sem, round_step, early, between, after, work):
        def at_steps(k, actions):
            for at, action in actions:
                pl.when(k == at)(action)

        def step(k, carry):
            at_steps(k, early)

            @pl.when((k % 2 == 1) & (k < n))
            def _():
                gather.wait(ROUNDS + k // 2, 2)

            @pl.when(jnp.logical_not(one_of(k, LATE)) & (k < n))
            def _():
                load(gather, buf, k, sem).start()
            load(gather, buf, k - 1, sem).wait()
            work((k - 1) % 2, block_of(k - 1))
            at_steps(k, between)
            for r in range(ROUNDS):
                @pl.when(k == round_step[r])
                def _():
                    gather.round(r)
            at_steps(k, after)

            @pl.when(one_of(k, LATE))
            def _():
                load(gather, buf, k, sem).start()
            return carry
        lax.fori_loop(1, n + 1, step, 0)

    barrier = pltpu.get_barrier_semaphore()
    for peer in peers.values():
        pl.semaphore_signal(barrier, inc=1, device_id={"tensor": peer}, device_id_type=MESH)

    first = [
        pltpu.make_async_copy(rr_ref, rr, x_send.at[0]),
        pltpu.make_async_copy(r_ref, ro_ref, x_send.at[1]),
        pltpu.make_async_copy(l_ref, lo_ref, d_send.at[0]),
        pltpu.make_async_copy(lr_ref, lroot.at[pl.ds(2 * ((y * (side // 2) + x // 2) * CORES + c), 2)], l_send.at[0]),
    ]
    own_load = pltpu.make_async_copy(g_ref, gbuf.at[0], load_sem.at[0])
    own_load.start()
    for copy in first:
        copy.start()

    pl.semaphore_wait(barrier, len(peers))
    grad.start()

    acc[...] = jnp.zeros_like(acc)
    own_load.wait()
    for h in (0, 1):
        gt[:, h * half_rows:(h + 1) * half_rows] = gbuf[0, h].T
    for copy in first:
        copy.wait()
    own_load.start()

    per_half = half_rows // tile

    def grad_work(slot, b):
        at = pl.multiple_of(b * cols, cols)
        rhs[:cols] = rr[:, pl.ds(at, cols)]
        rhs[cols:] = gbuf[slot, me // (n // 2), pl.ds(pl.multiple_of((me % (n // 2)) * lrows, lrows), lrows), :]

        def rows_step(t, carry):
            left = gbuf[slot, t // per_half, pl.ds(pl.multiple_of((t % per_half) * tile, tile), tile), :]
            out = pl.ds(pl.multiple_of(t * tile, tile), tile)
            acc[out, :] += lax.dot_general(left, rhs[...], (((1,), (1,)), ((), ())), preferred_element_type=jnp.float32)
            return carry
        lax.fori_loop(0, 2 * per_half, rows_step, 0)
        prod = jnp.dot(gt[:, :half_rows], gbuf[slot, 0], preferred_element_type=jnp.float32)
        prod += jnp.dot(gt[:, half_rows:], gbuf[slot, 1], preferred_element_type=jnp.float32)
        ro_ref[:, pl.ds(at, cols)] = EMA_DECAY * ro_ref[:, pl.ds(at, cols)] + (1.0 - EMA_DECAY) * prod


    dx = 1 - 2 * c
    helper = (y * side + (x + dx + side) % side) * CORES + c
    client = (y * side + (x - dx + side) % side) * CORES + c
    up = (((y + 1) % side) * side + x) * CORES + c
    down = (((y + side - 1) % side) * side + x) * CORES + c
    half_count, root_half, _ = lroot.shape
    pieces = ((0, root_half - root_half // 4), (root_half - root_half // 4, root_half // 4))

    def root_block(dy, q, p=0):
        oy, ox = (y + dy) % side, (x + 2 * q) % side
        core = c + p * (1 - 2 * c)
        return (oy * (side // 2) + ox // 2) * CORES + core, (oy * side + ox) * CORES + core

    def twin_turn(place):
        return g_recv.at[ROUNDS + 1 + place // CORES]

    twin_last = g_recv.at[ROUNDS + 1 + half_count // 4]

    def root_copy(peer, place, half, src=None, dst=None, recv=None, part=None, across=0):
        here = lroot.at[2 * place + half]
        if part is not None:
            here = here.at[pl.ds(*pieces[part])]
        if peer is twin and recv is None:
            recv = twin_turn(place)
        return pltpu.make_async_remote_copy(
            src_ref=here if src is None else src, dst_ref=here if dst is None else dst, send_sem=l_send.at[across],
            recv_sem=l_recv.at[recv] if isinstance(recv, int) else recv, device_id={"tensor": peer}, device_id_type=MESH)

    sent = [0, 0]

    def root_send(peer, place, half, part=None, across=0, **kw):
        sent[across] += root_half if part is None else pieces[part][1]
        root_copy(peer, place, half, part=part, across=across, **kw).start()

    def uncounted(action):
        before = list(sent)
        action()
        sent[:] = before

    def pair_wait(pair, sem):
        pltpu.make_async_copy(pair, pair, sem).wait()

    own_place, _ = root_block(0, 0)
    far_place, _ = root_block(0, 1)
    passing = (y * (side // 2) + ((x - dx + side) % side) // 2) * CORES + c

    def root_start_across():
        for half in (0, 1):
            root_send(helper, own_place, half, across=1, src=lr_ref.at[half], dst=relay.at[half], recv=relay_recv.at[half])

    def root_start():
        for half in (0, 1):
            root_send(up, own_place, half, src=lr_ref.at[half], recv=half)
            root_send(down, own_place, 1 - half, src=lr_ref.at[1 - half], recv=half)
        for half in (0, 1):
            root_send(twin, own_place, half, src=lr_ref.at[half])

    def root_relay(half):
        root_copy(helper, own_place, half, src=lr_ref.at[half], dst=relay.at[half], recv=relay_recv.at[half]).wait_recv()
        root_send(helper, passing, half, across=1, src=relay.at[half], recv=FAR_TURN + half)
        root_send(twin, passing, half, across=1, src=relay.at[half], dst=relay.at[2 + half], recv=g_recv.at[ROUNDS + 10])

    def passed_rows(p):
        if p:
            pair_wait(relay.at[pl.ds(2, 2)], g_recv.at[ROUNDS + 10])
        source = (y * side + (x - (1 - 2 * p) * dx + side) % side) * CORES + c + p * (1 - 2 * c)
        left = relay[2 * p:2 * p + 2].reshape(lrows, rows)
        do_ref[rows_of(source), :] = jnp.dot(left, xx[0], preferred_element_type=jnp.float32)

    def root_far():
        for half in (0, 1):
            pltpu.make_async_copy(lroot.at[0], lroot.at[0], l_recv.at[FAR_TURN + half]).wait()
            root_send(up, far_place, half, recv=3 + half)
            root_send(twin, far_place, half)
        for half in (1, 0):
            root_send(down, far_place, half, recv=4 - half)

    def root_round(r):
        q, stage = r // 3, r % 3
        pair_wait(lroot.at[pl.ds(0, 2)], l_recv.at[r])
        if stage == 2:
            below = above = root_block(2, q)[0]
        else:
            below, above = root_block(side - 1, q)[0], root_block(1, q)[0]
        if stage == 0:
            for peer, place, half in ((up, below, 0), (down, above, 1)):
                if q == 0:
                    root_send(peer, place, half, recv=2)
                else:
                    for part in (0, 1):
                        root_send(peer, place, half, part=part, recv=LAST_TURN + part)
        root_send(twin, below, stage % 2)
        root_send(twin, above, 1 - stage % 2)

    last_place, last_device = root_block(2, 1)
    twin_place, twin_device = root_block(2, 1, 1)

    def root_last(part):
        pair_wait(lroot.at[pl.ds(0, 2), pl.ds(*pieces[part])], l_recv.at[LAST_TURN + part])
        for half in (0, 1):
            root_send(twin, last_place, half, part=part, recv=twin_last if part else None)

    def root_last_twin(part):
        pair = lroot.at[pl.ds(2 * twin_place, 2), pl.ds(*pieces[part])]
        pair_wait(pair, twin_last if part else twin_turn(twin_place))

    steps(grad, gbuf, load_sem, GRAD_ROUND_STEP, [(RELAY_STEP, lambda: root_relay(0))],
          [(ROOT_ACROSS_STEP, root_start_across), (ROOT_ACROSS_STEP, lambda: pl.when(c == 1)(lambda: uncounted(root_start)))],
          [(ROOT_START_STEP, lambda: pl.when(c == 0)(root_start))], grad_work)

    side_cols = cols // 2

    def x_copy(h):
        at = pl.ds(h * side_cols, side_cols)
        return pltpu.make_async_remote_copy(
            src_ref=xx.at[0, :, at], dst_ref=xx.at[1, :, at], send_sem=x_send.at[h], recv_sem=x_recv.at[h],
            device_id={"tensor": helper}, device_id_type=MESH)

    xx[0] = acc[:, :cols].astype(jnp.bfloat16)
    root_relay(1)
    x_copy(0).start()
    x_copy(1).start()
    root_round(0)

    def left_step(t, carry):
        at = pl.ds(pl.multiple_of(t * lrows, lrows), lrows)
        lo_ref[:, at] = EMA_DECAY * lo_ref[:, at] + (1.0 - EMA_DECAY) * acc[at, cols:].T
        return carry
    lax.fori_loop(0, rows // lrows, left_step, 0)

    def at_step(i):
        e, p = i // 2, i % 2
        dy = lax.shift_right_logical(ROOT_Y, 2 * e) & 3
        q = lax.shift_right_logical(ROOT_X, 2 * e) & 3
        return root_block(dy, q, p)

    def twin_wait(i, place):
        @pl.when(i % 2 == 1)
        def _():
            pair_wait(lroot.at[pl.ds(2 * place, 2)], twin_turn(place))

    def product(place, which):
        left = lroot[pl.ds(2 * place, 2)].reshape(lrows, rows)
        return jnp.dot(left, xx[which], preferred_element_type=jnp.float32)

    def rows_of(device):
        return pl.ds(pl.multiple_of(device * lrows, lrows), lrows)

    def own_rows(i):
        place, device = at_step(i)
        do_ref[rows_of(device), :] = product(place, 0)

    def lent_copy(i, device):
        return pltpu.make_async_remote_copy(
            src_ref=lent.at[i], dst_ref=do_ref.at[rows_of(device)], send_sem=d_send.at[0], recv_sem=d_recv.at[0],
            device_id={"tensor": client}, device_id_type=MESH)

    def lent_rows(i):
        place, device = at_step(i)
        lent[i] = product(place, 1)
        lent_copy(i, device).start()

    def lent_side(i, h):
        place, _ = at_step(i)
        at = pl.ds(h * side_cols, side_cols)
        left = lroot[pl.ds(2 * place, 2)].reshape(lrows, rows)
        lent[i, :, at] = jnp.dot(left, xx[1, :, at], preferred_element_type=jnp.float32)

    def lent_side_copy(i, h):
        _, device = at_step(i)
        at = pl.ds(h * side_cols, side_cols)
        return pltpu.make_async_remote_copy(
            src_ref=lent.at[i, :, at], dst_ref=do_ref.at[rows_of(device), at], send_sem=d_send.at[0], recv_sem=d_recv.at[0],
            device_id={"tensor": client}, device_id_type=MESH)

    def loop(lo, hi, body):
        def step(i, carry):
            body(i)
            return carry
        lax.fori_loop(lo, hi, step, 0)

    def first_own(i):
        @pl.when(i == 2)
        def _():
            root_far()
            root_round(1)

        @pl.when(i == 8)
        def _():
            root_round(2)
        twin_wait(i, at_step(i)[0])
        own_rows(i)

    loop(0, 10, first_own)
    passed_rows(0)
    passed_rows(1)
    x_copy(0).wait_recv()
    def lent_step(j):
        return j + (j + 7) // 8 + j // 5

    loop(0, 8, lambda j: lent_side(lent_step(j), 0))
    x_copy(0).wait_send()
    x_copy(1).wait_send()
    pl.semaphore_signal(x_gone, inc=1, device_id={"tensor": twin}, device_id_type=MESH)
    pl.semaphore_wait(x_gone, 1)
    loop(0, 8, lambda j: lent_side_copy(lent_step(j), 0).start())
    root_round(3)
    x_copy(1).wait_recv()

    def second_side(j):
        i = lent_step(j)
        lent_side(i, 1)
        lent_side_copy(i, 1).start()
    loop(0, 8, second_side)
    root_round(4)

    def both(i):
        twin_wait(i, at_step(i)[0])
        lent_rows(i)
        own_rows(i)
    loop(10, 14, both)

    def lent_piece(i, place, device, part):
        first, count = pieces[part]
        left = jnp.concatenate([lroot[2 * place, pl.ds(first, count), :], lroot[2 * place + 1, pl.ds(first, count), :]], axis=0)
        prod = jnp.dot(left, xx[1], preferred_element_type=jnp.float32)
        for half in (0, 1):
            at = half * root_half + first
            lent[i, pl.ds(at, count), :] = prod[half * count:(half + 1) * count]
            pltpu.make_async_remote_copy(
                src_ref=lent.at[i, pl.ds(at, count)], dst_ref=do_ref.at[pl.ds(pl.multiple_of(device * lrows, lrows) + at, count)],
                send_sem=d_send.at[0], recv_sem=d_recv.at[0], device_id={"tensor": client}, device_id_type=MESH).start()

    def own_piece(part):
        root_last(part)
        lent_piece(14, last_place, last_device, part)

    def twin_piece(part):
        root_last_twin(part)
        lent_piece(15, twin_place, twin_device, part)

    @pl.when(c == 0)
    def _():
        own_piece(0)
        own_piece(1)
        twin_piece(0)
        twin_piece(1)

    @pl.when(c == 1)
    def _():
        uncounted(lambda: own_piece(0))
        twin_piece(0)
        twin_piece(1)
        uncounted(lambda: own_piece(1))

    loop(14, 16, own_rows)

    grad.drain()
    for across, count in enumerate(sent):
        whole = lroot.at[pl.ds(0, count // root_half)]
        pltpu.make_async_copy(whole, whole, l_send.at[across]).wait()
    given = lent.at[pl.ds(0, half_count // 2 - 2)]
    pltpu.make_async_copy(given, given, d_send.at[0]).wait()
    pltpu.make_async_copy(given, given, d_recv.at[0]).wait()


def store_kernel(*refs):
    count = (len(refs) - 1) // 2
    sems = refs[-1]
    pieces = 32
    for i in range(count):
        src, dst = refs[i], refs[count + i]
        step = src.shape[0] // pieces
        for j in range(pieces):
            part = pl.ds(j * step, step)
            pltpu.make_async_copy(src.at[part], dst.at[part], sems.at[i]).start()
    for i in range(count):
        pltpu.make_async_copy(refs[i], refs[count + i], sems.at[i]).wait()


def solution(mesh):
    row_spec = P(("layer", "tensor"), None)
    col_spec = P("layer", "tensor")
    n = mesh.shape["tensor"]
    side = math.isqrt(n // CORES)

    def local_step(g, l, r, lr, rr):
        rows, cols = g.shape
        lrows = l.shape[0]
        kept = n // 2
        hbm = pl.BlockSpec(memory_space=pltpu.HBM)
        vmem = pl.BlockSpec(memory_space=pltpu.VMEM)
        operands = [g.reshape(2, rows // 2, cols), l, r, lr.reshape(2, lrows // 2, rows), rr]
        left_new, right_new, direction, _ = pl.pallas_call(
            functools.partial(kernel, n, side),
            name="shampoo",
            out_shape=[
                pltpu.VMEM(l.shape, jnp.float32),
                pltpu.VMEM(r.shape, jnp.float32),
                pltpu.VMEM(g.shape, jnp.float32),
                pltpu.HBM((2 * n, rows // 2, cols), jnp.bfloat16),
            ],
            in_specs=[hbm] * 5,
            out_specs=[vmem, vmem, vmem, hbm],
            scratch_shapes=[
                pltpu.VMEM(rr.shape, jnp.bfloat16),
                pltpu.VMEM((cols, rows), jnp.bfloat16),
                pltpu.VMEM((rows, cols + lrows), jnp.float32),
                pltpu.VMEM((2, 2, rows // 2, cols), jnp.bfloat16),
                pltpu.VMEM((cols + lrows, cols), jnp.bfloat16),
                pltpu.VMEM((2, rows, cols), jnp.bfloat16),
                pltpu.VMEM((2 * kept, lrows // 2, rows), jnp.bfloat16),
                pltpu.VMEM((4, lrows // 2, rows), jnp.bfloat16),
                pltpu.VMEM((kept, lrows, cols), jnp.float32),
                pltpu.SemaphoreType.DMA((ROUNDS + n // 2,)),
                pltpu.SemaphoreType.DMA((1,)),
                pltpu.SemaphoreType.DMA((2,)),
                pltpu.SemaphoreType.DMA((ROOT_TURNS,)),
                pltpu.SemaphoreType.DMA((2,)),
                pltpu.SemaphoreType.DMA((2,)),
                pltpu.SemaphoreType.DMA((1,)),
                pltpu.SemaphoreType.DMA((2,)),
                pltpu.SemaphoreType.DMA((2,)),
                pltpu.SemaphoreType.DMA((1,)),
                pltpu.SemaphoreType.REGULAR,
            ],
            compiler_params=pltpu.CompilerParams(collective_id=0, has_side_effects=True, vmem_limit_bytes=48 * 2**20),
            cost_estimate=pl.CostEstimate(flops=2 * rows * cols * (2 * n * cols + 2 * rows), bytes_accessed=2 * n * rows * cols * 3, transcendentals=0),
        )(*[pltpu.with_memory_space_constraint(v, pltpu.HBM) for v in operands])
        results = [left_new, right_new, direction]
        return pl.pallas_call(
            store_kernel,
            name="store",
            out_shape=[jax.ShapeDtypeStruct(v.shape, v.dtype) for v in results],
            in_specs=[vmem] * 3,
            out_specs=[hbm] * 3,
            scratch_shapes=[pltpu.SemaphoreType.DMA((3,))],
            compiler_params=pltpu.CompilerParams(vmem_limit_bytes=1 * 2**20),
        )(*results)

    return jax.shard_map(local_step, mesh=mesh, in_specs=(col_spec, row_spec, row_spec, row_spec, row_spec), out_specs=(row_spec, row_spec, col_spec), check_vma=False)
```
